32 devices in a mesh: dp: 8 (over z, y), seq: 4 (over x, core).
Axes of the slice: x: 2, y: 2, z: 4, core: 2. Of those that a mesh axis runs over, the one named last changes fastest.
Arguments:
- tokens: bfloat16 [16, 1024, 1536], P('dp', 'seq'), may hold values from -6 to 6
- in_proj: bfloat16 [1536, 6448], P(('dp', 'seq')), may hold values from -0.15625 to 0.15625
- conv_weight: bfloat16 [4, 3328], P(None, ('dp', 'seq')), may hold values from -3 to 3
- conv_bias: bfloat16 [3328], P(('dp', 'seq')), may hold values from -0.5 to 0.5
- decay_log: float32 [48], replicated, may hold values from -6 to 0.5
- step_bias: float32 [48], replicated, may hold values from -4.5 to -2
- skip_gain: float32 [48], replicated, may hold values from 0.5 to 1.5
- norm_gain: bfloat16 [1536], P(('dp', 'seq')), may hold values from 0.099609375 to 1.8984375
- gated_gain: bfloat16 [3072], P(('dp', 'seq')), may hold values from 0.099609375 to 1.8984375
- out_proj: bfloat16 [3072, 1536], P(('dp', 'seq')), may hold values from -0.109375 to 0.109375
- cotangent: bfloat16 [16, 1024, 1536], P('dp', 'seq'), may hold values from -6 to 6
Outputs:
- block_out: bfloat16 [16, 1024, 1536], P('dp', 'seq')
- tokens_grad: bfloat16 [16, 1024, 1536], P('dp', 'seq')
- in_proj_grad: float32 [1536, 6448], P(('dp', 'seq'))
- conv_weight_grad: float32 [4, 3328], P(None, ('dp', 'seq'))
- conv_bias_grad: float32 [3328], P(('dp', 'seq'))
- decay_log_grad: float32 [48], replicated
- step_bias_grad: float32 [48], replicated
- skip_gain_grad: float32 [48], replicated
- norm_gain_grad: float32 [1536], P(('dp', 'seq'))
- gated_gain_grad: float32 [3072], P(('dp', 'seq'))
- out_proj_grad: float32 [3072, 1536], P(('dp', 'seq'))
The draws below stay inside these ranges and needn't reach their ends.
All inputs are finite; a program needn't handle non-finite values.
Results may differ from the reference program's by a relative error of at most 0.0062.
Values may be sent and summed in bfloat16 or wider, within the bound.
A program may use at most 256 MiB of HBM per device.

```python
import jax
import jax.numpy as jnp
from jax import lax

D = 1536
HEADS = 48
P_SIZE = 64
N = 128
KW = 4
GROUP = 256
DI = 3072
CD = 3328
E = 6448
LENGTH = 1024
SEQS = 16


def level_of(rng, dims, cuts, least, high):
    gain, own = 1.0, jax.random.fold_in(rng, 6)
    for dim, parts in cuts:
        heights = jnp.exp(jax.random.uniform(jax.random.fold_in(own, dim), (parts,), jnp.float32, least / len(cuts), high / len(cuts)))
        gain = gain * jnp.repeat(heights, dims[dim] // parts).reshape([-1 if axis == dim else 1 for axis in range(len(dims))])
    return gain


def noise(key, shape, scale, reach, cuts=(), kind=jnp.bfloat16):
    values = jax.random.normal(key, shape, jnp.float32) * scale
    if len(cuts) > 0:
        values = level_of(key, shape, cuts, -0.22, 0.18) * values
    return jnp.clip(values, min=-reach, max=reach).astype(kind)


def setup_inputs(seed: int = 0) -> dict:
    key_list = jax.random.split(jax.random.key(seed), 12)
    tokens = noise(key_list[0], (SEQS, LENGTH, D), 1.0, 6.0, ((0, 8), (1, 4)))
    in_proj = noise(key_list[1], (D, E), D ** -0.5, 0.15625, ((0, 32),))
    conv_weight = noise(key_list[2], (KW, CD), KW ** -0.5, 3.0, ((1, 32),))
    conv_bias = jnp.clip(jax.random.uniform(key_list[3], (CD,), jnp.float32, -0.5, 0.5) * level_of(key_list[3], (CD,), ((0, 32),), -0.4, 0.0), -0.5, 0.5).astype(jnp.bfloat16)
    decay_log = jnp.clip(jax.random.uniform(key_list[4], (HEADS,), jnp.float32, -6.0, 0.5), -6.0, 0.5)
    step_bias = jnp.clip(jax.random.uniform(key_list[5], (HEADS,), jnp.float32, -4.5, -2.0), -4.5, -2.0)
    skip_gain = jnp.clip(jax.random.uniform(key_list[6], (HEADS,), jnp.float32, 0.5, 1.5), 0.5, 1.5)
    norm_gain = jnp.clip(1.0 + 0.18 * jax.random.normal(key_list[7], (D,), jnp.float32), 0.099609375, 1.8984375).astype(jnp.bfloat16)
    gated_gain = jnp.clip(1.0 + 0.18 * jax.random.normal(key_list[8], (DI,), jnp.float32), 0.099609375, 1.8984375).astype(jnp.bfloat16)
    out_proj = noise(key_list[9], (DI, D), DI ** -0.5, 0.109375, ((0, 32),))
    cotangent = noise(key_list[10], (SEQS, LENGTH, D), 1.0, 6.0, ((0, 8), (1, 4)))
    return dict(tokens=tokens, in_proj=in_proj, conv_weight=conv_weight, conv_bias=conv_bias, decay_log=decay_log, step_bias=step_bias, skip_gain=skip_gain, norm_gain=norm_gain, gated_gain=gated_gain, out_proj=out_proj, cotangent=cotangent)


@jax.custom_vjp
def low(v):
    return lax.optimization_barrier(v.astype(jnp.bfloat16)).astype(jnp.float32)

@jax.custom_vjp
def low_back(v):
    return v

def low_keep(v):
    return (low(v), None)

def low_pass(kept, grad):
    return (grad,)

def back_keep(v):
    return (v, None)

def back_low(kept, grad):
    return (low(grad),)
low.defvjp(low_keep, low_pass)
low_back.defvjp(back_keep, back_low)
EPSILON = 1e-05
precise = lax.Precision.HIGHEST

def group_step(memory, pieces):
    values, inputs_b, inputs_c, step_sizes, decays = pieces
    running = jnp.cumsum(decays, axis=0)
    blocks = decays.shape[0]
    causal = (jnp.arange(blocks)[:, None] >= jnp.arange(blocks)[None, :])[:, :, None]
    spread = running[:, None, :] - running[None, :, :]
    within = jnp.where(causal, jnp.exp(jnp.where(causal, spread, 0.0)), 0.0)
    scores = jnp.dot(inputs_c, inputs_b.T, precision=precise)
    weights = scores[:, :, None] * within * step_sizes[None, :, :]
    output = jnp.einsum('ijh,jhp->ihp', weights, values, precision=precise)
    output = output + jnp.exp(running)[:, :, None] * jnp.einsum('in,hpn->ihp', inputs_c, memory, precision=precise)
    closing = running[-1]
    carried = jnp.exp(closing[None, :] - running) * step_sizes
    memory = memory * jnp.exp(closing)[:, None, None] + jnp.einsum('jh,jhp,jn->hpn', carried, values, inputs_b, precision=precise)
    return (memory, output)

def run_groups(values, inputs_b, inputs_c, step_sizes, decays):
    blocks = values.shape[0] // GROUP
    pieces = tuple((item.reshape((blocks, GROUP) + item.shape[1:]) for item in (values, inputs_b, inputs_c, step_sizes, decays)))
    memory = jnp.zeros((HEADS, P_SIZE, N), values.dtype)
    memory, outputs = lax.scan(jax.checkpoint(group_step), memory, pieces)
    return outputs.reshape(values.shape)

def forward(inputs, in_proj, conv_weight, conv_bias, decay_log, step_bias, skip_gain, norm_gain, gated_gain, out_proj):
    length = inputs.shape[0]
    inv_scale = lax.rsqrt(lax.optimization_barrier(jnp.mean(inputs * inputs, axis=-1, keepdims=True)) + EPSILON)
    normed = low(inputs * inv_scale * norm_gain)
    projected = low_back(jnp.dot(normed, in_proj, precision=precise))
    gate_half = projected[:, :DI]
    stream = projected[:, DI:DI + CD]
    raw_step = projected[:, DI + CD:]
    padded = jnp.concatenate([jnp.zeros((KW - 1, CD), stream.dtype), stream], axis=0)
    mixed_conv = conv_bias + jnp.zeros_like(stream)
    for offset in range(KW):
        mixed_conv = mixed_conv + conv_weight[offset] * padded[offset:offset + length]
    active = jax.nn.silu(mixed_conv)
    values = active[:, :DI].reshape(length, HEADS, P_SIZE)
    inputs_b = active[:, DI:DI + N]
    inputs_c = active[:, DI + N:]
    step_sizes = jax.nn.softplus(raw_step + step_bias)
    decays = -jnp.exp(decay_log) * step_sizes
    ssd_out = run_groups(values, inputs_b, inputs_c, step_sizes, decays)
    ssd_out = ssd_out + skip_gain[:, None] * values
    gated = ssd_out.reshape(length, DI) * jax.nn.silu(gate_half)
    gated_scale = lax.rsqrt(lax.optimization_barrier(jnp.mean(gated * gated, axis=-1, keepdims=True)) + EPSILON)
    shaped = low(gated * gated_scale * gated_gain)
    return inputs + jnp.dot(shaped, out_proj, precision=precise)

def reference(tokens, in_proj, conv_weight, conv_bias, decay_log, step_bias, skip_gain, norm_gain, gated_gain, out_proj, cotangent):
    params = tuple((item.astype(jnp.float32) for item in (in_proj, conv_weight, conv_bias, decay_log, step_bias, skip_gain, norm_gain, gated_gain, out_proj)))

    def per_sequence(totals, sequence_pair):
        inputs, upstream = sequence_pair
        result, pullback = jax.vjp(forward, inputs.astype(jnp.float32), *params)
        gradients = pullback(upstream.astype(jnp.float32))
        totals = tuple((total + grad for total, grad in zip(totals, gradients[1:])))
        return (totals, (result.astype(jnp.bfloat16), gradients[0].astype(jnp.bfloat16)))
    starting = tuple((jnp.zeros_like(item) for item in params))
    totals, (block_out, tokens_grad) = lax.scan(per_sequence, starting, (tokens, cotangent))
    return (block_out, tokens_grad, totals[0], totals[1], totals[2], totals[3], totals[4], totals[5], totals[6], totals[7], totals[8])
```

```python
import functools

import jax
import jax.numpy as jnp
from jax import lax
from jax.experimental import pallas as pl
from jax.experimental.pallas import tpu as pltpu
from jax.sharding import PartitionSpec as P

HEADS = 48
P_SIZE = 64
N = 128
KW = 4
DI = 3072
CD = 3328
LANES = 128
CHUNK = 128
FAR = -1e30

EPSILON = 1e-05
F32 = jnp.float32
BF16 = jnp.bfloat16


def dot(a, b, dims=((1,), (0,)), precision=None):
    return lax.dot_general(a, b, (dims, ((), ())), precision=precision, preferred_element_type=F32)


NT = ((1,), (1,))
HIGH = lax.Precision.HIGHEST


def pick(a, p, low):
    return jnp.where(low, a[:, 2 * p : 2 * p + 1], a[:, 2 * p + 1 : 2 * p + 2])


def chunk_parts(heads, rest_ref, xbuf, taps_ref, head_ref):
    size = rest_ref.shape[0]
    wide = taps_ref.shape[1]
    mixed = taps_ref[KW : KW + 1, :] + taps_ref[0:1, :] * xbuf[5 : 5 + size, :]
    for k in range(1, KW):
        mixed = mixed + taps_ref[k : k + 1, :] * xbuf[5 + k : 5 + k + size, :]
    sig = lax.logistic(mixed)
    lane = lax.broadcasted_iota(jnp.int32, (1, LANES), 1)
    raw = jnp.where(lane < heads, rest_ref[:, wide:], 0.0) + head_ref[1:2, :]
    step = jnp.maximum(raw, 0.0) + jnp.log1p(jnp.exp(-jnp.abs(raw)))
    decay = -jnp.exp(head_ref[0:1, :]) * step
    i = lax.broadcasted_iota(jnp.int32, (size, size), 0)
    j = lax.broadcasted_iota(jnp.int32, (size, size), 1)
    run = dot(jnp.where(i >= j, 1.0, 0.0), decay, precision=HIGH)
    return mixed, sig, raw, step, decay, run


def forward_kernel(heads, rest_ref, taps_ref, head_ref, ssd_ref, mem_ref, xbuf, mem):
    size = rest_ref.shape[0]
    wide = taps_ref.shape[1]
    inner = heads * P_SIZE
    first = pl.program_id(1) == 0

    @pl.when(first)
    def _():
        xbuf[0:8, :] = jnp.zeros((8, wide), F32)
        mem[...] = jnp.zeros_like(mem)

    @pl.when(jnp.logical_not(first))
    def _():
        xbuf[0:8, :] = xbuf[size : size + 8, :]

    xbuf[8 : 8 + size, :] = rest_ref[:, :wide]
    mixed, sig, _, step, _, run = chunk_parts(heads, rest_ref, xbuf, taps_ref, head_ref)
    act = mixed * sig
    run_t = run.T
    closing = run[size - 1 : size, :]
    last = jnp.exp(closing)
    left = jnp.exp(closing - run)
    grown = jnp.exp(run)
    b = act[:, inner : inner + N]
    c = act[:, inner + N :].astype(BF16)
    scores = dot(c, b.astype(BF16), NT)
    b_t = b.T.astype(BF16)
    mem_ref[0] = mem[...].astype(BF16)
    inter = dot(c, mem[...].astype(BF16))
    low = lax.broadcasted_iota(jnp.int32, (1, LANES), 1) < P_SIZE
    i = lax.broadcasted_iota(jnp.int32, (size, size), 0)
    j = lax.broadcasted_iota(jnp.int32, (size, size), 1)
    causal = i >= j
    for p in range(heads // 2):
        at = slice(p * LANES, (p + 1) * LANES)
        v = act[:, at]
        xv = pick(step, p, low) * v
        y = pick(head_ref[2:3, :], p, low) * v + pick(grown, p, low) * inter[:, at]
        for e in range(2):
            h = 2 * p + e
            gap = run[:, h : h + 1] - run_t[h : h + 1, :]
            w = (scores * jnp.exp(jnp.where(causal, gap, FAR))).astype(BF16)
            mine = jnp.where(low if e == 0 else jnp.logical_not(low), xv, 0.0).astype(BF16)
            y = y + dot(w, mine)
        ssd_ref[:, at] = y
        xc = (pick(left, p, low) * xv).astype(BF16)
        mem[:, at] = mem[:, at] * pick(last, p, low) + dot(b_t, xc)


def backward_kernel(
    heads,
    rest_ref,
    prev_ref,
    dy_ref,
    mem_ref,
    taps_ref,
    head_ref,
    out_ref,
    wgrad_ref,
    hgrad_ref,
    xbuf,
    gbuf,
    adj,
    dmix,
    dsum,
    uprod,
    zprod,
    rows_t,
    line,
):
    size = rest_ref.shape[0]
    wide = taps_ref.shape[1]
    inner = heads * P_SIZE
    chunks = pl.num_programs(1)
    step_id = pl.program_id(1)
    newest = step_id == 0
    oldest = step_id == chunks - 1
    begin = jnp.logical_and(pl.program_id(0) == 0, newest)
    finish = jnp.logical_and(pl.program_id(0) == pl.num_programs(0) - 1, oldest)

    @pl.when(begin)
    def _():
        wgrad_ref[...] = jnp.zeros_like(wgrad_ref)
        hgrad_ref[...] = jnp.zeros_like(hgrad_ref)
        rows_t[...] = jnp.zeros_like(rows_t)
        line[...] = jnp.zeros_like(line)

    @pl.when(newest)
    def _():
        gbuf[size : size + 8, :] = jnp.zeros((8, wide), F32)
        adj[...] = jnp.zeros_like(adj)

    @pl.when(jnp.logical_not(newest))
    def _():
        gbuf[size : size + 8, :] = gbuf[0:8, :]

    xbuf[0:8, :] = jnp.where(oldest, 0.0, prev_ref[:, :wide])
    xbuf[8 : 8 + size, :] = rest_ref[:, :wide]
    mixed, sig, raw, step, decay, run = chunk_parts(heads, rest_ref, xbuf, taps_ref, head_ref)
    act = mixed * sig
    run_t = run.T
    closing = run[size - 1 : size, :]
    last = jnp.exp(closing)
    left = jnp.exp(closing - run)
    grown = jnp.exp(run)
    b = act[:, inner : inner + N].astype(BF16)
    c = act[:, inner + N :].astype(BF16)
    c_t = act[:, inner + N :].T.astype(BF16)
    scores_t = dot(b, c, NT)
    low = lax.broadcasted_iota(jnp.int32, (1, LANES), 1) < P_SIZE
    lane = lax.broadcasted_iota(jnp.int32, (1, LANES), 1)
    j = lax.broadcasted_iota(jnp.int32, (size, size), 0)
    i = lax.broadcasted_iota(jnp.int32, (size, size), 1)
    causal = i >= j
    mem_b = mem_ref[0]
    adj_b = adj[...].astype(BF16)
    spread = dot(b, adj_b)
    inherit = dot(c, mem_b)
    scored = jnp.zeros((size, size), F32)
    cols = jnp.zeros((size, LANES), F32)
    for p in range(heads // 2):
        at = slice(p * LANES, (p + 1) * LANES)
        v = act[:, at]
        size_p = pick(step, p, low)
        xv = size_p * v
        dy = dy_ref[:, at]
        dyb = dy.astype(BF16)
        xvb = xv.astype(BF16)
        dxv = pick(left, p, low) * spread[:, at]
        zprod[:, at] = (dxv * xv).astype(BF16)
        dyg = pick(grown, p, low) * dy
        uprod[:, at] = (dyg * inherit[:, at]).astype(BF16)
        for e in range(2):
            h = 2 * p + e
            keep = low if e == 0 else jnp.logical_not(low)
            mine = jnp.where(keep, dy, 0.0).astype(BF16)
            gap = run_t[h : h + 1, :] - run[:, h : h + 1]
            near = jnp.exp(jnp.where(causal, gap, FAR))
            w_t = scores_t * near
            dw_t = dot(xvb, mine, NT)
            scored = scored + dw_t * near
            g_t = dw_t * w_t
            rows_t[h : h + 1, :] = jnp.sum(g_t, axis=0, keepdims=True)
            cols = jnp.where(lane == h, jnp.sum(g_t, axis=1, keepdims=True), cols)
            dxv = dxv + dot(w_t.astype(BF16), mine)
        dsum[:, at] = (dxv * v).astype(BF16)
        dmix[:, at] = size_p * dxv + pick(head_ref[2:3, :], p, low) * dy
        line[0:1, at] += jnp.sum(dy * v, axis=0, keepdims=True)
        line[1:2, at] = jnp.sum(adj[:, at] * mem_b[:, at].astype(F32), axis=0, keepdims=True) * pick(
            last, p, low
        )
        xc = (pick(left, p, low) * xv).astype(BF16)
        dygb = dyg.astype(BF16)
        db = dot(xc, adj_b[:, at], NT)
        dc = dot(dygb, mem_b[:, at], NT)
        if p == 0:
            dmix[:, inner : inner + N] = db
            dmix[:, inner + N :] = dc
        else:
            dmix[:, inner : inner + N] += db
            dmix[:, inner + N :] += dc
        adj[:, at] = adj[:, at] * pick(last, p, low) + dot(c_t, dygb)
    dmix[:, inner : inner + N] += dot(scored.astype(BF16), c)
    dmix[:, inner + N :] += dot(scored.T.astype(BF16), b)

    group = jnp.where(
        lax.broadcasted_iota(jnp.int32, (inner, LANES), 0) // P_SIZE
        == lax.broadcasted_iota(jnp.int32, (inner, LANES), 1),
        1.0,
        0.0,
    )
    group_b = group.astype(BF16)
    d_step = dot(dsum[...], group_b)
    u = dot(uprod[...], group_b)
    z = dot(zprod[...], group_b)
    sums = dot(line[...], group, precision=HIGH)
    d_run = rows_t[...].T - cols + u - z
    row = lax.broadcasted_iota(jnp.int32, (size, 1), 0)
    ending = sums[1:2, :] + jnp.sum(z, axis=0, keepdims=True)
    d_run = d_run + jnp.where(row == size - 1, ending, 0.0)
    d_decay = dot(jnp.where(causal, 1.0, 0.0), d_run, precision=HIGH)
    d_raw = (d_step - jnp.exp(head_ref[0:1, :]) * d_decay) * lax.logistic(raw)
    d_raw = jnp.where(lane < heads, d_raw, 0.0)
    hgrad_ref[0:1, :] += jnp.sum(d_decay * decay, axis=0, keepdims=True)
    hgrad_ref[1:2, :] += jnp.sum(d_raw, axis=0, keepdims=True)

    @pl.when(finish)
    def _():
        hgrad_ref[2:3, :] = sums[0:1, :]

    g = dmix[...] * (sig * (1.0 + mixed * (1.0 - sig)))
    gbuf[0:size, :] = g
    wgrad_ref[KW : KW + 1, :] += jnp.sum(g, axis=0, keepdims=True)
    for k in range(KW):
        wgrad_ref[k : k + 1, :] += jnp.sum(g * xbuf[5 + k : 5 + k + size, :], axis=0, keepdims=True)
    back = taps_ref[KW - 1 : KW, :] * g
    for k in range(KW - 1):
        back = back + taps_ref[k : k + 1, :] * gbuf[3 - k : 3 - k + size, :]
    out_ref[:, :wide] = back.astype(BF16)
    out_ref[:, wide:] = d_raw.astype(BF16)


def mixer_forward(rest, taps, head, heads, micro):
    count, full = rest.shape
    wide = taps.shape[1]
    inner = heads * P_SIZE
    chunks = count // micro // CHUNK
    return pl.pallas_call(
        functools.partial(forward_kernel, heads),
        grid=(micro, chunks),
        in_specs=[
            pl.BlockSpec((CHUNK, full), lambda m, c: (m * chunks + c, 0)),
            pl.BlockSpec((8, wide), lambda m, c: (0, 0)),
            pl.BlockSpec((8, LANES), lambda m, c: (0, 0)),
        ],
        out_specs=[
            pl.BlockSpec((CHUNK, inner), lambda m, c: (m * chunks + c, 0)),
            pl.BlockSpec((1, N, inner), lambda m, c: (m * chunks + c, 0, 0)),
        ],
        out_shape=[
            jax.ShapeDtypeStruct((count, inner), F32),
            jax.ShapeDtypeStruct((micro * chunks, N, inner), BF16),
        ],
        scratch_shapes=[pltpu.VMEM((CHUNK + 8, wide), F32), pltpu.VMEM((N, inner), F32)],
        compiler_params=pltpu.CompilerParams(dimension_semantics=("arbitrary", "arbitrary")),
        cost_estimate=pl.CostEstimate(flops=3 * 10**9, bytes_accessed=2 * 10**7, transcendentals=10**7),
        name="mixer_forward",
    )(rest, taps, head)


def mixer_backward(rest, dy, memory, taps, head, heads, micro):
    count, full = rest.shape
    wide = taps.shape[1]
    inner = heads * P_SIZE
    chunks = count // micro // CHUNK

    def at(m, c):
        return m * chunks + chunks - 1 - c

    return pl.pallas_call(
        functools.partial(backward_kernel, heads),
        grid=(micro, chunks),
        in_specs=[
            pl.BlockSpec((CHUNK, full), lambda m, c: (at(m, c), 0)),
            pl.BlockSpec((8, full), lambda m, c: (jnp.maximum(at(m, c) * (CHUNK // 8) - 1, 0), 0)),
            pl.BlockSpec((CHUNK, inner), lambda m, c: (at(m, c), 0)),
            pl.BlockSpec((1, N, inner), lambda m, c: (at(m, c), 0, 0)),
            pl.BlockSpec((8, wide), lambda m, c: (0, 0)),
            pl.BlockSpec((8, LANES), lambda m, c: (0, 0)),
        ],
        out_specs=[
            pl.BlockSpec((CHUNK, full), lambda m, c: (at(m, c), 0)),
            pl.BlockSpec((8, wide), lambda m, c: (0, 0)),
            pl.BlockSpec((8, LANES), lambda m, c: (0, 0)),
        ],
        out_shape=[
            jax.ShapeDtypeStruct((count, full), BF16),
            jax.ShapeDtypeStruct((8, wide), F32),
            jax.ShapeDtypeStruct((8, LANES), F32),
        ],
        scratch_shapes=[
            pltpu.VMEM((CHUNK + 8, wide), F32),
            pltpu.VMEM((CHUNK + 8, wide), F32),
            pltpu.VMEM((N, inner), F32),
            pltpu.VMEM((CHUNK, wide), F32),
            pltpu.VMEM((CHUNK, inner), BF16),
            pltpu.VMEM((CHUNK, inner), BF16),
            pltpu.VMEM((CHUNK, inner), BF16),
            pltpu.VMEM((LANES, CHUNK), F32),
            pltpu.VMEM((8, inner), F32),
        ],
        compiler_params=pltpu.CompilerParams(dimension_semantics=("arbitrary", "arbitrary")),
        cost_estimate=pl.CostEstimate(flops=10**10, bytes_accessed=4 * 10**7, transcendentals=10**7),
        name="mixer_backward",
    )(rest, rest, dy, memory, taps, head)


def weight_columns(in_proj, own, tp, heads):
    rows = in_proj.shape[0]
    inner = heads * P_SIZE
    cells = -(-own.shape[0] // rows)
    packed = jnp.pad(own, (0, rows * cells - own.shape[0])).reshape(rows, 1, cells)
    gate = in_proj[:, :DI].reshape(rows, tp, inner).transpose(1, 0, 2)
    rest = jnp.concatenate(
        [
            in_proj[:, DI : 2 * DI].reshape(rows, tp, inner),
            jnp.broadcast_to(in_proj[:, None, 2 * DI : 2 * DI + 2 * N], (rows, tp, 2 * N)),
            in_proj[:, 2 * DI + 2 * N :].reshape(rows, tp, heads),
            jnp.broadcast_to(packed, (rows, tp, cells)),
            jnp.zeros((rows, tp, LANES - heads - cells), BF16),
        ],
        axis=2,
    ).transpose(1, 0, 2)
    return rest, gate


def body(
    tokens,
    in_proj,
    conv_weight,
    conv_bias,
    decay_log,
    step_bias,
    skip_gain,
    norm_gain,
    gated_gain,
    out_proj,
    cotangent,
):
    dp, tp = lax.axis_size("dp"), lax.axis_size("seq")
    total = dp * tp
    s = lax.axis_index("seq")
    micro, part, width = tokens.shape
    heads = HEADS // tp
    inner = heads * P_SIZE
    rows = in_proj.shape[0]
    length = part * tp
    count = micro * length
    wide = inner + 2 * N
    chan = conv_bias.shape[0]

    own = jnp.concatenate([conv_weight.reshape(-1), conv_bias, norm_gain, gated_gain])
    rest, gate = weight_columns(in_proj, own, tp, heads)
    columns = jnp.concatenate([rest, gate], axis=2)
    columns = lax.all_to_all(columns, "seq", 0, 0).reshape(tp * rows, -1)
    w_rest = lax.all_gather(columns[:, : wide + LANES], "dp", axis=0, tiled=True)
    w_gate = lax.all_gather(columns[:, wide + LANES :], "dp", axis=0, tiled=True)
    tok = lax.all_gather(tokens, "seq", axis=1, tiled=True).reshape(count, width)
    turn = [(b * dp + a, a * tp + b) for a in range(dp) for b in range(tp)]
    w_out = lax.ppermute(out_proj, ("dp", "seq"), turn)
    w_out = lax.all_gather(w_out, "dp", axis=0, tiled=True)
    cot = lax.all_gather(cotangent, "seq", axis=1, tiled=True).reshape(count, width)

    cells = -(-own.shape[0] // rows)
    shared = w_rest[:, wide + heads : wide + heads + cells].reshape(total, rows * cells).astype(F32)
    w_conv = shared[:, : KW * chan].reshape(total, KW, chan).transpose(1, 0, 2).reshape(KW, CD)
    b_conv = shared[:, KW * chan : (KW + 1) * chan].reshape(1, CD)
    at = (KW + 1) * chan
    g_norm = shared[:, at : at + rows].reshape(width)
    g_gated = shared[:, at + rows : at + rows + gated_gain.shape[0]].reshape(DI)
    first, lane = s * inner, s * heads
    taps = jnp.concatenate([w_conv, b_conv, jnp.zeros((3, CD), F32)], axis=0)
    taps = jnp.concatenate([lax.dynamic_slice_in_dim(taps, first, inner, 1), taps[:, DI:]], axis=1)
    g_gated = lax.dynamic_slice_in_dim(g_gated, first, inner)
    head = jnp.stack([decay_log, step_bias, skip_gain])
    head = lax.dynamic_slice_in_dim(head, lane, heads, 1)
    head = jnp.pad(head, ((0, 5), (0, LANES - heads)))

    h = tok.astype(F32)
    r = lax.rsqrt(jnp.mean(h * h, axis=-1, keepdims=True) + EPSILON)
    normed = (h * r * g_norm).astype(BF16)
    proj_rest = jnp.dot(normed, w_rest, preferred_element_type=F32)
    ssd, memory = mixer_forward(proj_rest, taps, head, heads, micro)
    gate = jnp.dot(normed, w_gate, preferred_element_type=F32)
    sig = jax.nn.sigmoid(gate)
    act = gate * sig
    gated = ssd * act
    grad_shaped = jnp.dot(cot, w_out.T, preferred_element_type=F32)
    weighed = grad_shaped * g_gated
    stats = jnp.stack([jnp.sum(gated * gated, axis=1), jnp.sum(weighed * gated, axis=1)])
    stats = lax.psum(stats, "seq")
    q = lax.rsqrt(stats[0] / DI + EPSILON)[:, None]
    shaped = (gated * q * g_gated).astype(BF16)
    grad_gated = q * (weighed - gated * (q * q * (stats[1] / DI)[:, None]))
    grad_ssd = grad_gated * act
    grad_gate = (grad_gated * ssd * (sig + act * (1 - sig))).astype(BF16)

    out_part = jnp.dot(shaped, w_out, preferred_element_type=F32).astype(BF16)
    out_part = lax.psum_scatter(
        out_part.reshape(micro, length, width), "seq", scatter_dimension=1, tiled=True
    )
    h_own = tokens.astype(F32)
    block_out = (h_own + out_part.astype(F32)).astype(BF16)

    grad_out = jnp.dot(shaped.T, cot, preferred_element_type=F32).astype(BF16)
    grad_out = lax.psum_scatter(grad_out, "dp", scatter_dimension=0, tiled=True)
    grad_out = lax.ppermute(grad_out, ("dp", "seq"), [(b, a) for a, b in turn]).astype(F32)
    gated_gain_grad = jnp.sum(out_proj.astype(F32) * grad_out, axis=1) / gated_gain.astype(F32)
    gate_in = jnp.dot(normed.T, grad_gate, preferred_element_type=F32).astype(BF16)
    gate_in = lax.psum_scatter(gate_in, "dp", scatter_dimension=0, tiled=True)
    gate_in = lax.all_to_all(gate_in.reshape(tp, rows, inner), "seq", 0, 0)

    grad_rest, wgrad, hgrad = mixer_backward(proj_rest, grad_ssd, memory, taps, head, heads, micro)
    small = jnp.concatenate([wgrad[: KW + 1].reshape(-1), hgrad[:3].reshape(-1)])
    small = lax.all_gather(small, ("dp", "seq")).reshape(dp, tp, -1)
    small = jnp.sum(small, axis=0)
    convs = small[:, : (KW + 1) * wide].reshape(tp, KW + 1, wide)
    convs = jnp.concatenate(
        [
            convs[:, :, :inner].transpose(1, 0, 2).reshape(KW + 1, DI),
            jnp.sum(convs[:, :, inner:], axis=0),
        ],
        axis=1,
    )
    place = lax.axis_index("dp") * tp + s
    convs = lax.dynamic_slice_in_dim(convs, place * chan, chan, 1)
    head_grads = small[:, (KW + 1) * wide :].reshape(tp, 3, LANES)[:, :, :heads]
    head_grads = head_grads.transpose(1, 0, 2).reshape(3, HEADS)

    rest_in = jnp.dot(normed.T, grad_rest, preferred_element_type=F32).astype(BF16)
    rest_in = lax.psum_scatter(rest_in, "dp", scatter_dimension=0, tiled=True)
    rest_in = lax.all_to_all(rest_in.reshape(tp, rows, wide + LANES), "seq", 0, 0).astype(F32)

    def side(a):
        return a.astype(F32).transpose(1, 0, 2).reshape(rows, -1)

    in_grad = jnp.concatenate(
        [
            side(gate_in),
            side(rest_in[:, :, :inner]),
            jnp.sum(rest_in[:, :, inner:wide], axis=0),
            side(rest_in[:, :, wide : wide + heads]),
        ],
        axis=1,
    )
    norm_gain_grad = jnp.sum(in_proj.astype(F32) * in_grad, axis=1) / norm_gain.astype(F32)

    grad_normed = (
        lax.dot_general(grad_rest, w_rest, (((1,), (1,)), ((), ())), preferred_element_type=F32)
        + lax.dot_general(grad_gate, w_gate, (((1,), (1,)), ((), ())), preferred_element_type=F32)
    ).astype(BF16)
    grad_normed = lax.psum_scatter(
        grad_normed.reshape(micro, length, width), "seq", scatter_dimension=1, tiled=True
    ).astype(F32)
    r_own = lax.rsqrt(jnp.mean(h_own * h_own, axis=-1, keepdims=True) + EPSILON)
    n_own = h_own * r_own
    g = grad_normed * g_norm
    tokens_grad = cotangent.astype(F32) + r_own * (
        g - n_own * jnp.mean(g * n_own, axis=-1, keepdims=True)
    )
    return (
        block_out,
        tokens_grad.astype(BF16),
        in_grad,
        convs[:KW],
        convs[KW],
        head_grads[0],
        head_grads[1],
        head_grads[2],
        norm_gain_grad,
        gated_gain_grad,
        grad_out,
    )


def solution(mesh):
    both = ("dp", "seq")
    return jax.shard_map(
        body,
        mesh=mesh,
        in_specs=(
            P("dp", "seq", None),
            P(both, None),
            P(None, both),
            P(both),
            P(),
            P(),
            P(),
            P(both),
            P(both),
            P(both, None),
            P("dp", "seq", None),
        ),
        out_specs=(
            P("dp", "seq", None),
            P("dp", "seq", None),
            P(both, None),
            P(None, both),
            P(both),
            P(),
            P(),
            P(),
            P(both),
            P(both),
            P(both, None),
        ),
        check_vma=False,
    )
```

```python
import functools

import jax
import jax.numpy as jnp
from jax import lax
from jax.experimental import pallas as pl
from jax.experimental.pallas import tpu as pltpu
from jax.sharding import PartitionSpec as P

HEADS = 48
P_SIZE = 64
N = 128
KW = 4
DI = 3072
CD = 3328
LANES = 128
CHUNK = 128
FAR = -1e30

EPSILON = 1e-05
F32 = jnp.float32
BF16 = jnp.bfloat16


def dot(a, b, dims=((1,), (0,)), precision=None):
    return lax.dot_general(a, b, (dims, ((), ())), precision=precision, preferred_element_type=F32)


NT = ((1,), (1,))
HIGH = lax.Precision.HIGHEST


def pick(a, p, low):
    return jnp.where(low, a[:, 2 * p : 2 * p + 1], a[:, 2 * p + 1 : 2 * p + 2])


def chunk_parts(heads, rest_ref, xbuf, taps_ref, head_ref):
    size = rest_ref.shape[0]
    wide = taps_ref.shape[1]
    mixed = taps_ref[KW : KW + 1, :] + taps_ref[0:1, :] * xbuf[5 : 5 + size, :]
    for k in range(1, KW):
        mixed = mixed + taps_ref[k : k + 1, :] * xbuf[5 + k : 5 + k + size, :]
    sig = lax.logistic(mixed)
    lane = lax.broadcasted_iota(jnp.int32, (1, LANES), 1)
    raw = jnp.where(lane < heads, rest_ref[:, wide:], 0.0) + head_ref[1:2, :]
    step = jnp.maximum(raw, 0.0) + jnp.log1p(jnp.exp(-jnp.abs(raw)))
    decay = -jnp.exp(head_ref[0:1, :]) * step
    i = lax.broadcasted_iota(jnp.int32, (size, size), 0)
    j = lax.broadcasted_iota(jnp.int32, (size, size), 1)
    run = dot(jnp.where(i >= j, 1.0, 0.0), decay, precision=HIGH)
    return mixed, sig, raw, step, decay, run


def forward_kernel(heads, rest_ref, taps_ref, head_ref, ssd_ref, mem_ref, xbuf, mem):
    size = rest_ref.shape[0]
    wide = taps_ref.shape[1]
    inner = heads * P_SIZE
    first = pl.program_id(1) == 0

    @pl.when(first)
    def _():
        xbuf[0:8, :] = jnp.zeros((8, wide), F32)
        mem[...] = jnp.zeros_like(mem)

    @pl.when(jnp.logical_not(first))
    def _():
        xbuf[0:8, :] = xbuf[size : size + 8, :]

    xbuf[8 : 8 + size, :] = rest_ref[:, :wide]
    mixed, sig, _, step, _, run = chunk_parts(heads, rest_ref, xbuf, taps_ref, head_ref)
    act = mixed * sig
    run_t = run.T
    closing = run[size - 1 : size, :]
    last = jnp.exp(closing)
    left = jnp.exp(closing - run)
    grown = jnp.exp(run)
    b = act[:, inner : inner + N]
    c = act[:, inner + N :].astype(BF16)
    scores = dot(c, b.astype(BF16), NT)
    b_t = b.T.astype(BF16)
    mem_ref[0] = mem[...].astype(BF16)
    inter = dot(c, mem[...].astype(BF16))
    low = lax.broadcasted_iota(jnp.int32, (1, LANES), 1) < P_SIZE
    i = lax.broadcasted_iota(jnp.int32, (size, size), 0)
    j = lax.broadcasted_iota(jnp.int32, (size, size), 1)
    causal = i >= j
    for p in range(heads // 2):
        at = slice(p * LANES, (p + 1) * LANES)
        v = act[:, at]
        xv = pick(step, p, low) * v
        y = pick(head_ref[2:3, :], p, low) * v + pick(grown, p, low) * inter[:, at]
        for e in range(2):
            h = 2 * p + e
            gap = run[:, h : h + 1] - run_t[h : h + 1, :]
            w = (scores * jnp.exp(jnp.where(causal, gap, FAR))).astype(BF16)
            mine = jnp.where(low if e == 0 else jnp.logical_not(low), xv, 0.0).astype(BF16)
            y = y + dot(w, mine)
        ssd_ref[:, at] = y
        xc = (pick(left, p, low) * xv).astype(BF16)
        mem[:, at] = mem[:, at] * pick(last, p, low) + dot(b_t, xc)


def backward_kernel(
    heads,
    rest_ref,
    prev_ref,
    dy_ref,
    mem_ref,
    taps_ref,
    head_ref,
    out_ref,
    wgrad_ref,
    hgrad_ref,
    xbuf,
    gbuf,
    adj,
    dmix,
    dsum,
    uprod,
    zprod,
    rows_t,
    line,
):
    size = rest_ref.shape[0]
    wide = taps_ref.shape[1]
    inner = heads * P_SIZE
    chunks = pl.num_programs(1)
    step_id = pl.program_id(1)
    newest = step_id == 0
    oldest = step_id == chunks - 1
    begin = jnp.logical_and(pl.program_id(0) == 0, newest)
    finish = jnp.logical_and(pl.program_id(0) == pl.num_programs(0) - 1, oldest)

    @pl.when(begin)
    def _():
        wgrad_ref[...] = jnp.zeros_like(wgrad_ref)
        hgrad_ref[...] = jnp.zeros_like(hgrad_ref)
        rows_t[...] = jnp.zeros_like(rows_t)
        line[...] = jnp.zeros_like(line)

    @pl.when(newest)
    def _():
        gbuf[size : size + 8, :] = jnp.zeros((8, wide), F32)
        adj[...] = jnp.zeros_like(adj)

    @pl.when(jnp.logical_not(newest))
    def _():
        gbuf[size : size + 8, :] = gbuf[0:8, :]

    xbuf[0:8, :] = jnp.where(oldest, 0.0, prev_ref[:, :wide])
    xbuf[8 : 8 + size, :] = rest_ref[:, :wide]
    mixed, sig, raw, step, decay, run = chunk_parts(heads, rest_ref, xbuf, taps_ref, head_ref)
    act = mixed * sig
    run_t = run.T
    closing = run[size - 1 : size, :]
    last = jnp.exp(closing)
    left = jnp.exp(closing - run)
    grown = jnp.exp(run)
    b = act[:, inner : inner + N].astype(BF16)
    c = act[:, inner + N :].astype(BF16)
    c_t = act[:, inner + N :].T.astype(BF16)
    scores_t = dot(b, c, NT)
    low = lax.broadcasted_iota(jnp.int32, (1, LANES), 1) < P_SIZE
    lane = lax.broadcasted_iota(jnp.int32, (1, LANES), 1)
    j = lax.broadcasted_iota(jnp.int32, (size, size), 0)
    i = lax.broadcasted_iota(jnp.int32, (size, size), 1)
    causal = i >= j
    mem_b = mem_ref[0]
    adj_b = adj[...].astype(BF16)
    spread = dot(b, adj_b)
    inherit = dot(c, mem_b)
    scored = jnp.zeros((size, size), F32)
    cols = jnp.zeros((size, LANES), F32)
    for p in range(heads // 2):
        at = slice(p * LANES, (p + 1) * LANES)
        v = act[:, at]
        size_p = pick(step, p, low)
        xv = size_p * v
        dy = dy_ref[:, at]
        dyb = dy.astype(BF16)
        xvb = xv.astype(BF16)
        dxv = pick(left, p, low) * spread[:, at]
        zprod[:, at] = (dxv * xv).astype(BF16)
        dyg = pick(grown, p, low) * dy
        uprod[:, at] = (dyg * inherit[:, at]).astype(BF16)
        for e in range(2):
            h = 2 * p + e
            keep = low if e == 0 else jnp.logical_not(low)
            mine = jnp.where(keep, dy, 0.0).astype(BF16)
            gap = run_t[h : h + 1, :] - run[:, h : h + 1]
            near = jnp.exp(jnp.where(causal, gap, FAR))
            w_t = scores_t * near
            dw_t = dot(xvb, mine, NT)
            scored = scored + dw_t * near
            g_t = dw_t * w_t
            rows_t[h : h + 1, :] = jnp.sum(g_t, axis=0, keepdims=True)
            cols = jnp.where(lane == h, jnp.sum(g_t, axis=1, keepdims=True), cols)
            dxv = dxv + dot(w_t.astype(BF16), mine)
        dsum[:, at] = (dxv * v).astype(BF16)
        dmix[:, at] = size_p * dxv + pick(head_ref[2:3, :], p, low) * dy
        line[0:1, at] += jnp.sum(dy * v, axis=0, keepdims=True)
        line[1:2, at] = jnp.sum(adj[:, at] * mem_b[:, at].astype(F32), axis=0, keepdims=True) * pick(
            last, p, low
        )
        xc = (pick(left, p, low) * xv).astype(BF16)
        dygb = dyg.astype(BF16)
        db = dot(xc, adj_b[:, at], NT)
        dc = dot(dygb, mem_b[:, at], NT)
        if p == 0:
            dmix[:, inner : inner + N] = db
            dmix[:, inner + N :] = dc
        else:
            dmix[:, inner : inner + N] += db
            dmix[:, inner + N :] += dc
        adj[:, at] = adj[:, at] * pick(last, p, low) + dot(c_t, dygb)
    dmix[:, inner : inner + N] += dot(scored.astype(BF16), c)
    dmix[:, inner + N :] += dot(scored.T.astype(BF16), b)

    group = jnp.where(
        lax.broadcasted_iota(jnp.int32, (inner, LANES), 0) // P_SIZE
        == lax.broadcasted_iota(jnp.int32, (inner, LANES), 1),
        1.0,
        0.0,
    )
    group_b = group.astype(BF16)
    d_step = dot(dsum[...], group_b)
    u = dot(uprod[...], group_b)
    z = dot(zprod[...], group_b)
    sums = dot(line[...], group, precision=HIGH)
    d_run = rows_t[...].T - cols + u - z
    row = lax.broadcasted_iota(jnp.int32, (size, 1), 0)
    ending = sums[1:2, :] + jnp.sum(z, axis=0, keepdims=True)
    d_run = d_run + jnp.where(row == size - 1, ending, 0.0)
    d_decay = dot(jnp.where(causal, 1.0, 0.0), d_run, precision=HIGH)
    d_raw = (d_step - jnp.exp(head_ref[0:1, :]) * d_decay) * lax.logistic(raw)
    d_raw = jnp.where(lane < heads, d_raw, 0.0)
    hgrad_ref[0:1, :] += jnp.sum(d_decay * decay, axis=0, keepdims=True)
    hgrad_ref[1:2, :] += jnp.sum(d_raw, axis=0, keepdims=True)

    @pl.when(finish)
    def _():
        hgrad_ref[2:3, :] = sums[0:1, :]

    g = dmix[...] * (sig * (1.0 + mixed * (1.0 - sig)))
    gbuf[0:size, :] = g
    wgrad_ref[KW : KW + 1, :] += jnp.sum(g, axis=0, keepdims=True)
    for k in range(KW):
        wgrad_ref[k : k + 1, :] += jnp.sum(g * xbuf[5 + k : 5 + k + size, :], axis=0, keepdims=True)
    back = taps_ref[KW - 1 : KW, :] * g
    for k in range(KW - 1):
        back = back + taps_ref[k : k + 1, :] * gbuf[3 - k : 3 - k + size, :]
    out_ref[:, :wide] = back.astype(BF16)
    out_ref[:, wide:] = d_raw.astype(BF16)


def mixer_forward(rest, taps, head, heads, micro):
    count, full = rest.shape
    wide = taps.shape[1]
    inner = heads * P_SIZE
    chunks = count // micro // CHUNK
    return pl.pallas_call(
        functools.partial(forward_kernel, heads),
        grid=(micro, chunks),
        in_specs=[
            pl.BlockSpec((CHUNK, full), lambda m, c: (m * chunks + c, 0)),
            pl.BlockSpec((8, wide), lambda m, c: (0, 0)),
            pl.BlockSpec((8, LANES), lambda m, c: (0, 0)),
        ],
        out_specs=[
            pl.BlockSpec((CHUNK, inner), lambda m, c: (m * chunks + c, 0)),
            pl.BlockSpec((1, N, inner), lambda m, c: (m * chunks + c, 0, 0)),
        ],
        out_shape=[
            jax.ShapeDtypeStruct((count, inner), F32),
            jax.ShapeDtypeStruct((micro * chunks, N, inner), BF16),
        ],
        scratch_shapes=[pltpu.VMEM((CHUNK + 8, wide), F32), pltpu.VMEM((N, inner), F32)],
        compiler_params=pltpu.CompilerParams(dimension_semantics=("arbitrary", "arbitrary")),
        cost_estimate=pl.CostEstimate(flops=3 * 10**9, bytes_accessed=2 * 10**7, transcendentals=10**7),
        name="mixer_forward",
    )(rest, taps, head)


def mixer_backward(rest, dy, memory, taps, head, heads, micro):
    count, full = rest.shape
    wide = taps.shape[1]
    inner = heads * P_SIZE
    chunks = count // micro // CHUNK

    def at(m, c):
        return m * chunks + chunks - 1 - c

    return pl.pallas_call(
        functools.partial(backward_kernel, heads),
        grid=(micro, chunks),
        in_specs=[
            pl.BlockSpec((CHUNK, full), lambda m, c: (at(m, c), 0)),
            pl.BlockSpec((8, full), lambda m, c: (jnp.maximum(at(m, c) * (CHUNK // 8) - 1, 0), 0)),
            pl.BlockSpec((CHUNK, inner), lambda m, c: (at(m, c), 0)),
            pl.BlockSpec((1, N, inner), lambda m, c: (at(m, c), 0, 0)),
            pl.BlockSpec((8, wide), lambda m, c: (0, 0)),
            pl.BlockSpec((8, LANES), lambda m, c: (0, 0)),
        ],
        out_specs=[
            pl.BlockSpec((CHUNK, full), lambda m, c: (at(m, c), 0)),
            pl.BlockSpec((8, wide), lambda m, c: (0, 0)),
            pl.BlockSpec((8, LANES), lambda m, c: (0, 0)),
        ],
        out_shape=[
            jax.ShapeDtypeStruct((count, full), BF16),
            jax.ShapeDtypeStruct((8, wide), F32),
            jax.ShapeDtypeStruct((8, LANES), F32),
        ],
        scratch_shapes=[
            pltpu.VMEM((CHUNK + 8, wide), F32),
            pltpu.VMEM((CHUNK + 8, wide), F32),
            pltpu.VMEM((N, inner), F32),
            pltpu.VMEM((CHUNK, wide), F32),
            pltpu.VMEM((CHUNK, inner), BF16),
            pltpu.VMEM((CHUNK, inner), BF16),
            pltpu.VMEM((CHUNK, inner), BF16),
            pltpu.VMEM((LANES, CHUNK), F32),
            pltpu.VMEM((8, inner), F32),
        ],
        compiler_params=pltpu.CompilerParams(dimension_semantics=("arbitrary", "arbitrary")),
        cost_estimate=pl.CostEstimate(flops=10**10, bytes_accessed=4 * 10**7, transcendentals=10**7),
        name="mixer_backward",
    )(rest, rest, dy, memory, taps, head)


MESH = pl.DeviceIdType.MESH


def where_am_i(dp):
    d, s = lax.axis_index("dp"), lax.axis_index("seq")
    z, y = d // 2, d % 2
    x, c = s // 2, s % 2
    peers = [s + 1 - 2 * c, s + 2 - 4 * x, 3 - s]
    return d, s, z, y, x, c, peers, dp // 2


def push(src, dst, send_sem, recv_sem, d, s):
    return pltpu.make_async_remote_copy(
        src_ref=src,
        dst_ref=dst,
        send_sem=send_sem,
        recv_sem=recv_sem,
        device_id={"dp": d, "seq": s},
        device_id_type=MESH,
    )


def greet(partners):
    barrier = pltpu.get_barrier_semaphore()
    for cond, d, s in partners:

        def hello(d=d, s=s):
            pl.semaphore_signal(barrier, inc=1, device_id={"dp": d, "seq": s}, device_id_type=MESH)

        if cond is None:
            hello()
        else:
            pl.when(cond)(hello)
    count = 0
    for cond, _, _ in partners:
        count = count + (1 if cond is None else jnp.where(cond, 1, 0))
    pl.semaphore_wait(barrier, count)


class Sends:
    def __init__(self):
        self.items = []

    def start(self, cond, copy):
        if cond is None:
            copy.start()
        else:
            pl.when(cond)(copy.start)
        self.items.append((cond, copy))

    def drain(self):
        for cond, copy in self.items:
            if cond is None:
                copy.wait_send()
            else:
                pl.when(cond)(copy.wait_send)


def gather_kernel(
    dp, rest_ref, gate_ref, tok_ref, w_rest, w_gate, tok, own, a_send, a_recv, z_send, z_recv, y_send, y_recv, t_send, t_recv
):
    d, s, z, y, x, c, peers, deep = where_am_i(dp)
    part = tok_ref.shape[1]
    up, down, far = d + 2, d - 2, d + 1 - 2 * y
    greet(
        [(None, d, p) for p in peers]
        + [(None, far, s), (z < deep - 1, up, s), (z > 0, down, s)]
    )
    sends = Sends()
    parts = ((0, rest_ref, w_rest), (1, gate_ref, w_gate))

    def exchange(a, src, dst):
        for r, p in enumerate(peers):
            sends.start(None, push(src.at[p], dst.at[d, s], a_send.at[a, r], a_recv.at[a, r], d, p))

    def mine(k):
        return tok.at[:, pl.ds(k * part, part), :]

    exchange(*parts[0])
    locals_ = [
        pltpu.make_async_copy(rest_ref.at[s], w_rest.at[d, s], own.at[0]),
        pltpu.make_async_copy(gate_ref.at[s], w_gate.at[d, s], own.at[1]),
        pltpu.make_async_copy(tok_ref, mine(s), own.at[2]),
    ]
    for copy in locals_:
        copy.start()
    sends.start(None, push(tok_ref, mine(s), t_send.at[1], t_recv.at[1], d, peers[1]))
    sends.start(None, push(tok_ref, mine(s), t_send.at[0], t_recv.at[0], d, peers[0]))
    exchange(*parts[1])

    def arrive(dst, sem):
        push(dst, dst, sem, sem, d, peers[0]).wait_recv()

    def spread(a, dst):
        shard = dst.at[d]
        sends.start(z < deep - 1, push(shard, shard, z_send.at[a, 0, 0], z_recv.at[a, 0, 0], up, s))
        sends.start(z > 0, push(shard, shard, z_send.at[a, 1, 0], z_recv.at[a, 1, 0], down, s))
        sends.start(None, push(shard, shard, y_send.at[a, 0, 0], y_recv.at[a, 0, 0], far, s))
        for t in range(1, deep):
            for way in range(2):
                here = (z >= t) if way == 0 else (z + t <= deep - 1)
                more = jnp.logical_and(here, (z < deep - 1) if way == 0 else (z > 0))
                at = jnp.clip(d - 2 * t if way == 0 else d + 2 * t, 0, dp - 1)
                block = dst.at[at]
                pl.when(here)(functools.partial(arrive, block, z_recv.at[a, way, t - 1]))
                if t < deep - 1:
                    nxt = up if way == 0 else down
                    sends.start(
                        more, push(block, block, z_send.at[a, way, t], z_recv.at[a, way, t], nxt, s)
                    )
                sends.start(
                    here, push(block, block, y_send.at[a, way, t], y_recv.at[a, way, t], far, s)
                )

    def landed(a, dst):
        arrive(dst.at[d + 1 - 2 * y], y_recv.at[a, 0, 0])
        for t in range(1, deep):
            for way in range(2):
                here = (z >= t) if way == 0 else (z + t <= deep - 1)
                at = jnp.clip(far - 2 * t if way == 0 else far + 2 * t, 0, dp - 1)
                pl.when(here)(functools.partial(arrive, dst.at[at], y_recv.at[a, way, t]))

    for a, _, dst in parts:
        locals_[a].wait()
        for r, p in enumerate(peers):
            arrive(dst.at[d, p], a_recv.at[a, r])
        spread(a, dst)
    arrive(mine(peers[1]), t_recv.at[1])
    block = mine(peers[1])
    sends.start(None, push(block, block, t_send.at[2], t_recv.at[2], d, peers[0]))
    for a, _, dst in parts:
        landed(a, dst)
    arrive(mine(peers[0]), t_recv.at[0])
    arrive(mine(peers[2]), t_recv.at[2])
    locals_[2].wait()
    sends.drain()


def gather(rest, gate, tokens, dp):
    tp, rows = rest.shape[:2]
    micro, part, width = tokens.shape
    deep = dp // 2
    dma = pltpu.SemaphoreType.DMA
    vmem = pl.BlockSpec(memory_space=pltpu.VMEM)
    hbm = pl.BlockSpec(memory_space=pl.ANY)
    return pl.pallas_call(
        functools.partial(gather_kernel, dp),
        in_specs=[vmem] * 3,
        out_specs=[hbm] * 3,
        out_shape=[
            jax.ShapeDtypeStruct((dp, tp, rows, rest.shape[2]), BF16),
            jax.ShapeDtypeStruct((dp, tp, rows, gate.shape[2]), BF16),
            jax.ShapeDtypeStruct((micro, tp * part, width), BF16),
        ],
        scratch_shapes=[
            dma((3,)),
            dma((2, 3)),
            dma((2, 3)),
            dma((2, 2, deep - 1)),
            dma((2, 2, deep - 1)),
            dma((2, 2, deep)),
            dma((2, 2, deep)),
            dma((3,)),
            dma((3,)),
        ],
        compiler_params=pltpu.CompilerParams(collective_id=1, has_side_effects=True),
        cost_estimate=pl.CostEstimate(flops=5 * 10**10, bytes_accessed=3 * 10**7, transcendentals=0),
        name="weights_and_tokens",
    )(rest, gate, tokens)


def stats_kernel(dp, own_ref, out_ref, held, send, recv):
    d, s, *_, peers, _ = where_am_i(dp)
    greet([(None, d, p) for p in peers])
    copies = [
        push(own_ref, held.at[r], send.at[r], recv.at[r], d, p) for r, p in enumerate(peers)
    ]
    for copy in copies:
        copy.start()
    for copy in copies:
        copy.wait()
    out_ref[...] = (own_ref[...] + held[0]) + (held[1] + held[2])


def add_over_seq(stats, dp):
    dma = pltpu.SemaphoreType.DMA
    vmem = pl.BlockSpec(memory_space=pltpu.VMEM)
    return pl.pallas_call(
        functools.partial(stats_kernel, dp),
        in_specs=[vmem],
        out_specs=vmem,
        out_shape=jax.ShapeDtypeStruct(stats.shape, F32),
        scratch_shapes=[pltpu.VMEM((3,) + stats.shape, F32), dma((3,)), dma((3,))],
        compiler_params=pltpu.CompilerParams(collective_id=2, has_side_effects=True),
        name="stats_over_seq",
    )(stats)


def scatter_kernel(
    dp,
    grad_ref,
    normed_ref,
    small_ref,
    out_ref,
    own_ref,
    sums_ref,
    ybuf,
    zbuf,
    final,
    core_buf,
    x_buf,
    s_buf,
    y_send,
    y_recv,
    z_send,
    z_recv,
    a_send,
    a_recv,
    c_send,
    c_recv,
    x_send,
    x_recv,
    s_send,
    s_recv,
):
    d, s, z, y, x, c, peers, deep = where_am_i(dp)
    tp, rows = grad_ref.shape[1:3]
    micro, part, width = own_ref.shape
    up, down, far = d + 2, d - 2, d + 1 - 2 * y
    bits = dp.bit_length() - 1
    partners = []
    for k in range(bits):
        step = 2**k
        bit = (d // step) % 2
        partners.append(d + step - 2 * step * bit)
    greet(
        [(None, d, p) for p in peers]
        + [(None, far, s), (z < deep - 1, up, s), (z > 0, down, s)]
        + [(None, partners[k], s) for k in range(2, bits)]
    )
    sends = Sends()
    lower = z < deep // 2

    def place(j):
        low = jnp.where(j > z, deep - 1 - j, deep - 1 - z + j)
        high = jnp.where(j < z, j, z + deep - 1 - j)
        return jnp.where(j == z, deep - 1, jnp.where(lower, low, high))

    def turn(k):
        low = jnp.where(k < deep - 1 - z, deep - 1 - k, k - (deep - 1 - z))
        high = jnp.where(k < z, k, deep - 1 - (k - z))
        return jnp.where(lower, low, high) if k < deep - 1 else z

    def chunk(k):
        return normed_ref.at[:, pl.ds(k * part, part), :]

    def arrive(dst, sem):
        push(dst, dst, sem, sem, d, peers[0]).wait_recv()

    for q, xx in enumerate((1 - x, x)):
        src = chunk(xx * 2 + 1 - c)
        sends.start(None, push(src, core_buf.at[q], c_send.at[q], c_recv.at[q], d, peers[0]))
    order = [turn(k) for k in range(deep)]
    for k in range(deep):
        src = grad_ref.at[order[k] * 2 + 1 - y]
        sends.start(None, push(src, ybuf.at[k], y_send.at[k], y_recv.at[k], far, s))
    sums_ref[0] = small_ref[...]
    sends.start(None, push(small_ref, s_buf.at[0], s_send.at[0], s_recv.at[0], partners[0], s))

    def add_rows(count, work):
        lax.fori_loop(0, count, lambda i, carry: (work(i), carry)[1], 0)

    def add_normed(q, xx):
        mine = xx * 2 + c
        span = 16

        def work(i):
            m, row = i // (part // span), (i % (part // span)) * span
            row = pl.multiple_of(row, span)
            theirs = core_buf[q, m, pl.ds(row, span), :].astype(F32)
            ours = normed_ref[m, pl.ds(pl.multiple_of(mine * part + row, span), span), :].astype(F32)
            core_buf[q, m, pl.ds(row, span), :] = (theirs + ours).astype(BF16)

        add_rows(micro * (part // span), work)

    arrive(core_buf.at[0], c_recv.at[0])
    add_normed(0, 1 - x)
    sends.start(None, push(core_buf.at[0], x_buf, x_send.at[0], x_recv.at[0], d, peers[1]))
    arrive(core_buf.at[1], c_recv.at[1])

    def doubling(k):
        arrive(s_buf.at[k], s_recv.at[k])
        if k + 1 < bits:
            sums_ref[k + 1] = sums_ref[k] + s_buf[k]
            sends.start(
                None,
                push(sums_ref.at[k + 1], s_buf.at[k + 1], s_send.at[k + 1], s_recv.at[k + 1], partners[k + 1], s),
            )
        else:
            final_sum = sums_ref[k] + s_buf[k]
            sums_ref[bits] = final_sum

    def add_y(k):
        arrive(ybuf.at[k], y_recv.at[k])
        at = order[k] * 2 + y

        def work(i):
            ybuf[k, i] = (ybuf[k, i].astype(F32) + grad_ref[at, i].astype(F32)).astype(BF16)

        add_rows(tp, work)

    def send_z(t):
        for way in range(2):
            depth = z if way == 0 else deep - 1 - z
            j = deep - 1 - t + z if way == 0 else t + z - deep + 1
            j = jnp.clip(j, 0, deep - 1)
            k = place(j)
            nxt = up if way == 0 else down
            first = depth == 0
            dst = zbuf.at[way, t]
            sends.start(
                first, push(ybuf.at[k], dst, z_send.at[way, t], z_recv.at[way, t], nxt, s)
            )
            if t == 0:
                continue
            later = jnp.logical_and(depth > 0, depth <= t)

            @pl.when(later)
            def _():
                arrive(zbuf.at[way, t - 1], z_recv.at[way, t - 1])

                def work(i):
                    zbuf[way, t - 1, i] = (
                        zbuf[way, t - 1, i].astype(F32) + ybuf[k, i].astype(F32)
                    ).astype(BF16)

                add_rows(tp, work)

            sends.start(
                later,
                push(zbuf.at[way, t - 1], dst, z_send.at[way, t], z_recv.at[way, t], nxt, s),
            )

    for k in range(deep):
        add_y(k)
        if k < deep - 1:
            send_z(k)
        if k < bits:
            doubling(k)
    for k in range(deep, bits):
        doubling(k)
    for r, p in enumerate(peers):
        sends.start(
            None,
            push(sums_ref.at[bits], sums_ref.at[bits + 1 + s], s_send.at[bits + r], s_recv.at[bits + r], d, p),
        )
    sums_ref[bits + 1 + s] = sums_ref[bits]

    for way in range(2):
        depth = z if way == 0 else deep - 1 - z

        @pl.when(depth > 0)
        def _():
            arrive(zbuf.at[way, deep - 2], z_recv.at[way, deep - 2])

    def finish(ways, i):
        total = ybuf[deep - 1, i].astype(F32)
        for way in ways:
            total = total + zbuf[way, deep - 2, i].astype(F32)
        final[i] = total.astype(BF16)

    for cond, ways in (
        (z == 0, (1,)),
        (z == deep - 1, (0,)),
        (jnp.logical_and(z > 0, z < deep - 1), (0, 1)),
    ):

        @pl.when(cond)
        def _():
            add_rows(tp, functools.partial(finish, ways))

    for r, p in enumerate(peers):
        sends.start(None, push(final.at[p], out_ref.at[s], a_send.at[r], a_recv.at[r], d, p))
    out_ref[s] = final[s]

    arrive(x_buf, x_recv.at[0])
    span = 16

    def own_rows(i):
        m, row = i // (part // span), (i % (part // span)) * span
        row = pl.multiple_of(row, span)
        here = pl.multiple_of(s * part + row, span)
        own_ref[m, pl.ds(row, span), :] = (
            core_buf[1, m, pl.ds(row, span), :].astype(F32)
            + normed_ref[m, pl.ds(here, span), :].astype(F32)
            + x_buf[m, pl.ds(row, span), :].astype(F32)
        )

    add_rows(micro * (part // span), own_rows)
    for r, p in enumerate(peers):
        arrive(out_ref.at[p], a_recv.at[r])
        arrive(sums_ref.at[bits + 1 + p], s_recv.at[bits + r])
    sends.drain()


def scatter(grad, normed, small, dp):
    tp, rows, wide = grad.shape[1:]
    micro, length, width = normed.shape
    part = length // tp
    deep = dp // 2
    bits = dp.bit_length() - 1
    dma = pltpu.SemaphoreType.DMA
    vmem = pl.BlockSpec(memory_space=pltpu.VMEM)
    return pl.pallas_call(
        functools.partial(scatter_kernel, dp),
        in_specs=[vmem] * 3,
        out_specs=[vmem] * 3,
        out_shape=[
            jax.ShapeDtypeStruct((tp, rows, wide), BF16),
            jax.ShapeDtypeStruct((micro, part, width), F32),
            jax.ShapeDtypeStruct((bits + 1 + tp,) + small.shape, F32),
        ],
        scratch_shapes=[
            pltpu.VMEM((deep, tp, rows, wide), BF16),
            pltpu.VMEM((2, deep - 1, tp, rows, wide), BF16),
            pltpu.VMEM((tp, rows, wide), BF16),
            pltpu.VMEM((2, micro, part, width), BF16),
            pltpu.VMEM((micro, part, width), BF16),
            pltpu.VMEM((bits,) + small.shape, F32),
            dma((deep,)),
            dma((deep,)),
            dma((2, deep - 1)),
            dma((2, deep - 1)),
            dma((3,)),
            dma((3,)),
            dma((2,)),
            dma((2,)),
            dma((1,)),
            dma((1,)),
            dma((bits + 3,)),
            dma((bits + 3,)),
        ],
        compiler_params=pltpu.CompilerParams(
            collective_id=3, has_side_effects=True, vmem_limit_bytes=60 * 2**20
        ),
        cost_estimate=pl.CostEstimate(flops=5 * 10**10, bytes_accessed=3 * 10**7, transcendentals=0),
        name="gradients_to_owners",
    )(grad, normed, small)


def weight_columns(in_proj, own, tp, heads):
    rows = in_proj.shape[0]
    inner = heads * P_SIZE
    cells = -(-own.shape[0] // rows)
    packed = jnp.pad(own, (0, rows * cells - own.shape[0])).reshape(rows, 1, cells)
    gate = in_proj[:, :DI].reshape(rows, tp, inner).transpose(1, 0, 2)
    rest = jnp.concatenate(
        [
            in_proj[:, DI : 2 * DI].reshape(rows, tp, inner),
            jnp.broadcast_to(in_proj[:, None, 2 * DI : 2 * DI + 2 * N], (rows, tp, 2 * N)),
            in_proj[:, 2 * DI + 2 * N :].reshape(rows, tp, heads),
            jnp.broadcast_to(packed, (rows, tp, cells)),
            jnp.zeros((rows, tp, LANES - heads - cells), BF16),
        ],
        axis=2,
    ).transpose(1, 0, 2)
    return rest, gate


def body(
    tokens,
    in_proj,
    conv_weight,
    conv_bias,
    decay_log,
    step_bias,
    skip_gain,
    norm_gain,
    gated_gain,
    out_proj,
    cotangent,
):
    dp, tp = lax.axis_size("dp"), lax.axis_size("seq")
    total = dp * tp
    s = lax.axis_index("seq")
    micro, part, width = tokens.shape
    heads = HEADS // tp
    inner = heads * P_SIZE
    rows = in_proj.shape[0]
    length = part * tp
    count = micro * length
    wide = inner + 2 * N
    chan = conv_bias.shape[0]

    own = jnp.concatenate([conv_weight.reshape(-1), conv_bias, norm_gain, gated_gain])
    rest, gate = weight_columns(in_proj, own, tp, heads)
    w_rest, w_gate, tok = gather(rest, gate, tokens, dp)
    w_rest = w_rest.reshape(width, wide + LANES)
    w_gate = w_gate.reshape(width, inner)
    tok = tok.reshape(count, width)
    turn = [(b * dp + a, a * tp + b) for a in range(dp) for b in range(tp)]
    w_out = lax.ppermute(out_proj, ("dp", "seq"), turn)
    w_out = lax.all_gather(w_out, "dp", axis=0, tiled=True)
    cot = lax.all_gather(cotangent, "seq", axis=1, tiled=True).reshape(count, width)

    cells = -(-own.shape[0] // rows)
    shared = w_rest[:, wide + heads : wide + heads + cells].reshape(total, rows * cells).astype(F32)
    w_conv = shared[:, : KW * chan].reshape(total, KW, chan).transpose(1, 0, 2).reshape(KW, CD)
    b_conv = shared[:, KW * chan : (KW + 1) * chan].reshape(1, CD)
    at = (KW + 1) * chan
    g_norm = shared[:, at : at + rows].reshape(width)
    g_gated = shared[:, at + rows : at + rows + gated_gain.shape[0]].reshape(DI)
    first, lane = s * inner, s * heads
    taps = jnp.concatenate([w_conv, b_conv, jnp.zeros((3, CD), F32)], axis=0)
    taps = jnp.concatenate([lax.dynamic_slice_in_dim(taps, first, inner, 1), taps[:, DI:]], axis=1)
    g_gated = lax.dynamic_slice_in_dim(g_gated, first, inner)
    head = jnp.stack([decay_log, step_bias, skip_gain])
    head = lax.dynamic_slice_in_dim(head, lane, heads, 1)
    head = jnp.pad(head, ((0, 5), (0, LANES - heads)))

    h = tok.astype(F32)
    r = lax.rsqrt(jnp.mean(h * h, axis=-1, keepdims=True) + EPSILON)
    normed = (h * r * g_norm).astype(BF16)
    proj_rest = jnp.dot(normed, w_rest, preferred_element_type=F32)
    ssd, memory = mixer_forward(proj_rest, taps, head, heads, micro)
    gate = jnp.dot(normed, w_gate, preferred_element_type=F32)
    sig = jax.nn.sigmoid(gate)
    act = gate * sig
    gated = ssd * act
    grad_shaped = jnp.dot(cot, w_out.T, preferred_element_type=F32)
    weighed = grad_shaped * g_gated
    stats = jnp.stack([jnp.sum(gated * gated, axis=1), jnp.sum(weighed * gated, axis=1)])
    stats = add_over_seq(stats, dp)
    q = lax.rsqrt(stats[0] / DI + EPSILON)[:, None]
    shaped = (gated * q * g_gated).astype(BF16)
    grad_gated = q * (weighed - gated * (q * q * (stats[1] / DI)[:, None]))
    grad_ssd = grad_gated * act
    grad_gate = (grad_gated * ssd * (sig + act * (1 - sig))).astype(BF16)

    out_part = jnp.dot(shaped, w_out, preferred_element_type=F32).astype(BF16)
    out_part = lax.psum_scatter(
        out_part.reshape(micro, length, width), "seq", scatter_dimension=1, tiled=True
    )
    h_own = tokens.astype(F32)
    block_out = (h_own + out_part.astype(F32)).astype(BF16)

    grad_out = jnp.dot(shaped.T, cot, preferred_element_type=F32).astype(BF16)
    grad_out = lax.psum_scatter(grad_out, "dp", scatter_dimension=0, tiled=True)
    grad_out = lax.ppermute(grad_out, ("dp", "seq"), [(b, a) for a, b in turn]).astype(F32)
    gated_gain_grad = jnp.sum(out_proj.astype(F32) * grad_out, axis=1) / gated_gain.astype(F32)
    gate_in = jnp.dot(normed.T, grad_gate, preferred_element_type=F32).astype(BF16)
    gate_in = lax.psum_scatter(gate_in, "dp", scatter_dimension=0, tiled=True)
    gate_in = lax.all_to_all(gate_in.reshape(tp, rows, inner), "seq", 0, 0)

    grad_rest, wgrad, hgrad = mixer_backward(proj_rest, grad_ssd, memory, taps, head, heads, micro)
    small = jnp.concatenate([wgrad[: KW + 1].reshape(-1), hgrad[:3].reshape(-1)])
    lines = -(-small.shape[0] // (8 * LANES)) * 8
    small = jnp.pad(small, (0, lines * LANES - small.shape[0])).reshape(lines, LANES)
    rest_in = jnp.dot(normed.T, grad_rest, preferred_element_type=F32).astype(BF16)
    grad_normed = (
        lax.dot_general(grad_rest, w_rest, (((1,), (1,)), ((), ())), preferred_element_type=F32)
        + lax.dot_general(grad_gate, w_gate, (((1,), (1,)), ((), ())), preferred_element_type=F32)
    ).astype(BF16)
    rest_in, grad_normed, small = scatter(
        rest_in.reshape(dp, tp, rows, wide + LANES),
        grad_normed.reshape(micro, length, width),
        small,
        dp,
    )
    rest_in = rest_in.astype(F32)
    small = small[-tp:].reshape(tp, -1)
    convs = small[:, : (KW + 1) * wide].reshape(tp, KW + 1, wide)
    convs = jnp.concatenate(
        [
            convs[:, :, :inner].transpose(1, 0, 2).reshape(KW + 1, DI),
            jnp.sum(convs[:, :, inner:], axis=0),
        ],
        axis=1,
    )
    place = lax.axis_index("dp") * tp + s
    convs = lax.dynamic_slice_in_dim(convs, place * chan, chan, 1)
    head_grads = small[:, (KW + 1) * wide : (KW + 1) * wide + 3 * LANES].reshape(tp, 3, LANES)[:, :, :heads]
    head_grads = head_grads.transpose(1, 0, 2).reshape(3, HEADS)

    def side(a):
        return a.astype(F32).transpose(1, 0, 2).reshape(rows, -1)

    in_grad = jnp.concatenate(
        [
            side(gate_in),
            side(rest_in[:, :, :inner]),
            jnp.sum(rest_in[:, :, inner:wide], axis=0),
            side(rest_in[:, :, wide : wide + heads]),
        ],
        axis=1,
    )
    norm_gain_grad = jnp.sum(in_proj.astype(F32) * in_grad, axis=1) / norm_gain.astype(F32)

    r_own = lax.rsqrt(jnp.mean(h_own * h_own, axis=-1, keepdims=True) + EPSILON)
    n_own = h_own * r_own
    g = grad_normed * g_norm
    tokens_grad = cotangent.astype(F32) + r_own * (
        g - n_own * jnp.mean(g * n_own, axis=-1, keepdims=True)
    )
    return (
        block_out,
        tokens_grad.astype(BF16),
        in_grad,
        convs[:KW],
        convs[KW],
        head_grads[0],
        head_grads[1],
        head_grads[2],
        norm_gain_grad,
        gated_gain_grad,
        grad_out,
    )


def solution(mesh):
    both = ("dp", "seq")
    return jax.shard_map(
        body,
        mesh=mesh,
        in_specs=(
            P("dp", "seq", None),
            P(both, None),
            P(None, both),
            P(both),
            P(),
            P(),
            P(),
            P(both),
            P(both),
            P(both, None),
            P("dp", "seq", None),
        ),
        out_specs=(
            P("dp", "seq", None),
            P("dp", "seq", None),
            P(both, None),
            P(None, both),
            P(both),
            P(),
            P(),
            P(),
            P(both),
            P(both),
            P(both, None),
        ),
        check_vma=False,
    )
```

```python
import functools

import jax
import jax.numpy as jnp
from jax import lax
from jax.experimental import pallas as pl
from jax.experimental.pallas import tpu as pltpu
from jax.sharding import PartitionSpec as P

HEADS = 48
P_SIZE = 64
N = 128
KW = 4
DI = 3072
CD = 3328
LANES = 128
CHUNK = 128
FAR = -1e30

EPSILON = 1e-05
F32 = jnp.float32
BF16 = jnp.bfloat16


def dot(a, b, dims=((1,), (0,)), precision=None):
    return lax.dot_general(a, b, (dims, ((), ())), precision=precision, preferred_element_type=F32)


NT = ((1,), (1,))
HIGH = lax.Precision.HIGHEST


def pick(a, p, low):
    return jnp.where(low, a[:, 2 * p : 2 * p + 1], a[:, 2 * p + 1 : 2 * p + 2])


def chunk_parts(heads, rest_ref, xbuf, taps_ref, head_ref):
    size = rest_ref.shape[0]
    wide = taps_ref.shape[1]
    mixed = taps_ref[KW : KW + 1, :] + taps_ref[0:1, :] * xbuf[5 : 5 + size, :]
    for k in range(1, KW):
        mixed = mixed + taps_ref[k : k + 1, :] * xbuf[5 + k : 5 + k + size, :]
    sig = lax.logistic(mixed)
    lane = lax.broadcasted_iota(jnp.int32, (1, LANES), 1)
    raw = jnp.where(lane < heads, rest_ref[:, wide:], 0.0) + head_ref[1:2, :]
    step = jnp.maximum(raw, 0.0) + jnp.log1p(jnp.exp(-jnp.abs(raw)))
    decay = -jnp.exp(head_ref[0:1, :]) * step
    i = lax.broadcasted_iota(jnp.int32, (size, size), 0)
    j = lax.broadcasted_iota(jnp.int32, (size, size), 1)
    run = dot(jnp.where(i >= j, 1.0, 0.0), decay, precision=HIGH)
    return mixed, sig, raw, step, decay, run


def forward_kernel(heads, rest_ref, taps_ref, head_ref, ssd_ref, mem_ref, xbuf, mem):
    size = rest_ref.shape[0]
    wide = taps_ref.shape[1]
    inner = heads * P_SIZE
    first = pl.program_id(1) == 0

    @pl.when(first)
    def _():
        xbuf[0:8, :] = jnp.zeros((8, wide), F32)
        mem[...] = jnp.zeros_like(mem)

    @pl.when(jnp.logical_not(first))
    def _():
        xbuf[0:8, :] = xbuf[size : size + 8, :]

    xbuf[8 : 8 + size, :] = rest_ref[:, :wide]
    mixed, sig, _, step, _, run = chunk_parts(heads, rest_ref, xbuf, taps_ref, head_ref)
    act = mixed * sig
    run_t = run.T
    closing = run[size - 1 : size, :]
    last = jnp.exp(closing)
    left = jnp.exp(closing - run)
    grown = jnp.exp(run)
    b = act[:, inner : inner + N]
    c = act[:, inner + N :].astype(BF16)
    scores = dot(c, b.astype(BF16), NT)
    b_t = b.T.astype(BF16)
    mem_ref[0] = mem[...].astype(BF16)
    inter = dot(c, mem[...].astype(BF16))
    low = lax.broadcasted_iota(jnp.int32, (1, LANES), 1) < P_SIZE
    i = lax.broadcasted_iota(jnp.int32, (size, size), 0)
    j = lax.broadcasted_iota(jnp.int32, (size, size), 1)
    causal = i >= j
    for p in range(heads // 2):
        at = slice(p * LANES, (p + 1) * LANES)
        v = act[:, at]
        xv = pick(step, p, low) * v
        y = pick(head_ref[2:3, :], p, low) * v + pick(grown, p, low) * inter[:, at]
        for e in range(2):
            h = 2 * p + e
            gap = run[:, h : h + 1] - run_t[h : h + 1, :]
            w = (scores * jnp.exp(jnp.where(causal, gap, FAR))).astype(BF16)
            mine = jnp.where(low if e == 0 else jnp.logical_not(low), xv, 0.0).astype(BF16)
            y = y + dot(w, mine)
        ssd_ref[:, at] = y
        xc = (pick(left, p, low) * xv).astype(BF16)
        mem[:, at] = mem[:, at] * pick(last, p, low) + dot(b_t, xc)


def backward_kernel(
    heads,
    rest_ref,
    prev_ref,
    dy_ref,
    mem_ref,
    taps_ref,
    head_ref,
    out_ref,
    wgrad_ref,
    hgrad_ref,
    xbuf,
    gbuf,
    adj,
    dmix,
    dsum,
    uprod,
    zprod,
    rows_t,
    line,
):
    size = rest_ref.shape[0]
    wide = taps_ref.shape[1]
    inner = heads * P_SIZE
    chunks = pl.num_programs(1)
    step_id = pl.program_id(1)
    newest = step_id == 0
    oldest = step_id == chunks - 1
    begin = jnp.logical_and(pl.program_id(0) == 0, newest)
    finish = jnp.logical_and(pl.program_id(0) == pl.num_programs(0) - 1, oldest)

    @pl.when(begin)
    def _():
        wgrad_ref[...] = jnp.zeros_like(wgrad_ref)
        hgrad_ref[...] = jnp.zeros_like(hgrad_ref)
        rows_t[...] = jnp.zeros_like(rows_t)
        line[...] = jnp.zeros_like(line)

    @pl.when(newest)
    def _():
        gbuf[size : size + 8, :] = jnp.zeros((8, wide), F32)
        adj[...] = jnp.zeros_like(adj)

    @pl.when(jnp.logical_not(newest))
    def _():
        gbuf[size : size + 8, :] = gbuf[0:8, :]

    xbuf[0:8, :] = jnp.where(oldest, 0.0, prev_ref[:, :wide])
    xbuf[8 : 8 + size, :] = rest_ref[:, :wide]
    mixed, sig, raw, step, decay, run = chunk_parts(heads, rest_ref, xbuf, taps_ref, head_ref)
    act = mixed * sig
    run_t = run.T
    closing = run[size - 1 : size, :]
    last = jnp.exp(closing)
    left = jnp.exp(closing - run)
    grown = jnp.exp(run)
    b = act[:, inner : inner + N].astype(BF16)
    c = act[:, inner + N :].astype(BF16)
    c_t = act[:, inner + N :].T.astype(BF16)
    scores_t = dot(b, c, NT)
    low = lax.broadcasted_iota(jnp.int32, (1, LANES), 1) < P_SIZE
    lane = lax.broadcasted_iota(jnp.int32, (1, LANES), 1)
    j = lax.broadcasted_iota(jnp.int32, (size, size), 0)
    i = lax.broadcasted_iota(jnp.int32, (size, size), 1)
    causal = i >= j
    mem_b = mem_ref[0]
    adj_b = adj[...].astype(BF16)
    spread = dot(b, adj_b)
    inherit = dot(c, mem_b)
    scored = jnp.zeros((size, size), F32)
    cols = jnp.zeros((size, LANES), F32)
    for p in range(heads // 2):
        at = slice(p * LANES, (p + 1) * LANES)
        v = act[:, at]
        size_p = pick(step, p, low)
        xv = size_p * v
        dy = dy_ref[:, at]
        dyb = dy.astype(BF16)
        xvb = xv.astype(BF16)
        dxv = pick(left, p, low) * spread[:, at]
        zprod[:, at] = (dxv * xv).astype(BF16)
        dyg = pick(grown, p, low) * dy
        uprod[:, at] = (dyg * inherit[:, at]).astype(BF16)
        for e in range(2):
            h = 2 * p + e
            keep = low if e == 0 else jnp.logical_not(low)
            mine = jnp.where(keep, dy, 0.0).astype(BF16)
            gap = run_t[h : h + 1, :] - run[:, h : h + 1]
            near = jnp.exp(jnp.where(causal, gap, FAR))
            w_t = scores_t * near
            dw_t = dot(xvb, mine, NT)
            scored = scored + dw_t * near
            g_t = dw_t * w_t
            rows_t[h : h + 1, :] = jnp.sum(g_t, axis=0, keepdims=True)
            cols = jnp.where(lane == h, jnp.sum(g_t, axis=1, keepdims=True), cols)
            dxv = dxv + dot(w_t.astype(BF16), mine)
        dsum[:, at] = (dxv * v).astype(BF16)
        dmix[:, at] = size_p * dxv + pick(head_ref[2:3, :], p, low) * dy
        line[0:1, at] += jnp.sum(dy * v, axis=0, keepdims=True)
        line[1:2, at] = jnp.sum(adj[:, at] * mem_b[:, at].astype(F32), axis=0, keepdims=True) * pick(
            last, p, low
        )
        xc = (pick(left, p, low) * xv).astype(BF16)
        dygb = dyg.astype(BF16)
        db = dot(xc, adj_b[:, at], NT)
        dc = dot(dygb, mem_b[:, at], NT)
        if p == 0:
            dmix[:, inner : inner + N] = db
            dmix[:, inner + N :] = dc
        else:
            dmix[:, inner : inner + N] += db
            dmix[:, inner + N :] += dc
        adj[:, at] = adj[:, at] * pick(last, p, low) + dot(c_t, dygb)
    dmix[:, inner : inner + N] += dot(scored.astype(BF16), c)
    dmix[:, inner + N :] += dot(scored.T.astype(BF16), b)

    group = jnp.where(
        lax.broadcasted_iota(jnp.int32, (inner, LANES), 0) // P_SIZE
        == lax.broadcasted_iota(jnp.int32, (inner, LANES), 1),
        1.0,
        0.0,
    )
    group_b = group.astype(BF16)
    d_step = dot(dsum[...], group_b)
    u = dot(uprod[...], group_b)
    z = dot(zprod[...], group_b)
    sums = dot(line[...], group, precision=HIGH)
    d_run = rows_t[...].T - cols + u - z
    row = lax.broadcasted_iota(jnp.int32, (size, 1), 0)
    ending = sums[1:2, :] + jnp.sum(z, axis=0, keepdims=True)
    d_run = d_run + jnp.where(row == size - 1, ending, 0.0)
    d_decay = dot(jnp.where(causal, 1.0, 0.0), d_run, precision=HIGH)
    d_raw = (d_step - jnp.exp(head_ref[0:1, :]) * d_decay) * lax.logistic(raw)
    d_raw = jnp.where(lane < heads, d_raw, 0.0)
    hgrad_ref[0:1, :] += jnp.sum(d_decay * decay, axis=0, keepdims=True)
    hgrad_ref[1:2, :] += jnp.sum(d_raw, axis=0, keepdims=True)

    @pl.when(finish)
    def _():
        hgrad_ref[2:3, :] = sums[0:1, :]

    g = dmix[...] * (sig * (1.0 + mixed * (1.0 - sig)))
    gbuf[0:size, :] = g
    wgrad_ref[KW : KW + 1, :] += jnp.sum(g, axis=0, keepdims=True)
    for k in range(KW):
        wgrad_ref[k : k + 1, :] += jnp.sum(g * xbuf[5 + k : 5 + k + size, :], axis=0, keepdims=True)
    back = taps_ref[KW - 1 : KW, :] * g
    for k in range(KW - 1):
        back = back + taps_ref[k : k + 1, :] * gbuf[3 - k : 3 - k + size, :]
    out_ref[:, :wide] = back.astype(BF16)
    out_ref[:, wide:] = d_raw.astype(BF16)


def mixer_forward(rest, taps, head, heads, micro):
    count, full = rest.shape
    wide = taps.shape[1]
    inner = heads * P_SIZE
    chunks = count // micro // CHUNK
    return pl.pallas_call(
        functools.partial(forward_kernel, heads),
        grid=(micro, chunks),
        in_specs=[
            pl.BlockSpec((CHUNK, full), lambda m, c: (m * chunks + c, 0)),
            pl.BlockSpec((8, wide), lambda m, c: (0, 0)),
            pl.BlockSpec((8, LANES), lambda m, c: (0, 0)),
        ],
        out_specs=[
            pl.BlockSpec((CHUNK, inner), lambda m, c: (m * chunks + c, 0)),
            pl.BlockSpec((1, N, inner), lambda m, c: (m * chunks + c, 0, 0)),
        ],
        out_shape=[
            jax.ShapeDtypeStruct((count, inner), F32),
            jax.ShapeDtypeStruct((micro * chunks, N, inner), BF16),
        ],
        scratch_shapes=[pltpu.VMEM((CHUNK + 8, wide), F32), pltpu.VMEM((N, inner), F32)],
        compiler_params=pltpu.CompilerParams(dimension_semantics=("arbitrary", "arbitrary")),
        cost_estimate=pl.CostEstimate(flops=25 * 10**9, bytes_accessed=2 * 10**7, transcendentals=10**7),
        name="mixer_forward",
    )(rest, taps, head)


def mixer_backward(rest, dy, memory, taps, head, heads, micro):
    count, full = rest.shape
    wide = taps.shape[1]
    inner = heads * P_SIZE
    chunks = count // micro // CHUNK

    def at(m, c):
        return m * chunks + chunks - 1 - c

    return pl.pallas_call(
        functools.partial(backward_kernel, heads),
        grid=(micro, chunks),
        in_specs=[
            pl.BlockSpec((CHUNK, full), lambda m, c: (at(m, c), 0)),
            pl.BlockSpec((8, full), lambda m, c: (jnp.maximum(at(m, c) * (CHUNK // 8) - 1, 0), 0)),
            pl.BlockSpec((CHUNK, inner), lambda m, c: (at(m, c), 0)),
            pl.BlockSpec((1, N, inner), lambda m, c: (at(m, c), 0, 0)),
            pl.BlockSpec((8, wide), lambda m, c: (0, 0)),
            pl.BlockSpec((8, LANES), lambda m, c: (0, 0)),
        ],
        out_specs=[
            pl.BlockSpec((CHUNK, full), lambda m, c: (at(m, c), 0)),
            pl.BlockSpec((8, wide), lambda m, c: (0, 0)),
            pl.BlockSpec((8, LANES), lambda m, c: (0, 0)),
        ],
        out_shape=[
            jax.ShapeDtypeStruct((count, full), BF16),
            jax.ShapeDtypeStruct((8, wide), F32),
            jax.ShapeDtypeStruct((8, LANES), F32),
        ],
        scratch_shapes=[
            pltpu.VMEM((CHUNK + 8, wide), F32),
            pltpu.VMEM((CHUNK + 8, wide), F32),
            pltpu.VMEM((N, inner), F32),
            pltpu.VMEM((CHUNK, wide), F32),
            pltpu.VMEM((CHUNK, inner), BF16),
            pltpu.VMEM((CHUNK, inner), BF16),
            pltpu.VMEM((CHUNK, inner), BF16),
            pltpu.VMEM((LANES, CHUNK), F32),
            pltpu.VMEM((8, inner), F32),
        ],
        compiler_params=pltpu.CompilerParams(dimension_semantics=("arbitrary", "arbitrary")),
        cost_estimate=pl.CostEstimate(flops=7 * 10**10, bytes_accessed=4 * 10**7, transcendentals=10**7),
        name="mixer_backward",
    )(rest, rest, dy, memory, taps, head)


MESH = pl.DeviceIdType.MESH


def where_am_i(dp):
    d, s = lax.axis_index("dp"), lax.axis_index("seq")
    z, y = d // 2, d % 2
    x, c = s // 2, s % 2
    peers = [s + 1 - 2 * c, s + 2 - 4 * x, 3 - s]
    return d, s, z, y, x, c, peers, dp // 2


def push(src, dst, send_sem, recv_sem, d, s):
    return pltpu.make_async_remote_copy(
        src_ref=src,
        dst_ref=dst,
        send_sem=send_sem,
        recv_sem=recv_sem,
        device_id={"dp": d, "seq": s},
        device_id_type=MESH,
    )


def greet(partners):
    barrier = pltpu.get_barrier_semaphore()
    for cond, d, s in partners:

        def hello(d=d, s=s):
            pl.semaphore_signal(barrier, inc=1, device_id={"dp": d, "seq": s}, device_id_type=MESH)

        if cond is None:
            hello()
        else:
            pl.when(cond)(hello)
    count = 0
    for cond, _, _ in partners:
        count = count + (1 if cond is None else jnp.where(cond, 1, 0))
    pl.semaphore_wait(barrier, count)


class Sends:
    def __init__(self):
        self.items = []

    def start(self, cond, copy):
        if cond is None:
            copy.start()
        else:
            pl.when(cond)(copy.start)
        self.items.append((cond, copy))

    def drain(self):
        for cond, copy in self.items:
            if cond is None:
                copy.wait_send()
            else:
                pl.when(cond)(copy.wait_send)


def gather_kernel(
    dp, rest_ref, gate_ref, tok_ref, w_rest, w_gate, tok, own, a_send, a_recv, z_send, z_recv, y_send, y_recv, t_send, t_recv
):
    d, s, z, y, x, c, peers, deep = where_am_i(dp)
    part = tok_ref.shape[1]
    up, down, far = d + 2, d - 2, d + 1 - 2 * y
    greet(
        [(None, d, p) for p in peers]
        + [(None, far, s), (z < deep - 1, up, s), (z > 0, down, s)]
    )
    sends = Sends()
    parts = ((0, rest_ref, w_rest), (1, gate_ref, w_gate))

    def exchange(a, src, dst):
        for r, p in enumerate(peers):
            sends.start(None, push(src.at[p], dst.at[d, s], a_send.at[a, r], a_recv.at[a, r], d, p))

    def mine(k):
        return tok.at[:, pl.ds(k * part, part), :]

    exchange(*parts[0])
    locals_ = [
        pltpu.make_async_copy(rest_ref.at[s], w_rest.at[d, s], own.at[0]),
        pltpu.make_async_copy(gate_ref.at[s], w_gate.at[d, s], own.at[1]),
        pltpu.make_async_copy(tok_ref, mine(s), own.at[2]),
    ]
    for copy in locals_:
        copy.start()
    sends.start(None, push(tok_ref, mine(s), t_send.at[1], t_recv.at[1], d, peers[1]))
    sends.start(None, push(tok_ref, mine(s), t_send.at[0], t_recv.at[0], d, peers[0]))
    exchange(*parts[1])

    def arrive(dst, sem):
        push(dst, dst, sem, sem, d, peers[0]).wait_recv()

    def spread(a, dst):
        shard = dst.at[d]
        sends.start(z < deep - 1, push(shard, shard, z_send.at[a, 0, 0], z_recv.at[a, 0, 0], up, s))
        sends.start(z > 0, push(shard, shard, z_send.at[a, 1, 0], z_recv.at[a, 1, 0], down, s))
        sends.start(None, push(shard, shard, y_send.at[a, 0, 0], y_recv.at[a, 0, 0], far, s))
        for t in range(1, deep):
            for way in range(2):
                here = (z >= t) if way == 0 else (z + t <= deep - 1)
                more = jnp.logical_and(here, (z < deep - 1) if way == 0 else (z > 0))
                at = jnp.clip(d - 2 * t if way == 0 else d + 2 * t, 0, dp - 1)
                block = dst.at[at]
                pl.when(here)(functools.partial(arrive, block, z_recv.at[a, way, t - 1]))
                if t < deep - 1:
                    nxt = up if way == 0 else down
                    sends.start(
                        more, push(block, block, z_send.at[a, way, t], z_recv.at[a, way, t], nxt, s)
                    )
                sends.start(
                    here, push(block, block, y_send.at[a, way, t], y_recv.at[a, way, t], far, s)
                )

    def landed(a, dst):
        arrive(dst.at[d + 1 - 2 * y], y_recv.at[a, 0, 0])
        for t in range(1, deep):
            for way in range(2):
                here = (z >= t) if way == 0 else (z + t <= deep - 1)
                at = jnp.clip(far - 2 * t if way == 0 else far + 2 * t, 0, dp - 1)
                pl.when(here)(functools.partial(arrive, dst.at[at], y_recv.at[a, way, t]))

    for a, _, dst in parts:
        locals_[a].wait()
        for r, p in enumerate(peers):
            arrive(dst.at[d, p], a_recv.at[a, r])
        spread(a, dst)
    arrive(mine(peers[1]), t_recv.at[1])
    block = mine(peers[1])
    sends.start(None, push(block, block, t_send.at[2], t_recv.at[2], d, peers[0]))
    for a, _, dst in parts:
        landed(a, dst)
    arrive(mine(peers[0]), t_recv.at[0])
    arrive(mine(peers[2]), t_recv.at[2])
    locals_[2].wait()
    sends.drain()


def gather(rest, gate, tokens, dp):
    tp, rows = rest.shape[:2]
    micro, part, width = tokens.shape
    deep = dp // 2
    dma = pltpu.SemaphoreType.DMA
    vmem = pl.BlockSpec(memory_space=pltpu.VMEM)
    hbm = pl.BlockSpec(memory_space=pl.ANY)
    return pl.pallas_call(
        functools.partial(gather_kernel, dp),
        in_specs=[vmem] * 3,
        out_specs=[hbm] * 3,
        out_shape=[
            jax.ShapeDtypeStruct((dp, tp, rows, rest.shape[2]), BF16),
            jax.ShapeDtypeStruct((dp, tp, rows, gate.shape[2]), BF16),
            jax.ShapeDtypeStruct((micro, tp * part, width), BF16),
        ],
        scratch_shapes=[
            dma((3,)),
            dma((2, 3)),
            dma((2, 3)),
            dma((2, 2, deep - 1)),
            dma((2, 2, deep - 1)),
            dma((2, 2, deep)),
            dma((2, 2, deep)),
            dma((3,)),
            dma((3,)),
        ],
        compiler_params=pltpu.CompilerParams(collective_id=1, has_side_effects=True),
        cost_estimate=pl.CostEstimate(flops=5 * 10**10, bytes_accessed=3 * 10**7, transcendentals=0),
        name="weights_and_tokens",
    )(rest, gate, tokens)


def stats_kernel(dp, own_ref, out_ref, held, send, recv):
    d, s, *_, peers, _ = where_am_i(dp)
    greet([(None, d, p) for p in peers])
    copies = [
        push(own_ref, held.at[r], send.at[r], recv.at[r], d, p) for r, p in enumerate(peers)
    ]
    for copy in copies:
        copy.start()
    for copy in copies:
        copy.wait()
    out_ref[...] = (own_ref[...] + held[0]) + (held[1] + held[2])


def add_over_seq(stats, dp):
    dma = pltpu.SemaphoreType.DMA
    vmem = pl.BlockSpec(memory_space=pltpu.VMEM)
    return pl.pallas_call(
        functools.partial(stats_kernel, dp),
        in_specs=[vmem],
        out_specs=vmem,
        out_shape=jax.ShapeDtypeStruct(stats.shape, F32),
        scratch_shapes=[pltpu.VMEM((3,) + stats.shape, F32), dma((3,)), dma((3,))],
        compiler_params=pltpu.CompilerParams(collective_id=2, has_side_effects=True),
        name="stats_over_seq",
    )(stats)


def scatter_kernel(
    dp,
    grad_ref,
    normed_ref,
    small_ref,
    out_ref,
    own_ref,
    sums_ref,
    ybuf,
    zbuf,
    final,
    core_buf,
    x_buf,
    s_buf,
    y_send,
    y_recv,
    z_send,
    z_recv,
    a_send,
    a_recv,
    c_send,
    c_recv,
    x_send,
    x_recv,
    s_send,
    s_recv,
):
    d, s, z, y, x, c, peers, deep = where_am_i(dp)
    tp, rows = grad_ref.shape[1:3]
    micro, part, width = own_ref.shape
    up, down, far = d + 2, d - 2, d + 1 - 2 * y
    bits = dp.bit_length() - 1
    partners = []
    for k in range(bits):
        step = 2**k
        bit = (d // step) % 2
        partners.append(d + step - 2 * step * bit)
    greet(
        [(None, d, p) for p in peers]
        + [(None, far, s), (z < deep - 1, up, s), (z > 0, down, s)]
        + [(None, partners[k], s) for k in range(2, bits)]
    )
    sends = Sends()
    lower = z < deep // 2

    def place(j):
        low = jnp.where(j > z, deep - 1 - j, deep - 1 - z + j)
        high = jnp.where(j < z, j, z + deep - 1 - j)
        return jnp.where(j == z, deep - 1, jnp.where(lower, low, high))

    def turn(k):
        low = jnp.where(k < deep - 1 - z, deep - 1 - k, k - (deep - 1 - z))
        high = jnp.where(k < z, k, deep - 1 - (k - z))
        return jnp.where(lower, low, high) if k < deep - 1 else z

    def chunk(k):
        return normed_ref.at[:, pl.ds(k * part, part), :]

    def arrive(dst, sem):
        push(dst, dst, sem, sem, d, peers[0]).wait_recv()

    for q, xx in enumerate((1 - x, x)):
        src = chunk(xx * 2 + 1 - c)
        sends.start(None, push(src, core_buf.at[q], c_send.at[q], c_recv.at[q], d, peers[0]))
    order = [turn(k) for k in range(deep)]
    for k in range(deep):
        src = grad_ref.at[order[k] * 2 + 1 - y]
        sends.start(None, push(src, ybuf.at[k], y_send.at[k], y_recv.at[k], far, s))
    sums_ref[0] = small_ref[...]
    sends.start(None, push(small_ref, s_buf.at[0], s_send.at[0], s_recv.at[0], partners[0], s))

    def add_rows(count, work):
        lax.fori_loop(0, count, lambda i, carry: (work(i), carry)[1], 0)

    def add_normed(q, xx):
        mine = xx * 2 + c
        span = 16

        def work(i):
            m, row = i // (part // span), (i % (part // span)) * span
            row = pl.multiple_of(row, span)
            theirs = core_buf[q, m, pl.ds(row, span), :].astype(F32)
            ours = normed_ref[m, pl.ds(pl.multiple_of(mine * part + row, span), span), :].astype(F32)
            core_buf[q, m, pl.ds(row, span), :] = (theirs + ours).astype(BF16)

        add_rows(micro * (part // span), work)

    arrive(core_buf.at[0], c_recv.at[0])
    add_normed(0, 1 - x)
    sends.start(None, push(core_buf.at[0], x_buf, x_send.at[0], x_recv.at[0], d, peers[1]))
    arrive(core_buf.at[1], c_recv.at[1])

    def doubling(k):
        arrive(s_buf.at[k], s_recv.at[k])
        if k + 1 < bits:
            sums_ref[k + 1] = sums_ref[k] + s_buf[k]
            sends.start(
                None,
                push(sums_ref.at[k + 1], s_buf.at[k + 1], s_send.at[k + 1], s_recv.at[k + 1], partners[k + 1], s),
            )
        else:
            final_sum = sums_ref[k] + s_buf[k]
            sums_ref[bits] = final_sum

    def add_y(k):
        arrive(ybuf.at[k], y_recv.at[k])
        at = order[k] * 2 + y

        def work(i):
            ybuf[k, i] = (ybuf[k, i].astype(F32) + grad_ref[at, i].astype(F32)).astype(BF16)

        add_rows(tp, work)

    def send_z(t):
        for way in range(2):
            depth = z if way == 0 else deep - 1 - z
            j = deep - 1 - t + z if way == 0 else t + z - deep + 1
            j = jnp.clip(j, 0, deep - 1)
            k = place(j)
            nxt = up if way == 0 else down
            first = depth == 0
            dst = zbuf.at[way, t]
            sends.start(
                first, push(ybuf.at[k], dst, z_send.at[way, t], z_recv.at[way, t], nxt, s)
            )
            if t == 0:
                continue
            later = jnp.logical_and(depth > 0, depth <= t)

            @pl.when(later)
            def _():
                arrive(zbuf.at[way, t - 1], z_recv.at[way, t - 1])

                def work(i):
                    zbuf[way, t - 1, i] = (
                        zbuf[way, t - 1, i].astype(F32) + ybuf[k, i].astype(F32)
                    ).astype(BF16)

                add_rows(tp, work)

            sends.start(
                later,
                push(zbuf.at[way, t - 1], dst, z_send.at[way, t], z_recv.at[way, t], nxt, s),
            )

    for k in range(deep):
        add_y(k)
        if k < deep - 1:
            send_z(k)
        if k < bits:
            doubling(k)
    for k in range(deep, bits):
        doubling(k)
    for r, p in enumerate(peers):
        sends.start(
            None,
            push(sums_ref.at[bits], sums_ref.at[bits + 1 + s], s_send.at[bits + r], s_recv.at[bits + r], d, p),
        )
    sums_ref[bits + 1 + s] = sums_ref[bits]

    for way in range(2):
        depth = z if way == 0 else deep - 1 - z

        @pl.when(depth > 0)
        def _():
            arrive(zbuf.at[way, deep - 2], z_recv.at[way, deep - 2])

    def finish(ways, i):
        total = ybuf[deep - 1, i].astype(F32)
        for way in ways:
            total = total + zbuf[way, deep - 2, i].astype(F32)
        final[i] = total.astype(BF16)

    for cond, ways in (
        (z == 0, (1,)),
        (z == deep - 1, (0,)),
        (jnp.logical_and(z > 0, z < deep - 1), (0, 1)),
    ):

        @pl.when(cond)
        def _():
            add_rows(tp, functools.partial(finish, ways))

    for r, p in enumerate(peers):
        sends.start(None, push(final.at[p], out_ref.at[s], a_send.at[r], a_recv.at[r], d, p))
    out_ref[s] = final[s]

    arrive(x_buf, x_recv.at[0])
    span = 16

    def own_rows(i):
        m, row = i // (part // span), (i % (part // span)) * span
        row = pl.multiple_of(row, span)
        here = pl.multiple_of(s * part + row, span)
        own_ref[m, pl.ds(row, span), :] = (
            core_buf[1, m, pl.ds(row, span), :].astype(F32)
            + normed_ref[m, pl.ds(here, span), :].astype(F32)
            + x_buf[m, pl.ds(row, span), :].astype(F32)
        )

    add_rows(micro * (part // span), own_rows)
    for r, p in enumerate(peers):
        arrive(out_ref.at[p], a_recv.at[r])
        arrive(sums_ref.at[bits + 1 + p], s_recv.at[bits + r])
    sends.drain()


def scatter(grad, normed, small, dp):
    tp, rows, wide = grad.shape[1:]
    micro, length, width = normed.shape
    part = length // tp
    deep = dp // 2
    bits = dp.bit_length() - 1
    dma = pltpu.SemaphoreType.DMA
    vmem = pl.BlockSpec(memory_space=pltpu.VMEM)
    return pl.pallas_call(
        functools.partial(scatter_kernel, dp),
        in_specs=[vmem] * 3,
        out_specs=[vmem] * 3,
        out_shape=[
            jax.ShapeDtypeStruct((tp, rows, wide), BF16),
            jax.ShapeDtypeStruct((micro, part, width), F32),
            jax.ShapeDtypeStruct((bits + 1 + tp,) + small.shape, F32),
        ],
        scratch_shapes=[
            pltpu.VMEM((deep, tp, rows, wide), BF16),
            pltpu.VMEM((2, deep - 1, tp, rows, wide), BF16),
            pltpu.VMEM((tp, rows, wide), BF16),
            pltpu.VMEM((2, micro, part, width), BF16),
            pltpu.VMEM((micro, part, width), BF16),
            pltpu.VMEM((bits,) + small.shape, F32),
            dma((deep,)),
            dma((deep,)),
            dma((2, deep - 1)),
            dma((2, deep - 1)),
            dma((3,)),
            dma((3,)),
            dma((2,)),
            dma((2,)),
            dma((1,)),
            dma((1,)),
            dma((bits + 3,)),
            dma((bits + 3,)),
        ],
        compiler_params=pltpu.CompilerParams(
            collective_id=3, has_side_effects=True, vmem_limit_bytes=60 * 2**20
        ),
        cost_estimate=pl.CostEstimate(flops=5 * 10**10, bytes_accessed=3 * 10**7, transcendentals=0),
        name="gradients_to_owners",
    )(grad, normed, small)


CORES = [(0, 1), (1, 0), (2, 3), (3, 2)]
CHIPS = [(0, 2), (2, 0), (1, 3), (3, 1)]


def over_seq(shard):
    s = lax.axis_index("seq")
    micro, part, width = shard.shape
    other = lax.ppermute(shard, "seq", CHIPS)
    near = lax.ppermute(shard, "seq", CORES)
    cross = lax.ppermute(other, "seq", CORES)
    x, c = s // 2, s % 2
    whole = jnp.zeros((micro, 4 * part, width), shard.dtype)
    for piece, owner in ((shard, s), (near, s + 1 - 2 * c), (other, s + 2 - 4 * x), (cross, 3 - s)):
        whole = lax.dynamic_update_slice_in_dim(whole, piece, owner * part, 1)
    return whole


def over_cores(partial):
    s = lax.axis_index("seq")
    micro, length, width = partial.shape
    x, c = s // 2, s % 2
    grid = partial.reshape(micro, 2, 2, length // 4, width)
    theirs = lax.dynamic_index_in_dim(grid, 1 - c, 2, keepdims=False)
    mine = lax.dynamic_index_in_dim(grid, c, 2, keepdims=False).astype(F32)
    both = mine + lax.ppermute(theirs, "seq", CORES).astype(F32)
    away = lax.dynamic_index_in_dim(both, 1 - x, 1, keepdims=False).astype(BF16)
    here = lax.dynamic_index_in_dim(both, x, 1, keepdims=False)
    return here, away


def weight_columns(in_proj, own, tp, heads):
    rows = in_proj.shape[0]
    inner = heads * P_SIZE
    cells = -(-own.shape[0] // rows)
    packed = jnp.pad(own, (0, rows * cells - own.shape[0])).reshape(rows, 1, cells)
    gate = in_proj[:, :DI].reshape(rows, tp, inner).transpose(1, 0, 2)
    rest = jnp.concatenate(
        [
            in_proj[:, DI : 2 * DI].reshape(rows, tp, inner),
            jnp.broadcast_to(in_proj[:, None, 2 * DI : 2 * DI + 2 * N], (rows, tp, 2 * N)),
            in_proj[:, 2 * DI + 2 * N :].reshape(rows, tp, heads),
            jnp.broadcast_to(packed, (rows, tp, cells)),
            jnp.zeros((rows, tp, LANES - heads - cells), BF16),
        ],
        axis=2,
    ).transpose(1, 0, 2)
    return rest, gate


def body(
    tokens,
    in_proj,
    conv_weight,
    conv_bias,
    decay_log,
    step_bias,
    skip_gain,
    norm_gain,
    gated_gain,
    out_proj,
    cotangent,
):
    dp, tp = lax.axis_size("dp"), lax.axis_size("seq")
    total = dp * tp
    s = lax.axis_index("seq")
    micro, part, width = tokens.shape
    heads = HEADS // tp
    inner = heads * P_SIZE
    rows = in_proj.shape[0]
    length = part * tp
    count = micro * length
    wide = inner + 2 * N
    chan = conv_bias.shape[0]

    own = jnp.concatenate([conv_weight.reshape(-1), conv_bias, norm_gain, gated_gain])
    rest, gate = weight_columns(in_proj, own, tp, heads)
    w_rest, w_gate, tok = gather(rest, gate, tokens, dp)
    w_rest = w_rest.reshape(width, wide + LANES)
    w_gate = w_gate.reshape(width, inner)
    tok = tok.reshape(count, width)
    turn = [(b * dp + a, a * tp + b) for a in range(dp) for b in range(tp)]
    w_out = lax.ppermute(out_proj, ("dp", "seq"), turn)
    w_out, tok, upstream = lax.optimization_barrier((w_out, tok, cotangent))
    w_out = lax.all_gather(w_out, "dp", axis=0, tiled=True)
    cot = over_seq(upstream).reshape(count, width)

    cells = -(-own.shape[0] // rows)
    shared = w_rest[:, wide + heads : wide + heads + cells].reshape(total, rows * cells).astype(F32)
    w_conv = shared[:, : KW * chan].reshape(total, KW, chan).transpose(1, 0, 2).reshape(KW, CD)
    b_conv = shared[:, KW * chan : (KW + 1) * chan].reshape(1, CD)
    at = (KW + 1) * chan
    g_norm = shared[:, at : at + rows].reshape(width)
    g_gated = shared[:, at + rows : at + rows + gated_gain.shape[0]].reshape(DI)
    first, lane = s * inner, s * heads
    taps = jnp.concatenate([w_conv, b_conv, jnp.zeros((3, CD), F32)], axis=0)
    taps = jnp.concatenate([lax.dynamic_slice_in_dim(taps, first, inner, 1), taps[:, DI:]], axis=1)
    g_gated = lax.dynamic_slice_in_dim(g_gated, first, inner)
    head = jnp.stack([decay_log, step_bias, skip_gain])
    head = lax.dynamic_slice_in_dim(head, lane, heads, 1)
    head = jnp.pad(head, ((0, 5), (0, LANES - heads)))

    h = tok.astype(F32)
    r = lax.rsqrt(jnp.mean(h * h, axis=-1, keepdims=True) + EPSILON)
    normed = (h * r * g_norm).astype(BF16)
    proj_rest = jnp.dot(normed, w_rest, preferred_element_type=F32)
    ssd, memory = mixer_forward(proj_rest, taps, head, heads, micro)
    gate = jnp.dot(normed, w_gate, preferred_element_type=F32)
    sig = jax.nn.sigmoid(gate)
    act = gate * sig
    gated = ssd * act
    grad_shaped = jnp.dot(cot, w_out.T, preferred_element_type=F32)
    weighed = grad_shaped * g_gated
    stats = jnp.stack([jnp.sum(gated * gated, axis=1), jnp.sum(weighed * gated, axis=1)])
    stats = add_over_seq(stats, dp)
    q = lax.rsqrt(stats[0] / DI + EPSILON)[:, None]
    shaped = (gated * q * g_gated).astype(BF16)
    grad_gated = q * (weighed - gated * (q * q * (stats[1] / DI)[:, None]))
    grad_ssd = grad_gated * act
    grad_gate = (grad_gated * ssd * (sig + act * (1 - sig))).astype(BF16)

    out_part = jnp.dot(shaped, w_out, preferred_element_type=F32).astype(BF16)
    here, away = over_cores(out_part.reshape(micro, length, width))

    grad_out = jnp.dot(shaped.T, cot, preferred_element_type=F32).astype(BF16)
    gate_in = jnp.dot(normed.T, grad_gate, preferred_element_type=F32).astype(BF16)
    grad_ssd, grad_out, gate_in, here, away = lax.optimization_barrier(
        (grad_ssd, grad_out, gate_in, here, away)
    )
    h_own = tokens.astype(F32)
    block_out = (h_own + here + lax.ppermute(away, "seq", CHIPS).astype(F32)).astype(BF16)
    joint = jnp.concatenate(
        [grad_out.reshape(dp, -1, width), gate_in.reshape(dp, -1, width)], axis=1
    ).reshape(-1, width)
    joint = lax.psum_scatter(joint, "dp", scatter_dimension=0, tiled=True)
    grad_out = joint[: out_proj.shape[0]]
    gate_in = joint[out_proj.shape[0] :].reshape(tp * rows, inner)
    grad_out = lax.ppermute(grad_out, ("dp", "seq"), [(b, a) for a, b in turn]).astype(F32)
    gated_gain_grad = jnp.sum(out_proj.astype(F32) * grad_out, axis=1) / gated_gain.astype(F32)
    gate_in = lax.all_to_all(gate_in.reshape(tp, rows, inner), "seq", 0, 0)

    grad_rest, wgrad, hgrad = mixer_backward(proj_rest, grad_ssd, memory, taps, head, heads, micro)
    small = jnp.concatenate([wgrad[: KW + 1].reshape(-1), hgrad[:3].reshape(-1)])
    lines = -(-small.shape[0] // (8 * LANES)) * 8
    small = jnp.pad(small, (0, lines * LANES - small.shape[0])).reshape(lines, LANES)
    rest_in = jnp.dot(normed.T, grad_rest, preferred_element_type=F32).astype(BF16)
    grad_normed = (
        lax.dot_general(grad_rest, w_rest, (((1,), (1,)), ((), ())), preferred_element_type=F32)
        + lax.dot_general(grad_gate, w_gate, (((1,), (1,)), ((), ())), preferred_element_type=F32)
    ).astype(BF16)
    rest_in, grad_normed, small = scatter(
        rest_in.reshape(dp, tp, rows, wide + LANES),
        grad_normed.reshape(micro, length, width),
        small,
        dp,
    )
    rest_in = rest_in.astype(F32)
    small = small[-tp:].reshape(tp, -1)
    convs = small[:, : (KW + 1) * wide].reshape(tp, KW + 1, wide)
    convs = jnp.concatenate(
        [
            convs[:, :, :inner].transpose(1, 0, 2).reshape(KW + 1, DI),
            jnp.sum(convs[:, :, inner:], axis=0),
        ],
        axis=1,
    )
    place = lax.axis_index("dp") * tp + s
    convs = lax.dynamic_slice_in_dim(convs, place * chan, chan, 1)
    head_grads = small[:, (KW + 1) * wide : (KW + 1) * wide + 3 * LANES].reshape(tp, 3, LANES)[:, :, :heads]
    head_grads = head_grads.transpose(1, 0, 2).reshape(3, HEADS)

    def side(a):
        return a.astype(F32).transpose(1, 0, 2).reshape(rows, -1)

    in_grad = jnp.concatenate(
        [
            side(gate_in),
            side(rest_in[:, :, :inner]),
            jnp.sum(rest_in[:, :, inner:wide], axis=0),
            side(rest_in[:, :, wide : wide + heads]),
        ],
        axis=1,
    )
    norm_gain_grad = jnp.sum(in_proj.astype(F32) * in_grad, axis=1) / norm_gain.astype(F32)

    r_own = lax.rsqrt(jnp.mean(h_own * h_own, axis=-1, keepdims=True) + EPSILON)
    n_own = h_own * r_own
    g = grad_normed * g_norm
    tokens_grad = cotangent.astype(F32) + r_own * (
        g - n_own * jnp.mean(g * n_own, axis=-1, keepdims=True)
    )
    return (
        block_out,
        tokens_grad.astype(BF16),
        in_grad,
        convs[:KW],
        convs[KW],
        head_grads[0],
        head_grads[1],
        head_grads[2],
        norm_gain_grad,
        gated_gain_grad,
        grad_out,
    )


def solution(mesh):
    both = ("dp", "seq")
    return jax.shard_map(
        body,
        mesh=mesh,
        in_specs=(
            P("dp", "seq", None),
            P(both, None),
            P(None, both),
            P(both),
            P(),
            P(),
            P(),
            P(both),
            P(both),
            P(both, None),
            P("dp", "seq", None),
        ),
        out_specs=(
            P("dp", "seq", None),
            P("dp", "seq", None),
            P(both, None),
            P(None, both),
            P(both),
            P(),
            P(),
            P(),
            P(both),
            P(both),
            P(both, None),
        ),
        check_vma=False,
    )
```

```python
import functools

import jax
import jax.numpy as jnp
from jax import lax
from jax.experimental import pallas as pl
from jax.experimental.pallas import tpu as pltpu
from jax.sharding import PartitionSpec as P

HEADS = 48
P_SIZE = 64
N = 128
KW = 4
DI = 3072
CD = 3328
LANES = 128
CHUNK = 128
FAR = -1e30

EPSILON = 1e-05
F32 = jnp.float32
BF16 = jnp.bfloat16


def dot(a, b, dims=((1,), (0,)), precision=None):
    return lax.dot_general(a, b, (dims, ((), ())), precision=precision, preferred_element_type=F32)


NT = ((1,), (1,))
HIGH = lax.Precision.HIGHEST


def pick(a, p, low):
    return jnp.where(low, a[:, 2 * p : 2 * p + 1], a[:, 2 * p + 1 : 2 * p + 2])


def chunk_parts(heads, rest_ref, xbuf, taps_ref, head_ref):
    size = rest_ref.shape[0]
    wide = taps_ref.shape[1]
    mixed = taps_ref[KW : KW + 1, :] + taps_ref[0:1, :] * xbuf[5 : 5 + size, :]
    for k in range(1, KW):
        mixed = mixed + taps_ref[k : k + 1, :] * xbuf[5 + k : 5 + k + size, :]
    sig = lax.logistic(mixed)
    lane = lax.broadcasted_iota(jnp.int32, (1, LANES), 1)
    raw = jnp.where(lane < heads, rest_ref[:, wide:], 0.0) + head_ref[1:2, :]
    step = jnp.maximum(raw, 0.0) + jnp.log1p(jnp.exp(-jnp.abs(raw)))
    decay = -jnp.exp(head_ref[0:1, :]) * step
    i = lax.broadcasted_iota(jnp.int32, (size, size), 0)
    j = lax.broadcasted_iota(jnp.int32, (size, size), 1)
    run = dot(jnp.where(i >= j, 1.0, 0.0), decay, precision=HIGH)
    return mixed, sig, raw, step, decay, run


def forward_kernel(heads, rest_ref, taps_ref, head_ref, ssd_ref, mem_ref, xbuf, mem):
    size = rest_ref.shape[0]
    wide = taps_ref.shape[1]
    inner = heads * P_SIZE
    first = pl.program_id(1) == 0

    @pl.when(first)
    def _():
        xbuf[0:8, :] = jnp.zeros((8, wide), F32)
        mem[...] = jnp.zeros_like(mem)

    @pl.when(jnp.logical_not(first))
    def _():
        xbuf[0:8, :] = xbuf[size : size + 8, :]

    xbuf[8 : 8 + size, :] = rest_ref[:, :wide]
    mixed, sig, _, step, _, run = chunk_parts(heads, rest_ref, xbuf, taps_ref, head_ref)
    act = mixed * sig
    run_t = run.T
    closing = run[size - 1 : size, :]
    last = jnp.exp(closing)
    left = jnp.exp(closing - run)
    grown = jnp.exp(run)
    b = act[:, inner : inner + N]
    c = act[:, inner + N :].astype(BF16)
    scores = dot(c, b.astype(BF16), NT)
    b_t = b.T.astype(BF16)
    mem_ref[0] = mem[...].astype(BF16)
    inter = dot(c, mem[...].astype(BF16))
    low = lax.broadcasted_iota(jnp.int32, (1, LANES), 1) < P_SIZE
    i = lax.broadcasted_iota(jnp.int32, (size, size), 0)
    j = lax.broadcasted_iota(jnp.int32, (size, size), 1)
    causal = i >= j
    for p in range(heads // 2):
        at = slice(p * LANES, (p + 1) * LANES)
        v = act[:, at]
        xv = pick(step, p, low) * v
        y = pick(head_ref[2:3, :], p, low) * v + pick(grown, p, low) * inter[:, at]
        for e in range(2):
            h = 2 * p + e
            gap = run[:, h : h + 1] - run_t[h : h + 1, :]
            w = (scores * jnp.exp(jnp.where(causal, gap, FAR))).astype(BF16)
            mine = jnp.where(low if e == 0 else jnp.logical_not(low), xv, 0.0).astype(BF16)
            y = y + dot(w, mine)
        ssd_ref[:, at] = y
        xc = (pick(left, p, low) * xv).astype(BF16)
        mem[:, at] = mem[:, at] * pick(last, p, low) + dot(b_t, xc)


def backward_kernel(
    heads,
    rest_ref,
    prev_ref,
    dy_ref,
    mem_ref,
    taps_ref,
    head_ref,
    out_ref,
    wgrad_ref,
    hgrad_ref,
    xbuf,
    gbuf,
    adj,
    dmix,
    dsum,
    uprod,
    zprod,
    rows_t,
    line,
):
    size = rest_ref.shape[0]
    wide = taps_ref.shape[1]
    inner = heads * P_SIZE
    chunks = pl.num_programs(1)
    step_id = pl.program_id(1)
    newest = step_id == 0
    oldest = step_id == chunks - 1
    begin = jnp.logical_and(pl.program_id(0) == 0, newest)
    finish = jnp.logical_and(pl.program_id(0) == pl.num_programs(0) - 1, oldest)

    @pl.when(begin)
    def _():
        wgrad_ref[...] = jnp.zeros_like(wgrad_ref)
        hgrad_ref[...] = jnp.zeros_like(hgrad_ref)
        rows_t[...] = jnp.zeros_like(rows_t)
        line[...] = jnp.zeros_like(line)

    @pl.when(newest)
    def _():
        gbuf[size : size + 8, :] = jnp.zeros((8, wide), F32)
        adj[...] = jnp.zeros_like(adj)

    @pl.when(jnp.logical_not(newest))
    def _():
        gbuf[size : size + 8, :] = gbuf[0:8, :]

    xbuf[0:8, :] = jnp.where(oldest, 0.0, prev_ref[:, :wide])
    xbuf[8 : 8 + size, :] = rest_ref[:, :wide]
    mixed, sig, raw, step, decay, run = chunk_parts(heads, rest_ref, xbuf, taps_ref, head_ref)
    act = mixed * sig
    run_t = run.T
    closing = run[size - 1 : size, :]
    last = jnp.exp(closing)
    left = jnp.exp(closing - run)
    grown = jnp.exp(run)
    b = act[:, inner : inner + N].astype(BF16)
    c = act[:, inner + N :].astype(BF16)
    c_t = act[:, inner + N :].T.astype(BF16)
    scores_t = dot(b, c, NT)
    low = lax.broadcasted_iota(jnp.int32, (1, LANES), 1) < P_SIZE
    lane = lax.broadcasted_iota(jnp.int32, (1, LANES), 1)
    j = lax.broadcasted_iota(jnp.int32, (size, size), 0)
    i = lax.broadcasted_iota(jnp.int32, (size, size), 1)
    causal = i >= j
    mem_b = mem_ref[0]
    adj_b = adj[...].astype(BF16)
    spread = dot(b, adj_b)
    inherit = dot(c, mem_b)
    scored = jnp.zeros((size, size), F32)
    cols = jnp.zeros((size, LANES), F32)
    for p in range(heads // 2):
        at = slice(p * LANES, (p + 1) * LANES)
        v = act[:, at]
        size_p = pick(step, p, low)
        xv = size_p * v
        dy = dy_ref[:, at]
        dyb = dy.astype(BF16)
        xvb = xv.astype(BF16)
        dxv = pick(left, p, low) * spread[:, at]
        zprod[:, at] = (dxv * xv).astype(BF16)
        dyg = pick(grown, p, low) * dy
        uprod[:, at] = (dyg * inherit[:, at]).astype(BF16)
        for e in range(2):
            h = 2 * p + e
            keep = low if e == 0 else jnp.logical_not(low)
            mine = jnp.where(keep, dy, 0.0).astype(BF16)
            gap = run_t[h : h + 1, :] - run[:, h : h + 1]
            near = jnp.exp(jnp.where(causal, gap, FAR))
            w_t = scores_t * near
            dw_t = dot(xvb, mine, NT)
            scored = scored + dw_t * near
            g_t = dw_t * w_t
            rows_t[h : h + 1, :] = jnp.sum(g_t, axis=0, keepdims=True)
            cols = jnp.where(lane == h, jnp.sum(g_t, axis=1, keepdims=True), cols)
            dxv = dxv + dot(w_t.astype(BF16), mine)
        dsum[:, at] = (dxv * v).astype(BF16)
        dmix[:, at] = size_p * dxv + pick(head_ref[2:3, :], p, low) * dy
        line[0:1, at] += jnp.sum(dy * v, axis=0, keepdims=True)
        line[1:2, at] = jnp.sum(adj[:, at] * mem_b[:, at].astype(F32), axis=0, keepdims=True) * pick(
            last, p, low
        )
        xc = (pick(left, p, low) * xv).astype(BF16)
        dygb = dyg.astype(BF16)
        db = dot(xc, adj_b[:, at], NT)
        dc = dot(dygb, mem_b[:, at], NT)
        if p == 0:
            dmix[:, inner : inner + N] = db
            dmix[:, inner + N :] = dc
        else:
            dmix[:, inner : inner + N] += db
            dmix[:, inner + N :] += dc
        adj[:, at] = adj[:, at] * pick(last, p, low) + dot(c_t, dygb)
    dmix[:, inner : inner + N] += dot(scored.astype(BF16), c)
    dmix[:, inner + N :] += dot(scored.T.astype(BF16), b)

    group = jnp.where(
        lax.broadcasted_iota(jnp.int32, (inner, LANES), 0) // P_SIZE
        == lax.broadcasted_iota(jnp.int32, (inner, LANES), 1),
        1.0,
        0.0,
    )
    group_b = group.astype(BF16)
    d_step = dot(dsum[...], group_b)
    u = dot(uprod[...], group_b)
    z = dot(zprod[...], group_b)
    sums = dot(line[...], group, precision=HIGH)
    d_run = rows_t[...].T - cols + u - z
    row = lax.broadcasted_iota(jnp.int32, (size, 1), 0)
    ending = sums[1:2, :] + jnp.sum(z, axis=0, keepdims=True)
    d_run = d_run + jnp.where(row == size - 1, ending, 0.0)
    d_decay = dot(jnp.where(causal, 1.0, 0.0), d_run, precision=HIGH)
    d_raw = (d_step - jnp.exp(head_ref[0:1, :]) * d_decay) * lax.logistic(raw)
    d_raw = jnp.where(lane < heads, d_raw, 0.0)
    hgrad_ref[0:1, :] += jnp.sum(d_decay * decay, axis=0, keepdims=True)
    hgrad_ref[1:2, :] += jnp.sum(d_raw, axis=0, keepdims=True)

    @pl.when(finish)
    def _():
        hgrad_ref[2:3, :] = sums[0:1, :]

    g = dmix[...] * (sig * (1.0 + mixed * (1.0 - sig)))
    gbuf[0:size, :] = g
    wgrad_ref[KW : KW + 1, :] += jnp.sum(g, axis=0, keepdims=True)
    for k in range(KW):
        wgrad_ref[k : k + 1, :] += jnp.sum(g * xbuf[5 + k : 5 + k + size, :], axis=0, keepdims=True)
    back = taps_ref[KW - 1 : KW, :] * g
    for k in range(KW - 1):
        back = back + taps_ref[k : k + 1, :] * gbuf[3 - k : 3 - k + size, :]
    out_ref[:, :wide] = back.astype(BF16)
    out_ref[:, wide:] = d_raw.astype(BF16)


def mixer_forward(rest, taps, head, heads, micro):
    count, full = rest.shape
    wide = taps.shape[1]
    inner = heads * P_SIZE
    chunks = count // micro // CHUNK
    return pl.pallas_call(
        functools.partial(forward_kernel, heads),
        grid=(micro, chunks),
        in_specs=[
            pl.BlockSpec((CHUNK, full), lambda m, c: (m * chunks + c, 0)),
            pl.BlockSpec((8, wide), lambda m, c: (0, 0)),
            pl.BlockSpec((8, LANES), lambda m, c: (0, 0)),
        ],
        out_specs=[
            pl.BlockSpec((CHUNK, inner), lambda m, c: (m * chunks + c, 0)),
            pl.BlockSpec((1, N, inner), lambda m, c: (m * chunks + c, 0, 0)),
        ],
        out_shape=[
            jax.ShapeDtypeStruct((count, inner), F32),
            jax.ShapeDtypeStruct((micro * chunks, N, inner), BF16),
        ],
        scratch_shapes=[pltpu.VMEM((CHUNK + 8, wide), F32), pltpu.VMEM((N, inner), F32)],
        compiler_params=pltpu.CompilerParams(dimension_semantics=("arbitrary", "arbitrary")),
        cost_estimate=pl.CostEstimate(flops=25 * 10**9, bytes_accessed=2 * 10**7, transcendentals=10**7),
        name="mixer_forward",
    )(rest, taps, head)


def mixer_backward(rest, dy, memory, taps, head, heads, micro):
    count, full = rest.shape
    wide = taps.shape[1]
    inner = heads * P_SIZE
    chunks = count // micro // CHUNK

    def at(m, c):
        return m * chunks + chunks - 1 - c

    return pl.pallas_call(
        functools.partial(backward_kernel, heads),
        grid=(micro, chunks),
        in_specs=[
            pl.BlockSpec((CHUNK, full), lambda m, c: (at(m, c), 0)),
            pl.BlockSpec((8, full), lambda m, c: (jnp.maximum(at(m, c) * (CHUNK // 8) - 1, 0), 0)),
            pl.BlockSpec((CHUNK, inner), lambda m, c: (at(m, c), 0)),
            pl.BlockSpec((1, N, inner), lambda m, c: (at(m, c), 0, 0)),
            pl.BlockSpec((8, wide), lambda m, c: (0, 0)),
            pl.BlockSpec((8, LANES), lambda m, c: (0, 0)),
        ],
        out_specs=[
            pl.BlockSpec((CHUNK, full), lambda m, c: (at(m, c), 0)),
            pl.BlockSpec((8, wide), lambda m, c: (0, 0)),
            pl.BlockSpec((8, LANES), lambda m, c: (0, 0)),
        ],
        out_shape=[
            jax.ShapeDtypeStruct((count, full), BF16),
            jax.ShapeDtypeStruct((8, wide), F32),
            jax.ShapeDtypeStruct((8, LANES), F32),
        ],
        scratch_shapes=[
            pltpu.VMEM((CHUNK + 8, wide), F32),
            pltpu.VMEM((CHUNK + 8, wide), F32),
            pltpu.VMEM((N, inner), F32),
            pltpu.VMEM((CHUNK, wide), F32),
            pltpu.VMEM((CHUNK, inner), BF16),
            pltpu.VMEM((CHUNK, inner), BF16),
            pltpu.VMEM((CHUNK, inner), BF16),
            pltpu.VMEM((LANES, CHUNK), F32),
            pltpu.VMEM((8, inner), F32),
        ],
        compiler_params=pltpu.CompilerParams(dimension_semantics=("arbitrary", "arbitrary")),
        cost_estimate=pl.CostEstimate(flops=7 * 10**10, bytes_accessed=4 * 10**7, transcendentals=10**7),
        name="mixer_backward",
    )(rest, rest, dy, memory, taps, head)


MESH = pl.DeviceIdType.MESH


def where_am_i(dp):
    d, s = lax.axis_index("dp"), lax.axis_index("seq")
    z, y = d // 2, d % 2
    x, c = s // 2, s % 2
    peers = [s + 1 - 2 * c, s + 2 - 4 * x, 3 - s]
    return d, s, z, y, x, c, peers, dp // 2


def push(src, dst, send_sem, recv_sem, d, s):
    return pltpu.make_async_remote_copy(
        src_ref=src,
        dst_ref=dst,
        send_sem=send_sem,
        recv_sem=recv_sem,
        device_id={"dp": d, "seq": s},
        device_id_type=MESH,
    )


def greet(partners):
    barrier = pltpu.get_barrier_semaphore()
    for cond, d, s in partners:

        def hello(d=d, s=s):
            pl.semaphore_signal(barrier, inc=1, device_id={"dp": d, "seq": s}, device_id_type=MESH)

        if cond is None:
            hello()
        else:
            pl.when(cond)(hello)
    count = 0
    for cond, _, _ in partners:
        count = count + (1 if cond is None else jnp.where(cond, 1, 0))
    pl.semaphore_wait(barrier, count)


class Sends:
    def __init__(self):
        self.items = []

    def start(self, cond, copy):
        if cond is None:
            copy.start()
        else:
            pl.when(cond)(copy.start)
        self.items.append((cond, copy))

    def drain(self):
        for cond, copy in self.items:
            if cond is None:
                copy.wait_send()
            else:
                pl.when(cond)(copy.wait_send)


def gather_kernel(
    dp, rest_ref, gate_ref, tok_ref, w_rest, w_gate, tok, own, a_send, a_recv, z_send, z_recv, y_send, y_recv, t_send, t_recv
):
    d, s, z, y, x, c, peers, deep = where_am_i(dp)
    part = tok_ref.shape[1]
    up, down, far = d + 2, d - 2, d + 1 - 2 * y
    greet(
        [(None, d, p) for p in peers]
        + [(None, far, s), (z < deep - 1, up, s), (z > 0, down, s)]
    )
    sends = Sends()
    parts = ((0, rest_ref, w_rest), (1, gate_ref, w_gate))

    def exchange(a, src, dst):
        for r, p in enumerate(peers):
            sends.start(None, push(src.at[p], dst.at[d, s], a_send.at[a, r], a_recv.at[a, r], d, p))

    def mine(k):
        return tok.at[:, pl.ds(k * part, part), :]

    exchange(*parts[0])
    locals_ = [
        pltpu.make_async_copy(rest_ref.at[s], w_rest.at[d, s], own.at[0]),
        pltpu.make_async_copy(gate_ref.at[s], w_gate.at[d, s], own.at[1]),
        pltpu.make_async_copy(tok_ref, mine(s), own.at[2]),
    ]
    for copy in locals_:
        copy.start()
    sends.start(None, push(tok_ref, mine(s), t_send.at[1], t_recv.at[1], d, peers[1]))
    sends.start(None, push(tok_ref, mine(s), t_send.at[0], t_recv.at[0], d, peers[0]))
    exchange(*parts[1])

    def arrive(dst, sem):
        push(dst, dst, sem, sem, d, peers[0]).wait_recv()

    def spread(a, dst):
        shard = dst.at[d]
        sends.start(z < deep - 1, push(shard, shard, z_send.at[a, 0, 0], z_recv.at[a, 0, 0], up, s))
        sends.start(z > 0, push(shard, shard, z_send.at[a, 1, 0], z_recv.at[a, 1, 0], down, s))
        sends.start(None, push(shard, shard, y_send.at[a, 0, 0], y_recv.at[a, 0, 0], far, s))
        for t in range(1, deep):
            for way in range(2):
                here = (z >= t) if way == 0 else (z + t <= deep - 1)
                more = jnp.logical_and(here, (z < deep - 1) if way == 0 else (z > 0))
                at = jnp.clip(d - 2 * t if way == 0 else d + 2 * t, 0, dp - 1)
                block = dst.at[at]
                pl.when(here)(functools.partial(arrive, block, z_recv.at[a, way, t - 1]))
                if t < deep - 1:
                    nxt = up if way == 0 else down
                    sends.start(
                        more, push(block, block, z_send.at[a, way, t], z_recv.at[a, way, t], nxt, s)
                    )
                sends.start(
                    here, push(block, block, y_send.at[a, way, t], y_recv.at[a, way, t], far, s)
                )

    def landed(a, dst):
        arrive(dst.at[d + 1 - 2 * y], y_recv.at[a, 0, 0])
        for t in range(1, deep):
            for way in range(2):
                here = (z >= t) if way == 0 else (z + t <= deep - 1)
                at = jnp.clip(far - 2 * t if way == 0 else far + 2 * t, 0, dp - 1)
                pl.when(here)(functools.partial(arrive, dst.at[at], y_recv.at[a, way, t]))

    for a, _, dst in parts:
        locals_[a].wait()
        for r, p in enumerate(peers):
            arrive(dst.at[d, p], a_recv.at[a, r])
        spread(a, dst)
    arrive(mine(peers[1]), t_recv.at[1])
    block = mine(peers[1])
    sends.start(None, push(block, block, t_send.at[2], t_recv.at[2], d, peers[0]))
    for a, _, dst in parts:
        landed(a, dst)
    arrive(mine(peers[0]), t_recv.at[0])
    arrive(mine(peers[2]), t_recv.at[2])
    locals_[2].wait()
    sends.drain()


def gather(rest, gate, tokens, dp):
    tp, rows = rest.shape[:2]
    micro, part, width = tokens.shape
    deep = dp // 2
    dma = pltpu.SemaphoreType.DMA
    vmem = pl.BlockSpec(memory_space=pltpu.VMEM)
    hbm = pl.BlockSpec(memory_space=pl.ANY)
    return pl.pallas_call(
        functools.partial(gather_kernel, dp),
        in_specs=[vmem] * 3,
        out_specs=[hbm] * 3,
        out_shape=[
            jax.ShapeDtypeStruct((dp, tp, rows, rest.shape[2]), BF16),
            jax.ShapeDtypeStruct((dp, tp, rows, gate.shape[2]), BF16),
            jax.ShapeDtypeStruct((micro, tp * part, width), BF16),
        ],
        scratch_shapes=[
            dma((3,)),
            dma((2, 3)),
            dma((2, 3)),
            dma((2, 2, deep - 1)),
            dma((2, 2, deep - 1)),
            dma((2, 2, deep)),
            dma((2, 2, deep)),
            dma((3,)),
            dma((3,)),
        ],
        compiler_params=pltpu.CompilerParams(collective_id=1, has_side_effects=True),
        cost_estimate=pl.CostEstimate(flops=5 * 10**10, bytes_accessed=3 * 10**7, transcendentals=0),
        name="weights_and_tokens",
    )(rest, gate, tokens)


def stats_kernel(dp, own_ref, out_ref, held, send, recv):
    d, s, *_, peers, _ = where_am_i(dp)
    greet([(None, d, p) for p in peers])
    copies = [
        push(own_ref, held.at[r], send.at[r], recv.at[r], d, p) for r, p in enumerate(peers)
    ]
    for copy in copies:
        copy.start()
    for copy in copies:
        copy.wait()
    out_ref[...] = (own_ref[...] + held[0]) + (held[1] + held[2])


def add_over_seq(stats, dp):
    dma = pltpu.SemaphoreType.DMA
    vmem = pl.BlockSpec(memory_space=pltpu.VMEM)
    return pl.pallas_call(
        functools.partial(stats_kernel, dp),
        in_specs=[vmem],
        out_specs=vmem,
        out_shape=jax.ShapeDtypeStruct(stats.shape, F32),
        scratch_shapes=[pltpu.VMEM((3,) + stats.shape, F32), dma((3,)), dma((3,))],
        compiler_params=pltpu.CompilerParams(collective_id=2, has_side_effects=True),
        name="stats_over_seq",
    )(stats)


def scatter_kernel(
    dp,
    grad_hbm,
    rows_hbm,
    gates_hbm,
    w_rest_hbm,
    w_gate_hbm,
    small_ref,
    out_ref,
    own_ref,
    sums_ref,
    grad_ref,
    rows_ref,
    gates_ref,
    w_rest,
    w_gate,
    tile,
    ybuf,
    zbuf,
    final,
    core_buf,
    core_out,
    x_buf,
    x_out,
    s_buf,
    l_sem,
    y_send,
    y_recv,
    z_send,
    z_recv,
    a_send,
    a_recv,
    c_send,
    c_recv,
    x_send,
    x_recv,
    s_send,
    s_recv,
):
    d, s, z, y, x, c, peers, deep = where_am_i(dp)
    tp, rows = grad_hbm.shape[1:3]
    micro, part, width = own_ref.shape
    up, down, far = d + 2, d - 2, d + 1 - 2 * y
    bits = dp.bit_length() - 1
    partners = []
    for k in range(bits):
        step = 2**k
        bit = (d // step) % 2
        partners.append(d + step - 2 * step * bit)
    loads = [
        pltpu.make_async_copy(src, dst, l_sem.at[k])
        for k, (src, dst) in enumerate(
            (
                (w_rest_hbm, w_rest),
                (rows_hbm, rows_ref),
                (w_gate_hbm, w_gate),
                (gates_hbm, gates_ref),
                (grad_hbm, grad_ref),
            )
        )
    ]
    for copy in loads:
        copy.start()
    greet(
        [(None, d, p) for p in peers]
        + [(None, far, s), (z < deep - 1, up, s), (z > 0, down, s)]
        + [(None, partners[k], s) for k in range(2, bits)]
    )
    sends = Sends()
    lower = z < deep // 2

    def place(j):
        low = jnp.where(j > z, deep - 1 - j, deep - 1 - z + j)
        high = jnp.where(j < z, j, z + deep - 1 - j)
        return jnp.where(j == z, deep - 1, jnp.where(lower, low, high))

    def turn(k):
        low = jnp.where(k < deep - 1 - z, deep - 1 - k, k - (deep - 1 - z))
        high = jnp.where(k < z, k, deep - 1 - (k - z))
        return jnp.where(lower, low, high) if k < deep - 1 else z

    def arrive(dst, sem):
        push(dst, dst, sem, sem, d, peers[0]).wait_recv()

    order = [turn(k) for k in range(deep)]
    for k in range(deep):
        src = grad_hbm.at[order[k] * 2 + 1 - y]
        sends.start(None, push(src, ybuf.at[k], y_send.at[k], y_recv.at[k], far, s))
    sums_ref[0] = small_ref[...]
    sends.start(None, push(small_ref, s_buf.at[0], s_send.at[0], s_recv.at[0], partners[0], s))

    def each(count, work):
        lax.fori_loop(0, count, lambda i, carry: (work(i), carry)[1], 0)

    across = width // tile.shape[1]

    def product(owner, use):
        def work(i):
            m, n = i // across, i % across
            row = pl.multiple_of((m * tp + owner) * part, part)
            col = pl.multiple_of(n * tile.shape[1], tile.shape[1])
            lines = pl.ds(col, tile.shape[1])
            tile[...] = dot(rows_ref[pl.ds(row, part), :], w_rest[lines, :], NT) + dot(
                gates_ref[pl.ds(row, part), :], w_gate[lines, :], NT
            )
            use(m, lines)

        each(micro * across, work)

    def doubling(k):
        arrive(s_buf.at[k], s_recv.at[k])
        sums_ref[k + 1] = sums_ref[k] + s_buf[k]
        if k + 1 < bits:
            src = sums_ref.at[k + 1]
            sends.start(
                None, push(src, s_buf.at[k + 1], s_send.at[k + 1], s_recv.at[k + 1], partners[k + 1], s)
            )

    def add_y(k):
        arrive(ybuf.at[k], y_recv.at[k])
        at = order[k] * 2 + y

        def work(i):
            ybuf[k, i] = (ybuf[k, i].astype(F32) + grad_ref[at, i].astype(F32)).astype(BF16)

        each(tp, work)

    def send_z(t):
        for way in range(2):
            depth = z if way == 0 else deep - 1 - z
            j = deep - 1 - t + z if way == 0 else t + z - deep + 1
            j = jnp.clip(j, 0, deep - 1)
            k = place(j)
            nxt = up if way == 0 else down
            first = depth == 0
            dst = zbuf.at[way, t]
            sends.start(
                first, push(ybuf.at[k], dst, z_send.at[way, t], z_recv.at[way, t], nxt, s)
            )
            if t == 0:
                continue
            later = jnp.logical_and(depth > 0, depth <= t)

            @pl.when(later)
            def _():
                arrive(zbuf.at[way, t - 1], z_recv.at[way, t - 1])

                def work(i):
                    zbuf[way, t - 1, i] = (
                        zbuf[way, t - 1, i].astype(F32) + ybuf[k, i].astype(F32)
                    ).astype(BF16)

                each(tp, work)

            sends.start(
                later,
                push(zbuf.at[way, t - 1], dst, z_send.at[way, t], z_recv.at[way, t], nxt, s),
            )

    for copy in loads[:4]:
        copy.wait()

    def to_core(q):
        def use(m, lines):
            core_out[q, m, :, lines] = tile[...].astype(BF16)

        return use

    def to_chip(m, lines):
        x_out[m, :, lines] = (tile[...] + core_buf[0, m, :, lines].astype(F32)).astype(BF16)

    def keep(m, lines):
        own_ref[m, :, lines] = tile[...] + core_buf[1, m, :, lines].astype(F32)

    product((1 - x) * 2 + 1 - c, to_core(0))
    sends.start(
        None, push(core_out.at[0], core_buf.at[0], c_send.at[0], c_recv.at[0], d, peers[0])
    )
    arrive(core_buf.at[0], c_recv.at[0])
    product((1 - x) * 2 + c, to_chip)
    sends.start(None, push(x_out, x_buf, x_send.at[0], x_recv.at[0], d, peers[1]))
    loads[4].wait()
    add_y(0)
    send_z(0)
    doubling(0)
    product(x * 2 + 1 - c, to_core(1))
    sends.start(
        None, push(core_out.at[1], core_buf.at[1], c_send.at[1], c_recv.at[1], d, peers[0])
    )
    add_y(1)
    send_z(1)
    doubling(1)
    arrive(core_buf.at[1], c_recv.at[1])
    product(s, keep)
    for k in range(2, deep):
        add_y(k)
        if k < deep - 1:
            send_z(k)
        if k < bits:
            doubling(k)
    for k in range(deep, bits):
        doubling(k)
    for r, p in enumerate(peers):
        src, dst = sums_ref.at[bits], sums_ref.at[bits + 1 + s]
        sends.start(None, push(src, dst, s_send.at[bits + r], s_recv.at[bits + r], d, p))
    sums_ref[bits + 1 + s] = sums_ref[bits]

    for way in range(2):
        depth = z if way == 0 else deep - 1 - z

        @pl.when(depth > 0)
        def _():
            arrive(zbuf.at[way, deep - 2], z_recv.at[way, deep - 2])

    def finish(ways, i):
        total = ybuf[deep - 1, i].astype(F32)
        for way in ways:
            total = total + zbuf[way, deep - 2, i].astype(F32)
        final[i] = total.astype(BF16)

    for cond, ways in (
        (z == 0, (1,)),
        (z == deep - 1, (0,)),
        (jnp.logical_and(z > 0, z < deep - 1), (0, 1)),
    ):

        @pl.when(cond)
        def _():
            each(tp, functools.partial(finish, ways))

    for r, p in enumerate(peers):
        sends.start(None, push(final.at[p], out_ref.at[s], a_send.at[r], a_recv.at[r], d, p))
    out_ref[s] = final[s]

    arrive(x_buf, x_recv.at[0])
    span = 16

    def last(i):
        m, row = i // (part // span), (i % (part // span)) * span
        lines = pl.ds(pl.multiple_of(row, span), span)
        own_ref[m, lines, :] += x_buf[m, lines, :].astype(F32)

    each(micro * (part // span), last)
    for r, p in enumerate(peers):
        arrive(out_ref.at[p], a_recv.at[r])
        arrive(sums_ref.at[bits + 1 + p], s_recv.at[bits + r])
    sends.drain()


def scatter(grad, rows_grad, gates_grad, w_rest, w_gate, small, dp, micro):
    tp, rows, wide = grad.shape[1:]
    count, width = rows_grad.shape[0], w_rest.shape[0]
    part = count // micro // tp
    deep = dp // 2
    bits = dp.bit_length() - 1
    dma = pltpu.SemaphoreType.DMA
    vmem = pl.BlockSpec(memory_space=pltpu.VMEM)
    hbm = pl.BlockSpec(memory_space=pl.ANY)
    return pl.pallas_call(
        functools.partial(scatter_kernel, dp),
        in_specs=[hbm] * 5 + [vmem],
        out_specs=[vmem] * 3,
        out_shape=[
            jax.ShapeDtypeStruct((tp, rows, wide), BF16),
            jax.ShapeDtypeStruct((micro, part, width), F32),
            jax.ShapeDtypeStruct((bits + 1 + tp,) + small.shape, F32),
        ],
        scratch_shapes=[
            pltpu.VMEM(grad.shape, BF16),
            pltpu.VMEM(rows_grad.shape, BF16),
            pltpu.VMEM(gates_grad.shape, BF16),
            pltpu.VMEM(w_rest.shape, BF16),
            pltpu.VMEM(w_gate.shape, BF16),
            pltpu.VMEM((part, min(width, 512)), F32),
            pltpu.VMEM((deep, tp, rows, wide), BF16),
            pltpu.VMEM((2, deep - 1, tp, rows, wide), BF16),
            pltpu.VMEM((tp, rows, wide), BF16),
            pltpu.VMEM((2, micro, part, width), BF16),
            pltpu.VMEM((2, micro, part, width), BF16),
            pltpu.VMEM((micro, part, width), BF16),
            pltpu.VMEM((micro, part, width), BF16),
            pltpu.VMEM((bits,) + small.shape, F32),
            dma((5,)),
            dma((deep,)),
            dma((deep,)),
            dma((2, deep - 1)),
            dma((2, deep - 1)),
            dma((3,)),
            dma((3,)),
            dma((2,)),
            dma((2,)),
            dma((1,)),
            dma((1,)),
            dma((bits + 3,)),
            dma((bits + 3,)),
        ],
        compiler_params=pltpu.CompilerParams(
            collective_id=3, has_side_effects=True, vmem_limit_bytes=62 * 2**20
        ),
        cost_estimate=pl.CostEstimate(flops=6 * 10**10, bytes_accessed=3 * 10**7, transcendentals=0),
        name="gradients_to_owners",
    )(grad, rows_grad, gates_grad, w_rest, w_gate, small)


CORES = [(0, 1), (1, 0), (2, 3), (3, 2)]
CHIPS = [(0, 2), (2, 0), (1, 3), (3, 1)]


def over_seq(shard):
    s = lax.axis_index("seq")
    micro, part, width = shard.shape
    other = lax.ppermute(shard, "seq", CHIPS)
    near = lax.ppermute(shard, "seq", CORES)
    cross = lax.ppermute(other, "seq", CORES)
    x, c = s // 2, s % 2
    whole = jnp.zeros((micro, 4 * part, width), shard.dtype)
    for piece, owner in ((shard, s), (near, s + 1 - 2 * c), (other, s + 2 - 4 * x), (cross, 3 - s)):
        whole = lax.dynamic_update_slice_in_dim(whole, piece, owner * part, 1)
    return whole


def over_cores(partial):
    s = lax.axis_index("seq")
    micro, length, width = partial.shape
    x, c = s // 2, s % 2
    grid = partial.reshape(micro, 2, 2, length // 4, width)
    theirs = lax.dynamic_index_in_dim(grid, 1 - c, 2, keepdims=False)
    mine = lax.dynamic_index_in_dim(grid, c, 2, keepdims=False).astype(F32)
    both = mine + lax.ppermute(theirs, "seq", CORES).astype(F32)
    away = lax.dynamic_index_in_dim(both, 1 - x, 1, keepdims=False).astype(BF16)
    here = lax.dynamic_index_in_dim(both, x, 1, keepdims=False)
    return here, away


def weight_columns(in_proj, own, tp, heads):
    rows = in_proj.shape[0]
    inner = heads * P_SIZE
    cells = -(-own.shape[0] // rows)
    packed = jnp.pad(own, (0, rows * cells - own.shape[0])).reshape(rows, 1, cells)
    gate = in_proj[:, :DI].reshape(rows, tp, inner).transpose(1, 0, 2)
    rest = jnp.concatenate(
        [
            in_proj[:, DI : 2 * DI].reshape(rows, tp, inner),
            jnp.broadcast_to(in_proj[:, None, 2 * DI : 2 * DI + 2 * N], (rows, tp, 2 * N)),
            in_proj[:, 2 * DI + 2 * N :].reshape(rows, tp, heads),
            jnp.broadcast_to(packed, (rows, tp, cells)),
            jnp.zeros((rows, tp, LANES - heads - cells), BF16),
        ],
        axis=2,
    ).transpose(1, 0, 2)
    return rest, gate


def body(
    tokens,
    in_proj,
    conv_weight,
    conv_bias,
    decay_log,
    step_bias,
    skip_gain,
    norm_gain,
    gated_gain,
    out_proj,
    cotangent,
):
    dp, tp = lax.axis_size("dp"), lax.axis_size("seq")
    total = dp * tp
    s = lax.axis_index("seq")
    micro, part, width = tokens.shape
    heads = HEADS // tp
    inner = heads * P_SIZE
    rows = in_proj.shape[0]
    length = part * tp
    count = micro * length
    wide = inner + 2 * N
    chan = conv_bias.shape[0]

    own = jnp.concatenate([conv_weight.reshape(-1), conv_bias, norm_gain, gated_gain])
    rest, gate = weight_columns(in_proj, own, tp, heads)
    w_rest, w_gate, tok = gather(rest, gate, tokens, dp)
    w_rest = w_rest.reshape(width, wide + LANES)
    w_gate = w_gate.reshape(width, inner)
    tok = tok.reshape(count, width)
    turn = [(b * dp + a, a * tp + b) for a in range(dp) for b in range(tp)]
    w_out = lax.ppermute(out_proj, ("dp", "seq"), turn)
    w_out, tok, upstream = lax.optimization_barrier((w_out, tok, cotangent))
    w_out = lax.all_gather(w_out, "dp", axis=0, tiled=True)
    cot = over_seq(upstream).reshape(count, width)

    cells = -(-own.shape[0] // rows)
    shared = w_rest[:, wide + heads : wide + heads + cells].reshape(total, rows * cells).astype(F32)
    w_conv = shared[:, : KW * chan].reshape(total, KW, chan).transpose(1, 0, 2).reshape(KW, CD)
    b_conv = shared[:, KW * chan : (KW + 1) * chan].reshape(1, CD)
    at = (KW + 1) * chan
    g_norm = shared[:, at : at + rows].reshape(width)
    g_gated = shared[:, at + rows : at + rows + gated_gain.shape[0]].reshape(DI)
    first, lane = s * inner, s * heads
    taps = jnp.concatenate([w_conv, b_conv, jnp.zeros((3, CD), F32)], axis=0)
    taps = jnp.concatenate([lax.dynamic_slice_in_dim(taps, first, inner, 1), taps[:, DI:]], axis=1)
    g_gated = lax.dynamic_slice_in_dim(g_gated, first, inner)
    head = jnp.stack([decay_log, step_bias, skip_gain])
    head = lax.dynamic_slice_in_dim(head, lane, heads, 1)
    head = jnp.pad(head, ((0, 5), (0, LANES - heads)))

    h = tok.astype(F32)
    r = lax.rsqrt(jnp.mean(h * h, axis=-1, keepdims=True) + EPSILON)
    normed = (h * r * g_norm).astype(BF16)
    proj_rest = jnp.dot(normed, w_rest, preferred_element_type=F32)
    ssd, memory = mixer_forward(proj_rest, taps, head, heads, micro)
    gate = jnp.dot(normed, w_gate, preferred_element_type=F32)
    sig = jax.nn.sigmoid(gate)
    act = gate * sig
    gated = ssd * act
    grad_shaped = jnp.dot(cot, w_out.T, preferred_element_type=F32)
    weighed = grad_shaped * g_gated
    stats = jnp.stack([jnp.sum(gated * gated, axis=1), jnp.sum(weighed * gated, axis=1)])
    stats = add_over_seq(stats, dp)
    q = lax.rsqrt(stats[0] / DI + EPSILON)[:, None]
    shaped = (gated * q * g_gated).astype(BF16)
    grad_gated = q * (weighed - gated * (q * q * (stats[1] / DI)[:, None]))
    grad_ssd = grad_gated * act
    grad_gate = (grad_gated * ssd * (sig + act * (1 - sig))).astype(BF16)

    out_part = jnp.dot(shaped, w_out, preferred_element_type=F32).astype(BF16)
    here, away = over_cores(out_part.reshape(micro, length, width))

    grad_out = jnp.dot(shaped.T, cot, preferred_element_type=F32).astype(BF16)
    gate_in = jnp.dot(normed.T, grad_gate, preferred_element_type=F32).astype(BF16)
    grad_ssd, grad_out, gate_in, here, away = lax.optimization_barrier(
        (grad_ssd, grad_out, gate_in, here, away)
    )
    h_own = tokens.astype(F32)
    block_out = (h_own + here + lax.ppermute(away, "seq", CHIPS).astype(F32)).astype(BF16)
    joint = jnp.concatenate(
        [grad_out.reshape(dp, -1, width), gate_in.reshape(dp, -1, width)], axis=1
    ).reshape(-1, width)
    joint = lax.psum_scatter(joint, "dp", scatter_dimension=0, tiled=True)
    grad_out = joint[: out_proj.shape[0]]
    gate_in = joint[out_proj.shape[0] :].reshape(tp * rows, inner)
    grad_out = lax.ppermute(grad_out, ("dp", "seq"), [(b, a) for a, b in turn]).astype(F32)
    gated_gain_grad = jnp.sum(out_proj.astype(F32) * grad_out, axis=1) / gated_gain.astype(F32)
    gate_in = lax.all_to_all(gate_in.reshape(tp, rows, inner), "seq", 0, 0)

    grad_rest, wgrad, hgrad = mixer_backward(proj_rest, grad_ssd, memory, taps, head, heads, micro)
    small = jnp.concatenate([wgrad[: KW + 1].reshape(-1), hgrad[:3].reshape(-1)])
    lines = -(-small.shape[0] // (8 * LANES)) * 8
    small = jnp.pad(small, (0, lines * LANES - small.shape[0])).reshape(lines, LANES)
    rest_in = jnp.dot(normed.T, grad_rest, preferred_element_type=F32).astype(BF16)
    rest_in, grad_normed, small = scatter(
        rest_in.reshape(dp, tp, rows, wide + LANES),
        grad_rest,
        grad_gate,
        w_rest,
        w_gate,
        small,
        dp,
        micro,
    )
    rest_in = rest_in.astype(F32)
    small = small[-tp:].reshape(tp, -1)
    convs = small[:, : (KW + 1) * wide].reshape(tp, KW + 1, wide)
    convs = jnp.concatenate(
        [
            convs[:, :, :inner].transpose(1, 0, 2).reshape(KW + 1, DI),
            jnp.sum(convs[:, :, inner:], axis=0),
        ],
        axis=1,
    )
    place = lax.axis_index("dp") * tp + s
    convs = lax.dynamic_slice_in_dim(convs, place * chan, chan, 1)
    head_grads = small[:, (KW + 1) * wide : (KW + 1) * wide + 3 * LANES].reshape(tp, 3, LANES)[:, :, :heads]
    head_grads = head_grads.transpose(1, 0, 2).reshape(3, HEADS)

    def side(a):
        return a.astype(F32).transpose(1, 0, 2).reshape(rows, -1)

    in_grad = jnp.concatenate(
        [
            side(gate_in),
            side(rest_in[:, :, :inner]),
            jnp.sum(rest_in[:, :, inner:wide], axis=0),
            side(rest_in[:, :, wide : wide + heads]),
        ],
        axis=1,
    )
    norm_gain_grad = jnp.sum(in_proj.astype(F32) * in_grad, axis=1) / norm_gain.astype(F32)

    r_own = lax.rsqrt(jnp.mean(h_own * h_own, axis=-1, keepdims=True) + EPSILON)
    n_own = h_own * r_own
    g = grad_normed * g_norm
    tokens_grad = cotangent.astype(F32) + r_own * (
        g - n_own * jnp.mean(g * n_own, axis=-1, keepdims=True)
    )
    return (
        block_out,
        tokens_grad.astype(BF16),
        in_grad,
        convs[:KW],
        convs[KW],
        head_grads[0],
        head_grads[1],
        head_grads[2],
        norm_gain_grad,
        gated_gain_grad,
        grad_out,
    )


def solution(mesh):
    both = ("dp", "seq")
    return jax.shard_map(
        body,
        mesh=mesh,
        in_specs=(
            P("dp", "seq", None),
            P(both, None),
            P(None, both),
            P(both),
            P(),
            P(),
            P(),
            P(both),
            P(both),
            P(both, None),
            P("dp", "seq", None),
        ),
        out_specs=(
            P("dp", "seq", None),
            P("dp", "seq", None),
            P(both, None),
            P(None, both),
            P(both),
            P(),
            P(),
            P(),
            P(both),
            P(both),
            P(both, None),
        ),
        check_vma=False,
    )
```

```python
import functools

import jax
import jax.numpy as jnp
from jax import lax
from jax.experimental import pallas as pl
from jax.experimental.pallas import tpu as pltpu
from jax.sharding import PartitionSpec as P

HEADS = 48
P_SIZE = 64
N = 128
KW = 4
DI = 3072
CD = 3328
LANES = 128
FAR = -1e30

EPSILON = 1e-05
F32 = jnp.float32
BF16 = jnp.bfloat16


def dot(a, b, dims=((1,), (0,)), precision=None):
    return lax.dot_general(a, b, (dims, ((), ())), precision=precision, preferred_element_type=F32)


NT = ((1,), (1,))
HIGH = lax.Precision.HIGHEST


def pick(a, p, low):
    return jnp.where(low, a[:, 2 * p : 2 * p + 1], a[:, 2 * p + 1 : 2 * p + 2])


def chunk_parts(heads, rest_ref, xbuf, taps_ref, head_ref):
    size = rest_ref.shape[0]
    wide = taps_ref.shape[1]
    mixed = taps_ref[KW : KW + 1, :] + taps_ref[0:1, :] * xbuf[5 : 5 + size, :]
    for k in range(1, KW):
        mixed = mixed + taps_ref[k : k + 1, :] * xbuf[5 + k : 5 + k + size, :]
    sig = lax.logistic(mixed)
    lane = lax.broadcasted_iota(jnp.int32, (1, LANES), 1)
    raw = jnp.where(lane < heads, rest_ref[:, wide:], 0.0) + head_ref[1:2, :]
    step = jnp.maximum(raw, 0.0) + jnp.log1p(jnp.exp(-jnp.abs(raw)))
    decay = -jnp.exp(head_ref[0:1, :]) * step
    i = lax.broadcasted_iota(jnp.int32, (size, size), 0)
    j = lax.broadcasted_iota(jnp.int32, (size, size), 1)
    run = dot(jnp.where(i >= j, 1.0, 0.0), decay, precision=HIGH)
    return mixed, sig, raw, step, decay, run


def backward_kernel(
    heads,
    rest_ref,
    prev_ref,
    dy_ref,
    mem_ref,
    taps_ref,
    head_ref,
    out_ref,
    wgrad_ref,
    hgrad_ref,
    xbuf,
    gbuf,
    adj,
    dmix,
    dsum,
    uprod,
    zprod,
    rows_t,
    line,
):
    size = rest_ref.shape[0]
    wide = taps_ref.shape[1]
    inner = heads * P_SIZE
    chunks = pl.num_programs(1)
    step_id = pl.program_id(1)
    newest = step_id == 0
    oldest = step_id == chunks - 1
    begin = jnp.logical_and(pl.program_id(0) == 0, newest)
    finish = jnp.logical_and(pl.program_id(0) == pl.num_programs(0) - 1, oldest)

    @pl.when(begin)
    def _():
        wgrad_ref[...] = jnp.zeros_like(wgrad_ref)
        hgrad_ref[...] = jnp.zeros_like(hgrad_ref)
        rows_t[...] = jnp.zeros_like(rows_t)
        line[...] = jnp.zeros_like(line)

    @pl.when(newest)
    def _():
        gbuf[size : size + 8, :] = jnp.zeros((8, wide), F32)
        adj[...] = jnp.zeros_like(adj)

    @pl.when(jnp.logical_not(newest))
    def _():
        gbuf[size : size + 8, :] = gbuf[0:8, :]

    xbuf[0:8, :] = jnp.where(oldest, 0.0, prev_ref[:, :wide])
    xbuf[8 : 8 + size, :] = rest_ref[:, :wide]
    mixed, sig, raw, step, decay, run = chunk_parts(heads, rest_ref, xbuf, taps_ref, head_ref)
    act = mixed * sig
    run_t = run.T
    closing = run[size - 1 : size, :]
    last = jnp.exp(closing)
    left = jnp.exp(closing - run)
    grown = jnp.exp(run)
    b = act[:, inner : inner + N].astype(BF16)
    c = act[:, inner + N :].astype(BF16)
    c_t = act[:, inner + N :].T.astype(BF16)
    scores_t = dot(b, c, NT)
    low = lax.broadcasted_iota(jnp.int32, (1, LANES), 1) < P_SIZE
    lane = lax.broadcasted_iota(jnp.int32, (1, LANES), 1)
    j = lax.broadcasted_iota(jnp.int32, (size, size), 0)
    i = lax.broadcasted_iota(jnp.int32, (size, size), 1)
    causal = i >= j
    mem_b = mem_ref[0]
    adj_b = adj[...].astype(BF16)
    spread = dot(b, adj_b)
    inherit = dot(c, mem_b)
    scored = jnp.zeros((size, size), F32)
    cols = jnp.zeros((size, LANES), F32)
    for p in range(heads // 2):
        at = slice(p * LANES, (p + 1) * LANES)
        v = act[:, at]
        size_p = pick(step, p, low)
        xv = size_p * v
        dy = dy_ref[:, at]
        dyb = dy.astype(BF16)
        xvb = xv.astype(BF16)
        dxv = pick(left, p, low) * spread[:, at]
        zprod[:, at] = (dxv * xv).astype(BF16)
        dyg = pick(grown, p, low) * dy
        uprod[:, at] = (dyg * inherit[:, at]).astype(BF16)
        for e in range(2):
            h = 2 * p + e
            keep = low if e == 0 else jnp.logical_not(low)
            mine = jnp.where(keep, dy, 0.0).astype(BF16)
            gap = run_t[h : h + 1, :] - run[:, h : h + 1]
            near = jnp.exp(jnp.where(causal, gap, FAR))
            w_t = scores_t * near
            dw_t = dot(xvb, mine, NT)
            scored = scored + dw_t * near
            g_t = dw_t * w_t
            rows_t[h : h + 1, :] = jnp.sum(g_t, axis=0, keepdims=True)
            cols = jnp.where(lane == h, jnp.sum(g_t, axis=1, keepdims=True), cols)
            dxv = dxv + dot(w_t.astype(BF16), mine)
        dsum[:, at] = (dxv * v).astype(BF16)
        dmix[:, at] = size_p * dxv + pick(head_ref[2:3, :], p, low) * dy
        line[0:1, at] += jnp.sum(dy * v, axis=0, keepdims=True)
        line[1:2, at] = jnp.sum(adj[:, at] * mem_b[:, at].astype(F32), axis=0, keepdims=True) * pick(
            last, p, low
        )
        xc = (pick(left, p, low) * xv).astype(BF16)
        dygb = dyg.astype(BF16)
        db = dot(xc, adj_b[:, at], NT)
        dc = dot(dygb, mem_b[:, at], NT)
        if p == 0:
            dmix[:, inner : inner + N] = db
            dmix[:, inner + N :] = dc
        else:
            dmix[:, inner : inner + N] += db
            dmix[:, inner + N :] += dc
        adj[:, at] = adj[:, at] * pick(last, p, low) + dot(c_t, dygb)
    dmix[:, inner : inner + N] += dot(scored.astype(BF16), c)
    dmix[:, inner + N :] += dot(scored.T.astype(BF16), b)

    group = jnp.where(
        lax.broadcasted_iota(jnp.int32, (inner, LANES), 0) // P_SIZE
        == lax.broadcasted_iota(jnp.int32, (inner, LANES), 1),
        1.0,
        0.0,
    )
    group_b = group.astype(BF16)
    d_step = dot(dsum[...], group_b)
    u = dot(uprod[...], group_b)
    z = dot(zprod[...], group_b)
    sums = dot(line[...], group, precision=HIGH)
    d_run = rows_t[...].T - cols + u - z
    row = lax.broadcasted_iota(jnp.int32, (size, 1), 0)
    ending = sums[1:2, :] + jnp.sum(z, axis=0, keepdims=True)
    d_run = d_run + jnp.where(row == size - 1, ending, 0.0)
    d_decay = dot(jnp.where(causal, 1.0, 0.0), d_run, precision=HIGH)
    d_raw = (d_step - jnp.exp(head_ref[0:1, :]) * d_decay) * lax.logistic(raw)
    d_raw = jnp.where(lane < heads, d_raw, 0.0)
    hgrad_ref[0:1, :] += jnp.sum(d_decay * decay, axis=0, keepdims=True)
    hgrad_ref[1:2, :] += jnp.sum(d_raw, axis=0, keepdims=True)

    @pl.when(finish)
    def _():
        hgrad_ref[2:3, :] = sums[0:1, :]

    g = dmix[...] * (sig * (1.0 + mixed * (1.0 - sig)))
    gbuf[0:size, :] = g
    wgrad_ref[KW : KW + 1, :] += jnp.sum(g, axis=0, keepdims=True)
    for k in range(KW):
        wgrad_ref[k : k + 1, :] += jnp.sum(g * xbuf[5 + k : 5 + k + size, :], axis=0, keepdims=True)
    back = taps_ref[KW - 1 : KW, :] * g
    for k in range(KW - 1):
        back = back + taps_ref[k : k + 1, :] * gbuf[3 - k : 3 - k + size, :]
    out_ref[:, :wide] = back.astype(BF16)
    out_ref[:, wide:] = d_raw.astype(BF16)


MESH = pl.DeviceIdType.MESH


def where_am_i(dp):
    d, s = lax.axis_index("dp"), lax.axis_index("seq")
    z, y = d // 2, d % 2
    x, c = s // 2, s % 2
    peers = [s + 1 - 2 * c, s + 2 - 4 * x, 3 - s]
    return d, s, z, y, x, c, peers, dp // 2


def push(src, dst, send_sem, recv_sem, d, s):
    return pltpu.make_async_remote_copy(
        src_ref=src,
        dst_ref=dst,
        send_sem=send_sem,
        recv_sem=recv_sem,
        device_id={"dp": d, "seq": s},
        device_id_type=MESH,
    )


def greet(partners):
    barrier = pltpu.get_barrier_semaphore()
    for cond, d, s in partners:

        def hello(d=d, s=s):
            pl.semaphore_signal(barrier, inc=1, device_id={"dp": d, "seq": s}, device_id_type=MESH)

        if cond is None:
            hello()
        else:
            pl.when(cond)(hello)
    count = 0
    for cond, _, _ in partners:
        count = count + (1 if cond is None else jnp.where(cond, 1, 0))
    pl.semaphore_wait(barrier, count)


class Sends:
    def __init__(self):
        self.items = []

    def start(self, cond, copy):
        if cond is None:
            copy.start()
        else:
            pl.when(cond)(copy.start)
        self.items.append((cond, copy))

    def drain(self):
        for cond, copy in self.items:
            if cond is None:
                copy.wait_send()
            else:
                pl.when(cond)(copy.wait_send)


def stats_kernel(dp, own_ref, out_ref, held, send, recv):
    d, s, *_, peers, _ = where_am_i(dp)
    greet([(None, d, p) for p in peers])
    copies = [
        push(own_ref, held.at[r], send.at[r], recv.at[r], d, p) for r, p in enumerate(peers)
    ]
    for copy in copies:
        copy.start()
    for copy in copies:
        copy.wait()
    out_ref[...] = (own_ref[...] + held[0]) + (held[1] + held[2])


def add_over_seq(stats, dp):
    dma = pltpu.SemaphoreType.DMA
    vmem = pl.BlockSpec(memory_space=pltpu.VMEM)
    return pl.pallas_call(
        functools.partial(stats_kernel, dp),
        in_specs=[vmem],
        out_specs=vmem,
        out_shape=jax.ShapeDtypeStruct(stats.shape, F32),
        scratch_shapes=[pltpu.VMEM((3,) + stats.shape, F32), dma((3,)), dma((3,))],
        compiler_params=pltpu.CompilerParams(collective_id=2, has_side_effects=True),
        name="stats_over_seq",
    )(stats)


STRIPE = DI // 16


def swapped(s):
    return 2 * (s % 2) + s // 2


def stripe_owner(block, dp):
    u = dp // 4
    return block // (4 * u) * u + block % u


def stripe_seat(block, dp):
    return swapped(block // (dp // 4) % 4)


def stripe_block(d, s, dp):
    u = dp // 4
    return (d // u * 4 + swapped(s)) * u + d % u


def forward_chunk(heads, first, rest_ref, taps_ref, head_ref, ssd_ref, mem_ref, xbuf, mem):
    size = rest_ref.shape[0]
    wide = taps_ref.shape[1]
    inner = heads * P_SIZE

    @pl.when(first)
    def _():
        xbuf[0:8, :] = jnp.zeros((8, wide), F32)
        mem[...] = jnp.zeros_like(mem)

    @pl.when(jnp.logical_not(first))
    def _():
        xbuf[0:8, :] = xbuf[size : size + 8, :]

    xbuf[8 : 8 + size, :] = rest_ref[:, :wide]
    mixed, sig, _, step, _, run = chunk_parts(heads, rest_ref, xbuf, taps_ref, head_ref)
    act = mixed * sig
    run_t = run.T
    closing = run[size - 1 : size, :]
    last = jnp.exp(closing)
    left = jnp.exp(closing - run)
    grown = jnp.exp(run)
    b = act[:, inner : inner + N]
    c = act[:, inner + N :].astype(BF16)
    scores = dot(c, b.astype(BF16), NT)
    b_t = b.T.astype(BF16)
    mem_ref[...] = mem[...].astype(BF16)
    inter = dot(c, mem[...].astype(BF16))
    low = lax.broadcasted_iota(jnp.int32, (1, LANES), 1) < P_SIZE
    i = lax.broadcasted_iota(jnp.int32, (size, size), 0)
    j = lax.broadcasted_iota(jnp.int32, (size, size), 1)
    causal = i >= j
    for p in range(heads // 2):
        at = slice(p * LANES, (p + 1) * LANES)
        v = act[:, at]
        xv = pick(step, p, low) * v
        y = pick(head_ref[2:3, :], p, low) * v + pick(grown, p, low) * inter[:, at]
        for e in range(2):
            h = 2 * p + e
            gap = run[:, h : h + 1] - run_t[h : h + 1, :]
            w = (scores * jnp.exp(jnp.where(causal, gap, FAR))).astype(BF16)
            mine = jnp.where(low if e == 0 else jnp.logical_not(low), xv, 0.0).astype(BF16)
            y = y + dot(w, mine)
        ssd_ref[:, at] = y
        xc = (pick(left, p, low) * xv).astype(BF16)
        mem[:, at] = mem[:, at] * pick(last, p, low) + dot(b_t, xc)


def hop(v, size):
    return sum(jnp.where(v >= q * size, 1, 0) for q in range(1, 4))


def head_kernel(
    dp,
    heads,
    proj_ref,
    cw_ref,
    cb_ref,
    ng_ref,
    gg_ref,
    ph_ref,
    tok_ref,
    cot_ref,
    block_ref,
    normed_hbm,
    turned_hbm,
    proj_hbm,
    ssd_hbm,
    mem_hbm,
    gates_hbm,
    rest_hbm,
    gate_hbm,
    out_hbm,
    cot_hbm,
    taps_ref,
    gain_ref,
    gated_ref,
    head_ref,
    line,
    small_stage,
    val_stage,
    half_stage,
    gate_stage,
    small_all,
    val_in,
    half_in,
    gate_in,
    w_val,
    w_half,
    w_other,
    w_tail,
    w_gate,
    out_shard,
    tok,
    flipped,
    proj,
    ssd,
    gates,
    memory,
    xbuf,
    mem,
    l_sem,
    o_sem,
    f_sem,
    p_sem,
    g_sem,
    a_send,
    a_recv,
    z_send,
    z_recv,
    y_send,
    y_recv,
    t_send,
    t_recv,
):
    d, s, z, y, x, c, peers, deep = where_am_i(dp)
    tp, rows = val_stage.shape[:2]
    micro, part, width = tok_ref.shape
    total = dp * tp
    inner = heads * P_SIZE
    wide = inner + 2 * N
    chan, gpiece = cw_ref.shape[1], gg_ref.shape[1]
    up, down, far = d + 2, d - 2, d + 1 - 2 * y
    me = d * tp + s
    to_d, to_s, turned = stripe_owner(me, dp), stripe_seat(me, dp), stripe_block(d, s, dp)
    from_d, from_s = turned // tp, turned % tp
    moves = turned != me

    triple = HEADS // 16
    line[...] = jnp.zeros_like(line)
    line[0:KW, 0:chan] = cw_ref[...].astype(F32)
    line[KW : KW + 1, 0:chan] = cb_ref[...].astype(F32)
    line[KW + 1 : KW + 2, 0:rows] = ng_ref[...].astype(F32)
    line[KW + 2 : KW + 3, 0:gpiece] = gg_ref[...].astype(F32)
    raw = proj_ref[:, 2 * DI + 2 * N :]
    for b in range(4):
        seat = 2 * (b % 2) + b // 2
        for k in range(4):
            to, at = k * STRIPE, (4 * k + b) * STRIPE
            gate_stage[seat, :, to : to + STRIPE] = proj_ref[:, at : at + STRIPE]
            val_stage[seat, :, to : to + STRIPE] = proj_ref[:, DI + at : DI + at + STRIPE]
        at = 2 * DI + N * (seat % 2)
        half_stage[seat] = proj_ref[:, at : at + N]
        v = lax.broadcasted_iota(jnp.int32, (16, HEADS), 0)
        g = lax.broadcasted_iota(jnp.int32, (16, HEADS), 1)
        hit = jnp.logical_and(v < heads, g == v + 3 * triple * hop(v, triple) + triple * b)
        line[16:32, 0:rows] = dot(jnp.where(hit, 1.0, 0.0).astype(BF16), raw, NT)
        small_stage[seat] = line[...].astype(BF16)
    v = lax.broadcasted_iota(jnp.int32, (HEADS, LANES), 1)
    g = lax.broadcasted_iota(jnp.int32, (HEADS, LANES), 0)
    hit = jnp.logical_and(v < heads, g == v + 3 * triple * hop(v, triple) + triple * swapped(s))
    head_ref[...] = dot(ph_ref[...], jnp.where(hit, 1.0, 0.0), precision=HIGH)

    greet(
        [(None, d, p) for p in peers]
        + [(None, far, s), (z < deep - 1, up, s), (z > 0, down, s)]
        + [(moves, to_d, to_s), (moves, from_d, from_s)]
    )
    sends = Sends()

    def arrive(dst, sem):
        push(dst, dst, sem, sem, d, peers[0]).wait_recv()

    def mine(ref, k):
        return ref.at[:, pl.ds(k * part, part), :]

    def exchange(a, stage, target):
        for r, p in enumerate(peers):
            sends.start(
                None, push(stage.at[p], target(s), a_send.at[a, r], a_recv.at[a, r], d, p)
            )

    def exchanged(a, target):
        for r, p in enumerate(peers):
            arrive(target(p), a_recv.at[a, r])

    exchange(0, small_stage, lambda k: small_all.at[d, k])
    exchange(1, half_stage, lambda k: half_in.at[k])
    exchange(2, val_stage, lambda k: val_in.at[k])
    exchange(3, gate_stage, lambda k: gate_in.at[k])
    sends.start(moves, push(block_ref, out_shard, t_send.at[2], t_recv.at[2], to_d, to_s))
    sends.start(None, push(tok_ref, mine(tok, s), t_send.at[0], t_recv.at[0], d, peers[1]))
    sends.start(None, push(tok_ref, mine(tok, s), t_send.at[1], t_recv.at[1], d, peers[0]))
    sends.start(None, push(cot_ref, mine(cot_hbm, s), t_send.at[3], t_recv.at[3], d, peers[1]))
    sends.start(None, push(cot_ref, mine(cot_hbm, s), t_send.at[4], t_recv.at[4], d, peers[0]))
    saves = []

    def save(src, dst):
        copy = pltpu.make_async_copy(src, dst, l_sem.at[len(saves)])
        copy.start()
        saves.append(copy)

    save(cot_ref, mine(cot_hbm, s))
    small_all[d, s] = small_stage[s]
    half_in[s] = half_stage[s]
    val_in[s] = val_stage[s]
    gate_in[s] = gate_stage[s]
    tok[:, pl.ds(pl.multiple_of(s * part, part), part), :] = tok_ref[...]

    @pl.when(jnp.logical_not(moves))
    def _():
        out_shard[...] = block_ref[...]

    def begin(a, shard, dst):
        block = dst.at[d]
        sends.start(z < deep - 1, push(shard, block, z_send.at[a, 0, 0], z_recv.at[a, 0, 0], up, s))
        sends.start(z > 0, push(shard, block, z_send.at[a, 1, 0], z_recv.at[a, 1, 0], down, s))
        sends.start(None, push(shard, block, y_send.at[a, 0, 0], y_recv.at[a, 0, 0], far, s))

    def plan(a, dst, t):
        steps = []
        for way in range(2):
            here = (z >= t) if way == 0 else (z + t <= deep - 1)
            more = jnp.logical_and(here, (z < deep - 1) if way == 0 else (z > 0))
            at = jnp.clip(d - 2 * t if way == 0 else d + 2 * t, 0, dp - 1)
            block = dst.at[at]
            got = z_recv.at[a, way, t - 1]
            on = []
            if t < deep - 1:
                nxt = up if way == 0 else down
                on.append(
                    (more, push(block, block, z_send.at[a, way, t], z_recv.at[a, way, t], nxt, s))
                )
            on.append(
                (here, push(block, block, y_send.at[a, way, t], y_recv.at[a, way, t], far, s))
            )
            steps.append((here, push(block, block, got, got, d, peers[0]), on))
        return steps

    def run(steps):
        for here, wait, on in steps:
            pl.when(here)(wait.wait_recv)
            for cond, copy in on:
                pl.when(cond)(copy.start)

    def remember(steps):
        for _, _, on in steps:
            sends.items.extend(on)

    def relay(a, dst, t):
        steps = plan(a, dst, t)
        run(steps)
        remember(steps)

    def landed(a, dst):
        arrive(dst.at[far], y_recv.at[a, 0, 0])
        for t in range(1, deep):
            for way in range(2):
                here = (z >= t) if way == 0 else (z + t <= deep - 1)
                at = jnp.clip(far - 2 * t if way == 0 else far + 2 * t, 0, dp - 1)
                pl.when(here)(functools.partial(arrive, dst.at[at], y_recv.at[a, way, t]))

    def shard_of(a, pieces, dst):
        exchanged(a, lambda p: pieces.at[p])
        for k in range(tp):
            dst[d, k * rows : (k + 1) * rows, :] = pieces[k]
        begin(a, dst.at[d], dst)

    exchanged(0, lambda p: small_all.at[d, p])
    begin(0, small_all.at[d], small_all)
    shard_of(1, half_in, w_half)
    shard_of(2, val_in, w_val)
    for t in range(1, deep):
        relay(0, small_all, t)
        relay(1, w_half, t)
        relay(2, w_val, t)
    shard_of(3, gate_in, w_gate)
    pl.when(moves)(functools.partial(arrive, out_shard, t_recv.at[2]))
    begin(4, out_shard, out_hbm)
    save(out_shard, out_hbm.at[d])

    landed(0, small_all)

    def one_hot(columns, index, k, length):
        lane = lax.broadcasted_iota(jnp.int32, (LANES, columns), 1)
        at = lax.broadcasted_iota(jnp.int32, (LANES, columns), 0)
        hit = jnp.logical_and(at < length, index(lane) == k * length + at)
        return jnp.where(hit, 1.0, 0.0).astype(BF16)

    taps_ref[...] = jnp.zeros_like(taps_ref)
    gain_ref[...] = jnp.zeros_like(gain_ref)
    gated_ref[...] = jnp.zeros_like(gated_ref)

    def striped(v):
        return v + 3 * STRIPE * hop(v, STRIPE) + STRIPE * swapped(s)

    def lay_out(dd, carry):
        for kk in range(tp):
            k = dd * tp + kk
            values = small_all[dd, kk, 0:16, :]
            chans = one_hot(wide, lambda v: jnp.where(v < inner, striped(v), v - inner + DI), k, chan)
            taps_ref[...] += dot(values, chans)
            gain_ref[...] += dot(values, one_hot(width, lambda v: v, k, rows))
            gated_ref[...] += dot(values, one_hot(inner, striped, k, gpiece))
            turned = jnp.concatenate(
                [small_all[dd, kk, 16:32, :].astype(F32), jnp.zeros((LANES - 16, LANES), F32)], axis=0
            ).T
            w_tail[dd, kk * rows : (kk + 1) * rows, 2 * N :] = turned[:rows].astype(BF16)
        return carry

    lax.fori_loop(0, dp, lay_out, 0)
    landed(1, w_half)
    sends.start(None, push(w_half, w_other, t_send.at[6], t_recv.at[6], d, peers[0]))
    landed(2, w_val)
    save(w_val, rest_hbm.at[:, :, pl.ds(0, inner)])
    arrive(w_other, t_recv.at[6])

    def both_halves(dd, carry):
        w_tail[dd, :, pl.ds(pl.multiple_of(c * N, N), N)] = w_half[dd]
        w_tail[dd, :, pl.ds(pl.multiple_of((1 - c) * N, N), N)] = w_other[dd]
        return carry

    lax.fori_loop(0, dp, both_halves, 0)
    save(w_tail, rest_hbm.at[:, :, pl.ds(inner, w_tail.shape[2])])
    arrive(mine(tok, peers[1]), t_recv.at[0])
    block = mine(tok, peers[1])
    hand = push(block, block, t_send.at[5], t_recv.at[5], d, peers[0])
    hand.start()
    relay(3, w_gate, 1)
    relay(4, out_hbm, 1)
    arrive(mine(tok, peers[0]), t_recv.at[1])
    arrive(mine(tok, peers[2]), t_recv.at[5])
    hand.wait_send()

    tasks = [(a, ref, t) for t in range(2, deep) for a, ref in ((3, w_gate), (4, out_hbm))]
    chunks = micro * tp
    when = {}
    for n, task in enumerate(tasks):
        when.setdefault(min(n * 4 // len(tasks), chunks - 1), []).append(plan(*task))
    for plans in when.values():
        for steps in plans:
            remember(steps)

    def columns(i):
        return pl.ds(pl.multiple_of(i * part, part), part)

    def chunk(i, carry):
        m, k = i // tp, i % tp
        lines = pl.ds(pl.multiple_of(k * part, part), part)
        h = tok[m, lines, :].astype(F32)
        r = lax.rsqrt(jnp.mean(h * h, axis=-1, keepdims=True) + EPSILON)
        value = h * r * gain_ref[5:6, :]
        tok[m, lines, :] = value.astype(BF16)
        flipped[i] = value.T.astype(BF16)
        proj[i, :, 0:inner] = dot(tok[m, lines, :], w_val[...].reshape(width, inner))
        proj[i, :, inner:] = dot(tok[m, lines, :], w_tail[...].reshape(width, w_tail.shape[2]))
        forward_chunk(
            heads, k == 0, proj.at[i], taps_ref, head_ref, ssd.at[i], memory.at[i], xbuf, mem
        )
        pltpu.make_async_copy(tok.at[m, lines, :], normed_hbm.at[m, lines, :], o_sem.at[i]).start()
        pltpu.make_async_copy(flipped.at[i], turned_hbm.at[:, columns(i)], f_sem.at[i]).start()
        pltpu.make_async_copy(proj.at[i], proj_hbm.at[i], p_sem.at[i]).start()
        for n, plans in when.items():

            @pl.when(i == n)
            def _():
                for steps in plans:
                    run(steps)

        return carry

    lax.fori_loop(0, chunks, chunk, 0)
    save(ssd, ssd_hbm)
    save(memory, mem_hbm)
    arrive(mine(cot_hbm, peers[1]), t_recv.at[3])
    block = mine(cot_hbm, peers[1])
    sends.start(None, push(block, block, t_send.at[7], t_recv.at[7], d, peers[0]))
    landed(3, w_gate)
    save(w_gate, gate_hbm)

    def gating(i, carry):
        m, k = i // tp, i % tp
        lines = pl.ds(pl.multiple_of(k * part, part), part)
        gates[i] = dot(tok[m, lines, :], w_gate[...].reshape(width, inner))
        pltpu.make_async_copy(gates.at[i], gates_hbm.at[i], g_sem.at[i]).start()
        return carry

    lax.fori_loop(0, chunks, gating, 0)
    landed(4, out_hbm)
    arrive(mine(cot_hbm, peers[0]), t_recv.at[4])
    arrive(mine(cot_hbm, peers[2]), t_recv.at[7])

    def saved(i, carry):
        m, k = i // tp, i % tp
        lines = pl.ds(pl.multiple_of(k * part, part), part)
        pltpu.make_async_copy(tok.at[m, lines, :], normed_hbm.at[m, lines, :], o_sem.at[i]).wait()
        pltpu.make_async_copy(flipped.at[i], turned_hbm.at[:, columns(i)], f_sem.at[i]).wait()
        pltpu.make_async_copy(proj.at[i], proj_hbm.at[i], p_sem.at[i]).wait()
        pltpu.make_async_copy(gates.at[i], gates_hbm.at[i], g_sem.at[i]).wait()
        return carry

    lax.fori_loop(0, chunks, saved, 0)
    for copy in saves:
        copy.wait()
    sends.drain()


def head(in_proj, conv_weight, conv_bias, norm_gain, gated_gain, per_head, tokens, cotangent, out_proj, dp, tp):
    rows = in_proj.shape[0]
    heads = HEADS // tp
    inner = heads * P_SIZE
    full = inner + 2 * N + LANES
    micro, part, width = tokens.shape
    deep = dp // 2
    chunks = micro * tp
    block = tp * rows
    dma = pltpu.SemaphoreType.DMA
    vmem = pl.BlockSpec(memory_space=pltpu.VMEM)
    hbm = pl.BlockSpec(memory_space=pl.ANY)
    wide = inner + 2 * N

    def shape(*dims, kind=BF16):
        return jax.ShapeDtypeStruct(dims, kind)

    def room(*dims, kind=BF16):
        return pltpu.VMEM(dims, kind)

    return pl.pallas_call(
        functools.partial(head_kernel, dp, heads),
        in_specs=[vmem] * 9,
        out_specs=[hbm] * 10 + [vmem] * 4,
        out_shape=[
            shape(micro, tp * part, width),
            shape(width, chunks * part),
            shape(chunks, part, full, kind=F32),
            shape(chunks, part, inner, kind=F32),
            shape(chunks, N, inner),
            shape(chunks, part, inner, kind=F32),
            shape(dp, block, full),
            shape(dp, block, inner),
            shape(dp, out_proj.shape[0], width),
            shape(micro, tp * part, width),
            shape(16, wide, kind=F32),
            shape(16, width, kind=F32),
            shape(16, inner, kind=F32),
            shape(8, LANES, kind=F32),
        ],
        scratch_shapes=[
            room(32, LANES, kind=F32),
            room(tp, 32, LANES),
            room(tp, rows, inner),
            room(tp, rows, N),
            room(tp, rows, inner),
            room(dp, tp, 32, LANES),
            room(tp, rows, inner),
            room(tp, rows, N),
            room(tp, rows, inner),
            room(dp, block, inner),
            room(dp, block, N),
            room(dp, block, N),
            room(dp, block, 2 * N + LANES),
            room(dp, block, inner),
            room(*out_proj.shape),
            room(micro, tp * part, width),
            room(chunks, width, part),
            room(chunks, part, full, kind=F32),
            room(chunks, part, inner, kind=F32),
            room(chunks, part, inner, kind=F32),
            room(chunks, N, inner),
            room(part + 8, wide, kind=F32),
            room(N, inner, kind=F32),
            dma((8,)),
            dma((chunks,)),
            dma((chunks,)),
            dma((chunks,)),
            dma((chunks,)),
            dma((4, 3)),
            dma((4, 3)),
            dma((5, 2, deep - 1)),
            dma((5, 2, deep - 1)),
            dma((5, 2, deep)),
            dma((5, 2, deep)),
            dma((8,)),
            dma((8,)),
        ],
        compiler_params=pltpu.CompilerParams(
            collective_id=1, has_side_effects=True, vmem_limit_bytes=62 * 2**20
        ),
        cost_estimate=pl.CostEstimate(flops=10**11, bytes_accessed=5 * 10**7, transcendentals=0),
        name="gather_and_mix",
    )(in_proj, conv_weight, conv_bias, norm_gain, gated_gain, per_head, tokens, cotangent, out_proj)


class OwnerSum:
    def __init__(self, where, sends, source, mine, ybuf, zbuf, final, sems, theirs_ref=None):
        self.where, self.sends = where, sends
        self.mine, self.ybuf, self.zbuf, self.final = mine, ybuf, zbuf, final
        d, s, z, y, _, _, _, deep = where
        self.load_sem, y_send, self.y_recv, z_send, self.z_recv = sems
        lower = z < deep // 2

        def place(j):
            low = jnp.where(j > z, deep - 1 - j, deep - 1 - z + j)
            high = jnp.where(j < z, j, z + deep - 1 - j)
            return jnp.where(j == z, deep - 1, jnp.where(lower, low, high))

        def turn(k):
            low = jnp.where(k < deep - 1 - z, deep - 1 - k, k - (deep - 1 - z))
            high = jnp.where(k < z, k, deep - 1 - (k - z))
            return jnp.where(lower, low, high) if k < deep - 1 else z

        self.order = [turn(k) for k in range(deep)]
        self.y_items, self.loads = [], []
        for k, j in enumerate(self.order):
            theirs = source.at[j * 2 + 1 - y] if theirs_ref is None else theirs_ref.at[k]
            copy = push(theirs, ybuf.at[k], y_send.at[k], self.y_recv.at[k], d + 1 - 2 * y, s)
            self.y_items.append((None, copy))
            if theirs_ref is None:
                own = source.at[j * 2 + y]
                self.loads.append(pltpu.make_async_copy(own, mine.at[k], self.load_sem.at[k]))
        self.z_items = []
        for t in range(deep - 1):
            ways = []
            for way in range(2):
                depth = z if way == 0 else deep - 1 - z
                j = deep - 1 - t + z if way == 0 else t + z - deep + 1
                k = place(jnp.clip(j, 0, deep - 1))
                nxt = d + 2 if way == 0 else d - 2
                dst, ss, rs = zbuf.at[way, t], z_send.at[way, t], self.z_recv.at[way, t]
                first = (depth == 0, push(ybuf.at[k], dst, ss, rs, nxt, s))
                later = None
                if t > 0:
                    cond = jnp.logical_and(depth > 0, depth <= t)
                    later = (cond, push(zbuf.at[way, t - 1], dst, ss, rs, nxt, s))
                ways.append((k, first, later))
            self.z_items.append(ways)
        sends.items.extend(self.y_items)
        for ways in self.z_items:
            for _, first, later in ways:
                sends.items.append(first)
                if later is not None:
                    sends.items.append(later)

    def arrive(self, ref, sem):
        d, s = self.where[:2]
        push(ref, ref, sem, sem, d, self.where[6][0]).wait_recv()

    def begin(self):
        for _, copy in self.y_items:
            copy.start()
        for copy in self.loads:
            copy.start()

    def each(self, work):
        if self.mine.ndim == 4:
            count, cut = self.mine.shape[1], lambda i: i
        else:
            count, cut = self.mine.shape[1] // 16, lambda i: pl.ds(pl.multiple_of(i * 16, 16), 16)
        lax.fori_loop(0, count, lambda i, carry: (work(cut(i)), carry)[1], 0)

    def add(self, k):
        if self.loads:
            self.loads[k].wait()
        self.arrive(self.ybuf.at[k], self.y_recv.at[k])
        ybuf, mine = self.ybuf, self.mine

        def work(i):
            ybuf[k, i] = (ybuf[k, i].astype(F32) + mine[k, i].astype(F32)).astype(BF16)

        self.each(work)

    def send(self, t):
        zbuf, ybuf = self.zbuf, self.ybuf
        for way, (k, first, later) in enumerate(self.z_items[t]):
            pl.when(first[0])(first[1].start)
            if later is None:
                continue

            @pl.when(later[0])
            def _():
                self.arrive(zbuf.at[way, t - 1], self.z_recv.at[way, t - 1])

                def work(i):
                    zbuf[way, t - 1, i] = (
                        zbuf[way, t - 1, i].astype(F32) + ybuf[k, i].astype(F32)
                    ).astype(BF16)

                self.each(work)
                later[1].start()

    def finish(self):
        z, deep = self.where[2], self.where[7]
        zbuf, ybuf, final = self.zbuf, self.ybuf, self.final
        for way in range(2):
            depth = z if way == 0 else deep - 1 - z
            pl.when(depth > 0)(
                functools.partial(self.arrive, zbuf.at[way, deep - 2], self.z_recv.at[way, deep - 2])
            )

        def work(ways, i):
            total = ybuf[deep - 1, i].astype(F32)
            for way in ways:
                total = total + zbuf[way, deep - 2, i].astype(F32)
            final[i] = total.astype(BF16)

        for cond, ways in (
            (z == 0, (1,)),
            (z == deep - 1, (0,)),
            (jnp.logical_and(z > 0, z < deep - 1), (0, 1)),
        ):
            pl.when(cond)(functools.partial(self.each, functools.partial(work, ways)))


def middle_kernel(
    dp,
    heads,
    rest_ref,
    prev_ref,
    dy_ref,
    mem_ref,
    taps_ref,
    head_ref,
    part_hbm,
    gout_hbm,
    ggate_hbm,
    out_ref,
    wgrad_ref,
    hgrad_ref,
    own_hbm,
    gout_out,
    ggate_out,
    xbuf,
    gbuf,
    adj,
    dmix,
    dsum,
    uprod,
    zprod,
    rows_t,
    line,
    o_mine,
    o_y,
    o_z,
    o_final,
    g_mine,
    g_y,
    g_z,
    g_final,
    own,
    core_buf,
    x_buf,
    result,
    o_load,
    o_ysend,
    o_yrecv,
    o_zsend,
    o_zrecv,
    g_load,
    g_ysend,
    g_yrecv,
    g_zsend,
    g_zrecv,
    b_load,
    c_send,
    c_recv,
    m_send,
    m_recv,
    a_send,
    a_recv,
):
    where = where_am_i(dp)
    d, s, z, y, x, c, peers, deep = where
    micro, part, width = result.shape
    step = pl.program_id(0) * pl.num_programs(1) + pl.program_id(1)
    tp = ggate_hbm.shape[1]
    me = d * tp + s
    turned = stripe_block(d, s, dp)
    moves = turned != me
    to_d, to_s = turned // tp, turned % tp
    from_d, from_s = stripe_owner(me, dp), stripe_seat(me, dp)
    sends = Sends()
    gout = OwnerSum(
        where, sends, gout_hbm, o_mine, o_y, o_z, o_final, (o_load, o_ysend, o_yrecv, o_zsend, o_zrecv)
    )
    ggate = OwnerSum(
        where, sends, ggate_hbm, g_mine, g_y, g_z, g_final, (g_load, g_ysend, g_yrecv, g_zsend, g_zrecv)
    )

    def chunk(k):
        return part_hbm.at[:, pl.ds(k * part, part), :]

    cores, loads = [], []
    for q, xx in enumerate((1 - x, x)):
        cores.append(
            push(chunk(xx * 2 + 1 - c), core_buf.at[q], c_send.at[q], c_recv.at[q], d, peers[0])
        )
        loads.append(pltpu.make_async_copy(chunk(xx * 2 + c), own.at[q], b_load.at[q]))
    across = push(core_buf.at[0], x_buf, m_send.at[0], m_recv.at[0], d, peers[1])
    turning = push(o_final, gout_out, m_send.at[1], m_recv.at[1], to_d, to_s)
    staying = pltpu.make_async_copy(o_final, gout_out, b_load.at[2])
    swaps = [
        push(g_final.at[p], ggate_out.at[s], a_send.at[r], a_recv.at[r], d, p)
        for r, p in enumerate(peers)
    ]
    kept = pltpu.make_async_copy(g_final.at[s], ggate_out.at[s], b_load.at[3])
    saved = pltpu.make_async_copy(result, own_hbm, b_load.at[4])
    for copy in cores + [across] + swaps:
        sends.items.append((None, copy))
    sends.items.append((moves, turning))
    span = 16

    def by_rows(work):
        def one(i, carry):
            m, row = i // (part // span), (i % (part // span)) * span
            work(m, pl.ds(pl.multiple_of(row, span), span))
            return carry

        lax.fori_loop(0, micro * (part // span), one, 0)

    def start():
        greet(
            [(None, d, p) for p in peers]
            + [(None, d + 1 - 2 * y, s), (z < deep - 1, d + 2, s), (z > 0, d - 2, s)]
            + [(moves, to_d, to_s), (moves, from_d, from_s)]
        )
        for copy in cores + loads:
            copy.start()
        gout.begin()
        ggate.begin()

    def pass_on():
        loads[0].wait()
        cores[0].wait_recv()

        def work(m, rows):
            core_buf[0, m, rows, :] = (
                core_buf[0, m, rows, :].astype(F32) + own[0, m, rows, :].astype(F32)
            ).astype(BF16)

        by_rows(work)
        across.start()

    def collect():
        loads[1].wait()
        cores[1].wait_recv()
        across.wait_recv()

        def work(m, rows):
            result[m, rows, :] = (
                core_buf[1, m, rows, :].astype(F32)
                + own[1, m, rows, :].astype(F32)
                + x_buf[m, rows, :].astype(F32)
            )

        by_rows(work)
        saved.start()

    def hand_over():
        gout.finish()
        pl.when(moves)(turning.start)
        pl.when(jnp.logical_not(moves))(staying.start)

    def last():
        ggate.finish()
        for copy in swaps:
            copy.start()
        kept.start()
        pl.when(moves)(turning.wait_recv)
        pl.when(jnp.logical_not(moves))(staying.wait)
        for r, p in enumerate(peers):
            push(ggate_out.at[p], ggate_out.at[p], a_send.at[r], a_recv.at[r], d, p).wait_recv()
        kept.wait()
        saved.wait()
        sends.drain()

    stages = {}

    def at(n, task, *args):
        stages.setdefault(n, []).append(functools.partial(task, *args))

    at(0, start)
    at(1, pass_on)
    for k in range(deep):
        n = 1 + k * 3 // (deep - 1)
        at(n, gout.add, k)
        if k < deep - 1:
            at(n, gout.send, k)
    at(4, hand_over)
    at(5, ggate.add, 0)
    for k in range(deep - 1):
        n = 5 + k * 2 // (deep - 2)
        at(n, ggate.send, k)
        at(n, ggate.add, k + 1)
    at(6, collect)
    for n, tasks in stages.items():

        @pl.when(step == n)
        def _():
            for task in tasks:
                task()

    backward_kernel(
        heads,
        rest_ref,
        prev_ref,
        dy_ref,
        mem_ref,
        taps_ref,
        head_ref,
        out_ref,
        wgrad_ref,
        hgrad_ref,
        xbuf,
        gbuf,
        adj,
        dmix,
        dsum,
        uprod,
        zprod,
        rows_t,
        line,
    )
    pl.when(step == pl.num_programs(0) * pl.num_programs(1) - 1)(last)


def middle(rest, dy, memory, taps, head, partial, gout, ggate, dp, tp, heads, micro):
    count, full = rest.shape
    wide = taps.shape[1]
    inner = heads * P_SIZE
    _, length, width = partial.shape
    part = length // tp
    chunks = length // part
    deep = dp // 2
    dma = pltpu.SemaphoreType.DMA
    hbm = pl.BlockSpec(memory_space=pl.ANY)
    gout = gout.reshape(dp, 2, -1, width)

    def at(m, c):
        return m * chunks + chunks - 1 - c

    def sums(block):
        kinds = [(deep,), (deep,), (2, deep - 1), ()]
        return [pltpu.VMEM(kind + block, BF16) for kind in kinds]

    sems = [dma((deep,))] * 3 + [dma((2, deep - 1))] * 2
    out = pl.pallas_call(
        functools.partial(middle_kernel, dp, heads),
        grid=(micro, chunks),
        in_specs=[
            pl.BlockSpec((part, full), lambda m, c: (at(m, c), 0)),
            pl.BlockSpec((8, full), lambda m, c: (jnp.maximum(at(m, c) * (part // 8) - 1, 0), 0)),
            pl.BlockSpec((part, inner), lambda m, c: (at(m, c), 0)),
            pl.BlockSpec((1, N, inner), lambda m, c: (at(m, c), 0, 0)),
            pl.BlockSpec((8, wide), lambda m, c: (0, 0)),
            pl.BlockSpec((8, LANES), lambda m, c: (0, 0)),
            hbm,
            hbm,
            hbm,
        ],
        out_specs=[
            pl.BlockSpec((part, full), lambda m, c: (at(m, c), 0)),
            pl.BlockSpec((8, wide), lambda m, c: (0, 0)),
            pl.BlockSpec((8, LANES), lambda m, c: (0, 0)),
            hbm,
            hbm,
            hbm,
        ],
        out_shape=[
            jax.ShapeDtypeStruct((count, full), BF16),
            jax.ShapeDtypeStruct((8, wide), F32),
            jax.ShapeDtypeStruct((8, LANES), F32),
            jax.ShapeDtypeStruct((micro, part, width), F32),
            jax.ShapeDtypeStruct(gout.shape[1:], BF16),
            jax.ShapeDtypeStruct(ggate.shape[1:], BF16),
        ],
        scratch_shapes=[
            pltpu.VMEM((part + 8, wide), F32),
            pltpu.VMEM((part + 8, wide), F32),
            pltpu.VMEM((N, inner), F32),
            pltpu.VMEM((part, wide), F32),
            pltpu.VMEM((part, inner), BF16),
            pltpu.VMEM((part, inner), BF16),
            pltpu.VMEM((part, inner), BF16),
            pltpu.VMEM((LANES, part), F32),
            pltpu.VMEM((8, inner), F32),
        ]
        + sums(gout.shape[1:])
        + sums(ggate.shape[1:])
        + [
            pltpu.VMEM((2, micro, part, width), BF16),
            pltpu.VMEM((2, micro, part, width), BF16),
            pltpu.VMEM((micro, part, width), BF16),
            pltpu.VMEM((micro, part, width), F32),
        ]
        + sems
        + sems
        + [dma((5,)), dma((2,)), dma((2,)), dma((2,)), dma((2,)), dma((3,)), dma((3,))],
        compiler_params=pltpu.CompilerParams(
            dimension_semantics=("arbitrary", "arbitrary"),
            collective_id=4,
            has_side_effects=True,
            vmem_limit_bytes=62 * 2**20,
        ),
        cost_estimate=pl.CostEstimate(flops=7 * 10**10, bytes_accessed=4 * 10**7, transcendentals=0),
        name="mixer_backward_and_sums",
    )(rest, rest, dy, memory, taps, head, partial, gout, ggate)
    rest_grad, wgrad, hgrad, own, gout, ggate = out
    return rest_grad, wgrad, hgrad, own, gout.reshape(-1, width), ggate


def tail_kernel(
    dp,
    normed_hbm,
    rows_hbm,
    gates_hbm,
    w_rest_hbm,
    w_gate_hbm,
    small_ref,
    out_ref,
    own_ref,
    sums_ref,
    normed,
    rows_ref,
    gates_ref,
    w_rest,
    w_gate,
    tile,
    wtile,
    theirs,
    mine,
    ybuf,
    zbuf,
    final,
    handed,
    core_buf,
    core_out,
    x_buf,
    x_out,
    s_buf,
    l_sem,
    n_sem,
    y_send,
    y_recv,
    z_send,
    z_recv,
    a_send,
    a_recv,
    c_send,
    c_recv,
    x_send,
    x_recv,
    s_send,
    s_recv,
):
    where = where_am_i(dp)
    d, s, z, y, x, c, peers, deep = where
    tp, rows = out_ref.shape[:2]
    block = tp * rows
    micro, part, width = own_ref.shape
    full = rows_ref.shape[1]
    bits = dp.bit_length() - 1
    partners = []
    for k in range(bits):
        step = 2**k
        bit = (d // step) % 2
        partners.append(d + step - 2 * step * bit)
    sends = Sends()
    total = OwnerSum(
        where,
        sends,
        None,
        mine,
        ybuf,
        zbuf,
        final,
        (None, y_send, y_recv, z_send, z_recv),
        theirs,
    )
    loads = [
        pltpu.make_async_copy(src, dst, l_sem.at[k])
        for k, (src, dst) in enumerate(
            (
                (rows_hbm, rows_ref),
                (w_rest_hbm, w_rest),
                (gates_hbm, gates_ref),
                (w_gate_hbm, w_gate),
            )
        )
    ]
    fetches = []
    for k in range(deep):
        lines = pl.ds(pl.multiple_of(total.order[k] * 2 * block, 2 * block), 2 * block)
        fetches.append(pltpu.make_async_copy(normed_hbm.at[lines, :], normed.at[k], n_sem.at[k]))
    for copy in loads + fetches:
        copy.start()
    greet(
        [(None, d, p) for p in peers]
        + [(None, d + 1 - 2 * y, s), (z < deep - 1, d + 2, s), (z > 0, d - 2, s)]
        + [(None, partners[k], s) for k in range(2, bits)]
    )

    def arrive(dst, sem):
        push(dst, dst, sem, sem, d, peers[0]).wait_recv()

    sums_ref[0] = small_ref[...]
    sends.start(None, push(small_ref, s_buf.at[0], s_send.at[0], s_recv.at[0], partners[0], s))

    def each(count, work):
        lax.fori_loop(0, count, lambda i, carry: (work(i), carry)[1], 0)

    across = width // tile.shape[1]
    span = wtile.shape[1]

    def product(owner, use):
        def work(i):
            m, n = i // across, i % across
            row = pl.multiple_of((m * tp + owner) * part, part)
            col = pl.multiple_of(n * tile.shape[1], tile.shape[1])
            lines = pl.ds(col, tile.shape[1])
            tile[...] = dot(rows_ref[pl.ds(row, part), :], w_rest[lines, :], NT) + dot(
                gates_ref[pl.ds(row, part), :], w_gate[lines, :], NT
            )
            use(m, lines)

        each(micro * across, work)

    def weight(k):
        fetches[k].wait()

        def work(n):
            cols = pl.ds(pl.multiple_of(n * span, span), span)
            wtile[...] = dot(normed[k], rows_ref[:, cols])
            far = pl.ds(pl.multiple_of((1 - y) * block, block), block)
            near = pl.ds(pl.multiple_of(y * block, block), block)
            theirs[k, :, cols] = wtile[far, :].astype(BF16)
            mine[k, :, cols] = wtile[near, :].astype(BF16)

        each(full // span, work)
        total.y_items[k][1].start()

    def doubling(k):
        arrive(s_buf.at[k], s_recv.at[k])
        sums_ref[k + 1] = sums_ref[k] + s_buf[k]
        if k + 1 < bits:
            src = sums_ref.at[k + 1]
            sends.start(
                None, push(src, s_buf.at[k + 1], s_send.at[k + 1], s_recv.at[k + 1], partners[k + 1], s)
            )

    def to_core(q):
        def use(m, lines):
            core_out[q, m, :, lines] = tile[...].astype(BF16)

        return use

    def to_chip(m, lines):
        x_out[m, :, lines] = (tile[...] + core_buf[0, m, :, lines].astype(F32)).astype(BF16)

    def keep(m, lines):
        own_ref[m, :, lines] = tile[...] + core_buf[1, m, :, lines].astype(F32)

    for copy in loads:
        copy.wait()
    product((1 - x) * 2 + 1 - c, to_core(0))
    sends.start(
        None, push(core_out.at[0], core_buf.at[0], c_send.at[0], c_recv.at[0], d, peers[0])
    )
    weight(0)
    arrive(core_buf.at[0], c_recv.at[0])
    product((1 - x) * 2 + c, to_chip)
    sends.start(None, push(x_out, x_buf, x_send.at[0], x_recv.at[0], d, peers[1]))
    weight(1)
    total.add(0)
    total.send(0)
    doubling(0)
    for k in range(2, deep):
        weight(k)
    total.add(1)
    total.send(1)
    doubling(1)
    product(x * 2 + 1 - c, to_core(1))
    sends.start(
        None, push(core_out.at[1], core_buf.at[1], c_send.at[1], c_recv.at[1], d, peers[0])
    )
    for k in range(2, deep - 1):
        total.add(k)
        total.send(k)
        if k < bits:
            doubling(k)
    arrive(core_buf.at[1], c_recv.at[1])
    product(s, keep)
    for k in range(deep - 1, bits):
        doubling(k)
    for r, p in enumerate(peers):
        src, dst = sums_ref.at[bits], sums_ref.at[bits + 1 + s]
        sends.start(None, push(src, dst, s_send.at[bits + r], s_recv.at[bits + r], d, p))
    sums_ref[bits + 1 + s] = sums_ref[bits]
    total.add(deep - 1)
    total.finish()
    for p in range(tp):
        handed[p] = final[p * rows : (p + 1) * rows, :]
    for r, p in enumerate(peers):
        sends.start(None, push(handed.at[p], out_ref.at[s], a_send.at[r], a_recv.at[r], d, p))
    out_ref[s] = handed[s]

    arrive(x_buf, x_recv.at[0])

    def last(i):
        m, row = i // (part // 16), (i % (part // 16)) * 16
        lines = pl.ds(pl.multiple_of(row, 16), 16)
        own_ref[m, lines, :] += x_buf[m, lines, :].astype(F32)

    each(micro * (part // 16), last)
    for r, p in enumerate(peers):
        arrive(out_ref.at[p], a_recv.at[r])
        arrive(sums_ref.at[bits + 1 + p], s_recv.at[bits + r])
    sends.drain()


def tail(normed_t, rows_grad, gates_grad, w_rest, w_gate, small, dp, tp, micro):
    width, count = normed_t.shape
    full = rows_grad.shape[1]
    rows = width // dp // tp
    part = count // micro // tp
    deep = dp // 2
    bits = dp.bit_length() - 1
    block = tp * rows
    dma = pltpu.SemaphoreType.DMA
    vmem = pl.BlockSpec(memory_space=pltpu.VMEM)
    hbm = pl.BlockSpec(memory_space=pl.ANY)
    return pl.pallas_call(
        functools.partial(tail_kernel, dp),
        in_specs=[hbm] * 5 + [vmem],
        out_specs=[vmem] * 3,
        out_shape=[
            jax.ShapeDtypeStruct((tp, rows, full), BF16),
            jax.ShapeDtypeStruct((micro, part, width), F32),
            jax.ShapeDtypeStruct((bits + 1 + tp,) + small.shape, F32),
        ],
        scratch_shapes=[
            pltpu.VMEM((deep, 2 * block, count), BF16),
            pltpu.VMEM(rows_grad.shape, BF16),
            pltpu.VMEM(gates_grad.shape, BF16),
            pltpu.VMEM(w_rest.shape, BF16),
            pltpu.VMEM(w_gate.shape, BF16),
            pltpu.VMEM((part, min(width, 512)), F32),
            pltpu.VMEM((2 * block, 384 if full % 384 == 0 else LANES), F32),
            pltpu.VMEM((deep, block, full), BF16),
            pltpu.VMEM((deep, block, full), BF16),
            pltpu.VMEM((deep, block, full), BF16),
            pltpu.VMEM((2, deep - 1, block, full), BF16),
            pltpu.VMEM((block, full), BF16),
            pltpu.VMEM((tp, rows, full), BF16),
            pltpu.VMEM((2, micro, part, width), BF16),
            pltpu.VMEM((2, micro, part, width), BF16),
            pltpu.VMEM((micro, part, width), BF16),
            pltpu.VMEM((micro, part, width), BF16),
            pltpu.VMEM((bits,) + small.shape, F32),
            dma((4,)),
            dma((deep,)),
            dma((deep,)),
            dma((deep,)),
            dma((2, deep - 1)),
            dma((2, deep - 1)),
            dma((3,)),
            dma((3,)),
            dma((2,)),
            dma((2,)),
            dma((1,)),
            dma((1,)),
            dma((bits + 3,)),
            dma((bits + 3,)),
        ],
        compiler_params=pltpu.CompilerParams(
            collective_id=3, has_side_effects=True, vmem_limit_bytes=62 * 2**20
        ),
        cost_estimate=pl.CostEstimate(flops=6 * 10**10, bytes_accessed=3 * 10**7, transcendentals=0),
        name="gradients_to_owners",
    )(normed_t, rows_grad, gates_grad, w_rest, w_gate, small)


def from_seats(v, size):
    v = v.reshape(4, v.shape[1], 4, size)
    v = jnp.stack([v[2 * (k % 2) + k // 2] for k in range(4)], axis=2)
    return v.reshape(v.shape[0], -1)


def body(
    tokens,
    in_proj,
    conv_weight,
    conv_bias,
    decay_log,
    step_bias,
    skip_gain,
    norm_gain,
    gated_gain,
    out_proj,
    cotangent,
):
    dp, tp = lax.axis_size("dp"), lax.axis_size("seq")
    s = lax.axis_index("seq")
    micro, part, width = tokens.shape
    heads = HEADS // tp
    inner = heads * P_SIZE
    rows = in_proj.shape[0]
    length = part * tp
    count = micro * length
    wide = inner + 2 * N
    chan = conv_bias.shape[0]

    per_head = jnp.pad(jnp.stack([decay_log, step_bias, skip_gain]), ((0, 5), (0, 0)))
    (
        normed,
        normed_t,
        proj_rest,
        ssd,
        memory,
        gate,
        w_rest,
        w_gate,
        w_out,
        cot,
        taps,
        gains,
        g_gated,
        per_head,
    ) = head(
        in_proj,
        conv_weight,
        conv_bias[None],
        norm_gain[None],
        gated_gain[None],
        per_head,
        tokens,
        cotangent,
        out_proj,
        dp,
        tp,
    )
    proj_rest = proj_rest.reshape(count, wide + LANES)
    ssd = ssd.reshape(count, inner)
    w_rest = w_rest.reshape(width, wide + LANES)
    w_gate = w_gate.reshape(width, inner)
    w_out = w_out.reshape(inner, width)
    cot = cot.reshape(count, width)
    taps, g_norm, g_gated = taps[:8], gains[KW + 1], g_gated[KW + 2]

    gate = gate.reshape(count, inner)
    sig = jax.nn.sigmoid(gate)
    act = gate * sig
    gated = ssd * act
    grad_shaped = jnp.dot(cot, w_out.T, preferred_element_type=F32)
    weighed = grad_shaped * g_gated
    stats = jnp.stack([jnp.sum(gated * gated, axis=1), jnp.sum(weighed * gated, axis=1)])
    stats = add_over_seq(stats, dp)
    q = lax.rsqrt(stats[0] / DI + EPSILON)[:, None]
    shaped = (gated * q * g_gated).astype(BF16)
    grad_gated = q * (weighed - gated * (q * q * (stats[1] / DI)[:, None]))
    grad_ssd = grad_gated * act
    grad_gate = (grad_gated * ssd * (sig + act * (1 - sig))).astype(BF16)

    out_part = jnp.dot(shaped, w_out, preferred_element_type=F32).astype(BF16)
    grad_out = jnp.dot(shaped.T, cot, preferred_element_type=F32).astype(BF16)
    gate_in = jnp.dot(normed_t, grad_gate, preferred_element_type=F32).astype(BF16)
    grad_rest, wgrad, hgrad, out_part, grad_out, gate_in = middle(
        proj_rest,
        grad_ssd,
        memory,
        taps,
        per_head,
        out_part.reshape(micro, length, width),
        grad_out.reshape(dp, -1, width),
        gate_in.reshape(dp, tp, rows, inner),
        dp,
        tp,
        heads,
        micro,
    )
    h_own = tokens.astype(F32)
    block_out = (h_own + out_part).astype(BF16)
    grad_out = grad_out.astype(F32)
    gated_gain_grad = jnp.sum(out_proj.astype(F32) * grad_out, axis=1) / gated_gain.astype(F32)

    small = jnp.concatenate([wgrad[: KW + 1].reshape(-1), hgrad[:3].reshape(-1)])
    lines = -(-small.shape[0] // (8 * LANES)) * 8
    small = jnp.pad(small, (0, lines * LANES - small.shape[0])).reshape(lines, LANES)
    rest_in, grad_normed, small = tail(
        normed_t, grad_rest, grad_gate, w_rest, w_gate, small, dp, tp, micro
    )
    rest_in = rest_in.astype(F32)
    small = small[-tp:].reshape(tp, -1)
    convs = small[:, : (KW + 1) * wide].reshape(tp, KW + 1, wide)
    convs = jnp.concatenate(
        [from_seats(convs[:, :, :inner], STRIPE), jnp.sum(convs[:, :, inner:], axis=0)], axis=1
    )
    place = lax.axis_index("dp") * tp + s
    convs = lax.dynamic_slice_in_dim(convs, place * chan, chan, 1)
    head_grads = small[:, (KW + 1) * wide : (KW + 1) * wide + 3 * LANES].reshape(tp, 3, LANES)
    head_grads = from_seats(head_grads[:, :, :heads], HEADS // 16)

    in_grad = jnp.concatenate(
        [
            from_seats(gate_in.astype(F32), STRIPE),
            from_seats(rest_in[:, :, :inner], STRIPE),
            jnp.sum(rest_in[:, :, inner:wide], axis=0),
            from_seats(rest_in[:, :, wide : wide + heads], HEADS // 16),
        ],
        axis=1,
    )
    norm_gain_grad = jnp.sum(in_proj.astype(F32) * in_grad, axis=1) / norm_gain.astype(F32)

    r_own = lax.rsqrt(jnp.mean(h_own * h_own, axis=-1, keepdims=True) + EPSILON)
    n_own = h_own * r_own
    g = grad_normed * g_norm
    tokens_grad = cotangent.astype(F32) + r_own * (
        g - n_own * jnp.mean(g * n_own, axis=-1, keepdims=True)
    )
    return (
        block_out,
        tokens_grad.astype(BF16),
        in_grad,
        convs[:KW],
        convs[KW],
        head_grads[0],
        head_grads[1],
        head_grads[2],
        norm_gain_grad,
        gated_gain_grad,
        grad_out,
    )


def solution(mesh):
    both = ("dp", "seq")
    return jax.shard_map(
        body,
        mesh=mesh,
        in_specs=(
            P("dp", "seq", None),
            P(both, None),
            P(None, both),
            P(both),
            P(),
            P(),
            P(),
            P(both),
            P(both),
            P(both, None),
            P("dp", "seq", None),
        ),
        out_specs=(
            P("dp", "seq", None),
            P("dp", "seq", None),
            P(both, None),
            P(None, both),
            P(both),
            P(),
            P(),
            P(),
            P(both),
            P(both),
            P(both, None),
        ),
        check_vma=False,
    )
```

```python
import functools

import jax
import jax.numpy as jnp
from jax import lax
from jax.experimental import pallas as pl
from jax.experimental.pallas import tpu as pltpu
from jax.sharding import PartitionSpec as P

HEADS = 48
P_SIZE = 64
N = 128
KW = 4
DI = 3072
CD = 3328
LANES = 128
FAR = -1e30

EPSILON = 1e-05
F32 = jnp.float32
BF16 = jnp.bfloat16


def dot(a, b, dims=((1,), (0,)), precision=None):
    return lax.dot_general(a, b, (dims, ((), ())), precision=precision, preferred_element_type=F32)


NT = ((1,), (1,))
HIGH = lax.Precision.HIGHEST


def pick(a, p, low):
    return jnp.where(low, a[:, 2 * p : 2 * p + 1], a[:, 2 * p + 1 : 2 * p + 2])


def chunk_parts(heads, rest_ref, xbuf, taps_ref, head_ref):
    size = rest_ref.shape[0]
    wide = taps_ref.shape[1]
    mixed = taps_ref[KW : KW + 1, :] + taps_ref[0:1, :] * xbuf[5 : 5 + size, :]
    for k in range(1, KW):
        mixed = mixed + taps_ref[k : k + 1, :] * xbuf[5 + k : 5 + k + size, :]
    sig = lax.logistic(mixed)
    lane = lax.broadcasted_iota(jnp.int32, (1, LANES), 1)
    raw = jnp.where(lane < heads, rest_ref[:, wide:], 0.0) + head_ref[1:2, :]
    step = jnp.maximum(raw, 0.0) + jnp.log1p(jnp.exp(-jnp.abs(raw)))
    decay = -jnp.exp(head_ref[0:1, :]) * step
    i = lax.broadcasted_iota(jnp.int32, (size, size), 0)
    j = lax.broadcasted_iota(jnp.int32, (size, size), 1)
    run = dot(jnp.where(i >= j, 1.0, 0.0), decay, precision=HIGH)
    return mixed, sig, raw, step, decay, run


def backward_kernel(
    heads,
    rest_ref,
    prev_ref,
    dy_ref,
    mem_ref,
    taps_ref,
    head_ref,
    out_ref,
    wgrad_ref,
    hgrad_ref,
    xbuf,
    gbuf,
    adj,
    dmix,
    dsum,
    uprod,
    zprod,
    rows_t,
    line,
):
    size = rest_ref.shape[0]
    wide = taps_ref.shape[1]
    inner = heads * P_SIZE
    chunks = pl.num_programs(1)
    step_id = pl.program_id(1)
    newest = step_id == 0
    oldest = step_id == chunks - 1
    begin = jnp.logical_and(pl.program_id(0) == 0, newest)
    finish = jnp.logical_and(pl.program_id(0) == pl.num_programs(0) - 1, oldest)

    @pl.when(begin)
    def _():
        wgrad_ref[...] = jnp.zeros_like(wgrad_ref)
        hgrad_ref[...] = jnp.zeros_like(hgrad_ref)
        rows_t[...] = jnp.zeros_like(rows_t)
        line[...] = jnp.zeros_like(line)

    @pl.when(newest)
    def _():
        gbuf[size : size + 8, :] = jnp.zeros((8, wide), F32)
        adj[...] = jnp.zeros_like(adj)

    @pl.when(jnp.logical_not(newest))
    def _():
        gbuf[size : size + 8, :] = gbuf[0:8, :]

    xbuf[0:8, :] = jnp.where(oldest, 0.0, prev_ref[:, :wide])
    xbuf[8 : 8 + size, :] = rest_ref[:, :wide]
    mixed, sig, raw, step, decay, run = chunk_parts(heads, rest_ref, xbuf, taps_ref, head_ref)
    act = mixed * sig
    run_t = run.T
    closing = run[size - 1 : size, :]
    last = jnp.exp(closing)
    left = jnp.exp(closing - run)
    grown = jnp.exp(run)
    b = act[:, inner : inner + N].astype(BF16)
    c = act[:, inner + N :].astype(BF16)
    c_t = act[:, inner + N :].T.astype(BF16)
    scores_t = dot(b, c, NT)
    low = lax.broadcasted_iota(jnp.int32, (1, LANES), 1) < P_SIZE
    lane = lax.broadcasted_iota(jnp.int32, (1, LANES), 1)
    j = lax.broadcasted_iota(jnp.int32, (size, size), 0)
    i = lax.broadcasted_iota(jnp.int32, (size, size), 1)
    causal = i >= j
    mem_b = mem_ref[0]
    adj_b = adj[...].astype(BF16)
    spread = dot(b, adj_b)
    inherit = dot(c, mem_b)
    scored = jnp.zeros((size, size), F32)
    cols = jnp.zeros((size, LANES), F32)
    for p in range(heads // 2):
        at = slice(p * LANES, (p + 1) * LANES)
        v = act[:, at]
        size_p = pick(step, p, low)
        xv = size_p * v
        dy = dy_ref[:, at]
        dyb = dy.astype(BF16)
        xvb = xv.astype(BF16)
        dxv = pick(left, p, low) * spread[:, at]
        zprod[:, at] = (dxv * xv).astype(BF16)
        dyg = pick(grown, p, low) * dy
        uprod[:, at] = (dyg * inherit[:, at]).astype(BF16)
        for e in range(2):
            h = 2 * p + e
            keep = low if e == 0 else jnp.logical_not(low)
            mine = jnp.where(keep, dy, 0.0).astype(BF16)
            gap = run_t[h : h + 1, :] - run[:, h : h + 1]
            near = jnp.exp(jnp.where(causal, gap, FAR))
            w_t = scores_t * near
            dw_t = dot(xvb, mine, NT)
            scored = scored + dw_t * near
            g_t = dw_t * w_t
            rows_t[h : h + 1, :] = jnp.sum(g_t, axis=0, keepdims=True)
            cols = jnp.where(lane == h, jnp.sum(g_t, axis=1, keepdims=True), cols)
            dxv = dxv + dot(w_t.astype(BF16), mine)
        dsum[:, at] = (dxv * v).astype(BF16)
        dmix[:, at] = size_p * dxv + pick(head_ref[2:3, :], p, low) * dy
        line[0:1, at] += jnp.sum(dy * v, axis=0, keepdims=True)
        line[1:2, at] = jnp.sum(adj[:, at] * mem_b[:, at].astype(F32), axis=0, keepdims=True) * pick(
            last, p, low
        )
        xc = (pick(left, p, low) * xv).astype(BF16)
        dygb = dyg.astype(BF16)
        db = dot(xc, adj_b[:, at], NT)
        dc = dot(dygb, mem_b[:, at], NT)
        if p == 0:
            dmix[:, inner : inner + N] = db
            dmix[:, inner + N :] = dc
        else:
            dmix[:, inner : inner + N] += db
            dmix[:, inner + N :] += dc
        adj[:, at] = adj[:, at] * pick(last, p, low) + dot(c_t, dygb)
    dmix[:, inner : inner + N] += dot(scored.astype(BF16), c)
    dmix[:, inner + N :] += dot(scored.T.astype(BF16), b)

    group = jnp.where(
        lax.broadcasted_iota(jnp.int32, (inner, LANES), 0) // P_SIZE
        == lax.broadcasted_iota(jnp.int32, (inner, LANES), 1),
        1.0,
        0.0,
    )
    group_b = group.astype(BF16)
    d_step = dot(dsum[...], group_b)
    u = dot(uprod[...], group_b)
    z = dot(zprod[...], group_b)
    sums = dot(line[...], group, precision=HIGH)
    d_run = rows_t[...].T - cols + u - z
    row = lax.broadcasted_iota(jnp.int32, (size, 1), 0)
    ending = sums[1:2, :] + jnp.sum(z, axis=0, keepdims=True)
    d_run = d_run + jnp.where(row == size - 1, ending, 0.0)
    d_decay = dot(jnp.where(causal, 1.0, 0.0), d_run, precision=HIGH)
    d_raw = (d_step - jnp.exp(head_ref[0:1, :]) * d_decay) * lax.logistic(raw)
    d_raw = jnp.where(lane < heads, d_raw, 0.0)
    hgrad_ref[0:1, :] += jnp.sum(d_decay * decay, axis=0, keepdims=True)
    hgrad_ref[1:2, :] += jnp.sum(d_raw, axis=0, keepdims=True)

    @pl.when(finish)
    def _():
        hgrad_ref[2:3, :] = sums[0:1, :]

    g = dmix[...] * (sig * (1.0 + mixed * (1.0 - sig)))
    gbuf[0:size, :] = g
    wgrad_ref[KW : KW + 1, :] += jnp.sum(g, axis=0, keepdims=True)
    for k in range(KW):
        wgrad_ref[k : k + 1, :] += jnp.sum(g * xbuf[5 + k : 5 + k + size, :], axis=0, keepdims=True)
    back = taps_ref[KW - 1 : KW, :] * g
    for k in range(KW - 1):
        back = back + taps_ref[k : k + 1, :] * gbuf[3 - k : 3 - k + size, :]
    out_ref[:, :wide] = back.astype(BF16)
    out_ref[:, wide:] = d_raw.astype(BF16)


MESH = pl.DeviceIdType.MESH


def where_am_i(dp):
    d, s = lax.axis_index("dp"), lax.axis_index("seq")
    z, y = d // 2, d % 2
    x, c = s // 2, s % 2
    peers = [s + 1 - 2 * c, s + 2 - 4 * x, 3 - s]
    return d, s, z, y, x, c, peers, dp // 2


def push(src, dst, send_sem, recv_sem, d, s):
    return pltpu.make_async_remote_copy(
        src_ref=src,
        dst_ref=dst,
        send_sem=send_sem,
        recv_sem=recv_sem,
        device_id={"dp": d, "seq": s},
        device_id_type=MESH,
    )


def greet(partners):
    barrier = pltpu.get_barrier_semaphore()
    for cond, d, s in partners:

        def hello(d=d, s=s):
            pl.semaphore_signal(barrier, inc=1, device_id={"dp": d, "seq": s}, device_id_type=MESH)

        if cond is None:
            hello()
        else:
            pl.when(cond)(hello)
    count = 0
    for cond, _, _ in partners:
        count = count + (1 if cond is None else jnp.where(cond, 1, 0))
    pl.semaphore_wait(barrier, count)


class Sends:
    def __init__(self):
        self.items = []

    def start(self, cond, copy):
        if cond is None:
            copy.start()
        else:
            pl.when(cond)(copy.start)
        self.items.append((cond, copy))

    def drain(self):
        for cond, copy in self.items:
            if cond is None:
                copy.wait_send()
            else:
                pl.when(cond)(copy.wait_send)


STRIPE = DI // 16


def swapped(s):
    return 2 * (s % 2) + s // 2


def stripe_owner(block, dp):
    u = dp // 4
    return block // (4 * u) * u + block % u


def stripe_seat(block, dp):
    return swapped(block // (dp // 4) % 4)


def stripe_block(d, s, dp):
    u = dp // 4
    return (d // u * 4 + swapped(s)) * u + d % u


def forward_chunk(heads, first, rest_ref, taps_ref, head_ref, ssd_ref, mem_ref, xbuf, mem):
    size = rest_ref.shape[0]
    wide = taps_ref.shape[1]
    inner = heads * P_SIZE

    @pl.when(first)
    def _():
        xbuf[0:8, :] = jnp.zeros((8, wide), F32)
        mem[...] = jnp.zeros_like(mem)

    @pl.when(jnp.logical_not(first))
    def _():
        xbuf[0:8, :] = xbuf[size : size + 8, :]

    xbuf[8 : 8 + size, :] = rest_ref[:, :wide]
    mixed, sig, _, step, _, run = chunk_parts(heads, rest_ref, xbuf, taps_ref, head_ref)
    act = mixed * sig
    run_t = run.T
    closing = run[size - 1 : size, :]
    last = jnp.exp(closing)
    left = jnp.exp(closing - run)
    grown = jnp.exp(run)
    b = act[:, inner : inner + N]
    c = act[:, inner + N :].astype(BF16)
    scores = dot(c, b.astype(BF16), NT)
    b_t = b.T.astype(BF16)
    mem_ref[...] = mem[...].astype(BF16)
    inter = dot(c, mem[...].astype(BF16))
    low = lax.broadcasted_iota(jnp.int32, (1, LANES), 1) < P_SIZE
    i = lax.broadcasted_iota(jnp.int32, (size, size), 0)
    j = lax.broadcasted_iota(jnp.int32, (size, size), 1)
    causal = i >= j
    for p in range(heads // 2):
        at = slice(p * LANES, (p + 1) * LANES)
        v = act[:, at]
        xv = pick(step, p, low) * v
        y = pick(head_ref[2:3, :], p, low) * v + pick(grown, p, low) * inter[:, at]
        for e in range(2):
            h = 2 * p + e
            gap = run[:, h : h + 1] - run_t[h : h + 1, :]
            w = (scores * jnp.exp(jnp.where(causal, gap, FAR))).astype(BF16)
            mine = jnp.where(low if e == 0 else jnp.logical_not(low), xv, 0.0).astype(BF16)
            y = y + dot(w, mine)
        ssd_ref[:, at] = y
        xc = (pick(left, p, low) * xv).astype(BF16)
        mem[:, at] = mem[:, at] * pick(last, p, low) + dot(b_t, xc)


def hop(v, size):
    return sum(jnp.where(v >= q * size, 1, 0) for q in range(1, 4))


def head_kernel(
    dp,
    heads,
    proj_ref,
    cw_ref,
    cb_ref,
    ng_ref,
    gg_ref,
    ph_ref,
    tok_ref,
    cot_ref,
    block_ref,
    normed_hbm,
    turned_hbm,
    proj_hbm,
    ssd_hbm,
    mem_hbm,
    gates_hbm,
    rest_hbm,
    gate_hbm,
    out_hbm,
    cot_hbm,
    taps_ref,
    gain_ref,
    gated_ref,
    head_ref,
    line,
    small_stage,
    val_stage,
    half_stage,
    gate_stage,
    small_all,
    val_in,
    half_in,
    gate_in,
    w_val,
    w_half,
    w_other,
    w_tail,
    w_gate,
    out_shard,
    tok,
    flipped,
    proj,
    ssd,
    gates,
    memory,
    xbuf,
    mem,
    l_sem,
    o_sem,
    f_sem,
    p_sem,
    g_sem,
    a_send,
    a_recv,
    z_send,
    z_recv,
    y_send,
    y_recv,
    t_send,
    t_recv,
):
    d, s, z, y, x, c, peers, deep = where_am_i(dp)
    tp, rows = val_stage.shape[:2]
    micro, part, width = tok_ref.shape
    total = dp * tp
    inner = heads * P_SIZE
    wide = inner + 2 * N
    chan, gpiece = cw_ref.shape[1], gg_ref.shape[1]
    up, down, far = d + 2, d - 2, d + 1 - 2 * y
    me = d * tp + s
    to_d, to_s, turned = stripe_owner(me, dp), stripe_seat(me, dp), stripe_block(d, s, dp)
    from_d, from_s = turned // tp, turned % tp
    moves = turned != me

    triple = HEADS // 16
    line[...] = jnp.zeros_like(line)
    line[0:KW, 0:chan] = cw_ref[...].astype(F32)
    line[KW : KW + 1, 0:chan] = cb_ref[...].astype(F32)
    line[KW + 1 : KW + 2, 0:rows] = ng_ref[...].astype(F32)
    line[KW + 2 : KW + 3, 0:gpiece] = gg_ref[...].astype(F32)
    raw = proj_ref[:, 2 * DI + 2 * N :]
    for b in range(4):
        seat = 2 * (b % 2) + b // 2
        for k in range(4):
            to, at = k * STRIPE, (4 * k + b) * STRIPE
            gate_stage[seat, :, to : to + STRIPE] = proj_ref[:, at : at + STRIPE]
            val_stage[seat, :, to : to + STRIPE] = proj_ref[:, DI + at : DI + at + STRIPE]
        at = 2 * DI + N * (seat % 2)
        half_stage[seat] = proj_ref[:, at : at + N]
        v = lax.broadcasted_iota(jnp.int32, (16, HEADS), 0)
        g = lax.broadcasted_iota(jnp.int32, (16, HEADS), 1)
        hit = jnp.logical_and(v < heads, g == v + 3 * triple * hop(v, triple) + triple * b)
        line[16:32, 0:rows] = dot(jnp.where(hit, 1.0, 0.0).astype(BF16), raw, NT)
        small_stage[seat] = line[...].astype(BF16)
    v = lax.broadcasted_iota(jnp.int32, (HEADS, LANES), 1)
    g = lax.broadcasted_iota(jnp.int32, (HEADS, LANES), 0)
    hit = jnp.logical_and(v < heads, g == v + 3 * triple * hop(v, triple) + triple * swapped(s))
    head_ref[...] = dot(ph_ref[...], jnp.where(hit, 1.0, 0.0), precision=HIGH)

    greet(
        [(None, d, p) for p in peers]
        + [(None, far, s), (z < deep - 1, up, s), (z > 0, down, s)]
        + [(moves, to_d, to_s), (moves, from_d, from_s)]
    )
    sends = Sends()

    def arrive(dst, sem):
        push(dst, dst, sem, sem, d, peers[0]).wait_recv()

    def mine(ref, k):
        return ref.at[:, pl.ds(k * part, part), :]

    def exchange(a, stage, target):
        for r, p in enumerate(peers):
            sends.start(
                None, push(stage.at[p], target(s), a_send.at[a, r], a_recv.at[a, r], d, p)
            )

    def exchanged(a, target):
        for r, p in enumerate(peers):
            arrive(target(p), a_recv.at[a, r])

    exchange(0, small_stage, lambda k: small_all.at[d, k])
    exchange(1, half_stage, lambda k: half_in.at[k])
    exchange(2, val_stage, lambda k: val_in.at[k])
    exchange(3, gate_stage, lambda k: gate_in.at[k])
    sends.start(moves, push(block_ref, out_shard, t_send.at[2], t_recv.at[2], to_d, to_s))
    sends.start(None, push(tok_ref, mine(tok, s), t_send.at[0], t_recv.at[0], d, peers[1]))
    sends.start(None, push(tok_ref, mine(tok, s), t_send.at[1], t_recv.at[1], d, peers[0]))
    sends.start(None, push(cot_ref, mine(cot_hbm, s), t_send.at[3], t_recv.at[3], d, peers[1]))
    sends.start(None, push(cot_ref, mine(cot_hbm, s), t_send.at[4], t_recv.at[4], d, peers[0]))
    saves = []

    def save(src, dst):
        copy = pltpu.make_async_copy(src, dst, l_sem.at[len(saves)])
        copy.start()
        saves.append(copy)

    save(cot_ref, mine(cot_hbm, s))
    small_all[d, s] = small_stage[s]
    half_in[s] = half_stage[s]
    val_in[s] = val_stage[s]
    gate_in[s] = gate_stage[s]
    tok[:, pl.ds(pl.multiple_of(s * part, part), part), :] = tok_ref[...]

    @pl.when(jnp.logical_not(moves))
    def _():
        out_shard[...] = block_ref[...]

    def begin(a, shard, dst):
        block = dst.at[d]
        sends.start(z < deep - 1, push(shard, block, z_send.at[a, 0, 0], z_recv.at[a, 0, 0], up, s))
        sends.start(z > 0, push(shard, block, z_send.at[a, 1, 0], z_recv.at[a, 1, 0], down, s))
        sends.start(None, push(shard, block, y_send.at[a, 0, 0], y_recv.at[a, 0, 0], far, s))

    def plan(a, dst, t):
        steps = []
        for way in range(2):
            here = (z >= t) if way == 0 else (z + t <= deep - 1)
            more = jnp.logical_and(here, (z < deep - 1) if way == 0 else (z > 0))
            at = jnp.clip(d - 2 * t if way == 0 else d + 2 * t, 0, dp - 1)
            block = dst.at[at]
            got = z_recv.at[a, way, t - 1]
            on = []
            if t < deep - 1:
                nxt = up if way == 0 else down
                on.append(
                    (more, push(block, block, z_send.at[a, way, t], z_recv.at[a, way, t], nxt, s))
                )
            on.append(
                (here, push(block, block, y_send.at[a, way, t], y_recv.at[a, way, t], far, s))
            )
            steps.append((here, push(block, block, got, got, d, peers[0]), on))
        return steps

    def run(steps):
        for here, wait, on in steps:
            pl.when(here)(wait.wait_recv)
            for cond, copy in on:
                pl.when(cond)(copy.start)

    def remember(steps):
        for _, _, on in steps:
            sends.items.extend(on)

    def relay(a, dst, t):
        steps = plan(a, dst, t)
        run(steps)
        remember(steps)

    def landed(a, dst):
        arrive(dst.at[far], y_recv.at[a, 0, 0])
        for t in range(1, deep):
            for way in range(2):
                here = (z >= t) if way == 0 else (z + t <= deep - 1)
                at = jnp.clip(far - 2 * t if way == 0 else far + 2 * t, 0, dp - 1)
                pl.when(here)(functools.partial(arrive, dst.at[at], y_recv.at[a, way, t]))

    def shard_of(a, pieces, dst):
        exchanged(a, lambda p: pieces.at[p])
        for k in range(tp):
            dst[d, k * rows : (k + 1) * rows, :] = pieces[k]
        begin(a, dst.at[d], dst)

    exchanged(0, lambda p: small_all.at[d, p])
    begin(0, small_all.at[d], small_all)
    shard_of(1, half_in, w_half)
    shard_of(2, val_in, w_val)
    for t in range(1, deep):
        relay(0, small_all, t)
        relay(1, w_half, t)
        relay(2, w_val, t)
    shard_of(3, gate_in, w_gate)
    pl.when(moves)(functools.partial(arrive, out_shard, t_recv.at[2]))
    begin(4, out_shard, out_hbm)
    save(out_shard, out_hbm.at[d])

    landed(0, small_all)

    def one_hot(columns, index, k, length):
        lane = lax.broadcasted_iota(jnp.int32, (LANES, columns), 1)
        at = lax.broadcasted_iota(jnp.int32, (LANES, columns), 0)
        hit = jnp.logical_and(at < length, index(lane) == k * length + at)
        return jnp.where(hit, 1.0, 0.0).astype(BF16)

    taps_ref[...] = jnp.zeros_like(taps_ref)
    gain_ref[...] = jnp.zeros_like(gain_ref)
    gated_ref[...] = jnp.zeros_like(gated_ref)

    def striped(v):
        return v + 3 * STRIPE * hop(v, STRIPE) + STRIPE * swapped(s)

    def lay_out(dd, carry):
        for kk in range(tp):
            k = dd * tp + kk
            values = small_all[dd, kk, 0:16, :]
            chans = one_hot(wide, lambda v: jnp.where(v < inner, striped(v), v - inner + DI), k, chan)
            taps_ref[...] += dot(values, chans)[:8]
            gain_ref[...] += dot(values, one_hot(width, lambda v: v, k, rows))
            gated_ref[...] += dot(values, one_hot(inner, striped, k, gpiece))
            turned = jnp.concatenate(
                [small_all[dd, kk, 16:32, :].astype(F32), jnp.zeros((LANES - 16, LANES), F32)], axis=0
            ).T
            w_tail[dd, kk * rows : (kk + 1) * rows, 2 * N :] = turned[:rows].astype(BF16)
        return carry

    lax.fori_loop(0, dp, lay_out, 0)
    landed(1, w_half)
    sends.start(None, push(w_half, w_other, t_send.at[6], t_recv.at[6], d, peers[0]))
    landed(2, w_val)
    save(w_val, rest_hbm.at[:, :, pl.ds(0, inner)])
    arrive(w_other, t_recv.at[6])

    def both_halves(dd, carry):
        w_tail[dd, :, pl.ds(pl.multiple_of(c * N, N), N)] = w_half[dd]
        w_tail[dd, :, pl.ds(pl.multiple_of((1 - c) * N, N), N)] = w_other[dd]
        return carry

    lax.fori_loop(0, dp, both_halves, 0)
    save(w_tail, rest_hbm.at[:, :, pl.ds(inner, w_tail.shape[2])])
    arrive(mine(tok, peers[1]), t_recv.at[0])
    block = mine(tok, peers[1])
    hand = push(block, block, t_send.at[5], t_recv.at[5], d, peers[0])
    hand.start()
    relay(3, w_gate, 1)
    relay(4, out_hbm, 1)
    arrive(mine(tok, peers[0]), t_recv.at[1])
    arrive(mine(tok, peers[2]), t_recv.at[5])
    hand.wait_send()

    tasks = [(a, ref, t) for t in range(2, deep) for a, ref in ((3, w_gate), (4, out_hbm))]
    chunks = micro * tp
    when = {}
    for n, task in enumerate(tasks):
        when.setdefault(min(n * 4 // len(tasks), chunks - 1), []).append(plan(*task))
    for plans in when.values():
        for steps in plans:
            remember(steps)

    def columns(i):
        return pl.ds(pl.multiple_of(i * part, part), part)

    def chunk(i, carry):
        m, k = i // tp, i % tp
        lines = pl.ds(pl.multiple_of(k * part, part), part)
        h = tok[m, lines, :].astype(F32)
        r = lax.rsqrt(jnp.mean(h * h, axis=-1, keepdims=True) + EPSILON)
        value = h * r * gain_ref[5:6, :]
        tok[m, lines, :] = value.astype(BF16)
        flipped[i] = value.T.astype(BF16)
        proj[i, :, 0:inner] = dot(tok[m, lines, :], w_val[...].reshape(width, inner))
        proj[i, :, inner:] = dot(tok[m, lines, :], w_tail[...].reshape(width, w_tail.shape[2]))
        forward_chunk(
            heads, k == 0, proj.at[i], taps_ref, head_ref, ssd.at[i], memory.at[i], xbuf, mem
        )
        pltpu.make_async_copy(tok.at[m, lines, :], normed_hbm.at[m, lines, :], o_sem.at[i]).start()
        pltpu.make_async_copy(flipped.at[i], turned_hbm.at[:, columns(i)], f_sem.at[i]).start()
        pltpu.make_async_copy(proj.at[i], proj_hbm.at[i], p_sem.at[i]).start()
        for n, plans in when.items():

            @pl.when(i == n)
            def _():
                for steps in plans:
                    run(steps)

        return carry

    lax.fori_loop(0, chunks, chunk, 0)
    save(ssd, ssd_hbm)
    save(memory, mem_hbm)
    arrive(mine(cot_hbm, peers[1]), t_recv.at[3])
    block = mine(cot_hbm, peers[1])
    sends.start(None, push(block, block, t_send.at[7], t_recv.at[7], d, peers[0]))
    landed(3, w_gate)
    save(w_gate, gate_hbm)

    def gating(i, carry):
        m, k = i // tp, i % tp
        lines = pl.ds(pl.multiple_of(k * part, part), part)
        gates[i] = dot(tok[m, lines, :], w_gate[...].reshape(width, inner))
        pltpu.make_async_copy(gates.at[i], gates_hbm.at[i], g_sem.at[i]).start()
        return carry

    lax.fori_loop(0, chunks, gating, 0)
    landed(4, out_hbm)
    arrive(mine(cot_hbm, peers[0]), t_recv.at[4])
    arrive(mine(cot_hbm, peers[2]), t_recv.at[7])

    def saved(i, carry):
        m, k = i // tp, i % tp
        lines = pl.ds(pl.multiple_of(k * part, part), part)
        pltpu.make_async_copy(tok.at[m, lines, :], normed_hbm.at[m, lines, :], o_sem.at[i]).wait()
        pltpu.make_async_copy(flipped.at[i], turned_hbm.at[:, columns(i)], f_sem.at[i]).wait()
        pltpu.make_async_copy(proj.at[i], proj_hbm.at[i], p_sem.at[i]).wait()
        pltpu.make_async_copy(gates.at[i], gates_hbm.at[i], g_sem.at[i]).wait()
        return carry

    lax.fori_loop(0, chunks, saved, 0)
    for copy in saves:
        copy.wait()
    sends.drain()


def head(in_proj, conv_weight, conv_bias, norm_gain, gated_gain, per_head, tokens, cotangent, out_proj, dp, tp):
    rows = in_proj.shape[0]
    heads = HEADS // tp
    inner = heads * P_SIZE
    full = inner + 2 * N + LANES
    micro, part, width = tokens.shape
    deep = dp // 2
    chunks = micro * tp
    block = tp * rows
    dma = pltpu.SemaphoreType.DMA
    vmem = pl.BlockSpec(memory_space=pltpu.VMEM)
    hbm = pl.BlockSpec(memory_space=pl.ANY)
    wide = inner + 2 * N

    def shape(*dims, kind=BF16):
        return jax.ShapeDtypeStruct(dims, kind)

    def room(*dims, kind=BF16):
        return pltpu.VMEM(dims, kind)

    return pl.pallas_call(
        functools.partial(head_kernel, dp, heads),
        in_specs=[vmem] * 9,
        out_specs=[hbm] * 10 + [vmem] * 4,
        out_shape=[
            shape(micro, tp * part, width),
            shape(width, chunks * part),
            shape(chunks, part, full, kind=F32),
            shape(chunks, part, inner, kind=F32),
            shape(chunks, N, inner),
            shape(chunks, part, inner, kind=F32),
            shape(dp, block, full),
            shape(dp, block, inner),
            shape(dp, out_proj.shape[0], width),
            shape(micro, tp * part, width),
            shape(8, wide, kind=F32),
            shape(16, width, kind=F32),
            shape(16, inner, kind=F32),
            shape(8, LANES, kind=F32),
        ],
        scratch_shapes=[
            room(32, LANES, kind=F32),
            room(tp, 32, LANES),
            room(tp, rows, inner),
            room(tp, rows, N),
            room(tp, rows, inner),
            room(dp, tp, 32, LANES),
            room(tp, rows, inner),
            room(tp, rows, N),
            room(tp, rows, inner),
            room(dp, block, inner),
            room(dp, block, N),
            room(dp, block, N),
            room(dp, block, 2 * N + LANES),
            room(dp, block, inner),
            room(*out_proj.shape),
            room(micro, tp * part, width),
            room(chunks, width, part),
            room(chunks, part, full, kind=F32),
            room(chunks, part, inner, kind=F32),
            room(chunks, part, inner, kind=F32),
            room(chunks, N, inner),
            room(part + 8, wide, kind=F32),
            room(N, inner, kind=F32),
            dma((8,)),
            dma((chunks,)),
            dma((chunks,)),
            dma((chunks,)),
            dma((chunks,)),
            dma((4, 3)),
            dma((4, 3)),
            dma((5, 2, deep - 1)),
            dma((5, 2, deep - 1)),
            dma((5, 2, deep)),
            dma((5, 2, deep)),
            dma((8,)),
            dma((8,)),
        ],
        compiler_params=pltpu.CompilerParams(
            collective_id=1, has_side_effects=True, vmem_limit_bytes=62 * 2**20
        ),
        cost_estimate=pl.CostEstimate(flops=10**11, bytes_accessed=5 * 10**7, transcendentals=0),
        name="gather_and_mix",
    )(in_proj, conv_weight, conv_bias, norm_gain, gated_gain, per_head, tokens, cotangent, out_proj)


class OwnerSum:
    def __init__(self, where, sends, source, mine, ybuf, zbuf, final, sems, theirs_ref=None):
        self.where, self.sends = where, sends
        self.mine, self.ybuf, self.zbuf, self.final = mine, ybuf, zbuf, final
        d, s, z, y, _, _, _, deep = where
        self.load_sem, y_send, self.y_recv, z_send, self.z_recv = sems
        lower = z < deep // 2

        def place(j):
            low = jnp.where(j > z, deep - 1 - j, deep - 1 - z + j)
            high = jnp.where(j < z, j, z + deep - 1 - j)
            return jnp.where(j == z, deep - 1, jnp.where(lower, low, high))

        def turn(k):
            low = jnp.where(k < deep - 1 - z, deep - 1 - k, k - (deep - 1 - z))
            high = jnp.where(k < z, k, deep - 1 - (k - z))
            return jnp.where(lower, low, high) if k < deep - 1 else z

        self.order = [turn(k) for k in range(deep)]
        self.y_items, self.loads = [], []
        for k, j in enumerate(self.order):
            theirs = source.at[j * 2 + 1 - y] if theirs_ref is None else theirs_ref.at[k]
            copy = push(theirs, ybuf.at[k], y_send.at[k], self.y_recv.at[k], d + 1 - 2 * y, s)
            self.y_items.append((None, copy))
            if theirs_ref is None:
                own = source.at[j * 2 + y]
                self.loads.append(pltpu.make_async_copy(own, mine.at[k], self.load_sem.at[k]))
        self.z_items = []
        for t in range(deep - 1):
            ways = []
            for way in range(2):
                depth = z if way == 0 else deep - 1 - z
                j = deep - 1 - t + z if way == 0 else t + z - deep + 1
                k = place(jnp.clip(j, 0, deep - 1))
                nxt = d + 2 if way == 0 else d - 2
                dst, ss, rs = zbuf.at[way, t], z_send.at[way, t], self.z_recv.at[way, t]
                first = (depth == 0, push(ybuf.at[k], dst, ss, rs, nxt, s))
                later = None
                if t > 0:
                    cond = jnp.logical_and(depth > 0, depth <= t)
                    later = (cond, push(zbuf.at[way, t - 1], dst, ss, rs, nxt, s))
                ways.append((k, first, later))
            self.z_items.append(ways)
        sends.items.extend(self.y_items)
        for ways in self.z_items:
            for _, first, later in ways:
                sends.items.append(first)
                if later is not None:
                    sends.items.append(later)

    def arrive(self, ref, sem):
        d, s = self.where[:2]
        push(ref, ref, sem, sem, d, self.where[6][0]).wait_recv()

    def begin(self):
        for _, copy in self.y_items:
            copy.start()
        for copy in self.loads:
            copy.start()

    def each(self, work):
        if self.mine.ndim == 4:
            count, cut = self.mine.shape[1], lambda i: i
        else:
            count, cut = self.mine.shape[1] // 16, lambda i: pl.ds(pl.multiple_of(i * 16, 16), 16)
        lax.fori_loop(0, count, lambda i, carry: (work(cut(i)), carry)[1], 0)

    def add(self, k):
        if self.loads:
            self.loads[k].wait()
        self.arrive(self.ybuf.at[k], self.y_recv.at[k])
        ybuf, mine = self.ybuf, self.mine

        def work(i):
            ybuf[k, i] = (ybuf[k, i].astype(F32) + mine[k, i].astype(F32)).astype(BF16)

        self.each(work)

    def send(self, t):
        zbuf, ybuf = self.zbuf, self.ybuf
        for way, (k, first, later) in enumerate(self.z_items[t]):
            pl.when(first[0])(first[1].start)
            if later is None:
                continue

            @pl.when(later[0])
            def _():
                self.arrive(zbuf.at[way, t - 1], self.z_recv.at[way, t - 1])

                def work(i):
                    zbuf[way, t - 1, i] = (
                        zbuf[way, t - 1, i].astype(F32) + ybuf[k, i].astype(F32)
                    ).astype(BF16)

                self.each(work)
                later[1].start()

    def finish(self):
        z, deep = self.where[2], self.where[7]
        zbuf, ybuf, final = self.zbuf, self.ybuf, self.final
        for way in range(2):
            depth = z if way == 0 else deep - 1 - z
            pl.when(depth > 0)(
                functools.partial(self.arrive, zbuf.at[way, deep - 2], self.z_recv.at[way, deep - 2])
            )

        def work(ways, i):
            total = ybuf[deep - 1, i].astype(F32)
            for way in ways:
                total = total + zbuf[way, deep - 2, i].astype(F32)
            final[i] = total.astype(BF16)

        for cond, ways in (
            (z == 0, (1,)),
            (z == deep - 1, (0,)),
            (jnp.logical_and(z > 0, z < deep - 1), (0, 1)),
        ):
            pl.when(cond)(functools.partial(self.each, functools.partial(work, ways)))


def middle_kernel(
    dp,
    heads,
    rest_ref,
    prev_ref,
    dy_ref,
    mem_ref,
    taps_ref,
    head_ref,
    part_hbm,
    gout_hbm,
    ggate_hbm,
    tok_hbm,
    out_ref,
    wgrad_ref,
    hgrad_ref,
    own_hbm,
    gout_out,
    ggate_out,
    xbuf,
    gbuf,
    adj,
    dmix,
    dsum,
    uprod,
    zprod,
    rows_t,
    line,
    o_mine,
    o_y,
    o_z,
    o_final,
    g_mine,
    g_y,
    g_z,
    g_final,
    own,
    core_buf,
    x_buf,
    tok,
    result,
    o_load,
    o_ysend,
    o_yrecv,
    o_zsend,
    o_zrecv,
    g_load,
    g_ysend,
    g_yrecv,
    g_zsend,
    g_zrecv,
    b_load,
    c_send,
    c_recv,
    m_send,
    m_recv,
    a_send,
    a_recv,
):
    where = where_am_i(dp)
    d, s, z, y, x, c, peers, deep = where
    micro, part, width = result.shape
    step = pl.program_id(0) * pl.num_programs(1) + pl.program_id(1)
    tp = ggate_hbm.shape[1]
    me = d * tp + s
    turned = stripe_block(d, s, dp)
    moves = turned != me
    to_d, to_s = turned // tp, turned % tp
    from_d, from_s = stripe_owner(me, dp), stripe_seat(me, dp)
    sends = Sends()
    gout = OwnerSum(
        where, sends, gout_hbm, o_mine, o_y, o_z, o_final, (o_load, o_ysend, o_yrecv, o_zsend, o_zrecv)
    )
    ggate = OwnerSum(
        where, sends, ggate_hbm, g_mine, g_y, g_z, g_final, (g_load, g_ysend, g_yrecv, g_zsend, g_zrecv)
    )

    def chunk(k):
        return part_hbm.at[:, pl.ds(k * part, part), :]

    cores, loads = [], []
    for q, xx in enumerate((1 - x, x)):
        cores.append(
            push(chunk(xx * 2 + 1 - c), core_buf.at[q], c_send.at[q], c_recv.at[q], d, peers[0])
        )
        loads.append(pltpu.make_async_copy(chunk(xx * 2 + c), own.at[q], b_load.at[q]))
    across = push(core_buf.at[0], x_buf, m_send.at[0], m_recv.at[0], d, peers[1])
    turning = push(o_final, gout_out, m_send.at[1], m_recv.at[1], to_d, to_s)
    staying = pltpu.make_async_copy(o_final, gout_out, b_load.at[2])
    swaps = [
        push(g_final.at[p], ggate_out.at[s], a_send.at[r], a_recv.at[r], d, p)
        for r, p in enumerate(peers)
    ]
    kept = pltpu.make_async_copy(g_final.at[s], ggate_out.at[s], b_load.at[3])
    saved = pltpu.make_async_copy(result, own_hbm, b_load.at[4])
    loads.append(pltpu.make_async_copy(tok_hbm, tok, b_load.at[5]))
    for copy in cores + [across] + swaps:
        sends.items.append((None, copy))
    sends.items.append((moves, turning))
    span = 16

    def by_rows(work):
        def one(i, carry):
            m, row = i // (part // span), (i % (part // span)) * span
            work(m, pl.ds(pl.multiple_of(row, span), span))
            return carry

        lax.fori_loop(0, micro * (part // span), one, 0)

    def start():
        greet(
            [(None, d, p) for p in peers]
            + [(None, d + 1 - 2 * y, s), (z < deep - 1, d + 2, s), (z > 0, d - 2, s)]
            + [(moves, to_d, to_s), (moves, from_d, from_s)]
        )
        for copy in cores + loads:
            copy.start()
        gout.begin()
        ggate.begin()

    def pass_on():
        loads[0].wait()
        cores[0].wait_recv()

        def work(m, rows):
            core_buf[0, m, rows, :] = (
                core_buf[0, m, rows, :].astype(F32) + own[0, m, rows, :].astype(F32)
            ).astype(BF16)

        by_rows(work)
        across.start()

    def collect():
        loads[1].wait()
        loads[2].wait()
        cores[1].wait_recv()
        across.wait_recv()

        def work(m, rows):
            result[m, rows, :] = (
                core_buf[1, m, rows, :].astype(F32)
                + own[1, m, rows, :].astype(F32)
                + x_buf[m, rows, :].astype(F32)
                + tok[m, rows, :].astype(F32)
            ).astype(BF16)

        by_rows(work)
        saved.start()

    def hand_over():
        gout.finish()
        pl.when(moves)(turning.start)
        pl.when(jnp.logical_not(moves))(staying.start)

    def last():
        ggate.finish()
        for copy in swaps:
            copy.start()
        kept.start()
        pl.when(moves)(turning.wait_recv)
        pl.when(jnp.logical_not(moves))(staying.wait)
        for r, p in enumerate(peers):
            push(ggate_out.at[p], ggate_out.at[p], a_send.at[r], a_recv.at[r], d, p).wait_recv()
        kept.wait()
        saved.wait()
        sends.drain()

    stages = {}

    def at(n, task, *args):
        stages.setdefault(n, []).append(functools.partial(task, *args))

    at(0, start)
    at(1, pass_on)
    for k in range(deep):
        n = 1 + k * 3 // (deep - 1)
        at(n, gout.add, k)
        if k < deep - 1:
            at(n, gout.send, k)
    at(4, hand_over)
    at(5, ggate.add, 0)
    for k in range(deep - 1):
        n = 5 + k * 2 // (deep - 2)
        at(n, ggate.send, k)
        at(n, ggate.add, k + 1)
    at(6, collect)
    for n, tasks in stages.items():

        @pl.when(step == n)
        def _():
            for task in tasks:
                task()

    backward_kernel(
        heads,
        rest_ref,
        prev_ref,
        dy_ref,
        mem_ref,
        taps_ref,
        head_ref,
        out_ref,
        wgrad_ref,
        hgrad_ref,
        xbuf,
        gbuf,
        adj,
        dmix,
        dsum,
        uprod,
        zprod,
        rows_t,
        line,
    )
    pl.when(step == pl.num_programs(0) * pl.num_programs(1) - 1)(last)


def middle(rest, dy, memory, taps, head, partial, gout, ggate, tokens, dp, tp, heads, micro):
    count, full = rest.shape
    wide = taps.shape[1]
    inner = heads * P_SIZE
    _, length, width = partial.shape
    part = length // tp
    chunks = length // part
    deep = dp // 2
    dma = pltpu.SemaphoreType.DMA
    hbm = pl.BlockSpec(memory_space=pl.ANY)
    gout = gout.reshape(dp, 2, -1, width)

    def at(m, c):
        return m * chunks + chunks - 1 - c

    def sums(block):
        kinds = [(deep,), (deep,), (2, deep - 1), ()]
        return [pltpu.VMEM(kind + block, BF16) for kind in kinds]

    sems = [dma((deep,))] * 3 + [dma((2, deep - 1))] * 2
    out = pl.pallas_call(
        functools.partial(middle_kernel, dp, heads),
        grid=(micro, chunks),
        in_specs=[
            pl.BlockSpec((part, full), lambda m, c: (at(m, c), 0)),
            pl.BlockSpec((8, full), lambda m, c: (jnp.maximum(at(m, c) * (part // 8) - 1, 0), 0)),
            pl.BlockSpec((part, inner), lambda m, c: (at(m, c), 0)),
            pl.BlockSpec((1, N, inner), lambda m, c: (at(m, c), 0, 0)),
            pl.BlockSpec((8, wide), lambda m, c: (0, 0)),
            pl.BlockSpec((8, LANES), lambda m, c: (0, 0)),
            hbm,
            hbm,
            hbm,
            hbm,
        ],
        out_specs=[
            pl.BlockSpec((part, full), lambda m, c: (at(m, c), 0)),
            pl.BlockSpec((8, wide), lambda m, c: (0, 0)),
            pl.BlockSpec((8, LANES), lambda m, c: (0, 0)),
            hbm,
            hbm,
            hbm,
        ],
        out_shape=[
            jax.ShapeDtypeStruct((count, full), BF16),
            jax.ShapeDtypeStruct((8, wide), F32),
            jax.ShapeDtypeStruct((8, LANES), F32),
            jax.ShapeDtypeStruct((micro, part, width), BF16),
            jax.ShapeDtypeStruct(gout.shape[1:], BF16),
            jax.ShapeDtypeStruct(ggate.shape[1:], BF16),
        ],
        scratch_shapes=[
            pltpu.VMEM((part + 8, wide), F32),
            pltpu.VMEM((part + 8, wide), F32),
            pltpu.VMEM((N, inner), F32),
            pltpu.VMEM((part, wide), F32),
            pltpu.VMEM((part, inner), BF16),
            pltpu.VMEM((part, inner), BF16),
            pltpu.VMEM((part, inner), BF16),
            pltpu.VMEM((LANES, part), F32),
            pltpu.VMEM((8, inner), F32),
        ]
        + sums(gout.shape[1:])
        + sums(ggate.shape[1:])
        + [
            pltpu.VMEM((2, micro, part, width), BF16),
            pltpu.VMEM((2, micro, part, width), BF16),
            pltpu.VMEM((micro, part, width), BF16),
            pltpu.VMEM((micro, part, width), BF16),
            pltpu.VMEM((micro, part, width), BF16),
        ]
        + sems
        + sems
        + [dma((6,)), dma((2,)), dma((2,)), dma((2,)), dma((2,)), dma((3,)), dma((3,))],
        compiler_params=pltpu.CompilerParams(
            dimension_semantics=("arbitrary", "arbitrary"),
            collective_id=4,
            has_side_effects=True,
            vmem_limit_bytes=62 * 2**20,
        ),
        cost_estimate=pl.CostEstimate(flops=7 * 10**10, bytes_accessed=4 * 10**7, transcendentals=0),
        name="mixer_backward_and_sums",
    )(rest, rest, dy, memory, taps, head, partial, gout, ggate, tokens)
    rest_grad, wgrad, hgrad, own, gout, ggate = out
    return rest_grad, wgrad, hgrad, own, gout.reshape(-1, width), ggate


def gating_kernel(
    dp,
    ssd_hbm,
    gate_hbm,
    cot_hbm,
    out_hbm,
    turned_hbm,
    gain_ref,
    grad_ssd_hbm,
    grad_gate_hbm,
    part_hbm,
    gout_hbm,
    ggate_hbm,
    ssd,
    gate,
    cot,
    w_out,
    turned,
    weighed,
    shaped_t,
    grad_gate,
    partial,
    gout,
    ggate,
    stats,
    held,
    l_sem,
    c_sem,
    s_sem,
    g_sem,
    p_sem,
    o_sem,
    send,
    recv,
):
    d, s, *_, peers, _ = where_am_i(dp)
    chunks, part, inner = ssd.shape
    width = cot.shape[2]
    count = chunks * part

    def loads(i):
        return [
            pltpu.make_async_copy(cot_hbm.at[i], cot.at[i], c_sem.at[0, i]),
            pltpu.make_async_copy(ssd_hbm.at[i], ssd.at[i], c_sem.at[1, i]),
            pltpu.make_async_copy(gate_hbm.at[i], gate.at[i], c_sem.at[2, i]),
        ]

    first = pltpu.make_async_copy(out_hbm, w_out, l_sem.at[0])
    other = pltpu.make_async_copy(turned_hbm, turned, l_sem.at[1])
    first.start()
    for i in range(chunks):
        for copy in loads(i):
            copy.start()
    other.start()
    greet([(None, d, p) for p in peers])
    first.wait()

    def gated_parts(i):
        g = gate[i]
        sig = lax.logistic(g)
        act = g * sig
        return sig, act, ssd[i] * act

    def measure(i, carry):
        for copy in loads(i):
            copy.wait()
        w = dot(cot[i], w_out[...], NT) * gain_ref[KW + 2 : KW + 3, :]
        weighed[i] = w
        _, _, gated = gated_parts(i)
        lane = lax.broadcasted_iota(jnp.int32, (part, LANES), 1)
        both = jnp.where(lane == 0, jnp.sum(gated * gated, axis=1, keepdims=True), 0.0)
        both = jnp.where(lane == 1, jnp.sum(w * gated, axis=1, keepdims=True), both)
        stats[i] = both.T[:8, :]
        return carry

    lax.fori_loop(0, chunks, measure, 0)
    copies = [push(stats, held.at[r], send.at[r], recv.at[r], d, p) for r, p in enumerate(peers)]
    for copy in copies:
        copy.start()
    for copy in copies:
        copy.wait()

    def out_copies(i):
        return [
            pltpu.make_async_copy(weighed.at[i], grad_ssd_hbm.at[i], s_sem.at[i]),
            pltpu.make_async_copy(grad_gate.at[i], grad_gate_hbm.at[i], g_sem.at[i]),
            pltpu.make_async_copy(partial.at[i], part_hbm.at[i], p_sem.at[i]),
        ]

    def columns(i):
        return pl.ds(pl.multiple_of(i * part, part), part)

    def shape_chunk(i, carry):
        sums = (stats[i] + held[0, i]) + (held[1, i] + held[2, i])
        sums = jnp.concatenate([sums, jnp.zeros((LANES - 8, part), F32)], axis=0).T
        q = lax.rsqrt(sums[:, 0:1] / DI + EPSILON)
        pull = q * q * (sums[:, 1:2] / DI)
        sig, act, gated = gated_parts(i)
        value = gated * q * gain_ref[KW + 2 : KW + 3, :]
        shaped_t[:, columns(i)] = value.T.astype(BF16)
        partial[i] = dot(value.astype(BF16), w_out[...]).astype(BF16)
        grad = q * (weighed[i] - gated * pull)
        grad_gate[i] = (grad * ssd[i] * (sig + act * (1.0 - sig))).astype(BF16)
        weighed[i] = grad * act
        for copy in out_copies(i):
            copy.start()
        return carry

    lax.fori_loop(0, chunks, shape_chunk, 0)
    other.wait()
    high, across = min(384, inner), min(512, width)

    def out_tile(i, carry):
        a = pl.ds(pl.multiple_of(i // (width // across) * high, high), high)
        b = pl.ds(pl.multiple_of(i % (width // across) * across, across), across)
        gout[a, b] = dot(shaped_t[a, :], cot[:, :, b].reshape(count, across)).astype(BF16)
        return carry

    lax.fori_loop(0, (inner // high) * (width // across), out_tile, 0)
    save_out = pltpu.make_async_copy(gout, gout_hbm, o_sem.at[0])
    save_out.start()

    def gate_tile(i, carry):
        a = pl.ds(pl.multiple_of(i // 2 * across, across), across)
        b = pl.ds(pl.multiple_of(i % 2 * (inner // 2), inner // 2), inner // 2)
        ggate[a, b] = dot(turned[a, :], grad_gate[:, :, b].reshape(count, inner // 2)).astype(BF16)
        return carry

    lax.fori_loop(0, (width // across) * 2, gate_tile, 0)
    save_gate = pltpu.make_async_copy(ggate, ggate_hbm, o_sem.at[1])
    save_gate.start()

    def saved(i, carry):
        for copy in out_copies(i):
            copy.wait()
        return carry

    lax.fori_loop(0, chunks, saved, 0)
    save_out.wait()
    save_gate.wait()


def gating(ssd, gate, cot, w_out, normed_t, gains, dp):
    chunks, part, inner = ssd.shape
    width, count = normed_t.shape
    cot = cot.reshape(chunks, part, width)
    dma = pltpu.SemaphoreType.DMA
    vmem = pl.BlockSpec(memory_space=pltpu.VMEM)
    hbm = pl.BlockSpec(memory_space=pl.ANY)

    def shape(*dims, kind=BF16):
        return jax.ShapeDtypeStruct(dims, kind)

    def room(*dims, kind=BF16):
        return pltpu.VMEM(dims, kind)

    return pl.pallas_call(
        functools.partial(gating_kernel, dp),
        in_specs=[hbm] * 5 + [vmem],
        out_specs=[hbm] * 5,
        out_shape=[
            shape(chunks, part, inner, kind=F32),
            shape(chunks, part, inner),
            shape(chunks, part, width),
            shape(inner, width),
            shape(width, inner),
        ],
        scratch_shapes=[
            room(chunks, part, inner, kind=F32),
            room(chunks, part, inner, kind=F32),
            room(chunks, part, width),
            room(inner, width),
            room(width, count),
            room(chunks, part, inner, kind=F32),
            room(inner, count),
            room(chunks, part, inner),
            room(chunks, part, width),
            room(inner, width),
            room(width, inner),
            room(chunks, 8, part, kind=F32),
            room(3, chunks, 8, part, kind=F32),
            dma((2,)),
            dma((3, chunks)),
            dma((chunks,)),
            dma((chunks,)),
            dma((chunks,)),
            dma((2,)),
            dma((3,)),
            dma((3,)),
        ],
        compiler_params=pltpu.CompilerParams(
            collective_id=2, has_side_effects=True, vmem_limit_bytes=63 * 2**20
        ),
        cost_estimate=pl.CostEstimate(flops=3 * 10**10, bytes_accessed=5 * 10**7, transcendentals=0),
        name="gating_and_gradients",
    )(ssd, gate, cot, w_out, normed_t, gains)


def tail_kernel(
    dp,
    normed_hbm,
    rows_hbm,
    gates_hbm,
    w_rest_hbm,
    w_gate_hbm,
    tok_hbm,
    cot_hbm,
    gate_hbm,
    gout_hbm,
    proj_ref,
    block_ref,
    gain_ref,
    small_ref,
    tokens_ref,
    grad_ref,
    dots_ref,
    gout_ref,
    gdots_ref,
    taps_ref,
    bias_ref,
    heads_ref,
    out_ref,
    own_ref,
    sums_ref,
    tok,
    cot,
    gate_in,
    gout,
    normed,
    rows_ref,
    gates_ref,
    w_rest,
    w_gate,
    tile,
    wtile,
    theirs,
    mine,
    ybuf,
    zbuf,
    final,
    handed,
    core_buf,
    core_out,
    x_buf,
    x_out,
    s_buf,
    l_sem,
    n_sem,
    y_send,
    y_recv,
    z_send,
    z_recv,
    a_send,
    a_recv,
    c_send,
    c_recv,
    x_send,
    x_recv,
    s_send,
    s_recv,
):
    where = where_am_i(dp)
    d, s, z, y, x, c, peers, deep = where
    tp, rows = out_ref.shape[:2]
    block = tp * rows
    micro, part, width = own_ref.shape
    full = rows_ref.shape[1]
    bits = dp.bit_length() - 1
    partners = []
    for k in range(bits):
        step = 2**k
        bit = (d // step) % 2
        partners.append(d + step - 2 * step * bit)
    sends = Sends()
    total = OwnerSum(
        where,
        sends,
        None,
        mine,
        ybuf,
        zbuf,
        final,
        (None, y_send, y_recv, z_send, z_recv),
        theirs,
    )
    loads = [
        pltpu.make_async_copy(src, dst, l_sem.at[k])
        for k, (src, dst) in enumerate(
            (
                (rows_hbm, rows_ref),
                (w_rest_hbm, w_rest),
                (gates_hbm, gates_ref),
                (w_gate_hbm, w_gate),
                (tok_hbm, tok),
                (cot_hbm, cot),
                (gate_hbm, gate_in),
                (gout_hbm, gout),
            )
        )
    ]
    fetches = []
    for k in range(deep):
        lines = pl.ds(pl.multiple_of(total.order[k] * 2 * block, 2 * block), 2 * block)
        fetches.append(pltpu.make_async_copy(normed_hbm.at[lines, :], normed.at[k], n_sem.at[k]))
    for copy in loads + fetches:
        copy.start()
    greet(
        [(None, d, p) for p in peers]
        + [(None, d + 1 - 2 * y, s), (z < deep - 1, d + 2, s), (z > 0, d - 2, s)]
        + [(None, partners[k], s) for k in range(2, bits)]
    )

    def arrive(dst, sem):
        push(dst, dst, sem, sem, d, peers[0]).wait_recv()

    sums_ref[0] = small_ref[...]
    sends.start(None, push(small_ref, s_buf.at[0], s_send.at[0], s_recv.at[0], partners[0], s))

    def each(count, work):
        lax.fori_loop(0, count, lambda i, carry: (work(i), carry)[1], 0)

    across = width // tile.shape[1]
    span = wtile.shape[1]

    def product(owner, use):
        def work(i):
            m, n = i // across, i % across
            row = pl.multiple_of((m * tp + owner) * part, part)
            col = pl.multiple_of(n * tile.shape[1], tile.shape[1])
            lines = pl.ds(col, tile.shape[1])
            tile[...] = dot(rows_ref[pl.ds(row, part), :], w_rest[lines, :], NT) + dot(
                gates_ref[pl.ds(row, part), :], w_gate[lines, :], NT
            )
            use(m, lines)

        each(micro * across, work)

    def weight(k):
        fetches[k].wait()

        def work(n):
            cols = pl.ds(pl.multiple_of(n * span, span), span)
            wtile[...] = dot(normed[k], rows_ref[:, cols])
            far = pl.ds(pl.multiple_of((1 - y) * block, block), block)
            near = pl.ds(pl.multiple_of(y * block, block), block)
            theirs[k, :, cols] = wtile[far, :].astype(BF16)
            mine[k, :, cols] = wtile[near, :].astype(BF16)

        each(full // span, work)
        total.y_items[k][1].start()

    def doubling(k):
        arrive(s_buf.at[k], s_recv.at[k])
        sums_ref[k + 1] = sums_ref[k] + s_buf[k]
        if k + 1 < bits:
            src = sums_ref.at[k + 1]
            sends.start(
                None, push(src, s_buf.at[k + 1], s_send.at[k + 1], s_recv.at[k + 1], partners[k + 1], s)
            )

    def to_core(q):
        def use(m, lines):
            core_out[q, m, :, lines] = tile[...].astype(BF16)

        return use

    def to_chip(m, lines):
        x_out[m, :, lines] = (tile[...] + core_buf[0, m, :, lines].astype(F32)).astype(BF16)

    def keep(m, lines):
        own_ref[m, :, lines] = tile[...] + core_buf[1, m, :, lines].astype(F32)

    for copy in loads[:4]:
        copy.wait()
    product((1 - x) * 2 + 1 - c, to_core(0))
    sends.start(
        None, push(core_out.at[0], core_buf.at[0], c_send.at[0], c_recv.at[0], d, peers[0])
    )
    weight(0)
    arrive(core_buf.at[0], c_recv.at[0])
    product((1 - x) * 2 + c, to_chip)
    sends.start(None, push(x_out, x_buf, x_send.at[0], x_recv.at[0], d, peers[1]))
    weight(1)
    total.add(0)
    total.send(0)
    doubling(0)
    for k in range(2, deep):
        weight(k)
    total.add(1)
    total.send(1)
    doubling(1)
    product(x * 2 + 1 - c, to_core(1))
    sends.start(
        None, push(core_out.at[1], core_buf.at[1], c_send.at[1], c_recv.at[1], d, peers[0])
    )
    for k in range(2, deep - 1):
        total.add(k)
        total.send(k)
        if k < bits:
            doubling(k)
    arrive(core_buf.at[1], c_recv.at[1])
    product(s, keep)
    for k in range(deep - 1, bits):
        doubling(k)
    for r, p in enumerate(peers):
        src, dst = sums_ref.at[bits], sums_ref.at[bits + 1 + s]
        sends.start(None, push(src, dst, s_send.at[bits + r], s_recv.at[bits + r], d, p))
    sums_ref[bits + 1 + s] = sums_ref[bits]
    for copy in loads[4:]:
        copy.wait()
    inner = gate_in.shape[2]
    wide = inner + 2 * N
    heads = inner // P_SIZE
    triple = HEADS // 16
    for b in range(4):
        seat = 2 * (b % 2) + b // 2
        for k in range(4):
            at = (4 * k + b) * STRIPE
            grad_ref[:, at : at + STRIPE] = gate_in[seat, :, k * STRIPE : (k + 1) * STRIPE].astype(F32)
    gout_ref[...] = gout[...].astype(F32)
    gdots_ref[...] = jnp.sum(gout_ref[...] * block_ref[...].astype(F32), axis=1, keepdims=True)
    for r, p in enumerate(peers):
        arrive(sums_ref.at[bits + 1 + p], s_recv.at[bits + r])
    chan = taps_ref.shape[1]
    convs = jnp.zeros((8, chan), F32)
    per_head = jnp.zeros((8, HEADS), F32)
    v = lax.broadcasted_iota(jnp.int32, (wide, chan), 0)
    g = lax.broadcasted_iota(jnp.int32, (wide, chan), 1) + chan * (d * tp + s)
    lane = lax.broadcasted_iota(jnp.int32, (LANES, HEADS), 0)
    head = lax.broadcasted_iota(jnp.int32, (LANES, HEADS), 1)
    place = []
    for p in range(tp):
        b = 2 * (p % 2) + p // 2
        from_v = jnp.where(v < inner, v + 3 * STRIPE * hop(v, STRIPE) + STRIPE * b, v - inner + DI)
        sums = sums_ref[bits + 1 + p]
        convs = convs + dot(sums[:, :wide], jnp.where(from_v == g, 1.0, 0.0), precision=HIGH)
        hit = jnp.logical_and(lane < heads, head == lane + 3 * triple * hop(lane, triple) + triple * b)
        place.append(jnp.where(hit, 1.0, 0.0))
        per_head = per_head + dot(sums[:, wide:], place[p], precision=HIGH)
    taps_ref[...] = convs[:KW]
    bias_ref[...] = convs[KW : KW + 1]
    heads_ref[...] = per_head
    total.add(deep - 1)
    total.finish()
    for p in range(tp):
        handed[p] = final[p * rows : (p + 1) * rows, :]
    for r, p in enumerate(peers):
        sends.start(None, push(handed.at[p], out_ref.at[s], a_send.at[r], a_recv.at[r], d, p))
    out_ref[s] = handed[s]

    arrive(x_buf, x_recv.at[0])

    def last(i):
        m, row = i // (part // 16), (i % (part // 16)) * 16
        lines = pl.ds(pl.multiple_of(row, 16), 16)
        h = tok[m, lines, :].astype(F32)
        r = lax.rsqrt(jnp.mean(h * h, axis=-1, keepdims=True) + EPSILON)
        n = h * r
        grad = (own_ref[m, lines, :] + x_buf[m, lines, :].astype(F32)) * gain_ref[KW + 1 : KW + 2, :]
        grad = grad - n * jnp.mean(grad * n, axis=-1, keepdims=True)
        tokens_ref[m, lines, :] = (cot[m, lines, :].astype(F32) + r * grad).astype(BF16)

    each(micro * (part // 16), last)
    for r, p in enumerate(peers):
        arrive(out_ref.at[p], a_recv.at[r])
    both = jnp.zeros((rows, 2 * N), F32)
    steps = jnp.zeros((rows, HEADS), F32)
    for b in range(4):
        seat = 2 * (b % 2) + b // 2
        for k in range(4):
            at = DI + (4 * k + b) * STRIPE
            piece = out_ref[seat, :, k * STRIPE : (k + 1) * STRIPE]
            grad_ref[:, at : at + STRIPE] = piece.astype(F32)
        both = both + out_ref[seat, :, inner:wide].astype(F32)
        steps = steps + dot(out_ref[seat, :, wide:], place[seat].astype(BF16))
    grad_ref[:, 2 * DI : 2 * DI + 2 * N] = both
    grad_ref[:, 2 * DI + 2 * N :] = steps
    dots_ref[...] = jnp.sum(grad_ref[...] * proj_ref[...].astype(F32), axis=1, keepdims=True)
    sends.drain()


def tail(
    normed_t, rows_grad, gates_grad, w_rest, w_gate, tokens, cotangent, gate_in, gout, in_proj, out_proj, gains, small, chan, dp
):
    width, count = normed_t.shape
    micro = tokens.shape[0]
    tp = gate_in.shape[0]
    full = rows_grad.shape[1]
    rows = width // dp // tp
    part = count // micro // tp
    deep = dp // 2
    bits = dp.bit_length() - 1
    block = tp * rows
    dma = pltpu.SemaphoreType.DMA
    vmem = pl.BlockSpec(memory_space=pltpu.VMEM)
    hbm = pl.BlockSpec(memory_space=pl.ANY)
    return pl.pallas_call(
        functools.partial(tail_kernel, dp),
        in_specs=[hbm] * 9 + [vmem] * 4,
        out_specs=[vmem] * 8,
        out_shape=[
            jax.ShapeDtypeStruct(tokens.shape, BF16),
            jax.ShapeDtypeStruct(in_proj.shape, F32),
            jax.ShapeDtypeStruct((rows, 1), F32),
            jax.ShapeDtypeStruct(gout.shape, F32),
            jax.ShapeDtypeStruct((gout.shape[0], 1), F32),
            jax.ShapeDtypeStruct((KW, chan), F32),
            jax.ShapeDtypeStruct((1, chan), F32),
            jax.ShapeDtypeStruct((8, HEADS), F32),
        ],
        scratch_shapes=[
            pltpu.VMEM((tp, rows, full), BF16),
            pltpu.VMEM((micro, part, width), F32),
            pltpu.VMEM((bits + 1 + tp,) + small.shape, F32),
            pltpu.VMEM(tokens.shape, BF16),
            pltpu.VMEM(tokens.shape, BF16),
            pltpu.VMEM(gate_in.shape, BF16),
            pltpu.VMEM(gout.shape, BF16),
            pltpu.VMEM((deep, 2 * block, count), BF16),
            pltpu.VMEM(rows_grad.shape, BF16),
            pltpu.VMEM(gates_grad.shape, BF16),
            pltpu.VMEM(w_rest.shape, BF16),
            pltpu.VMEM(w_gate.shape, BF16),
            pltpu.VMEM((part, min(width, 512)), F32),
            pltpu.VMEM((2 * block, 384 if full % 384 == 0 else LANES), F32),
            pltpu.VMEM((deep, block, full), BF16),
            pltpu.VMEM((deep, block, full), BF16),
            pltpu.VMEM((deep, block, full), BF16),
            pltpu.VMEM((2, deep - 1, block, full), BF16),
            pltpu.VMEM((block, full), BF16),
            pltpu.VMEM((tp, rows, full), BF16),
            pltpu.VMEM((2, micro, part, width), BF16),
            pltpu.VMEM((2, micro, part, width), BF16),
            pltpu.VMEM((micro, part, width), BF16),
            pltpu.VMEM((micro, part, width), BF16),
            pltpu.VMEM((bits,) + small.shape, F32),
            dma((8,)),
            dma((deep,)),
            dma((deep,)),
            dma((deep,)),
            dma((2, deep - 1)),
            dma((2, deep - 1)),
            dma((3,)),
            dma((3,)),
            dma((2,)),
            dma((2,)),
            dma((1,)),
            dma((1,)),
            dma((bits + 3,)),
            dma((bits + 3,)),
        ],
        compiler_params=pltpu.CompilerParams(
            collective_id=3, has_side_effects=True, vmem_limit_bytes=62 * 2**20
        ),
        cost_estimate=pl.CostEstimate(flops=6 * 10**10, bytes_accessed=3 * 10**7, transcendentals=0),
        name="gradients_to_owners",
    )(
        normed_t,
        rows_grad,
        gates_grad,
        w_rest,
        w_gate,
        tokens,
        cotangent,
        gate_in,
        gout,
        in_proj,
        out_proj,
        gains,
        small,
    )


def body(
    tokens,
    in_proj,
    conv_weight,
    conv_bias,
    decay_log,
    step_bias,
    skip_gain,
    norm_gain,
    gated_gain,
    out_proj,
    cotangent,
):
    dp, tp = lax.axis_size("dp"), lax.axis_size("seq")
    s = lax.axis_index("seq")
    micro, part, width = tokens.shape
    heads = HEADS // tp
    inner = heads * P_SIZE
    rows = in_proj.shape[0]
    length = part * tp
    count = micro * length
    wide = inner + 2 * N
    chan = conv_bias.shape[0]

    per_head = jnp.pad(jnp.stack([decay_log, step_bias, skip_gain]), ((0, 5), (0, 0)))
    (
        normed,
        normed_t,
        proj_rest,
        ssd,
        memory,
        gate,
        w_rest,
        w_gate,
        w_out,
        cot,
        taps,
        gains,
        g_gated,
        per_head,
    ) = head(
        in_proj,
        conv_weight,
        conv_bias[None],
        norm_gain[None],
        gated_gain[None],
        per_head,
        tokens,
        cotangent,
        out_proj,
        dp,
        tp,
    )
    proj_rest = proj_rest.reshape(count, wide + LANES)
    w_rest = w_rest.reshape(width, wide + LANES)
    w_gate = w_gate.reshape(width, inner)
    grad_ssd, grad_gate, out_part, grad_out, gate_in = gating(
        ssd, gate, cot, w_out.reshape(inner, width), normed_t, g_gated, dp
    )
    grad_ssd = grad_ssd.reshape(count, inner)
    grad_gate = grad_gate.reshape(count, inner)
    grad_rest, wgrad, hgrad, out_part, grad_out, gate_in = middle(
        proj_rest,
        grad_ssd,
        memory,
        taps,
        per_head,
        out_part.reshape(micro, length, width),
        grad_out.reshape(dp, -1, width),
        gate_in.reshape(dp, tp, rows, inner),
        tokens,
        dp,
        tp,
        heads,
        micro,
    )
    small = jnp.concatenate([wgrad, hgrad], axis=1)
    tokens_grad, in_grad, dots, grad_out, gdots, conv_grad, bias_grad, head_grads = tail(
        normed_t,
        grad_rest,
        grad_gate,
        w_rest,
        w_gate,
        tokens,
        cotangent,
        gate_in,
        grad_out,
        in_proj,
        out_proj,
        gains,
        small,
        chan,
        dp,
    )
    return (
        out_part,
        tokens_grad,
        in_grad,
        conv_grad,
        bias_grad[0],
        head_grads[0],
        head_grads[1],
        head_grads[2],
        dots[:, 0] / norm_gain.astype(F32),
        gdots[:, 0] / gated_gain.astype(F32),
        grad_out,
    )


def solution(mesh):
    both = ("dp", "seq")
    return jax.shard_map(
        body,
        mesh=mesh,
        in_specs=(
            P("dp", "seq", None),
            P(both, None),
            P(None, both),
            P(both),
            P(),
            P(),
            P(),
            P(both),
            P(both),
            P(both, None),
            P("dp", "seq", None),
        ),
        out_specs=(
            P("dp", "seq", None),
            P("dp", "seq", None),
            P(both, None),
            P(None, both),
            P(both),
            P(),
            P(),
            P(),
            P(both),
            P(both),
            P(both, None),
        ),
        check_vma=False,
    )
```

```python
import functools

import jax
import jax.numpy as jnp
from jax import lax
from jax.experimental import pallas as pl
from jax.experimental.pallas import tpu as pltpu
from jax.sharding import PartitionSpec as P

HEADS = 48
P_SIZE = 64
N = 128
KW = 4
DI = 3072
CD = 3328
LANES = 128
FAR = -1e30

EPSILON = 1e-05
F32 = jnp.float32
BF16 = jnp.bfloat16


def dot(a, b, dims=((1,), (0,)), precision=None):
    return lax.dot_general(a, b, (dims, ((), ())), precision=precision, preferred_element_type=F32)


NT = ((1,), (1,))
HIGH = lax.Precision.HIGHEST


def pick(a, p, low):
    return jnp.where(low, a[:, 2 * p : 2 * p + 1], a[:, 2 * p + 1 : 2 * p + 2])


def chunk_parts(heads, rest_ref, xbuf, taps_ref, head_ref):
    size = rest_ref.shape[0]
    wide = taps_ref.shape[1]
    mixed = taps_ref[KW : KW + 1, :] + taps_ref[0:1, :] * xbuf[5 : 5 + size, :]
    for k in range(1, KW):
        mixed = mixed + taps_ref[k : k + 1, :] * xbuf[5 + k : 5 + k + size, :]
    sig = lax.logistic(mixed)
    lane = lax.broadcasted_iota(jnp.int32, (1, LANES), 1)
    raw = jnp.where(lane < heads, rest_ref[:, wide:], 0.0) + head_ref[1:2, :]
    step = jnp.maximum(raw, 0.0) + jnp.log1p(jnp.exp(-jnp.abs(raw)))
    decay = -jnp.exp(head_ref[0:1, :]) * step
    i = lax.broadcasted_iota(jnp.int32, (size, size), 0)
    j = lax.broadcasted_iota(jnp.int32, (size, size), 1)
    run = dot(jnp.where(i >= j, 1.0, 0.0), decay, precision=HIGH)
    return mixed, sig, raw, step, decay, run


def backward_kernel(
    heads,
    rest_ref,
    prev_ref,
    dy_ref,
    mem_ref,
    taps_ref,
    head_ref,
    out_ref,
    wgrad_ref,
    hgrad_ref,
    xbuf,
    gbuf,
    adj,
    dmix,
    dsum,
    uprod,
    zprod,
    rows_t,
    line,
):
    size = rest_ref.shape[0]
    wide = taps_ref.shape[1]
    inner = heads * P_SIZE
    chunks = pl.num_programs(1)
    step_id = pl.program_id(1)
    newest = step_id == 0
    oldest = step_id == chunks - 1
    begin = jnp.logical_and(pl.program_id(0) == 0, newest)
    finish = jnp.logical_and(pl.program_id(0) == pl.num_programs(0) - 1, oldest)

    @pl.when(begin)
    def _():
        wgrad_ref[...] = jnp.zeros_like(wgrad_ref)
        hgrad_ref[...] = jnp.zeros_like(hgrad_ref)
        rows_t[...] = jnp.zeros_like(rows_t)
        line[...] = jnp.zeros_like(line)

    @pl.when(newest)
    def _():
        gbuf[size : size + 8, :] = jnp.zeros((8, wide), F32)
        adj[...] = jnp.zeros_like(adj)

    @pl.when(jnp.logical_not(newest))
    def _():
        gbuf[size : size + 8, :] = gbuf[0:8, :]

    xbuf[0:8, :] = jnp.where(oldest, 0.0, prev_ref[:, :wide])
    xbuf[8 : 8 + size, :] = rest_ref[:, :wide]
    mixed, sig, raw, step, decay, run = chunk_parts(heads, rest_ref, xbuf, taps_ref, head_ref)
    act = mixed * sig
    run_t = run.T
    closing = run[size - 1 : size, :]
    last = jnp.exp(closing)
    left = jnp.exp(closing - run)
    grown = jnp.exp(run)
    b = act[:, inner : inner + N].astype(BF16)
    c = act[:, inner + N :].astype(BF16)
    c_t = act[:, inner + N :].T.astype(BF16)
    scores_t = dot(b, c, NT)
    low = lax.broadcasted_iota(jnp.int32, (1, LANES), 1) < P_SIZE
    lane = lax.broadcasted_iota(jnp.int32, (1, LANES), 1)
    j = lax.broadcasted_iota(jnp.int32, (size, size), 0)
    i = lax.broadcasted_iota(jnp.int32, (size, size), 1)
    causal = i >= j
    mem_b = mem_ref[0]
    adj_b = adj[...].astype(BF16)
    spread = dot(b, adj_b)
    inherit = dot(c, mem_b)
    scored = jnp.zeros((size, size), F32)
    cols = jnp.zeros((size, LANES), F32)
    for p in range(heads // 2):
        at = slice(p * LANES, (p + 1) * LANES)
        v = act[:, at]
        size_p = pick(step, p, low)
        xv = size_p * v
        dy = dy_ref[:, at]
        dyb = dy.astype(BF16)
        xvb = xv.astype(BF16)
        dxv = pick(left, p, low) * spread[:, at]
        zprod[:, at] = (dxv * xv).astype(BF16)
        dyg = pick(grown, p, low) * dy
        uprod[:, at] = (dyg * inherit[:, at]).astype(BF16)
        for e in range(2):
            h = 2 * p + e
            keep = low if e == 0 else jnp.logical_not(low)
            mine = jnp.where(keep, dy, 0.0).astype(BF16)
            gap = run_t[h : h + 1, :] - run[:, h : h + 1]
            near = jnp.exp(jnp.where(causal, gap, FAR))
            w_t = scores_t * near
            dw_t = dot(xvb, mine, NT)
            scored = scored + dw_t * near
            g_t = dw_t * w_t
            rows_t[h : h + 1, :] = jnp.sum(g_t, axis=0, keepdims=True)
            cols = jnp.where(lane == h, jnp.sum(g_t, axis=1, keepdims=True), cols)
            dxv = dxv + dot(w_t.astype(BF16), mine)
        dsum[:, at] = (dxv * v).astype(BF16)
        dmix[:, at] = size_p * dxv + pick(head_ref[2:3, :], p, low) * dy
        line[0:1, at] += jnp.sum(dy * v, axis=0, keepdims=True)
        line[1:2, at] = jnp.sum(adj[:, at] * mem_b[:, at].astype(F32), axis=0, keepdims=True) * pick(
            last, p, low
        )
        xc = (pick(left, p, low) * xv).astype(BF16)
        dygb = dyg.astype(BF16)
        db = dot(xc, adj_b[:, at], NT)
        dc = dot(dygb, mem_b[:, at], NT)
        if p == 0:
            dmix[:, inner : inner + N] = db
            dmix[:, inner + N :] = dc
        else:
            dmix[:, inner : inner + N] += db
            dmix[:, inner + N :] += dc
        adj[:, at] = adj[:, at] * pick(last, p, low) + dot(c_t, dygb)
    dmix[:, inner : inner + N] += dot(scored.astype(BF16), c)
    dmix[:, inner + N :] += dot(scored.T.astype(BF16), b)

    group = jnp.where(
        lax.broadcasted_iota(jnp.int32, (inner, LANES), 0) // P_SIZE
        == lax.broadcasted_iota(jnp.int32, (inner, LANES), 1),
        1.0,
        0.0,
    )
    group_b = group.astype(BF16)
    d_step = dot(dsum[...], group_b)
    u = dot(uprod[...], group_b)
    z = dot(zprod[...], group_b)
    sums = dot(line[...], group, precision=HIGH)
    d_run = rows_t[...].T - cols + u - z
    row = lax.broadcasted_iota(jnp.int32, (size, 1), 0)
    ending = sums[1:2, :] + jnp.sum(z, axis=0, keepdims=True)
    d_run = d_run + jnp.where(row == size - 1, ending, 0.0)
    d_decay = dot(jnp.where(causal, 1.0, 0.0), d_run, precision=HIGH)
    d_raw = (d_step - jnp.exp(head_ref[0:1, :]) * d_decay) * lax.logistic(raw)
    d_raw = jnp.where(lane < heads, d_raw, 0.0)
    hgrad_ref[0:1, :] += jnp.sum(d_decay * decay, axis=0, keepdims=True)
    hgrad_ref[1:2, :] += jnp.sum(d_raw, axis=0, keepdims=True)

    @pl.when(finish)
    def _():
        hgrad_ref[2:3, :] = sums[0:1, :]

    g = dmix[...] * (sig * (1.0 + mixed * (1.0 - sig)))
    gbuf[0:size, :] = g
    wgrad_ref[KW : KW + 1, :] += jnp.sum(g, axis=0, keepdims=True)
    for k in range(KW):
        wgrad_ref[k : k + 1, :] += jnp.sum(g * xbuf[5 + k : 5 + k + size, :], axis=0, keepdims=True)
    back = taps_ref[KW - 1 : KW, :] * g
    for k in range(KW - 1):
        back = back + taps_ref[k : k + 1, :] * gbuf[3 - k : 3 - k + size, :]
    out_ref[:, :wide] = back.astype(BF16)
    out_ref[:, wide:] = d_raw.astype(BF16)


MESH = pl.DeviceIdType.MESH


def where_am_i(dp):
    d, s = lax.axis_index("dp"), lax.axis_index("seq")
    z, y = d // 2, d % 2
    x, c = s // 2, s % 2
    peers = [s + 1 - 2 * c, s + 2 - 4 * x, 3 - s]
    return d, s, z, y, x, c, peers, dp // 2


def push(src, dst, send_sem, recv_sem, d, s):
    return pltpu.make_async_remote_copy(
        src_ref=src,
        dst_ref=dst,
        send_sem=send_sem,
        recv_sem=recv_sem,
        device_id={"dp": d, "seq": s},
        device_id_type=MESH,
    )


def greet(partners):
    barrier = pltpu.get_barrier_semaphore()
    for cond, d, s in partners:

        def hello(d=d, s=s):
            pl.semaphore_signal(barrier, inc=1, device_id={"dp": d, "seq": s}, device_id_type=MESH)

        if cond is None:
            hello()
        else:
            pl.when(cond)(hello)
    count = 0
    for cond, _, _ in partners:
        count = count + (1 if cond is None else jnp.where(cond, 1, 0))
    pl.semaphore_wait(barrier, count)


class Sends:
    def __init__(self):
        self.items = []

    def start(self, cond, copy):
        if cond is None:
            copy.start()
        else:
            pl.when(cond)(copy.start)
        self.items.append((cond, copy))

    def drain(self):
        for cond, copy in self.items:
            if cond is None:
                copy.wait_send()
            else:
                pl.when(cond)(copy.wait_send)


STRIPE = DI // 16


def swapped(s):
    return 2 * (s % 2) + s // 2


def stripe_owner(block, dp):
    u = dp // 4
    return block // (4 * u) * u + block % u


def stripe_seat(block, dp):
    return swapped(block // (dp // 4) % 4)


def stripe_block(d, s, dp):
    u = dp // 4
    return (d // u * 4 + swapped(s)) * u + d % u


def forward_chunk(heads, first, rest_ref, taps_ref, head_ref, ssd_ref, mem_ref, xbuf, mem):
    size = rest_ref.shape[0]
    wide = taps_ref.shape[1]
    inner = heads * P_SIZE

    @pl.when(first)
    def _():
        xbuf[0:8, :] = jnp.zeros((8, wide), F32)
        mem[...] = jnp.zeros_like(mem)

    @pl.when(jnp.logical_not(first))
    def _():
        xbuf[0:8, :] = xbuf[size : size + 8, :]

    xbuf[8 : 8 + size, :] = rest_ref[:, :wide]
    mixed, sig, _, step, _, run = chunk_parts(heads, rest_ref, xbuf, taps_ref, head_ref)
    act = mixed * sig
    run_t = run.T
    closing = run[size - 1 : size, :]
    last = jnp.exp(closing)
    left = jnp.exp(closing - run)
    grown = jnp.exp(run)
    b = act[:, inner : inner + N]
    c = act[:, inner + N :].astype(BF16)
    scores = dot(c, b.astype(BF16), NT)
    b_t = b.T.astype(BF16)
    mem_ref[...] = mem[...].astype(BF16)
    inter = dot(c, mem[...].astype(BF16))
    low = lax.broadcasted_iota(jnp.int32, (1, LANES), 1) < P_SIZE
    i = lax.broadcasted_iota(jnp.int32, (size, size), 0)
    j = lax.broadcasted_iota(jnp.int32, (size, size), 1)
    causal = i >= j
    for p in range(heads // 2):
        at = slice(p * LANES, (p + 1) * LANES)
        v = act[:, at]
        xv = pick(step, p, low) * v
        y = pick(head_ref[2:3, :], p, low) * v + pick(grown, p, low) * inter[:, at]
        for e in range(2):
            h = 2 * p + e
            gap = run[:, h : h + 1] - run_t[h : h + 1, :]
            w = (scores * jnp.exp(jnp.where(causal, gap, FAR))).astype(BF16)
            mine = jnp.where(low if e == 0 else jnp.logical_not(low), xv, 0.0).astype(BF16)
            y = y + dot(w, mine)
        ssd_ref[:, at] = y
        xc = (pick(left, p, low) * xv).astype(BF16)
        mem[:, at] = mem[:, at] * pick(last, p, low) + dot(b_t, xc)


def hop(v, size):
    return sum(jnp.where(v >= q * size, 1, 0) for q in range(1, 4))


def head_kernel(
    dp,
    heads,
    proj_ref,
    cw_ref,
    cb_ref,
    ng_ref,
    gg_ref,
    ph_ref,
    tok_ref,
    cot_ref,
    block_ref,
    normed_hbm,
    turned_hbm,
    proj_hbm,
    ssd_hbm,
    mem_hbm,
    gates_hbm,
    rest_hbm,
    gate_hbm,
    out_hbm,
    cot_hbm,
    taps_ref,
    gain_ref,
    gated_ref,
    head_ref,
    line,
    small_stage,
    val_stage,
    half_stage,
    gate_stage,
    small_all,
    val_in,
    half_in,
    gate_in,
    w_val,
    w_half,
    w_other,
    w_tail,
    w_gate,
    out_shard,
    tok,
    flipped,
    proj,
    ssd,
    gates,
    memory,
    xbuf,
    mem,
    l_sem,
    o_sem,
    f_sem,
    p_sem,
    g_sem,
    a_send,
    a_recv,
    z_send,
    z_recv,
    y_send,
    y_recv,
    t_send,
    t_recv,
):
    d, s, z, y, x, c, peers, deep = where_am_i(dp)
    tp, rows = val_stage.shape[:2]
    micro, part, width = tok_ref.shape
    total = dp * tp
    inner = heads * P_SIZE
    wide = inner + 2 * N
    chan, gpiece = cw_ref.shape[1], gg_ref.shape[1]
    up, down, far = d + 2, d - 2, d + 1 - 2 * y
    me = d * tp + s
    to_d, to_s, turned = stripe_owner(me, dp), stripe_seat(me, dp), stripe_block(d, s, dp)
    from_d, from_s = turned // tp, turned % tp
    moves = turned != me

    triple = HEADS // 16
    line[...] = jnp.zeros_like(line)
    line[0:KW, 0:chan] = cw_ref[...].astype(F32)
    line[KW : KW + 1, 0:chan] = cb_ref[...].astype(F32)
    line[KW + 1 : KW + 2, 0:rows] = ng_ref[...].astype(F32)
    line[KW + 2 : KW + 3, 0:gpiece] = gg_ref[...].astype(F32)
    raw = proj_ref[:, 2 * DI + 2 * N :]
    for b in range(4):
        seat = 2 * (b % 2) + b // 2
        for k in range(4):
            to, at = k * STRIPE, (4 * k + b) * STRIPE
            gate_stage[seat, :, to : to + STRIPE] = proj_ref[:, at : at + STRIPE]
            val_stage[seat, :, to : to + STRIPE] = proj_ref[:, DI + at : DI + at + STRIPE]
        at = 2 * DI + N * (seat % 2)
        half_stage[seat] = proj_ref[:, at : at + N]
        v = lax.broadcasted_iota(jnp.int32, (16, HEADS), 0)
        g = lax.broadcasted_iota(jnp.int32, (16, HEADS), 1)
        hit = jnp.logical_and(v < heads, g == v + 3 * triple * hop(v, triple) + triple * b)
        line[16:32, 0:rows] = dot(jnp.where(hit, 1.0, 0.0).astype(BF16), raw, NT)
        small_stage[seat] = line[...].astype(BF16)
    v = lax.broadcasted_iota(jnp.int32, (HEADS, LANES), 1)
    g = lax.broadcasted_iota(jnp.int32, (HEADS, LANES), 0)
    hit = jnp.logical_and(v < heads, g == v + 3 * triple * hop(v, triple) + triple * swapped(s))
    head_ref[...] = dot(ph_ref[...], jnp.where(hit, 1.0, 0.0), precision=HIGH)

    greet(
        [(None, d, p) for p in peers]
        + [(None, far, s), (z < deep - 1, up, s), (z > 0, down, s)]
        + [(moves, to_d, to_s), (moves, from_d, from_s)]
    )
    sends = Sends()

    def arrive(dst, sem):
        push(dst, dst, sem, sem, d, peers[0]).wait_recv()

    def mine(ref, k):
        return ref.at[:, pl.ds(k * part, part), :]

    def exchange(a, stage, target):
        for r, p in enumerate(peers):
            sends.start(
                None, push(stage.at[p], target(s), a_send.at[a, r], a_recv.at[a, r], d, p)
            )

    def exchanged(a, target):
        for r, p in enumerate(peers):
            arrive(target(p), a_recv.at[a, r])

    exchange(0, small_stage, lambda k: small_all.at[d, k])
    exchange(1, half_stage, lambda k: half_in.at[k])
    exchange(2, val_stage, lambda k: val_in.at[k])
    exchange(3, gate_stage, lambda k: gate_in.at[k])
    sends.start(moves, push(block_ref, out_shard, t_send.at[2], t_recv.at[2], to_d, to_s))
    sends.start(None, push(tok_ref, mine(tok, s), t_send.at[0], t_recv.at[0], d, peers[1]))
    sends.start(None, push(tok_ref, mine(tok, s), t_send.at[1], t_recv.at[1], d, peers[0]))
    sends.start(None, push(cot_ref, mine(cot_hbm, s), t_send.at[3], t_recv.at[3], d, peers[1]))
    sends.start(None, push(cot_ref, mine(cot_hbm, s), t_send.at[4], t_recv.at[4], d, peers[0]))
    saves = []

    def save(src, dst):
        copy = pltpu.make_async_copy(src, dst, l_sem.at[len(saves)])
        copy.start()
        saves.append(copy)

    save(cot_ref, mine(cot_hbm, s))
    small_all[d, s] = small_stage[s]
    half_in[s] = half_stage[s]
    val_in[s] = val_stage[s]
    gate_in[s] = gate_stage[s]
    tok[:, pl.ds(pl.multiple_of(s * part, part), part), :] = tok_ref[...]

    @pl.when(jnp.logical_not(moves))
    def _():
        out_shard[...] = block_ref[...]

    def begin(a, shard, dst):
        block = dst.at[d]
        sends.start(z < deep - 1, push(shard, block, z_send.at[a, 0, 0], z_recv.at[a, 0, 0], up, s))
        sends.start(z > 0, push(shard, block, z_send.at[a, 1, 0], z_recv.at[a, 1, 0], down, s))
        sends.start(None, push(shard, block, y_send.at[a, 0, 0], y_recv.at[a, 0, 0], far, s))

    def plan(a, dst, t):
        steps = []
        for way in range(2):
            here = (z >= t) if way == 0 else (z + t <= deep - 1)
            more = jnp.logical_and(here, (z < deep - 1) if way == 0 else (z > 0))
            at = jnp.clip(d - 2 * t if way == 0 else d + 2 * t, 0, dp - 1)
            block = dst.at[at]
            got = z_recv.at[a, way, t - 1]
            on = []
            if t < deep - 1:
                nxt = up if way == 0 else down
                on.append(
                    (more, push(block, block, z_send.at[a, way, t], z_recv.at[a, way, t], nxt, s))
                )
            on.append(
                (here, push(block, block, y_send.at[a, way, t], y_recv.at[a, way, t], far, s))
            )
            steps.append((here, push(block, block, got, got, d, peers[0]), on))
        return steps

    def run(steps):
        for here, wait, on in steps:
            if wait is not None:
                pl.when(here)(wait.wait_recv)
            for cond, copy in on:
                pl.when(cond)(copy.start)

    def remember(steps):
        for _, _, on in steps:
            sends.items.extend(on)

    def relay(a, dst, t):
        steps = plan(a, dst, t)
        run(steps)
        remember(steps)

    def pair(ref, t, way):
        at = jnp.clip(z - t if way == 0 else z + t, 0, deep - 1)
        return ref.at[pl.ds(2 * at, 2)]

    def plan_pair(a, ref, t):
        steps = []
        for way in range(2):
            here = (z >= t) if way == 0 else (z + t <= deep - 1)
            more = jnp.logical_and(here, (z < deep - 1) if way == 0 else (z > 0))
            block = pair(ref, t, way)
            on = []
            if t < deep - 1:
                nxt = up if way == 0 else down
                on.append(
                    (more, push(block, block, z_send.at[a, way, t], z_recv.at[a, way, t], nxt, s))
                )
            got = z_recv.at[a, way, max(t - 1, 0)]
            steps.append((here, push(block, block, got, got, d, peers[0]) if t else None, on))
        return steps

    def landed(a, dst):
        arrive(dst.at[far], y_recv.at[a, 0, 0])
        for t in range(1, deep):
            for way in range(2):
                here = (z >= t) if way == 0 else (z + t <= deep - 1)
                at = jnp.clip(far - 2 * t if way == 0 else far + 2 * t, 0, dp - 1)
                pl.when(here)(functools.partial(arrive, dst.at[at], y_recv.at[a, way, t]))

    def shard_of(a, pieces, dst):
        exchanged(a, lambda p: pieces.at[p])
        for k in range(tp):
            dst[d, k * rows : (k + 1) * rows, :] = pieces[k]
        begin(a, dst.at[d], dst)

    exchanged(0, lambda p: small_all.at[d, p])
    begin(0, small_all.at[d], small_all)
    shard_of(1, half_in, w_half)
    shard_of(2, val_in, w_val)
    for t in range(1, deep):
        relay(0, small_all, t)
        relay(1, w_half, t)
        relay(2, w_val, t)
    exchanged(3, lambda p: gate_in.at[p])
    for k in range(tp):
        w_gate[d, k * rows : (k + 1) * rows, :] = gate_in[k]
    cut = max(tp * rows // 32, 1) * 16
    lower = w_gate.at[:, pl.ds(0, cut), :]
    upper = w_gate.at[:, pl.ds(cut, tp * rows - cut), :]
    crossing = push(upper.at[d], upper.at[d], y_send.at[5, 0, 0], y_recv.at[5, 0, 0], far, s)
    sends.start(None, crossing)
    begin(3, lower.at[d], lower)
    pl.when(moves)(functools.partial(arrive, out_shard, t_recv.at[2]))
    begin(4, out_shard, out_hbm)
    save(out_shard, out_hbm.at[d])

    landed(0, small_all)

    def one_hot(columns, index, k, length):
        lane = lax.broadcasted_iota(jnp.int32, (LANES, columns), 1)
        at = lax.broadcasted_iota(jnp.int32, (LANES, columns), 0)
        hit = jnp.logical_and(at < length, index(lane) == k * length + at)
        return jnp.where(hit, 1.0, 0.0).astype(BF16)

    taps_ref[...] = jnp.zeros_like(taps_ref)
    gain_ref[...] = jnp.zeros_like(gain_ref)
    gated_ref[...] = jnp.zeros_like(gated_ref)

    def striped(v):
        return v + 3 * STRIPE * hop(v, STRIPE) + STRIPE * swapped(s)

    def lay_out(dd, carry):
        for kk in range(tp):
            k = dd * tp + kk
            values = small_all[dd, kk, 0:16, :]
            chans = one_hot(wide, lambda v: jnp.where(v < inner, striped(v), v - inner + DI), k, chan)
            taps_ref[...] += dot(values, chans)[:8]
            gain_ref[...] += dot(values, one_hot(width, lambda v: v, k, rows))
            gated_ref[...] += dot(values, one_hot(inner, striped, k, gpiece))
            turned = jnp.concatenate(
                [small_all[dd, kk, 16:32, :].astype(F32), jnp.zeros((LANES - 16, LANES), F32)], axis=0
            ).T
            w_tail[dd, kk * rows : (kk + 1) * rows, 2 * N :] = turned[:rows].astype(BF16)
        return carry

    lax.fori_loop(0, dp, lay_out, 0)
    landed(1, w_half)
    sends.start(None, push(w_half, w_other, t_send.at[6], t_recv.at[6], d, peers[0]))
    landed(2, w_val)
    save(w_val, rest_hbm.at[:, :, pl.ds(0, inner)])
    arrive(w_other, t_recv.at[6])

    def both_halves(dd, carry):
        w_tail[dd, :, pl.ds(pl.multiple_of(c * N, N), N)] = w_half[dd]
        w_tail[dd, :, pl.ds(pl.multiple_of((1 - c) * N, N), N)] = w_other[dd]
        return carry

    lax.fori_loop(0, dp, both_halves, 0)
    save(w_tail, rest_hbm.at[:, :, pl.ds(inner, w_tail.shape[2])])
    arrive(mine(tok, peers[1]), t_recv.at[0])
    block = mine(tok, peers[1])
    hand = push(block, block, t_send.at[5], t_recv.at[5], d, peers[0])
    hand.start()
    crossing.wait_recv()
    steps = plan_pair(5, upper, 0)
    run(steps)
    remember(steps)
    relay(3, lower, 1)
    relay(4, out_hbm, 1)
    arrive(mine(tok, peers[0]), t_recv.at[1])
    arrive(mine(tok, peers[2]), t_recv.at[5])
    hand.wait_send()

    tasks = []
    for t in range(2, deep):
        tasks += [(plan, 3, lower, t), (plan_pair, 5, upper, t - 1), (plan, 4, out_hbm, t)]
    tasks.append((plan_pair, 5, upper, deep - 1))
    chunks = micro * tp
    when = {}
    for n, task in enumerate(tasks):
        steps = task[0](*task[1:])
        when.setdefault(min(n * 6 // len(tasks), chunks - 1), []).append(steps)
    for plans in when.values():
        for steps in plans:
            remember(steps)

    def columns(i):
        return pl.ds(pl.multiple_of(i * part, part), part)

    def chunk(i, carry):
        m, k = i // tp, i % tp
        lines = pl.ds(pl.multiple_of(k * part, part), part)
        h = tok[m, lines, :].astype(F32)
        r = lax.rsqrt(jnp.mean(h * h, axis=-1, keepdims=True) + EPSILON)
        value = h * r * gain_ref[5:6, :]
        tok[m, lines, :] = value.astype(BF16)
        flipped[i] = value.T.astype(BF16)
        proj[i, :, 0:inner] = dot(tok[m, lines, :], w_val[...].reshape(width, inner))
        proj[i, :, inner:] = dot(tok[m, lines, :], w_tail[...].reshape(width, w_tail.shape[2]))
        forward_chunk(
            heads, k == 0, proj.at[i], taps_ref, head_ref, ssd.at[i], memory.at[i], xbuf, mem
        )
        pltpu.make_async_copy(tok.at[m, lines, :], normed_hbm.at[m, lines, :], o_sem.at[i]).start()
        pltpu.make_async_copy(flipped.at[i], turned_hbm.at[:, columns(i)], f_sem.at[i]).start()
        pltpu.make_async_copy(proj.at[i], proj_hbm.at[i], p_sem.at[i]).start()
        for n, plans in when.items():

            @pl.when(i == n)
            def _():
                for steps in plans:
                    run(steps)

        return carry

    lax.fori_loop(0, chunks, chunk, 0)
    save(ssd, ssd_hbm)
    save(memory, mem_hbm)
    arrive(mine(cot_hbm, peers[1]), t_recv.at[3])
    block = mine(cot_hbm, peers[1])
    sends.start(None, push(block, block, t_send.at[7], t_recv.at[7], d, peers[0]))
    landed(3, lower)
    save(w_gate, gate_hbm)

    def gating(i, carry):
        m, k = i // tp, i % tp
        lines = pl.ds(pl.multiple_of(k * part, part), part)
        gates[i] = dot(tok[m, lines, :], w_gate[...].reshape(width, inner))
        pltpu.make_async_copy(gates.at[i], gates_hbm.at[i], g_sem.at[i]).start()
        return carry

    lax.fori_loop(0, chunks, gating, 0)
    landed(4, out_hbm)
    arrive(mine(cot_hbm, peers[0]), t_recv.at[4])
    arrive(mine(cot_hbm, peers[2]), t_recv.at[7])

    def saved(i, carry):
        m, k = i // tp, i % tp
        lines = pl.ds(pl.multiple_of(k * part, part), part)
        pltpu.make_async_copy(tok.at[m, lines, :], normed_hbm.at[m, lines, :], o_sem.at[i]).wait()
        pltpu.make_async_copy(flipped.at[i], turned_hbm.at[:, columns(i)], f_sem.at[i]).wait()
        pltpu.make_async_copy(proj.at[i], proj_hbm.at[i], p_sem.at[i]).wait()
        pltpu.make_async_copy(gates.at[i], gates_hbm.at[i], g_sem.at[i]).wait()
        return carry

    lax.fori_loop(0, chunks, saved, 0)
    for copy in saves:
        copy.wait()
    sends.drain()


def head(in_proj, conv_weight, conv_bias, norm_gain, gated_gain, per_head, tokens, cotangent, out_proj, dp, tp):
    rows = in_proj.shape[0]
    heads = HEADS // tp
    inner = heads * P_SIZE
    full = inner + 2 * N + LANES
    micro, part, width = tokens.shape
    deep = dp // 2
    chunks = micro * tp
    block = tp * rows
    dma = pltpu.SemaphoreType.DMA
    vmem = pl.BlockSpec(memory_space=pltpu.VMEM)
    hbm = pl.BlockSpec(memory_space=pl.ANY)
    wide = inner + 2 * N

    def shape(*dims, kind=BF16):
        return jax.ShapeDtypeStruct(dims, kind)

    def room(*dims, kind=BF16):
        return pltpu.VMEM(dims, kind)

    return pl.pallas_call(
        functools.partial(head_kernel, dp, heads),
        in_specs=[vmem] * 9,
        out_specs=[hbm] * 10 + [vmem] * 4,
        out_shape=[
            shape(micro, tp * part, width),
            shape(width, chunks * part),
            shape(chunks, part, full, kind=F32),
            shape(chunks, part, inner, kind=F32),
            shape(chunks, N, inner),
            shape(chunks, part, inner, kind=F32),
            shape(dp, block, full),
            shape(dp, block, inner),
            shape(dp, out_proj.shape[0], width),
            shape(micro, tp * part, width),
            shape(8, wide, kind=F32),
            shape(16, width, kind=F32),
            shape(16, inner, kind=F32),
            shape(8, LANES, kind=F32),
        ],
        scratch_shapes=[
            room(32, LANES, kind=F32),
            room(tp, 32, LANES),
            room(tp, rows, inner),
            room(tp, rows, N),
            room(tp, rows, inner),
            room(dp, tp, 32, LANES),
            room(tp, rows, inner),
            room(tp, rows, N),
            room(tp, rows, inner),
            room(dp, block, inner),
            room(dp, block, N),
            room(dp, block, N),
            room(dp, block, 2 * N + LANES),
            room(dp, block, inner),
            room(*out_proj.shape),
            room(micro, tp * part, width),
            room(chunks, width, part),
            room(chunks, part, full, kind=F32),
            room(chunks, part, inner, kind=F32),
            room(chunks, part, inner, kind=F32),
            room(chunks, N, inner),
            room(part + 8, wide, kind=F32),
            room(N, inner, kind=F32),
            dma((8,)),
            dma((chunks,)),
            dma((chunks,)),
            dma((chunks,)),
            dma((chunks,)),
            dma((4, 3)),
            dma((4, 3)),
            dma((6, 2, deep - 1)),
            dma((6, 2, deep - 1)),
            dma((6, 2, deep)),
            dma((6, 2, deep)),
            dma((8,)),
            dma((8,)),
        ],
        compiler_params=pltpu.CompilerParams(
            collective_id=1, has_side_effects=True, vmem_limit_bytes=62 * 2**20
        ),
        cost_estimate=pl.CostEstimate(flops=10**11, bytes_accessed=5 * 10**7, transcendentals=0),
        name="gather_and_mix",
    )(in_proj, conv_weight, conv_bias, norm_gain, gated_gain, per_head, tokens, cotangent, out_proj)


class OwnerSum:
    def __init__(self, where, sends, source, mine, ybuf, zbuf, final, sems, theirs_ref=None):
        self.where, self.sends = where, sends
        self.mine, self.ybuf, self.zbuf, self.final = mine, ybuf, zbuf, final
        d, s, z, y, _, _, _, deep = where
        self.load_sem, y_send, self.y_recv, z_send, self.z_recv = sems
        lower = z < deep // 2

        def place(j):
            low = jnp.where(j > z, deep - 1 - j, deep - 1 - z + j)
            high = jnp.where(j < z, j, z + deep - 1 - j)
            return jnp.where(j == z, deep - 1, jnp.where(lower, low, high))

        def turn(k):
            low = jnp.where(k < deep - 1 - z, deep - 1 - k, k - (deep - 1 - z))
            high = jnp.where(k < z, k, deep - 1 - (k - z))
            return jnp.where(lower, low, high) if k < deep - 1 else z

        self.order = [turn(k) for k in range(deep)]
        self.y_items, self.loads = [], []
        for k, j in enumerate(self.order):
            theirs = source.at[j * 2 + 1 - y] if theirs_ref is None else theirs_ref.at[k]
            copy = push(theirs, ybuf.at[k], y_send.at[k], self.y_recv.at[k], d + 1 - 2 * y, s)
            self.y_items.append((None, copy))
            if theirs_ref is None:
                own = source.at[j * 2 + y]
                self.loads.append(pltpu.make_async_copy(own, mine.at[k], self.load_sem.at[k]))
        self.z_items = []
        for t in range(deep - 1):
            ways = []
            for way in range(2):
                depth = z if way == 0 else deep - 1 - z
                j = deep - 1 - t + z if way == 0 else t + z - deep + 1
                k = place(jnp.clip(j, 0, deep - 1))
                nxt = d + 2 if way == 0 else d - 2
                dst, ss, rs = zbuf.at[way, t], z_send.at[way, t], self.z_recv.at[way, t]
                first = (depth == 0, push(ybuf.at[k], dst, ss, rs, nxt, s))
                later = None
                if t > 0:
                    cond = jnp.logical_and(depth > 0, depth <= t)
                    later = (cond, push(zbuf.at[way, t - 1], dst, ss, rs, nxt, s))
                ways.append((k, first, later))
            self.z_items.append(ways)
        sends.items.extend(self.y_items)
        for ways in self.z_items:
            for _, first, later in ways:
                sends.items.append(first)
                if later is not None:
                    sends.items.append(later)

    def arrive(self, ref, sem):
        d, s = self.where[:2]
        push(ref, ref, sem, sem, d, self.where[6][0]).wait_recv()

    def begin(self):
        for _, copy in self.y_items:
            copy.start()
        for copy in self.loads:
            copy.start()

    def each(self, work):
        if self.mine.ndim == 4:
            count, cut = self.mine.shape[1], lambda i: i
        else:
            count, cut = self.mine.shape[1] // 16, lambda i: pl.ds(pl.multiple_of(i * 16, 16), 16)
        lax.fori_loop(0, count, lambda i, carry: (work(cut(i)), carry)[1], 0)

    def add(self, k):
        if self.loads:
            self.loads[k].wait()
        self.arrive(self.ybuf.at[k], self.y_recv.at[k])
        ybuf, mine = self.ybuf, self.mine

        def work(i):
            ybuf[k, i] = (ybuf[k, i].astype(F32) + mine[k, i].astype(F32)).astype(BF16)

        self.each(work)

    def send(self, t):
        zbuf, ybuf = self.zbuf, self.ybuf
        for way, (k, first, later) in enumerate(self.z_items[t]):
            pl.when(first[0])(first[1].start)
            if later is None:
                continue

            @pl.when(later[0])
            def _():
                self.arrive(zbuf.at[way, t - 1], self.z_recv.at[way, t - 1])

                def work(i):
                    zbuf[way, t - 1, i] = (
                        zbuf[way, t - 1, i].astype(F32) + ybuf[k, i].astype(F32)
                    ).astype(BF16)

                self.each(work)
                later[1].start()

    def finish(self):
        z, deep = self.where[2], self.where[7]
        zbuf, ybuf, final = self.zbuf, self.ybuf, self.final
        for way in range(2):
            depth = z if way == 0 else deep - 1 - z
            pl.when(depth > 0)(
                functools.partial(self.arrive, zbuf.at[way, deep - 2], self.z_recv.at[way, deep - 2])
            )

        def work(ways, i):
            total = ybuf[deep - 1, i].astype(F32)
            for way in ways:
                total = total + zbuf[way, deep - 2, i].astype(F32)
            final[i] = total.astype(BF16)

        for cond, ways in (
            (z == 0, (1,)),
            (z == deep - 1, (0,)),
            (jnp.logical_and(z > 0, z < deep - 1), (0, 1)),
        ):
            pl.when(cond)(functools.partial(self.each, functools.partial(work, ways)))


def middle_kernel(
    dp,
    heads,
    rest_ref,
    prev_ref,
    dy_ref,
    mem_ref,
    taps_ref,
    head_ref,
    part_hbm,
    gout_hbm,
    ggate_hbm,
    tok_hbm,
    out_ref,
    wgrad_ref,
    hgrad_ref,
    own_hbm,
    gout_out,
    ggate_out,
    xbuf,
    gbuf,
    adj,
    dmix,
    dsum,
    uprod,
    zprod,
    rows_t,
    line,
    o_mine,
    o_y,
    o_z,
    o_final,
    g_mine,
    g_y,
    g_z,
    g_final,
    own,
    core_buf,
    x_buf,
    tok,
    result,
    o_load,
    o_ysend,
    o_yrecv,
    o_zsend,
    o_zrecv,
    g_load,
    g_ysend,
    g_yrecv,
    g_zsend,
    g_zrecv,
    b_load,
    c_send,
    c_recv,
    m_send,
    m_recv,
    a_send,
    a_recv,
):
    where = where_am_i(dp)
    d, s, z, y, x, c, peers, deep = where
    micro, part, width = result.shape
    step = pl.program_id(0) * pl.num_programs(1) + pl.program_id(1)
    tp = ggate_hbm.shape[1]
    me = d * tp + s
    turned = stripe_block(d, s, dp)
    moves = turned != me
    to_d, to_s = turned // tp, turned % tp
    from_d, from_s = stripe_owner(me, dp), stripe_seat(me, dp)
    sends = Sends()
    gout = OwnerSum(
        where, sends, gout_hbm, o_mine, o_y, o_z, o_final, (o_load, o_ysend, o_yrecv, o_zsend, o_zrecv)
    )
    ggate = OwnerSum(
        where, sends, ggate_hbm, g_mine, g_y, g_z, g_final, (g_load, g_ysend, g_yrecv, g_zsend, g_zrecv)
    )

    def chunk(k):
        return part_hbm.at[:, pl.ds(k * part, part), :]

    cores, loads = [], []
    for q, xx in enumerate((1 - x, x)):
        cores.append(
            push(chunk(xx * 2 + 1 - c), core_buf.at[q], c_send.at[q], c_recv.at[q], d, peers[0])
        )
        loads.append(pltpu.make_async_copy(chunk(xx * 2 + c), own.at[q], b_load.at[q]))
    across = push(core_buf.at[0], x_buf, m_send.at[0], m_recv.at[0], d, peers[1])
    turning = push(o_final, gout_out, m_send.at[1], m_recv.at[1], to_d, to_s)
    staying = pltpu.make_async_copy(o_final, gout_out, b_load.at[2])
    swaps = [
        push(g_final.at[p], ggate_out.at[s], a_send.at[r], a_recv.at[r], d, p)
        for r, p in enumerate(peers)
    ]
    kept = pltpu.make_async_copy(g_final.at[s], ggate_out.at[s], b_load.at[3])
    saved = pltpu.make_async_copy(result, own_hbm, b_load.at[4])
    loads.append(pltpu.make_async_copy(tok_hbm, tok, b_load.at[5]))
    for copy in cores + [across] + swaps:
        sends.items.append((None, copy))
    sends.items.append((moves, turning))
    span = 16

    def by_rows(work):
        def one(i, carry):
            m, row = i // (part // span), (i % (part // span)) * span
            work(m, pl.ds(pl.multiple_of(row, span), span))
            return carry

        lax.fori_loop(0, micro * (part // span), one, 0)

    def start():
        greet(
            [(None, d, p) for p in peers]
            + [(None, d + 1 - 2 * y, s), (z < deep - 1, d + 2, s), (z > 0, d - 2, s)]
            + [(moves, to_d, to_s), (moves, from_d, from_s)]
        )
        for copy in cores + loads:
            copy.start()
        gout.begin()
        ggate.begin()

    def pass_on():
        loads[0].wait()
        cores[0].wait_recv()

        def work(m, rows):
            core_buf[0, m, rows, :] = (
                core_buf[0, m, rows, :].astype(F32) + own[0, m, rows, :].astype(F32)
            ).astype(BF16)

        by_rows(work)
        across.start()

    def collect():
        loads[1].wait()
        loads[2].wait()
        cores[1].wait_recv()
        across.wait_recv()

        def work(m, rows):
            result[m, rows, :] = (
                core_buf[1, m, rows, :].astype(F32)
                + own[1, m, rows, :].astype(F32)
                + x_buf[m, rows, :].astype(F32)
                + tok[m, rows, :].astype(F32)
            ).astype(BF16)

        by_rows(work)
        saved.start()

    def hand_over():
        gout.finish()
        pl.when(moves)(turning.start)
        pl.when(jnp.logical_not(moves))(staying.start)

    def last():
        ggate.finish()
        for copy in swaps:
            copy.start()
        kept.start()
        pl.when(moves)(turning.wait_recv)
        pl.when(jnp.logical_not(moves))(staying.wait)
        for r, p in enumerate(peers):
            push(ggate_out.at[p], ggate_out.at[p], a_send.at[r], a_recv.at[r], d, p).wait_recv()
        kept.wait()
        saved.wait()
        sends.drain()

    stages = {}

    def at(n, task, *args):
        stages.setdefault(n, []).append(functools.partial(task, *args))

    at(0, start)
    at(1, pass_on)
    for k in range(deep):
        n = 1 + k * 3 // (deep - 1)
        at(n, gout.add, k)
        if k < deep - 1:
            at(n, gout.send, k)
    at(4, hand_over)
    at(5, ggate.add, 0)
    for k in range(deep - 1):
        n = 5 + k * 2 // (deep - 2)
        at(n, ggate.send, k)
        at(n, ggate.add, k + 1)
    at(6, collect)
    for n, tasks in stages.items():

        @pl.when(step == n)
        def _():
            for task in tasks:
                task()

    backward_kernel(
        heads,
        rest_ref,
        prev_ref,
        dy_ref,
        mem_ref,
        taps_ref,
        head_ref,
        out_ref,
        wgrad_ref,
        hgrad_ref,
        xbuf,
        gbuf,
        adj,
        dmix,
        dsum,
        uprod,
        zprod,
        rows_t,
        line,
    )
    pl.when(step == pl.num_programs(0) * pl.num_programs(1) - 1)(last)


def middle(rest, dy, memory, taps, head, partial, gout, ggate, tokens, dp, tp, heads, micro):
    count, full = rest.shape
    wide = taps.shape[1]
    inner = heads * P_SIZE
    _, length, width = partial.shape
    part = length // tp
    chunks = length // part
    deep = dp // 2
    dma = pltpu.SemaphoreType.DMA
    hbm = pl.BlockSpec(memory_space=pl.ANY)
    gout = gout.reshape(dp, 2, -1, width)

    def at(m, c):
        return m * chunks + chunks - 1 - c

    def sums(block):
        kinds = [(deep,), (deep,), (2, deep - 1), ()]
        return [pltpu.VMEM(kind + block, BF16) for kind in kinds]

    sems = [dma((deep,))] * 3 + [dma((2, deep - 1))] * 2
    out = pl.pallas_call(
        functools.partial(middle_kernel, dp, heads),
        grid=(micro, chunks),
        in_specs=[
            pl.BlockSpec((part, full), lambda m, c: (at(m, c), 0)),
            pl.BlockSpec((8, full), lambda m, c: (jnp.maximum(at(m, c) * (part // 8) - 1, 0), 0)),
            pl.BlockSpec((part, inner), lambda m, c: (at(m, c), 0)),
            pl.BlockSpec((1, N, inner), lambda m, c: (at(m, c), 0, 0)),
            pl.BlockSpec((8, wide), lambda m, c: (0, 0)),
            pl.BlockSpec((8, LANES), lambda m, c: (0, 0)),
            hbm,
            hbm,
            hbm,
            hbm,
        ],
        out_specs=[
            pl.BlockSpec((part, full), lambda m, c: (at(m, c), 0)),
            pl.BlockSpec((8, wide), lambda m, c: (0, 0)),
            pl.BlockSpec((8, LANES), lambda m, c: (0, 0)),
            hbm,
            hbm,
            hbm,
        ],
        out_shape=[
            jax.ShapeDtypeStruct((count, full), BF16),
            jax.ShapeDtypeStruct((8, wide), F32),
            jax.ShapeDtypeStruct((8, LANES), F32),
            jax.ShapeDtypeStruct((micro, part, width), BF16),
            jax.ShapeDtypeStruct(gout.shape[1:], BF16),
            jax.ShapeDtypeStruct(ggate.shape[1:], BF16),
        ],
        scratch_shapes=[
            pltpu.VMEM((part + 8, wide), F32),
            pltpu.VMEM((part + 8, wide), F32),
            pltpu.VMEM((N, inner), F32),
            pltpu.VMEM((part, wide), F32),
            pltpu.VMEM((part, inner), BF16),
            pltpu.VMEM((part, inner), BF16),
            pltpu.VMEM((part, inner), BF16),
            pltpu.VMEM((LANES, part), F32),
            pltpu.VMEM((8, inner), F32),
        ]
        + sums(gout.shape[1:])
        + sums(ggate.shape[1:])
        + [
            pltpu.VMEM((2, micro, part, width), BF16),
            pltpu.VMEM((2, micro, part, width), BF16),
            pltpu.VMEM((micro, part, width), BF16),
            pltpu.VMEM((micro, part, width), BF16),
            pltpu.VMEM((micro, part, width), BF16),
        ]
        + sems
        + sems
        + [dma((6,)), dma((2,)), dma((2,)), dma((2,)), dma((2,)), dma((3,)), dma((3,))],
        compiler_params=pltpu.CompilerParams(
            dimension_semantics=("arbitrary", "arbitrary"),
            collective_id=4,
            has_side_effects=True,
            vmem_limit_bytes=62 * 2**20,
        ),
        cost_estimate=pl.CostEstimate(flops=7 * 10**10, bytes_accessed=4 * 10**7, transcendentals=0),
        name="mixer_backward_and_sums",
    )(rest, rest, dy, memory, taps, head, partial, gout, ggate, tokens)
    rest_grad, wgrad, hgrad, own, gout, ggate = out
    return rest_grad, wgrad, hgrad, own, gout.reshape(-1, width), ggate


def gating_kernel(
    dp,
    ssd_hbm,
    gate_hbm,
    cot_hbm,
    out_hbm,
    turned_hbm,
    gain_ref,
    grad_ssd_hbm,
    grad_gate_hbm,
    part_hbm,
    gout_hbm,
    ggate_hbm,
    ssd,
    gate,
    cot,
    w_out,
    turned,
    weighed,
    shaped_t,
    grad_gate,
    partial,
    gout,
    ggate,
    stats,
    held,
    l_sem,
    c_sem,
    s_sem,
    g_sem,
    p_sem,
    o_sem,
    send,
    recv,
):
    d, s, *_, peers, _ = where_am_i(dp)
    chunks, part, inner = ssd.shape
    width = cot.shape[2]
    count = chunks * part

    def loads(i):
        return [
            pltpu.make_async_copy(cot_hbm.at[i], cot.at[i], c_sem.at[0, i]),
            pltpu.make_async_copy(ssd_hbm.at[i], ssd.at[i], c_sem.at[1, i]),
            pltpu.make_async_copy(gate_hbm.at[i], gate.at[i], c_sem.at[2, i]),
        ]

    first = pltpu.make_async_copy(out_hbm, w_out, l_sem.at[0])
    other = pltpu.make_async_copy(turned_hbm, turned, l_sem.at[1])
    first.start()
    for i in range(chunks):
        for copy in loads(i):
            copy.start()
    other.start()
    greet([(None, d, p) for p in peers])
    first.wait()

    def gated_parts(i):
        g = gate[i]
        sig = lax.logistic(g)
        act = g * sig
        return sig, act, ssd[i] * act

    def measure(i, carry):
        for copy in loads(i):
            copy.wait()
        w = dot(cot[i], w_out[...], NT) * gain_ref[KW + 2 : KW + 3, :]
        weighed[i] = w
        _, _, gated = gated_parts(i)
        lane = lax.broadcasted_iota(jnp.int32, (part, LANES), 1)
        both = jnp.where(lane == 0, jnp.sum(gated * gated, axis=1, keepdims=True), 0.0)
        both = jnp.where(lane == 1, jnp.sum(w * gated, axis=1, keepdims=True), both)
        stats[i] = both.T[:8, :]
        return carry

    lax.fori_loop(0, chunks, measure, 0)
    copies = [push(stats, held.at[r], send.at[r], recv.at[r], d, p) for r, p in enumerate(peers)]
    for copy in copies:
        copy.start()
    for copy in copies:
        copy.wait()

    def out_copies(i):
        return [
            pltpu.make_async_copy(weighed.at[i], grad_ssd_hbm.at[i], s_sem.at[i]),
            pltpu.make_async_copy(grad_gate.at[i], grad_gate_hbm.at[i], g_sem.at[i]),
            pltpu.make_async_copy(partial.at[i], part_hbm.at[i], p_sem.at[i]),
        ]

    def columns(i):
        return pl.ds(pl.multiple_of(i * part, part), part)

    def shape_chunk(i, carry):
        sums = (stats[i] + held[0, i]) + (held[1, i] + held[2, i])
        sums = jnp.concatenate([sums, jnp.zeros((LANES - 8, part), F32)], axis=0).T
        q = lax.rsqrt(sums[:, 0:1] / DI + EPSILON)
        pull = q * q * (sums[:, 1:2] / DI)
        sig, act, gated = gated_parts(i)
        value = gated * q * gain_ref[KW + 2 : KW + 3, :]
        shaped_t[:, columns(i)] = value.T.astype(BF16)
        partial[i] = dot(value.astype(BF16), w_out[...]).astype(BF16)
        grad = q * (weighed[i] - gated * pull)
        grad_gate[i] = (grad * ssd[i] * (sig + act * (1.0 - sig))).astype(BF16)
        weighed[i] = grad * act
        for copy in out_copies(i):
            copy.start()
        return carry

    lax.fori_loop(0, chunks, shape_chunk, 0)
    other.wait()
    high, across = min(384, inner), min(512, width)

    def out_tile(i, carry):
        a = pl.ds(pl.multiple_of(i // (width // across) * high, high), high)
        b = pl.ds(pl.multiple_of(i % (width // across) * across, across), across)
        gout[a, b] = dot(shaped_t[a, :], cot[:, :, b].reshape(count, across)).astype(BF16)
        return carry

    lax.fori_loop(0, (inner // high) * (width // across), out_tile, 0)
    save_out = pltpu.make_async_copy(gout, gout_hbm, o_sem.at[0])
    save_out.start()

    def gate_tile(i, carry):
        a = pl.ds(pl.multiple_of(i // 2 * across, across), across)
        b = pl.ds(pl.multiple_of(i % 2 * (inner // 2), inner // 2), inner // 2)
        ggate[a, b] = dot(turned[a, :], grad_gate[:, :, b].reshape(count, inner // 2)).astype(BF16)
        return carry

    lax.fori_loop(0, (width // across) * 2, gate_tile, 0)
    save_gate = pltpu.make_async_copy(ggate, ggate_hbm, o_sem.at[1])
    save_gate.start()

    def saved(i, carry):
        for copy in out_copies(i):
            copy.wait()
        return carry

    lax.fori_loop(0, chunks, saved, 0)
    save_out.wait()
    save_gate.wait()


def gating(ssd, gate, cot, w_out, normed_t, gains, dp):
    chunks, part, inner = ssd.shape
    width, count = normed_t.shape
    cot = cot.reshape(chunks, part, width)
    dma = pltpu.SemaphoreType.DMA
    vmem = pl.BlockSpec(memory_space=pltpu.VMEM)
    hbm = pl.BlockSpec(memory_space=pl.ANY)

    def shape(*dims, kind=BF16):
        return jax.ShapeDtypeStruct(dims, kind)

    def room(*dims, kind=BF16):
        return pltpu.VMEM(dims, kind)

    return pl.pallas_call(
        functools.partial(gating_kernel, dp),
        in_specs=[hbm] * 5 + [vmem],
        out_specs=[hbm] * 5,
        out_shape=[
            shape(chunks, part, inner, kind=F32),
            shape(chunks, part, inner),
            shape(chunks, part, width),
            shape(inner, width),
            shape(width, inner),
        ],
        scratch_shapes=[
            room(chunks, part, inner, kind=F32),
            room(chunks, part, inner, kind=F32),
            room(chunks, part, width),
            room(inner, width),
            room(width, count),
            room(chunks, part, inner, kind=F32),
            room(inner, count),
            room(chunks, part, inner),
            room(chunks, part, width),
            room(inner, width),
            room(width, inner),
            room(chunks, 8, part, kind=F32),
            room(3, chunks, 8, part, kind=F32),
            dma((2,)),
            dma((3, chunks)),
            dma((chunks,)),
            dma((chunks,)),
            dma((chunks,)),
            dma((2,)),
            dma((3,)),
            dma((3,)),
        ],
        compiler_params=pltpu.CompilerParams(
            collective_id=2, has_side_effects=True, vmem_limit_bytes=63 * 2**20
        ),
        cost_estimate=pl.CostEstimate(flops=3 * 10**10, bytes_accessed=5 * 10**7, transcendentals=0),
        name="gating_and_gradients",
    )(ssd, gate, cot, w_out, normed_t, gains)


def tail_kernel(
    dp,
    normed_hbm,
    rows_hbm,
    gates_hbm,
    w_rest_hbm,
    w_gate_hbm,
    tok_hbm,
    cot_hbm,
    gate_hbm,
    gout_hbm,
    proj_ref,
    block_ref,
    gain_ref,
    small_ref,
    tokens_ref,
    grad_ref,
    dots_ref,
    gout_ref,
    gdots_ref,
    taps_ref,
    bias_ref,
    heads_ref,
    out_ref,
    own_ref,
    sums_ref,
    tok,
    cot,
    gate_in,
    gout,
    normed,
    rows_ref,
    gates_ref,
    w_rest,
    w_gate,
    tile,
    wtile,
    btile,
    b_own,
    b_out,
    b_in,
    theirs,
    mine,
    ybuf,
    zbuf,
    final,
    handed,
    core_buf,
    core_out,
    x_buf,
    x_out,
    s_buf,
    l_sem,
    n_sem,
    b_send,
    b_recv,
    y_send,
    y_recv,
    z_send,
    z_recv,
    a_send,
    a_recv,
    c_send,
    c_recv,
    x_send,
    x_recv,
    s_send,
    s_recv,
):
    where = where_am_i(dp)
    d, s, z, y, x, c, peers, deep = where
    tp, rows = out_ref.shape[:2]
    block = tp * rows
    micro, part, width = own_ref.shape
    inner = gates_ref.shape[1]
    bits = dp.bit_length() - 1
    partners = []
    for k in range(bits):
        step = 2**k
        bit = (d // step) % 2
        partners.append(d + step - 2 * step * bit)
    sends = Sends()
    total = OwnerSum(
        where,
        sends,
        None,
        mine,
        ybuf,
        zbuf,
        final,
        (None, y_send, y_recv, z_send, z_recv),
        theirs,
    )
    loads = [
        pltpu.make_async_copy(src, dst, l_sem.at[k])
        for k, (src, dst) in enumerate(
            (
                (rows_hbm, rows_ref),
                (w_rest_hbm, w_rest),
                (gates_hbm, gates_ref),
                (w_gate_hbm, w_gate),
                (tok_hbm, tok),
                (cot_hbm, cot),
                (gate_hbm, gate_in),
                (gout_hbm, gout),
            )
        )
    ]
    fetches = []
    for k in range(deep):
        lines = pl.ds(pl.multiple_of(total.order[k] * 2 * block, 2 * block), 2 * block)
        fetches.append(pltpu.make_async_copy(normed_hbm.at[lines, :], normed.at[k], n_sem.at[k]))
    for copy in loads + fetches:
        copy.start()
    greet(
        [(None, d, p) for p in peers]
        + [(None, d + 1 - 2 * y, s), (z < deep - 1, d + 2, s), (z > 0, d - 2, s)]
        + [(None, partners[k], s) for k in range(2, bits)]
    )

    def arrive(dst, sem):
        push(dst, dst, sem, sem, d, peers[0]).wait_recv()

    sums_ref[0] = small_ref[...]
    sends.start(None, push(small_ref, s_buf.at[0], s_send.at[0], s_recv.at[0], partners[0], s))

    def each(count, work):
        lax.fori_loop(0, count, lambda i, carry: (work(i), carry)[1], 0)

    across = width // tile.shape[1]
    span = wtile.shape[1]

    def product(owner, use):
        def work(i):
            m, n = i // across, i % across
            row = pl.multiple_of((m * tp + owner) * part, part)
            col = pl.multiple_of(n * tile.shape[1], tile.shape[1])
            lines = pl.ds(col, tile.shape[1])
            tile[...] = dot(rows_ref[pl.ds(row, part), :], w_rest[lines, :], NT) + dot(
                gates_ref[pl.ds(row, part), :], w_gate[lines, :], NT
            )
            use(m, lines)

        each(micro * across, work)

    def weight(k):
        fetches[k].wait()
        far = pl.ds(pl.multiple_of((1 - y) * block, block), block)
        near = pl.ds(pl.multiple_of(y * block, block), block)

        def work(n):
            cols = pl.ds(pl.multiple_of(n * span, span), span)
            wtile[...] = dot(normed[k], rows_ref[:, cols])
            theirs[k, :, cols] = wtile[far, :].astype(BF16)
            mine[k, :, cols] = wtile[near, :].astype(BF16)

        lines = pl.ds(inner, 2 * N)
        btile[...] = dot(normed[k], rows_ref[:, lines])
        ours = pl.ds(pl.multiple_of(c * N, N), N)
        b_out[k] = btile[:, pl.ds(pl.multiple_of((1 - c) * N, N), N)].astype(BF16)
        b_own[...] = btile[:, ours]
        swap = push(b_out.at[k], b_in.at[k], b_send.at[k], b_recv.at[k], d, peers[0])
        sends.start(None, swap)
        each(inner // span, work)
        b_tail = dot(normed[k], rows_ref[:, inner + 2 * N :])
        btile[:, N:] = b_tail
        arrive(b_in.at[k], b_recv.at[k])
        btile[:, 0:N] = b_own[...] + b_in[k].astype(F32)
        theirs[k, :, inner:] = btile[far, :].astype(BF16)
        mine[k, :, inner:] = btile[near, :].astype(BF16)
        total.y_items[k][1].start()

    def doubling(k):
        arrive(s_buf.at[k], s_recv.at[k])
        sums_ref[k + 1] = sums_ref[k] + s_buf[k]
        if k + 1 < bits:
            src = sums_ref.at[k + 1]
            sends.start(
                None, push(src, s_buf.at[k + 1], s_send.at[k + 1], s_recv.at[k + 1], partners[k + 1], s)
            )

    def to_core(q):
        def use(m, lines):
            core_out[q, m, :, lines] = tile[...].astype(BF16)

        return use

    def to_chip(m, lines):
        x_out[m, :, lines] = (tile[...] + core_buf[0, m, :, lines].astype(F32)).astype(BF16)

    def keep(m, lines):
        own_ref[m, :, lines] = tile[...] + core_buf[1, m, :, lines].astype(F32)

    for copy in loads[:4]:
        copy.wait()
    product((1 - x) * 2 + 1 - c, to_core(0))
    sends.start(
        None, push(core_out.at[0], core_buf.at[0], c_send.at[0], c_recv.at[0], d, peers[0])
    )
    weight(0)
    arrive(core_buf.at[0], c_recv.at[0])
    product((1 - x) * 2 + c, to_chip)
    sends.start(None, push(x_out, x_buf, x_send.at[0], x_recv.at[0], d, peers[1]))
    weight(1)
    total.add(0)
    total.send(0)
    doubling(0)
    for k in range(2, deep):
        weight(k)
    total.add(1)
    total.send(1)
    doubling(1)
    product(x * 2 + 1 - c, to_core(1))
    sends.start(
        None, push(core_out.at[1], core_buf.at[1], c_send.at[1], c_recv.at[1], d, peers[0])
    )
    for k in range(2, deep - 1):
        total.add(k)
        total.send(k)
        if k < bits:
            doubling(k)
    arrive(core_buf.at[1], c_recv.at[1])
    product(s, keep)
    for k in range(deep - 1, bits):
        doubling(k)
    for r, p in enumerate(peers):
        src, dst = sums_ref.at[bits], sums_ref.at[bits + 1 + s]
        sends.start(None, push(src, dst, s_send.at[bits + r], s_recv.at[bits + r], d, p))
    sums_ref[bits + 1 + s] = sums_ref[bits]
    for copy in loads[4:]:
        copy.wait()
    wide = inner + 2 * N
    heads = inner // P_SIZE
    triple = HEADS // 16
    for b in range(4):
        seat = 2 * (b % 2) + b // 2
        for k in range(4):
            at = (4 * k + b) * STRIPE
            grad_ref[:, at : at + STRIPE] = gate_in[seat, :, k * STRIPE : (k + 1) * STRIPE].astype(F32)
    gout_ref[...] = gout[...].astype(F32)
    gdots_ref[...] = jnp.sum(gout_ref[...] * block_ref[...].astype(F32), axis=1, keepdims=True)
    for r, p in enumerate(peers):
        arrive(sums_ref.at[bits + 1 + p], s_recv.at[bits + r])
    chan = taps_ref.shape[1]
    convs = jnp.zeros((8, chan), F32)
    per_head = jnp.zeros((8, HEADS), F32)
    v = lax.broadcasted_iota(jnp.int32, (wide, chan), 0)
    g = lax.broadcasted_iota(jnp.int32, (wide, chan), 1) + chan * (d * tp + s)
    lane = lax.broadcasted_iota(jnp.int32, (LANES, HEADS), 0)
    head = lax.broadcasted_iota(jnp.int32, (LANES, HEADS), 1)
    place = []
    for p in range(tp):
        b = 2 * (p % 2) + p // 2
        from_v = jnp.where(v < inner, v + 3 * STRIPE * hop(v, STRIPE) + STRIPE * b, v - inner + DI)
        sums = sums_ref[bits + 1 + p]
        convs = convs + dot(sums[:, :wide], jnp.where(from_v == g, 1.0, 0.0), precision=HIGH)
        hit = jnp.logical_and(lane < heads, head == lane + 3 * triple * hop(lane, triple) + triple * b)
        place.append(jnp.where(hit, 1.0, 0.0))
        per_head = per_head + dot(sums[:, wide:], place[p], precision=HIGH)
    taps_ref[...] = convs[:KW]
    bias_ref[...] = convs[KW : KW + 1]
    heads_ref[...] = per_head
    total.add(deep - 1)
    total.finish()
    for p in range(tp):
        handed[p] = final[p * rows : (p + 1) * rows, :]
    for r, p in enumerate(peers):
        sends.start(None, push(handed.at[p], out_ref.at[s], a_send.at[r], a_recv.at[r], d, p))
    out_ref[s] = handed[s]

    arrive(x_buf, x_recv.at[0])

    def last(i):
        m, row = i // (part // 16), (i % (part // 16)) * 16
        lines = pl.ds(pl.multiple_of(row, 16), 16)
        h = tok[m, lines, :].astype(F32)
        r = lax.rsqrt(jnp.mean(h * h, axis=-1, keepdims=True) + EPSILON)
        n = h * r
        grad = (own_ref[m, lines, :] + x_buf[m, lines, :].astype(F32)) * gain_ref[KW + 1 : KW + 2, :]
        grad = grad - n * jnp.mean(grad * n, axis=-1, keepdims=True)
        tokens_ref[m, lines, :] = (cot[m, lines, :].astype(F32) + r * grad).astype(BF16)

    each(micro * (part // 16), last)
    for r, p in enumerate(peers):
        arrive(out_ref.at[p], a_recv.at[r])
    both = [jnp.zeros((rows, N), F32), jnp.zeros((rows, N), F32)]
    steps = jnp.zeros((rows, HEADS), F32)
    for b in range(4):
        seat = 2 * (b % 2) + b // 2
        for k in range(4):
            at = DI + (4 * k + b) * STRIPE
            piece = out_ref[seat, :, k * STRIPE : (k + 1) * STRIPE]
            grad_ref[:, at : at + STRIPE] = piece.astype(F32)
        both[seat % 2] = both[seat % 2] + out_ref[seat, :, inner : inner + N].astype(F32)
        steps = steps + dot(out_ref[seat, :, inner + N :], place[seat].astype(BF16))
    grad_ref[:, 2 * DI : 2 * DI + N] = both[0]
    grad_ref[:, 2 * DI + N : 2 * DI + 2 * N] = both[1]
    grad_ref[:, 2 * DI + 2 * N :] = steps
    dots_ref[...] = jnp.sum(grad_ref[...] * proj_ref[...].astype(F32), axis=1, keepdims=True)
    sends.drain()


def tail(
    normed_t, rows_grad, gates_grad, w_rest, w_gate, tokens, cotangent, gate_in, gout, in_proj, out_proj, gains, small, chan, dp
):
    width, count = normed_t.shape
    micro = tokens.shape[0]
    tp = gate_in.shape[0]
    full = gates_grad.shape[1] + N + LANES
    rows = width // dp // tp
    part = count // micro // tp
    deep = dp // 2
    bits = dp.bit_length() - 1
    block = tp * rows
    dma = pltpu.SemaphoreType.DMA
    vmem = pl.BlockSpec(memory_space=pltpu.VMEM)
    hbm = pl.BlockSpec(memory_space=pl.ANY)
    return pl.pallas_call(
        functools.partial(tail_kernel, dp),
        in_specs=[hbm] * 9 + [vmem] * 4,
        out_specs=[vmem] * 8,
        out_shape=[
            jax.ShapeDtypeStruct(tokens.shape, BF16),
            jax.ShapeDtypeStruct(in_proj.shape, F32),
            jax.ShapeDtypeStruct((rows, 1), F32),
            jax.ShapeDtypeStruct(gout.shape, F32),
            jax.ShapeDtypeStruct((gout.shape[0], 1), F32),
            jax.ShapeDtypeStruct((KW, chan), F32),
            jax.ShapeDtypeStruct((1, chan), F32),
            jax.ShapeDtypeStruct((8, HEADS), F32),
        ],
        scratch_shapes=[
            pltpu.VMEM((tp, rows, full), BF16),
            pltpu.VMEM((micro, part, width), F32),
            pltpu.VMEM((bits + 1 + tp,) + small.shape, F32),
            pltpu.VMEM(tokens.shape, BF16),
            pltpu.VMEM(tokens.shape, BF16),
            pltpu.VMEM(gate_in.shape, BF16),
            pltpu.VMEM(gout.shape, BF16),
            pltpu.VMEM((deep, 2 * block, count), BF16),
            pltpu.VMEM(rows_grad.shape, BF16),
            pltpu.VMEM(gates_grad.shape, BF16),
            pltpu.VMEM(w_rest.shape, BF16),
            pltpu.VMEM(w_gate.shape, BF16),
            pltpu.VMEM((part, min(width, 512)), F32),
            pltpu.VMEM((2 * block, 384), F32),
            pltpu.VMEM((2 * block, 2 * N), F32),
            pltpu.VMEM((2 * block, N), F32),
            pltpu.VMEM((deep, 2 * block, N), BF16),
            pltpu.VMEM((deep, 2 * block, N), BF16),
            pltpu.VMEM((deep, block, full), BF16),
            pltpu.VMEM((deep, block, full), BF16),
            pltpu.VMEM((deep, block, full), BF16),
            pltpu.VMEM((2, deep - 1, block, full), BF16),
            pltpu.VMEM((block, full), BF16),
            pltpu.VMEM((tp, rows, full), BF16),
            pltpu.VMEM((2, micro, part, width), BF16),
            pltpu.VMEM((2, micro, part, width), BF16),
            pltpu.VMEM((micro, part, width), BF16),
            pltpu.VMEM((micro, part, width), BF16),
            pltpu.VMEM((bits,) + small.shape, F32),
            dma((8,)),
            dma((deep,)),
            dma((deep,)),
            dma((deep,)),
            dma((deep,)),
            dma((deep,)),
            dma((2, deep - 1)),
            dma((2, deep - 1)),
            dma((3,)),
            dma((3,)),
            dma((2,)),
            dma((2,)),
            dma((1,)),
            dma((1,)),
            dma((bits + 3,)),
            dma((bits + 3,)),
        ],
        compiler_params=pltpu.CompilerParams(
            collective_id=3, has_side_effects=True, vmem_limit_bytes=62 * 2**20
        ),
        cost_estimate=pl.CostEstimate(flops=6 * 10**10, bytes_accessed=3 * 10**7, transcendentals=0),
        name="gradients_to_owners",
    )(
        normed_t,
        rows_grad,
        gates_grad,
        w_rest,
        w_gate,
        tokens,
        cotangent,
        gate_in,
        gout,
        in_proj,
        out_proj,
        gains,
        small,
    )


def body(
    tokens,
    in_proj,
    conv_weight,
    conv_bias,
    decay_log,
    step_bias,
    skip_gain,
    norm_gain,
    gated_gain,
    out_proj,
    cotangent,
):
    dp, tp = lax.axis_size("dp"), lax.axis_size("seq")
    s = lax.axis_index("seq")
    micro, part, width = tokens.shape
    heads = HEADS // tp
    inner = heads * P_SIZE
    rows = in_proj.shape[0]
    length = part * tp
    count = micro * length
    wide = inner + 2 * N
    chan = conv_bias.shape[0]

    per_head = jnp.pad(jnp.stack([decay_log, step_bias, skip_gain]), ((0, 5), (0, 0)))
    (
        normed,
        normed_t,
        proj_rest,
        ssd,
        memory,
        gate,
        w_rest,
        w_gate,
        w_out,
        cot,
        taps,
        gains,
        g_gated,
        per_head,
    ) = head(
        in_proj,
        conv_weight,
        conv_bias[None],
        norm_gain[None],
        gated_gain[None],
        per_head,
        tokens,
        cotangent,
        out_proj,
        dp,
        tp,
    )
    proj_rest = proj_rest.reshape(count, wide + LANES)
    w_rest = w_rest.reshape(width, wide + LANES)
    w_gate = w_gate.reshape(width, inner)
    grad_ssd, grad_gate, out_part, grad_out, gate_in = gating(
        ssd, gate, cot, w_out.reshape(inner, width), normed_t, g_gated, dp
    )
    grad_ssd = grad_ssd.reshape(count, inner)
    grad_gate = grad_gate.reshape(count, inner)
    grad_rest, wgrad, hgrad, out_part, grad_out, gate_in = middle(
        proj_rest,
        grad_ssd,
        memory,
        taps,
        per_head,
        out_part.reshape(micro, length, width),
        grad_out.reshape(dp, -1, width),
        gate_in.reshape(dp, tp, rows, inner),
        tokens,
        dp,
        tp,
        heads,
        micro,
    )
    small = jnp.concatenate([wgrad, hgrad], axis=1)
    tokens_grad, in_grad, dots, grad_out, gdots, conv_grad, bias_grad, head_grads = tail(
        normed_t,
        grad_rest,
        grad_gate,
        w_rest,
        w_gate,
        tokens,
        cotangent,
        gate_in,
        grad_out,
        in_proj,
        out_proj,
        gains,
        small,
        chan,
        dp,
    )
    return (
        out_part,
        tokens_grad,
        in_grad,
        conv_grad,
        bias_grad[0],
        head_grads[0],
        head_grads[1],
        head_grads[2],
        dots[:, 0] / norm_gain.astype(F32),
        gdots[:, 0] / gated_gain.astype(F32),
        grad_out,
    )


def solution(mesh):
    both = ("dp", "seq")
    return jax.shard_map(
        body,
        mesh=mesh,
        in_specs=(
            P("dp", "seq", None),
            P(both, None),
            P(None, both),
            P(both),
            P(),
            P(),
            P(),
            P(both),
            P(both),
            P(both, None),
            P("dp", "seq", None),
        ),
        out_specs=(
            P("dp", "seq", None),
            P("dp", "seq", None),
            P(both, None),
            P(None, both),
            P(both),
            P(),
            P(),
            P(),
            P(both),
            P(both),
            P(both, None),
        ),
        check_vma=False,
    )
```

```python
import functools

import jax
import jax.numpy as jnp
from jax import lax
from jax.experimental import pallas as pl
from jax.experimental.pallas import tpu as pltpu
from jax.sharding import PartitionSpec as P

HEADS = 48
P_SIZE = 64
N = 128
KW = 4
DI = 3072
CD = 3328
LANES = 128
FAR = -1e30

EPSILON = 1e-05
F32 = jnp.float32
BF16 = jnp.bfloat16


def dot(a, b, dims=((1,), (0,)), precision=None):
    return lax.dot_general(a, b, (dims, ((), ())), precision=precision, preferred_element_type=F32)


NT = ((1,), (1,))
HIGH = lax.Precision.HIGHEST


def pick(a, p, low):
    return jnp.where(low, a[:, 2 * p : 2 * p + 1], a[:, 2 * p + 1 : 2 * p + 2])


def chunk_parts(heads, rest_ref, xbuf, taps_ref, head_ref):
    size = rest_ref.shape[0]
    wide = taps_ref.shape[1]
    mixed = taps_ref[KW : KW + 1, :] + taps_ref[0:1, :] * xbuf[5 : 5 + size, :]
    for k in range(1, KW):
        mixed = mixed + taps_ref[k : k + 1, :] * xbuf[5 + k : 5 + k + size, :]
    sig = lax.logistic(mixed)
    return (mixed, sig) + step_parts(heads, rest_ref, taps_ref, head_ref)


def step_parts(heads, rest_ref, taps_ref, head_ref):
    size = rest_ref.shape[0]
    wide = taps_ref.shape[1]
    lane = lax.broadcasted_iota(jnp.int32, (1, LANES), 1)
    raw = jnp.where(lane < heads, rest_ref[:, wide:], 0.0) + head_ref[1:2, :]
    step = jnp.maximum(raw, 0.0) + jnp.log1p(jnp.exp(-jnp.abs(raw)))
    decay = -jnp.exp(head_ref[0:1, :]) * step
    i = lax.broadcasted_iota(jnp.int32, (size, size), 0)
    j = lax.broadcasted_iota(jnp.int32, (size, size), 1)
    run = dot(jnp.where(i >= j, 1.0, 0.0), decay, precision=HIGH)
    return raw, step, decay, run


def backward_kernel(
    heads,
    rest_ref,
    prev_ref,
    dy_ref,
    mem_ref,
    taps_ref,
    head_ref,
    out_ref,
    wgrad_ref,
    hgrad_ref,
    xbuf,
    gbuf,
    adj,
    dmix,
    dsum,
    uprod,
    zprod,
    rows_t,
    line,
    acts,
    slopes,
):
    size = rest_ref.shape[0]
    wide = taps_ref.shape[1]
    inner = heads * P_SIZE
    chunks = pl.num_programs(1)
    step_id = pl.program_id(1)
    newest = step_id == 0
    oldest = step_id == chunks - 1
    begin = jnp.logical_and(pl.program_id(0) == 0, newest)
    finish = jnp.logical_and(pl.program_id(0) == pl.num_programs(0) - 1, oldest)

    @pl.when(begin)
    def _():
        wgrad_ref[...] = jnp.zeros_like(wgrad_ref)
        hgrad_ref[...] = jnp.zeros_like(hgrad_ref)
        rows_t[...] = jnp.zeros_like(rows_t)
        line[...] = jnp.zeros_like(line)

    @pl.when(newest)
    def _():
        gbuf[size : size + 8, :] = jnp.zeros((8, wide), F32)
        adj[...] = jnp.zeros_like(adj)

    @pl.when(jnp.logical_not(newest))
    def _():
        gbuf[size : size + 8, :] = gbuf[0:8, :]

    xbuf[0:8, :] = jnp.where(oldest, 0.0, prev_ref[:, :wide])
    xbuf[8 : 8 + size, :] = rest_ref[:, :wide]
    for n in range(wide // LANES):
        at = slice(n * LANES, (n + 1) * LANES)
        mixed = taps_ref[KW : KW + 1, at] + taps_ref[0:1, at] * xbuf[5 : 5 + size, at]
        for k in range(1, KW):
            mixed = mixed + taps_ref[k : k + 1, at] * xbuf[5 + k : 5 + k + size, at]
        sig = lax.logistic(mixed)
        acts[:, at] = mixed * sig
        slopes[:, at] = sig * (1.0 + mixed * (1.0 - sig))
    raw, step, decay, run = step_parts(heads, rest_ref, taps_ref, head_ref)
    run_t = run.T
    closing = run[size - 1 : size, :]
    last = jnp.exp(closing)
    left = jnp.exp(closing - run)
    grown = jnp.exp(run)
    b = acts[:, inner : inner + N].astype(BF16)
    c = acts[:, inner + N :].astype(BF16)
    c_t = acts[:, inner + N :].T.astype(BF16)
    scores_t = dot(b, c, NT)
    low = lax.broadcasted_iota(jnp.int32, (1, LANES), 1) < P_SIZE
    lane = lax.broadcasted_iota(jnp.int32, (1, LANES), 1)
    j = lax.broadcasted_iota(jnp.int32, (size, size), 0)
    i = lax.broadcasted_iota(jnp.int32, (size, size), 1)
    causal = i >= j
    mem_b = mem_ref[0]
    adj_b = adj[...].astype(BF16)
    spread = dot(b, adj_b)
    inherit = dot(c, mem_b)
    scored = jnp.zeros((size, size), F32)
    cols = jnp.zeros((size, LANES), F32)
    for p in range(heads // 2):
        at = slice(p * LANES, (p + 1) * LANES)
        v = acts[:, at]
        size_p = pick(step, p, low)
        xv = size_p * v
        dy = dy_ref[:, at]
        dyb = dy.astype(BF16)
        xvb = xv.astype(BF16)
        dxv = pick(left, p, low) * spread[:, at]
        zprod[:, at] = (dxv * xv).astype(BF16)
        dyg = pick(grown, p, low) * dy
        uprod[:, at] = (dyg * inherit[:, at]).astype(BF16)
        for e in range(2):
            h = 2 * p + e
            keep = low if e == 0 else jnp.logical_not(low)
            mine = jnp.where(keep, dy, 0.0).astype(BF16)
            gap = run_t[h : h + 1, :] - run[:, h : h + 1]
            near = jnp.exp(jnp.where(causal, gap, FAR))
            w_t = scores_t * near
            dw_t = dot(xvb, mine, NT)
            scored = scored + dw_t * near
            g_t = dw_t * w_t
            rows_t[h : h + 1, :] = jnp.sum(g_t, axis=0, keepdims=True)
            cols = jnp.where(lane == h, jnp.sum(g_t, axis=1, keepdims=True), cols)
            dxv = dxv + dot(w_t.astype(BF16), mine)
        dsum[:, at] = (dxv * v).astype(BF16)
        dmix[:, at] = size_p * dxv + pick(head_ref[2:3, :], p, low) * dy
        line[0:1, at] += jnp.sum(dy * v, axis=0, keepdims=True)
        line[1:2, at] = jnp.sum(adj[:, at] * mem_b[:, at].astype(F32), axis=0, keepdims=True) * pick(
            last, p, low
        )
        xc = (pick(left, p, low) * xv).astype(BF16)
        dygb = dyg.astype(BF16)
        db = dot(xc, adj_b[:, at], NT)
        dc = dot(dygb, mem_b[:, at], NT)
        if p == 0:
            dmix[:, inner : inner + N] = db
            dmix[:, inner + N :] = dc
        else:
            dmix[:, inner : inner + N] += db
            dmix[:, inner + N :] += dc
        adj[:, at] = adj[:, at] * pick(last, p, low) + dot(c_t, dygb)
    dmix[:, inner : inner + N] += dot(scored.astype(BF16), c)
    dmix[:, inner + N :] += dot(scored.T.astype(BF16), b)

    group = jnp.where(
        lax.broadcasted_iota(jnp.int32, (inner, LANES), 0) // P_SIZE
        == lax.broadcasted_iota(jnp.int32, (inner, LANES), 1),
        1.0,
        0.0,
    )
    group_b = group.astype(BF16)
    d_step = dot(dsum[...], group_b)
    u = dot(uprod[...], group_b)
    z = dot(zprod[...], group_b)
    sums = dot(line[...], group, precision=HIGH)
    d_run = rows_t[...].T - cols + u - z
    row = lax.broadcasted_iota(jnp.int32, (size, 1), 0)
    ending = sums[1:2, :] + jnp.sum(z, axis=0, keepdims=True)
    d_run = d_run + jnp.where(row == size - 1, ending, 0.0)
    d_decay = dot(jnp.where(causal, 1.0, 0.0), d_run, precision=HIGH)
    d_raw = (d_step - jnp.exp(head_ref[0:1, :]) * d_decay) * lax.logistic(raw)
    d_raw = jnp.where(lane < heads, d_raw, 0.0)
    hgrad_ref[0:1, :] += jnp.sum(d_decay * decay, axis=0, keepdims=True)
    hgrad_ref[1:2, :] += jnp.sum(d_raw, axis=0, keepdims=True)

    @pl.when(finish)
    def _():
        hgrad_ref[2:3, :] = sums[0:1, :]

    for n in range(wide // LANES):
        at = slice(n * LANES, (n + 1) * LANES)
        g = dmix[:, at] * slopes[:, at]
        gbuf[0:size, at] = g
        wgrad_ref[KW : KW + 1, at] += jnp.sum(g, axis=0, keepdims=True)
        for k in range(KW):
            lag = xbuf[5 + k : 5 + k + size, at]
            wgrad_ref[k : k + 1, at] += jnp.sum(g * lag, axis=0, keepdims=True)
        back = taps_ref[KW - 1 : KW, at] * g
        for k in range(KW - 1):
            back = back + taps_ref[k : k + 1, at] * gbuf[3 - k : 3 - k + size, at]
        out_ref[:, at] = back.astype(BF16)
    out_ref[:, wide:] = d_raw.astype(BF16)


MESH = pl.DeviceIdType.MESH


def where_am_i(dp):
    d, s = lax.axis_index("dp"), lax.axis_index("seq")
    z, y = d // 2, d % 2
    x, c = s // 2, s % 2
    peers = [s + 1 - 2 * c, s + 2 - 4 * x, 3 - s]
    return d, s, z, y, x, c, peers, dp // 2


def push(src, dst, send_sem, recv_sem, d, s):
    return pltpu.make_async_remote_copy(
        src_ref=src,
        dst_ref=dst,
        send_sem=send_sem,
        recv_sem=recv_sem,
        device_id={"dp": d, "seq": s},
        device_id_type=MESH,
    )


def greet(partners):
    barrier = pltpu.get_barrier_semaphore()
    for cond, d, s in partners:

        def hello(d=d, s=s):
            pl.semaphore_signal(barrier, inc=1, device_id={"dp": d, "seq": s}, device_id_type=MESH)

        if cond is None:
            hello()
        else:
            pl.when(cond)(hello)
    count = 0
    for cond, _, _ in partners:
        count = count + (1 if cond is None else jnp.where(cond, 1, 0))
    pl.semaphore_wait(barrier, count)


class Sends:
    def __init__(self):
        self.items = []

    def start(self, cond, copy):
        if cond is None:
            copy.start()
        else:
            pl.when(cond)(copy.start)
        self.items.append((cond, copy))

    def drain(self):
        for cond, copy in self.items:
            if cond is None:
                copy.wait_send()
            else:
                pl.when(cond)(copy.wait_send)


STRIPE = DI // 16


def swapped(s):
    return 2 * (s % 2) + s // 2


def stripe_owner(block, dp):
    u = dp // 4
    return block // (4 * u) * u + block % u


def stripe_seat(block, dp):
    return swapped(block // (dp // 4) % 4)


def stripe_block(d, s, dp):
    u = dp // 4
    return (d // u * 4 + swapped(s)) * u + d % u


def forward_chunk(heads, first, rest_ref, taps_ref, head_ref, ssd_ref, mem_ref, xbuf, mem):
    size = rest_ref.shape[0]
    wide = taps_ref.shape[1]
    inner = heads * P_SIZE

    @pl.when(first)
    def _():
        xbuf[0:8, :] = jnp.zeros((8, wide), F32)
        mem[...] = jnp.zeros_like(mem)

    @pl.when(jnp.logical_not(first))
    def _():
        xbuf[0:8, :] = xbuf[size : size + 8, :]

    xbuf[8 : 8 + size, :] = rest_ref[:, :wide]
    mixed, sig, _, step, _, run = chunk_parts(heads, rest_ref, xbuf, taps_ref, head_ref)
    act = mixed * sig
    run_t = run.T
    closing = run[size - 1 : size, :]
    last = jnp.exp(closing)
    left = jnp.exp(closing - run)
    grown = jnp.exp(run)
    b = act[:, inner : inner + N]
    c = act[:, inner + N :].astype(BF16)
    scores = dot(c, b.astype(BF16), NT)
    b_t = b.T.astype(BF16)
    mem_ref[...] = mem[...].astype(BF16)
    inter = dot(c, mem[...].astype(BF16))
    low = lax.broadcasted_iota(jnp.int32, (1, LANES), 1) < P_SIZE
    i = lax.broadcasted_iota(jnp.int32, (size, size), 0)
    j = lax.broadcasted_iota(jnp.int32, (size, size), 1)
    causal = i >= j
    for p in range(heads // 2):
        at = slice(p * LANES, (p + 1) * LANES)
        v = act[:, at]
        xv = pick(step, p, low) * v
        y = pick(head_ref[2:3, :], p, low) * v + pick(grown, p, low) * inter[:, at]
        for e in range(2):
            h = 2 * p + e
            gap = run[:, h : h + 1] - run_t[h : h + 1, :]
            w = (scores * jnp.exp(jnp.where(causal, gap, FAR))).astype(BF16)
            mine = jnp.where(low if e == 0 else jnp.logical_not(low), xv, 0.0).astype(BF16)
            y = y + dot(w, mine)
        ssd_ref[:, at] = y
        xc = (pick(left, p, low) * xv).astype(BF16)
        mem[:, at] = mem[:, at] * pick(last, p, low) + dot(b_t, xc)


def hop(v, size):
    return sum(jnp.where(v >= q * size, 1, 0) for q in range(1, 4))


def head_kernel(
    dp,
    heads,
    proj_ref,
    cw_ref,
    cb_ref,
    ng_ref,
    gg_ref,
    ph_ref,
    tok_ref,
    cot_ref,
    block_ref,
    normed_hbm,
    turned_hbm,
    proj_hbm,
    ssd_hbm,
    mem_hbm,
    gates_hbm,
    rest_hbm,
    gate_hbm,
    out_hbm,
    cot_hbm,
    taps_ref,
    gain_ref,
    gated_ref,
    head_ref,
    line,
    small_stage,
    val_stage,
    half_stage,
    gate_stage,
    small_all,
    val_in,
    half_in,
    gate_in,
    w_val,
    w_half,
    w_other,
    w_tail,
    w_gate,
    out_shard,
    tok,
    flipped,
    proj,
    ssd,
    gates,
    memory,
    xbuf,
    mem,
    l_sem,
    o_sem,
    f_sem,
    p_sem,
    g_sem,
    a_send,
    a_recv,
    z_send,
    z_recv,
    y_send,
    y_recv,
    t_send,
    t_recv,
):
    d, s, z, y, x, c, peers, deep = where_am_i(dp)
    tp, rows = val_stage.shape[:2]
    micro, part, width = tok_ref.shape
    total = dp * tp
    inner = heads * P_SIZE
    wide = inner + 2 * N
    chan, gpiece = cw_ref.shape[1], gg_ref.shape[1]
    up, down, far = d + 2, d - 2, d + 1 - 2 * y
    me = d * tp + s
    to_d, to_s, turned = stripe_owner(me, dp), stripe_seat(me, dp), stripe_block(d, s, dp)
    from_d, from_s = turned // tp, turned % tp
    moves = turned != me

    triple = HEADS // 16
    line[...] = jnp.zeros_like(line)
    line[0:KW, 0:chan] = cw_ref[...].astype(F32)
    line[KW : KW + 1, 0:chan] = cb_ref[...].astype(F32)
    line[KW + 1 : KW + 2, 0:rows] = ng_ref[...].astype(F32)
    line[KW + 2 : KW + 3, 0:gpiece] = gg_ref[...].astype(F32)
    raw = proj_ref[:, 2 * DI + 2 * N :]
    for b in range(4):
        seat = 2 * (b % 2) + b // 2
        for k in range(4):
            to, at = k * STRIPE, (4 * k + b) * STRIPE
            gate_stage[seat, :, to : to + STRIPE] = proj_ref[:, at : at + STRIPE]
            val_stage[seat, :, to : to + STRIPE] = proj_ref[:, DI + at : DI + at + STRIPE]
        at = 2 * DI + N * (seat % 2)
        half_stage[seat] = proj_ref[:, at : at + N]
        v = lax.broadcasted_iota(jnp.int32, (16, HEADS), 0)
        g = lax.broadcasted_iota(jnp.int32, (16, HEADS), 1)
        hit = jnp.logical_and(v < heads, g == v + 3 * triple * hop(v, triple) + triple * b)
        line[16:32, 0:rows] = dot(jnp.where(hit, 1.0, 0.0).astype(BF16), raw, NT)
        small_stage[seat] = line[...].astype(BF16)
    v = lax.broadcasted_iota(jnp.int32, (HEADS, LANES), 1)
    g = lax.broadcasted_iota(jnp.int32, (HEADS, LANES), 0)
    hit = jnp.logical_and(v < heads, g == v + 3 * triple * hop(v, triple) + triple * swapped(s))
    head_ref[...] = dot(ph_ref[...], jnp.where(hit, 1.0, 0.0), precision=HIGH)

    greet(
        [(None, d, p) for p in peers]
        + [(None, far, s), (z < deep - 1, up, s), (z > 0, down, s)]
        + [(moves, to_d, to_s), (moves, from_d, from_s)]
    )
    sends = Sends()

    def arrive(dst, sem):
        push(dst, dst, sem, sem, d, peers[0]).wait_recv()

    def mine(ref, k):
        return ref.at[:, pl.ds(k * part, part), :]

    def exchange(a, stage, target):
        for r, p in enumerate(peers):
            sends.start(
                None, push(stage.at[p], target(s), a_send.at[a, r], a_recv.at[a, r], d, p)
            )

    def exchanged(a, target):
        for r, p in enumerate(peers):
            arrive(target(p), a_recv.at[a, r])

    exchange(0, small_stage, lambda k: small_all.at[d, k])
    exchange(1, half_stage, lambda k: half_in.at[k])
    exchange(2, val_stage, lambda k: val_in.at[k])
    exchange(3, gate_stage, lambda k: gate_in.at[k])
    sends.start(moves, push(block_ref, out_shard, t_send.at[2], t_recv.at[2], to_d, to_s))
    sends.start(None, push(tok_ref, mine(tok, s), t_send.at[0], t_recv.at[0], d, peers[1]))
    sends.start(None, push(tok_ref, mine(tok, s), t_send.at[1], t_recv.at[1], d, peers[0]))
    sends.start(None, push(cot_ref, mine(cot_hbm, s), t_send.at[3], t_recv.at[3], d, peers[1]))
    sends.start(None, push(cot_ref, mine(cot_hbm, s), t_send.at[4], t_recv.at[4], d, peers[0]))
    saves = []

    def save(src, dst):
        copy = pltpu.make_async_copy(src, dst, l_sem.at[len(saves)])
        copy.start()
        saves.append(copy)

    save(cot_ref, mine(cot_hbm, s))
    small_all[d, s] = small_stage[s]
    half_in[s] = half_stage[s]
    val_in[s] = val_stage[s]
    gate_in[s] = gate_stage[s]
    tok[:, pl.ds(pl.multiple_of(s * part, part), part), :] = tok_ref[...]

    @pl.when(jnp.logical_not(moves))
    def _():
        out_shard[...] = block_ref[...]

    def begin(a, shard, dst):
        block = dst.at[d]
        sends.start(z < deep - 1, push(shard, block, z_send.at[a, 0, 0], z_recv.at[a, 0, 0], up, s))
        sends.start(z > 0, push(shard, block, z_send.at[a, 1, 0], z_recv.at[a, 1, 0], down, s))
        sends.start(None, push(shard, block, y_send.at[a, 0, 0], y_recv.at[a, 0, 0], far, s))

    def plan(a, dst, t):
        steps = []
        for way in range(2):
            here = (z >= t) if way == 0 else (z + t <= deep - 1)
            more = jnp.logical_and(here, (z < deep - 1) if way == 0 else (z > 0))
            at = jnp.clip(d - 2 * t if way == 0 else d + 2 * t, 0, dp - 1)
            block = dst.at[at]
            got = z_recv.at[a, way, t - 1]
            on = []
            if t < deep - 1:
                nxt = up if way == 0 else down
                on.append(
                    (more, push(block, block, z_send.at[a, way, t], z_recv.at[a, way, t], nxt, s))
                )
            on.append(
                (here, push(block, block, y_send.at[a, way, t], y_recv.at[a, way, t], far, s))
            )
            steps.append((here, push(block, block, got, got, d, peers[0]), on))
        return steps

    def run(steps):
        for here, wait, on in steps:
            pl.when(here)(wait.wait_recv)
            for cond, copy in on:
                pl.when(cond)(copy.start)

    def remember(steps):
        for _, _, on in steps:
            sends.items.extend(on)

    def relay(a, dst, t):
        steps = plan(a, dst, t)
        run(steps)
        remember(steps)

    def landed(a, dst):
        arrive(dst.at[far], y_recv.at[a, 0, 0])
        for t in range(1, deep):
            for way in range(2):
                here = (z >= t) if way == 0 else (z + t <= deep - 1)
                at = jnp.clip(far - 2 * t if way == 0 else far + 2 * t, 0, dp - 1)
                pl.when(here)(functools.partial(arrive, dst.at[at], y_recv.at[a, way, t]))

    def shard_of(a, pieces, dst):
        exchanged(a, lambda p: pieces.at[p])
        for k in range(tp):
            dst[d, k * rows : (k + 1) * rows, :] = pieces[k]
        begin(a, dst.at[d], dst)

    exchanged(0, lambda p: small_all.at[d, p])
    begin(0, small_all.at[d], small_all)
    shard_of(1, half_in, w_half)
    shard_of(2, val_in, w_val)
    for t in range(1, deep):
        relay(0, small_all, t)
        relay(1, w_half, t)
        relay(2, w_val, t)
    shard_of(3, gate_in, w_gate)
    pl.when(moves)(functools.partial(arrive, out_shard, t_recv.at[2]))
    begin(4, out_shard, out_hbm)
    save(out_shard, out_hbm.at[d])

    landed(0, small_all)

    def one_hot(columns, index, k, length):
        lane = lax.broadcasted_iota(jnp.int32, (LANES, columns), 1)
        at = lax.broadcasted_iota(jnp.int32, (LANES, columns), 0)
        hit = jnp.logical_and(at < length, index(lane) == k * length + at)
        return jnp.where(hit, 1.0, 0.0).astype(BF16)

    taps_ref[...] = jnp.zeros_like(taps_ref)
    gain_ref[...] = jnp.zeros_like(gain_ref)
    gated_ref[...] = jnp.zeros_like(gated_ref)

    def striped(v):
        return v + 3 * STRIPE * hop(v, STRIPE) + STRIPE * swapped(s)

    def lay_out(dd, carry):
        for kk in range(tp):
            k = dd * tp + kk
            values = small_all[dd, kk, 0:16, :]
            chans = one_hot(wide, lambda v: jnp.where(v < inner, striped(v), v - inner + DI), k, chan)
            taps_ref[...] += dot(values, chans)[:8]
            gain_ref[...] += dot(values, one_hot(width, lambda v: v, k, rows))
            gated_ref[...] += dot(values, one_hot(inner, striped, k, gpiece))
            turned = jnp.concatenate(
                [small_all[dd, kk, 16:32, :].astype(F32), jnp.zeros((LANES - 16, LANES), F32)], axis=0
            ).T
            w_tail[dd, kk * rows : (kk + 1) * rows, 2 * N :] = turned[:rows].astype(BF16)
        return carry

    lax.fori_loop(0, dp, lay_out, 0)
    landed(1, w_half)
    sends.start(None, push(w_half, w_other, t_send.at[6], t_recv.at[6], d, peers[0]))
    landed(2, w_val)
    save(w_val, rest_hbm.at[:, :, pl.ds(0, inner)])
    arrive(w_other, t_recv.at[6])

    def both_halves(dd, carry):
        w_tail[dd, :, pl.ds(pl.multiple_of(c * N, N), N)] = w_half[dd]
        w_tail[dd, :, pl.ds(pl.multiple_of((1 - c) * N, N), N)] = w_other[dd]
        return carry

    lax.fori_loop(0, dp, both_halves, 0)
    save(w_tail, rest_hbm.at[:, :, pl.ds(inner, w_tail.shape[2])])
    arrive(mine(tok, peers[1]), t_recv.at[0])
    block = mine(tok, peers[1])
    hand = push(block, block, t_send.at[5], t_recv.at[5], d, peers[0])
    hand.start()
    relay(3, w_gate, 1)
    relay(4, out_hbm, 1)
    arrive(mine(tok, peers[0]), t_recv.at[1])
    arrive(mine(tok, peers[2]), t_recv.at[5])
    hand.wait_send()

    tasks = [(a, ref, t) for t in range(2, deep) for a, ref in ((3, w_gate), (4, out_hbm))]
    chunks = micro * tp
    when = {}
    for n, task in enumerate(tasks):
        when.setdefault(min(n * 4 // len(tasks), chunks - 1), []).append(plan(*task))
    for plans in when.values():
        for steps in plans:
            remember(steps)

    def columns(i):
        return pl.ds(pl.multiple_of(i * part, part), part)

    def chunk(i, carry):
        m, k = i // tp, i % tp
        lines = pl.ds(pl.multiple_of(k * part, part), part)
        h = tok[m, lines, :].astype(F32)
        r = lax.rsqrt(jnp.mean(h * h, axis=-1, keepdims=True) + EPSILON)
        value = h * r * gain_ref[5:6, :]
        tok[m, lines, :] = value.astype(BF16)
        flipped[i] = value.T.astype(BF16)
        proj[i, :, 0:inner] = dot(tok[m, lines, :], w_val[...].reshape(width, inner))
        proj[i, :, inner:] = dot(tok[m, lines, :], w_tail[...].reshape(width, w_tail.shape[2]))
        forward_chunk(
            heads, k == 0, proj.at[i], taps_ref, head_ref, ssd.at[i], memory.at[i], xbuf, mem
        )
        pltpu.make_async_copy(tok.at[m, lines, :], normed_hbm.at[m, lines, :], o_sem.at[i]).start()
        pltpu.make_async_copy(flipped.at[i], turned_hbm.at[:, columns(i)], f_sem.at[i]).start()
        pltpu.make_async_copy(proj.at[i], proj_hbm.at[i], p_sem.at[i]).start()
        for n, plans in when.items():

            @pl.when(i == n)
            def _():
                for steps in plans:
                    run(steps)

        return carry

    lax.fori_loop(0, chunks, chunk, 0)
    save(ssd, ssd_hbm)
    save(memory, mem_hbm)
    arrive(mine(cot_hbm, peers[1]), t_recv.at[3])
    block = mine(cot_hbm, peers[1])
    sends.start(None, push(block, block, t_send.at[7], t_recv.at[7], d, peers[0]))
    landed(3, w_gate)
    save(w_gate, gate_hbm)

    def gating(i, carry):
        m, k = i // tp, i % tp
        lines = pl.ds(pl.multiple_of(k * part, part), part)
        gates[i] = dot(tok[m, lines, :], w_gate[...].reshape(width, inner))
        pltpu.make_async_copy(gates.at[i], gates_hbm.at[i], g_sem.at[i]).start()
        return carry

    lax.fori_loop(0, chunks, gating, 0)
    landed(4, out_hbm)
    arrive(mine(cot_hbm, peers[0]), t_recv.at[4])
    arrive(mine(cot_hbm, peers[2]), t_recv.at[7])

    def saved(i, carry):
        m, k = i // tp, i % tp
        lines = pl.ds(pl.multiple_of(k * part, part), part)
        pltpu.make_async_copy(tok.at[m, lines, :], normed_hbm.at[m, lines, :], o_sem.at[i]).wait()
        pltpu.make_async_copy(flipped.at[i], turned_hbm.at[:, columns(i)], f_sem.at[i]).wait()
        pltpu.make_async_copy(proj.at[i], proj_hbm.at[i], p_sem.at[i]).wait()
        pltpu.make_async_copy(gates.at[i], gates_hbm.at[i], g_sem.at[i]).wait()
        return carry

    lax.fori_loop(0, chunks, saved, 0)
    for copy in saves:
        copy.wait()
    sends.drain()


def head(in_proj, conv_weight, conv_bias, norm_gain, gated_gain, per_head, tokens, cotangent, out_proj, dp, tp):
    rows = in_proj.shape[0]
    heads = HEADS // tp
    inner = heads * P_SIZE
    full = inner + 2 * N + LANES
    micro, part, width = tokens.shape
    deep = dp // 2
    chunks = micro * tp
    block = tp * rows
    dma = pltpu.SemaphoreType.DMA
    vmem = pl.BlockSpec(memory_space=pltpu.VMEM)
    hbm = pl.BlockSpec(memory_space=pl.ANY)
    wide = inner + 2 * N

    def shape(*dims, kind=BF16):
        return jax.ShapeDtypeStruct(dims, kind)

    def room(*dims, kind=BF16):
        return pltpu.VMEM(dims, kind)

    return pl.pallas_call(
        functools.partial(head_kernel, dp, heads),
        in_specs=[vmem] * 9,
        out_specs=[hbm] * 10 + [vmem] * 4,
        out_shape=[
            shape(micro, tp * part, width),
            shape(width, chunks * part),
            shape(chunks, part, full, kind=F32),
            shape(chunks, part, inner, kind=F32),
            shape(chunks, N, inner),
            shape(chunks, part, inner, kind=F32),
            shape(dp, block, full),
            shape(dp, block, inner),
            shape(dp, out_proj.shape[0], width),
            shape(micro, tp * part, width),
            shape(8, wide, kind=F32),
            shape(16, width, kind=F32),
            shape(16, inner, kind=F32),
            shape(8, LANES, kind=F32),
        ],
        scratch_shapes=[
            room(32, LANES, kind=F32),
            room(tp, 32, LANES),
            room(tp, rows, inner),
            room(tp, rows, N),
            room(tp, rows, inner),
            room(dp, tp, 32, LANES),
            room(tp, rows, inner),
            room(tp, rows, N),
            room(tp, rows, inner),
            room(dp, block, inner),
            room(dp, block, N),
            room(dp, block, N),
            room(dp, block, 2 * N + LANES),
            room(dp, block, inner),
            room(*out_proj.shape),
            room(micro, tp * part, width),
            room(chunks, width, part),
            room(chunks, part, full, kind=F32),
            room(chunks, part, inner, kind=F32),
            room(chunks, part, inner, kind=F32),
            room(chunks, N, inner),
            room(part + 8, wide, kind=F32),
            room(N, inner, kind=F32),
            dma((8,)),
            dma((chunks,)),
            dma((chunks,)),
            dma((chunks,)),
            dma((chunks,)),
            dma((4, 3)),
            dma((4, 3)),
            dma((5, 2, deep - 1)),
            dma((5, 2, deep - 1)),
            dma((5, 2, deep)),
            dma((5, 2, deep)),
            dma((8,)),
            dma((8,)),
        ],
        compiler_params=pltpu.CompilerParams(
            collective_id=1, has_side_effects=True, vmem_limit_bytes=62 * 2**20
        ),
        cost_estimate=pl.CostEstimate(flops=10**11, bytes_accessed=5 * 10**7, transcendentals=0),
        name="gather_and_mix",
    )(in_proj, conv_weight, conv_bias, norm_gain, gated_gain, per_head, tokens, cotangent, out_proj)


class OwnerSum:
    def __init__(self, where, sends, source, mine, ybuf, zbuf, final, sems, theirs_ref=None):
        self.where, self.sends = where, sends
        self.mine, self.ybuf, self.zbuf, self.final = mine, ybuf, zbuf, final
        d, s, z, y, _, _, _, deep = where
        self.load_sem, y_send, self.y_recv, z_send, self.z_recv = sems
        lower = z < deep // 2

        def place(j):
            low = jnp.where(j > z, deep - 1 - j, deep - 1 - z + j)
            high = jnp.where(j < z, j, z + deep - 1 - j)
            return jnp.where(j == z, deep - 1, jnp.where(lower, low, high))

        def turn(k):
            low = jnp.where(k < deep - 1 - z, deep - 1 - k, k - (deep - 1 - z))
            high = jnp.where(k < z, k, deep - 1 - (k - z))
            return jnp.where(lower, low, high) if k < deep - 1 else z

        self.order = [turn(k) for k in range(deep)]
        self.y_items, self.loads = [], []
        for k, j in enumerate(self.order):
            theirs = source.at[j * 2 + 1 - y] if theirs_ref is None else theirs_ref.at[k]
            copy = push(theirs, ybuf.at[k], y_send.at[k], self.y_recv.at[k], d + 1 - 2 * y, s)
            self.y_items.append((None, copy))
            if theirs_ref is None:
                own = source.at[j * 2 + y]
                self.loads.append(pltpu.make_async_copy(own, mine.at[k], self.load_sem.at[k]))
        self.z_items = []
        for t in range(deep - 1):
            ways = []
            for way in range(2):
                depth = z if way == 0 else deep - 1 - z
                j = deep - 1 - t + z if way == 0 else t + z - deep + 1
                k = place(jnp.clip(j, 0, deep - 1))
                nxt = d + 2 if way == 0 else d - 2
                dst, ss, rs = zbuf.at[way, t], z_send.at[way, t], self.z_recv.at[way, t]
                first = (depth == 0, push(ybuf.at[k], dst, ss, rs, nxt, s))
                later = None
                if t > 0:
                    cond = jnp.logical_and(depth > 0, depth <= t)
                    later = (cond, push(zbuf.at[way, t - 1], dst, ss, rs, nxt, s))
                ways.append((k, first, later))
            self.z_items.append(ways)
        sends.items.extend(self.y_items)
        for ways in self.z_items:
            for _, first, later in ways:
                sends.items.append(first)
                if later is not None:
                    sends.items.append(later)

    def arrive(self, ref, sem):
        d, s = self.where[:2]
        push(ref, ref, sem, sem, d, self.where[6][0]).wait_recv()

    def begin(self):
        for _, copy in self.y_items:
            copy.start()
        for copy in self.loads:
            copy.start()

    def each(self, work):
        if self.mine.ndim == 4:
            count, cut = self.mine.shape[1], lambda i: i
        else:
            count, cut = self.mine.shape[1] // 16, lambda i: pl.ds(pl.multiple_of(i * 16, 16), 16)
        lax.fori_loop(0, count, lambda i, carry: (work(cut(i)), carry)[1], 0)

    def add(self, k):
        if self.loads:
            self.loads[k].wait()
        self.arrive(self.ybuf.at[k], self.y_recv.at[k])
        ybuf, mine = self.ybuf, self.mine

        def work(i):
            ybuf[k, i] = (ybuf[k, i].astype(F32) + mine[k, i].astype(F32)).astype(BF16)

        self.each(work)

    def send(self, t):
        zbuf, ybuf = self.zbuf, self.ybuf
        for way, (k, first, later) in enumerate(self.z_items[t]):
            pl.when(first[0])(first[1].start)
            if later is None:
                continue

            @pl.when(later[0])
            def _():
                self.arrive(zbuf.at[way, t - 1], self.z_recv.at[way, t - 1])

                def work(i):
                    zbuf[way, t - 1, i] = (
                        zbuf[way, t - 1, i].astype(F32) + ybuf[k, i].astype(F32)
                    ).astype(BF16)

                self.each(work)
                later[1].start()

    def finish(self):
        z, deep = self.where[2], self.where[7]
        zbuf, ybuf, final = self.zbuf, self.ybuf, self.final
        for way in range(2):
            depth = z if way == 0 else deep - 1 - z
            pl.when(depth > 0)(
                functools.partial(self.arrive, zbuf.at[way, deep - 2], self.z_recv.at[way, deep - 2])
            )

        def work(ways, i):
            total = ybuf[deep - 1, i].astype(F32)
            for way in ways:
                total = total + zbuf[way, deep - 2, i].astype(F32)
            final[i] = total.astype(BF16)

        for cond, ways in (
            (z == 0, (1,)),
            (z == deep - 1, (0,)),
            (jnp.logical_and(z > 0, z < deep - 1), (0, 1)),
        ):
            pl.when(cond)(functools.partial(self.each, functools.partial(work, ways)))


def middle_kernel(
    dp,
    heads,
    rest_ref,
    prev_ref,
    dy_ref,
    mem_ref,
    taps_ref,
    head_ref,
    part_hbm,
    gout_hbm,
    ggate_hbm,
    tok_hbm,
    out_ref,
    wgrad_ref,
    hgrad_ref,
    own_hbm,
    gout_out,
    ggate_out,
    xbuf,
    gbuf,
    adj,
    dmix,
    dsum,
    uprod,
    zprod,
    rows_t,
    line,
    acts,
    slopes,
    o_mine,
    o_y,
    o_z,
    o_final,
    g_mine,
    g_y,
    g_z,
    g_final,
    own,
    core_buf,
    x_buf,
    tok,
    result,
    o_load,
    o_ysend,
    o_yrecv,
    o_zsend,
    o_zrecv,
    g_load,
    g_ysend,
    g_yrecv,
    g_zsend,
    g_zrecv,
    b_load,
    c_send,
    c_recv,
    m_send,
    m_recv,
    a_send,
    a_recv,
):
    where = where_am_i(dp)
    d, s, z, y, x, c, peers, deep = where
    micro, part, width = result.shape
    step = pl.program_id(0) * pl.num_programs(1) + pl.program_id(1)
    tp = ggate_hbm.shape[1]
    me = d * tp + s
    turned = stripe_block(d, s, dp)
    moves = turned != me
    to_d, to_s = turned // tp, turned % tp
    from_d, from_s = stripe_owner(me, dp), stripe_seat(me, dp)
    sends = Sends()
    gout = OwnerSum(
        where, sends, gout_hbm, o_mine, o_y, o_z, o_final, (o_load, o_ysend, o_yrecv, o_zsend, o_zrecv)
    )
    ggate = OwnerSum(
        where, sends, ggate_hbm, g_mine, g_y, g_z, g_final, (g_load, g_ysend, g_yrecv, g_zsend, g_zrecv)
    )

    def chunk(k):
        return part_hbm.at[:, pl.ds(k * part, part), :]

    cores, loads = [], []
    for q, xx in enumerate((1 - x, x)):
        cores.append(
            push(chunk(xx * 2 + 1 - c), core_buf.at[q], c_send.at[q], c_recv.at[q], d, peers[0])
        )
        loads.append(pltpu.make_async_copy(chunk(xx * 2 + c), own.at[q], b_load.at[q]))
    across = push(core_buf.at[0], x_buf, m_send.at[0], m_recv.at[0], d, peers[1])
    turning = push(o_final, gout_out, m_send.at[1], m_recv.at[1], to_d, to_s)
    staying = pltpu.make_async_copy(o_final, gout_out, b_load.at[2])
    swaps = [
        push(g_final.at[p], ggate_out.at[s], a_send.at[r], a_recv.at[r], d, p)
        for r, p in enumerate(peers)
    ]
    kept = pltpu.make_async_copy(g_final.at[s], ggate_out.at[s], b_load.at[3])
    saved = pltpu.make_async_copy(result, own_hbm, b_load.at[4])
    loads.append(pltpu.make_async_copy(tok_hbm, tok, b_load.at[5]))
    for copy in cores + [across] + swaps:
        sends.items.append((None, copy))
    sends.items.append((moves, turning))
    span = 16

    def by_rows(work):
        def one(i, carry):
            m, row = i // (part // span), (i % (part // span)) * span
            work(m, pl.ds(pl.multiple_of(row, span), span))
            return carry

        lax.fori_loop(0, micro * (part // span), one, 0)

    def start():
        greet(
            [(None, d, p) for p in peers]
            + [(None, d + 1 - 2 * y, s), (z < deep - 1, d + 2, s), (z > 0, d - 2, s)]
            + [(moves, to_d, to_s), (moves, from_d, from_s)]
        )
        for copy in cores + loads:
            copy.start()
        gout.begin()
        ggate.begin()

    def pass_on():
        loads[0].wait()
        cores[0].wait_recv()

        def work(m, rows):
            core_buf[0, m, rows, :] = (
                core_buf[0, m, rows, :].astype(F32) + own[0, m, rows, :].astype(F32)
            ).astype(BF16)

        by_rows(work)
        across.start()

    def collect():
        loads[1].wait()
        loads[2].wait()
        cores[1].wait_recv()
        across.wait_recv()

        def work(m, rows):
            result[m, rows, :] = (
                core_buf[1, m, rows, :].astype(F32)
                + own[1, m, rows, :].astype(F32)
                + x_buf[m, rows, :].astype(F32)
                + tok[m, rows, :].astype(F32)
            ).astype(BF16)

        by_rows(work)
        saved.start()

    def hand_over():
        gout.finish()
        pl.when(moves)(turning.start)
        pl.when(jnp.logical_not(moves))(staying.start)

    def last():
        ggate.add(deep - 1)
        ggate.finish()
        for copy in swaps:
            copy.start()
        kept.start()
        pl.when(moves)(turning.wait_recv)
        pl.when(jnp.logical_not(moves))(staying.wait)
        for r, p in enumerate(peers):
            push(ggate_out.at[p], ggate_out.at[p], a_send.at[r], a_recv.at[r], d, p).wait_recv()
        kept.wait()
        saved.wait()
        sends.drain()

    stages = {}

    def at(n, task, *args):
        stages.setdefault(n, []).append(functools.partial(task, *args))

    at(0, start)
    at(1, pass_on)
    for k in range(deep - 1):
        n = k * 2 // (deep - 2)
        at(2 + n, gout.add, k)
        at(2 + n, gout.send, k)
    at(4, gout.add, deep - 1)
    at(5, hand_over)
    for k in range(deep - 1):
        n = k * 2 // (deep - 2)
        at(5 + n, ggate.add, k)
        at(5 + n, ggate.send, k)
    at(6, collect)
    for n, tasks in stages.items():

        @pl.when(step == n)
        def _():
            for task in tasks:
                task()

    backward_kernel(
        heads,
        rest_ref,
        prev_ref,
        dy_ref,
        mem_ref,
        taps_ref,
        head_ref,
        out_ref,
        wgrad_ref,
        hgrad_ref,
        xbuf,
        gbuf,
        adj,
        dmix,
        dsum,
        uprod,
        zprod,
        rows_t,
        line,
        acts,
        slopes,
    )
    pl.when(step == pl.num_programs(0) * pl.num_programs(1) - 1)(last)


def middle(rest, dy, memory, taps, head, partial, gout, ggate, tokens, dp, tp, heads, micro):
    count, full = rest.shape
    wide = taps.shape[1]
    inner = heads * P_SIZE
    _, length, width = partial.shape
    part = length // tp
    chunks = length // part
    deep = dp // 2
    dma = pltpu.SemaphoreType.DMA
    hbm = pl.BlockSpec(memory_space=pl.ANY)
    gout = gout.reshape(dp, 2, -1, width)

    def at(m, c):
        return m * chunks + chunks - 1 - c

    def sums(block):
        kinds = [(deep,), (deep,), (2, deep - 1), ()]
        return [pltpu.VMEM(kind + block, BF16) for kind in kinds]

    sems = [dma((deep,))] * 3 + [dma((2, deep - 1))] * 2
    out = pl.pallas_call(
        functools.partial(middle_kernel, dp, heads),
        grid=(micro, chunks),
        in_specs=[
            pl.BlockSpec((part, full), lambda m, c: (at(m, c), 0)),
            pl.BlockSpec((8, full), lambda m, c: (jnp.maximum(at(m, c) * (part // 8) - 1, 0), 0)),
            pl.BlockSpec((part, inner), lambda m, c: (at(m, c), 0)),
            pl.BlockSpec((1, N, inner), lambda m, c: (at(m, c), 0, 0)),
            pl.BlockSpec((8, wide), lambda m, c: (0, 0)),
            pl.BlockSpec((8, LANES), lambda m, c: (0, 0)),
            hbm,
            hbm,
            hbm,
            hbm,
        ],
        out_specs=[
            pl.BlockSpec((part, full), lambda m, c: (at(m, c), 0)),
            pl.BlockSpec((8, wide), lambda m, c: (0, 0)),
            pl.BlockSpec((8, LANES), lambda m, c: (0, 0)),
            hbm,
            hbm,
            hbm,
        ],
        out_shape=[
            jax.ShapeDtypeStruct((count, full), BF16),
            jax.ShapeDtypeStruct((8, wide), F32),
            jax.ShapeDtypeStruct((8, LANES), F32),
            jax.ShapeDtypeStruct((micro, part, width), BF16),
            jax.ShapeDtypeStruct(gout.shape[1:], BF16),
            jax.ShapeDtypeStruct(ggate.shape[1:], BF16),
        ],
        scratch_shapes=[
            pltpu.VMEM((part + 8, wide), F32),
            pltpu.VMEM((part + 8, wide), F32),
            pltpu.VMEM((N, inner), F32),
            pltpu.VMEM((part, wide), F32),
            pltpu.VMEM((part, inner), BF16),
            pltpu.VMEM((part, inner), BF16),
            pltpu.VMEM((part, inner), BF16),
            pltpu.VMEM((LANES, part), F32),
            pltpu.VMEM((8, inner), F32),
            pltpu.VMEM((part, wide), F32),
            pltpu.VMEM((part, wide), F32),
        ]
        + sums(gout.shape[1:])
        + sums(ggate.shape[1:])
        + [
            pltpu.VMEM((2, micro, part, width), BF16),
            pltpu.VMEM((2, micro, part, width), BF16),
            pltpu.VMEM((micro, part, width), BF16),
            pltpu.VMEM((micro, part, width), BF16),
            pltpu.VMEM((micro, part, width), BF16),
        ]
        + sems
        + sems
        + [dma((6,)), dma((2,)), dma((2,)), dma((2,)), dma((2,)), dma((3,)), dma((3,))],
        compiler_params=pltpu.CompilerParams(
            dimension_semantics=("arbitrary", "arbitrary"),
            collective_id=4,
            has_side_effects=True,
            vmem_limit_bytes=62 * 2**20,
        ),
        cost_estimate=pl.CostEstimate(flops=7 * 10**10, bytes_accessed=4 * 10**7, transcendentals=0),
        name="mixer_backward_and_sums",
    )(rest, rest, dy, memory, taps, head, partial, gout, ggate, tokens)
    rest_grad, wgrad, hgrad, own, gout, ggate = out
    return rest_grad, wgrad, hgrad, own, gout.reshape(-1, width), ggate


def gating_kernel(
    dp,
    ssd_hbm,
    gate_hbm,
    cot_hbm,
    out_hbm,
    turned_hbm,
    gain_ref,
    grad_ssd_hbm,
    grad_gate_hbm,
    part_hbm,
    gout_hbm,
    ggate_hbm,
    ssd,
    gate,
    cot,
    w_out,
    turned,
    weighed,
    shaped_t,
    grad_gate,
    partial,
    gout,
    ggate,
    stats,
    held,
    l_sem,
    c_sem,
    s_sem,
    g_sem,
    p_sem,
    o_sem,
    send,
    recv,
):
    d, s, *_, peers, _ = where_am_i(dp)
    chunks, part, inner = ssd.shape
    width = cot.shape[2]
    count = chunks * part

    def loads(i):
        return [
            pltpu.make_async_copy(cot_hbm.at[i], cot.at[i], c_sem.at[0, i]),
            pltpu.make_async_copy(ssd_hbm.at[i], ssd.at[i], c_sem.at[1, i]),
            pltpu.make_async_copy(gate_hbm.at[i], gate.at[i], c_sem.at[2, i]),
        ]

    first = pltpu.make_async_copy(out_hbm, w_out, l_sem.at[0])
    other = pltpu.make_async_copy(turned_hbm, turned, l_sem.at[1])
    first.start()
    for i in range(chunks):
        for copy in loads(i):
            copy.start()
    other.start()
    greet([(None, d, p) for p in peers])
    first.wait()

    def gated_parts(i):
        g = gate[i]
        sig = lax.logistic(g)
        act = g * sig
        return sig, act, ssd[i] * act

    def measure(i, carry):
        for copy in loads(i):
            copy.wait()
        w = dot(cot[i], w_out[...], NT) * gain_ref[KW + 2 : KW + 3, :]
        weighed[i] = w
        _, _, gated = gated_parts(i)
        lane = lax.broadcasted_iota(jnp.int32, (part, LANES), 1)
        both = jnp.where(lane == 0, jnp.sum(gated * gated, axis=1, keepdims=True), 0.0)
        both = jnp.where(lane == 1, jnp.sum(w * gated, axis=1, keepdims=True), both)
        stats[i] = both.T[:8, :]
        return carry

    lax.fori_loop(0, chunks, measure, 0)
    copies = [push(stats, held.at[r], send.at[r], recv.at[r], d, p) for r, p in enumerate(peers)]
    for copy in copies:
        copy.start()
    for copy in copies:
        copy.wait()

    def out_copies(i):
        return [
            pltpu.make_async_copy(weighed.at[i], grad_ssd_hbm.at[i], s_sem.at[i]),
            pltpu.make_async_copy(grad_gate.at[i], grad_gate_hbm.at[i], g_sem.at[i]),
            pltpu.make_async_copy(partial.at[i], part_hbm.at[i], p_sem.at[i]),
        ]

    def columns(i):
        return pl.ds(pl.multiple_of(i * part, part), part)

    def shape_chunk(i, carry):
        sums = (stats[i] + held[0, i]) + (held[1, i] + held[2, i])
        sums = jnp.concatenate([sums, jnp.zeros((LANES - 8, part), F32)], axis=0).T
        q = lax.rsqrt(sums[:, 0:1] / DI + EPSILON)
        pull = q * q * (sums[:, 1:2] / DI)
        sig, act, gated = gated_parts(i)
        value = gated * q * gain_ref[KW + 2 : KW + 3, :]
        shaped_t[:, columns(i)] = value.T.astype(BF16)
        partial[i] = dot(value.astype(BF16), w_out[...]).astype(BF16)
        grad = q * (weighed[i] - gated * pull)
        grad_gate[i] = (grad * ssd[i] * (sig + act * (1.0 - sig))).astype(BF16)
        weighed[i] = grad * act
        for copy in out_copies(i):
            copy.start()
        return carry

    lax.fori_loop(0, chunks, shape_chunk, 0)
    other.wait()
    high, across = min(384, inner), min(512, width)

    def out_tile(i, carry):
        a = pl.ds(pl.multiple_of(i // (width // across) * high, high), high)
        b = pl.ds(pl.multiple_of(i % (width // across) * across, across), across)
        gout[a, b] = dot(shaped_t[a, :], cot[:, :, b].reshape(count, across)).astype(BF16)
        return carry

    lax.fori_loop(0, (inner // high) * (width // across), out_tile, 0)
    save_out = pltpu.make_async_copy(gout, gout_hbm, o_sem.at[0])
    save_out.start()

    def gate_tile(i, carry):
        a = pl.ds(pl.multiple_of(i // 2 * across, across), across)
        b = pl.ds(pl.multiple_of(i % 2 * (inner // 2), inner // 2), inner // 2)
        ggate[a, b] = dot(turned[a, :], grad_gate[:, :, b].reshape(count, inner // 2)).astype(BF16)
        return carry

    lax.fori_loop(0, (width // across) * 2, gate_tile, 0)
    save_gate = pltpu.make_async_copy(ggate, ggate_hbm, o_sem.at[1])
    save_gate.start()

    def saved(i, carry):
        for copy in out_copies(i):
            copy.wait()
        return carry

    lax.fori_loop(0, chunks, saved, 0)
    save_out.wait()
    save_gate.wait()


def gating(ssd, gate, cot, w_out, normed_t, gains, dp):
    chunks, part, inner = ssd.shape
    width, count = normed_t.shape
    cot = cot.reshape(chunks, part, width)
    dma = pltpu.SemaphoreType.DMA
    vmem = pl.BlockSpec(memory_space=pltpu.VMEM)
    hbm = pl.BlockSpec(memory_space=pl.ANY)

    def shape(*dims, kind=BF16):
        return jax.ShapeDtypeStruct(dims, kind)

    def room(*dims, kind=BF16):
        return pltpu.VMEM(dims, kind)

    return pl.pallas_call(
        functools.partial(gating_kernel, dp),
        in_specs=[hbm] * 5 + [vmem],
        out_specs=[hbm] * 5,
        out_shape=[
            shape(chunks, part, inner, kind=F32),
            shape(chunks, part, inner),
            shape(chunks, part, width),
            shape(inner, width),
            shape(width, inner),
        ],
        scratch_shapes=[
            room(chunks, part, inner, kind=F32),
            room(chunks, part, inner, kind=F32),
            room(chunks, part, width),
            room(inner, width),
            room(width, count),
            room(chunks, part, inner, kind=F32),
            room(inner, count),
            room(chunks, part, inner),
            room(chunks, part, width),
            room(inner, width),
            room(width, inner),
            room(chunks, 8, part, kind=F32),
            room(3, chunks, 8, part, kind=F32),
            dma((2,)),
            dma((3, chunks)),
            dma((chunks,)),
            dma((chunks,)),
            dma((chunks,)),
            dma((2,)),
            dma((3,)),
            dma((3,)),
        ],
        compiler_params=pltpu.CompilerParams(
            collective_id=2, has_side_effects=True, vmem_limit_bytes=63 * 2**20
        ),
        cost_estimate=pl.CostEstimate(flops=3 * 10**10, bytes_accessed=5 * 10**7, transcendentals=0),
        name="gating_and_gradients",
    )(ssd, gate, cot, w_out, normed_t, gains)


def tail_kernel(
    dp,
    normed_hbm,
    rows_hbm,
    gates_hbm,
    w_rest_hbm,
    w_gate_hbm,
    tok_hbm,
    cot_hbm,
    gate_hbm,
    gout_hbm,
    proj_ref,
    block_ref,
    gain_ref,
    wgrad_ref,
    hgrad_ref,
    tokens_ref,
    grad_ref,
    dots_ref,
    gout_ref,
    gdots_ref,
    taps_ref,
    bias_ref,
    heads_ref,
    out_ref,
    own_ref,
    sums_ref,
    tok,
    cot,
    gate_in,
    gout,
    normed,
    rows_ref,
    gates_ref,
    w_rest,
    w_gate,
    tile,
    wtile,
    btile,
    b_own,
    b_out,
    b_in,
    theirs,
    mine,
    ybuf,
    zbuf,
    final,
    handed,
    core_buf,
    core_out,
    x_buf,
    x_out,
    s_buf,
    l_sem,
    n_sem,
    b_send,
    b_recv,
    y_send,
    y_recv,
    z_send,
    z_recv,
    a_send,
    a_recv,
    c_send,
    c_recv,
    x_send,
    x_recv,
    s_send,
    s_recv,
):
    where = where_am_i(dp)
    d, s, z, y, x, c, peers, deep = where
    tp, rows = out_ref.shape[:2]
    block = tp * rows
    micro, part, width = own_ref.shape
    inner = gates_ref.shape[1]
    bits = dp.bit_length() - 1
    partners = []
    for k in range(bits):
        step = 2**k
        bit = (d // step) % 2
        partners.append(d + step - 2 * step * bit)
    sends = Sends()
    total = OwnerSum(
        where,
        sends,
        None,
        mine,
        ybuf,
        zbuf,
        final,
        (None, y_send, y_recv, z_send, z_recv),
        theirs,
    )
    loads = [
        pltpu.make_async_copy(src, dst, l_sem.at[k])
        for k, (src, dst) in enumerate(
            (
                (rows_hbm, rows_ref),
                (w_rest_hbm, w_rest),
                (gates_hbm, gates_ref),
                (w_gate_hbm, w_gate),
                (tok_hbm, tok),
                (cot_hbm, cot),
                (gate_hbm, gate_in),
                (gout_hbm, gout),
            )
        )
    ]
    fetches = []
    for k in range(deep):
        lines = pl.ds(pl.multiple_of(total.order[k] * 2 * block, 2 * block), 2 * block)
        fetches.append(pltpu.make_async_copy(normed_hbm.at[lines, :], normed.at[k], n_sem.at[k]))
    for copy in loads + fetches:
        copy.start()
    greet(
        [(None, d, p) for p in peers]
        + [(None, d + 1 - 2 * y, s), (z < deep - 1, d + 2, s), (z > 0, d - 2, s)]
        + [(None, partners[k], s) for k in range(2, bits)]
    )

    def arrive(dst, sem):
        push(dst, dst, sem, sem, d, peers[0]).wait_recv()

    sums_ref[0, :, 0 : wgrad_ref.shape[1]] = wgrad_ref[...]
    sums_ref[0, :, wgrad_ref.shape[1] :] = hgrad_ref[...]

    def each(count, work):
        lax.fori_loop(0, count, lambda i, carry: (work(i), carry)[1], 0)

    across = width // tile.shape[1]
    span = wtile.shape[1]

    def product(owner, use):
        def work(i):
            m, n = i // across, i % across
            row = pl.multiple_of((m * tp + owner) * part, part)
            col = pl.multiple_of(n * tile.shape[1], tile.shape[1])
            lines = pl.ds(col, tile.shape[1])
            tile[...] = dot(rows_ref[pl.ds(row, part), :], w_rest[lines, :], NT) + dot(
                gates_ref[pl.ds(row, part), :], w_gate[lines, :], NT
            )
            use(m, lines)

        each(micro * across, work)

    def weight(k):
        fetches[k].wait()
        far = pl.ds(pl.multiple_of((1 - y) * block, block), block)
        near = pl.ds(pl.multiple_of(y * block, block), block)

        def work(n):
            cols = pl.ds(pl.multiple_of(n * span, span), span)
            wtile[...] = dot(normed[k], rows_ref[:, cols])
            theirs[k, :, cols] = wtile[far, :].astype(BF16)
            mine[k, :, cols] = wtile[near, :].astype(BF16)

        lines = pl.ds(inner, 2 * N)
        btile[...] = dot(normed[k], rows_ref[:, lines])
        ours = pl.ds(pl.multiple_of(c * N, N), N)
        b_out[k] = btile[:, pl.ds(pl.multiple_of((1 - c) * N, N), N)].astype(BF16)
        b_own[...] = btile[:, ours]
        swap = push(b_out.at[k], b_in.at[k], b_send.at[k], b_recv.at[k], d, peers[0])
        sends.start(None, swap)
        each(inner // span, work)
        b_tail = dot(normed[k], rows_ref[:, inner + 2 * N :])
        btile[:, N:] = b_tail
        arrive(b_in.at[k], b_recv.at[k])
        btile[:, 0:N] = b_own[...] + b_in[k].astype(F32)
        theirs[k, :, inner:] = btile[far, :].astype(BF16)
        mine[k, :, inner:] = btile[near, :].astype(BF16)
        total.y_items[k][1].start()

    def doubling(k):
        arrive(s_buf.at[k], s_recv.at[k])
        sums_ref[k + 1] = sums_ref[k] + s_buf[k]
        if k + 1 < bits:
            src = sums_ref.at[k + 1]
            sends.start(
                None, push(src, s_buf.at[k + 1], s_send.at[k + 1], s_recv.at[k + 1], partners[k + 1], s)
            )

    def to_core(q):
        def use(m, lines):
            core_out[q, m, :, lines] = tile[...].astype(BF16)

        return use

    def to_chip(m, lines):
        x_out[m, :, lines] = (tile[...] + core_buf[0, m, :, lines].astype(F32)).astype(BF16)

    def keep(m, lines):
        own_ref[m, :, lines] = tile[...] + core_buf[1, m, :, lines].astype(F32)

    for copy in loads[:4]:
        copy.wait()
    src = sums_ref.at[0]
    sends.start(None, push(src, s_buf.at[0], s_send.at[0], s_recv.at[0], partners[0], s))
    product((1 - x) * 2 + 1 - c, to_core(0))
    sends.start(
        None, push(core_out.at[0], core_buf.at[0], c_send.at[0], c_recv.at[0], d, peers[0])
    )
    weight(0)
    arrive(core_buf.at[0], c_recv.at[0])
    product((1 - x) * 2 + c, to_chip)
    sends.start(None, push(x_out, x_buf, x_send.at[0], x_recv.at[0], d, peers[1]))
    weight(1)
    total.add(0)
    total.send(0)
    doubling(0)
    for k in range(2, deep):
        weight(k)
    total.add(1)
    total.send(1)
    doubling(1)
    product(x * 2 + 1 - c, to_core(1))
    sends.start(
        None, push(core_out.at[1], core_buf.at[1], c_send.at[1], c_recv.at[1], d, peers[0])
    )
    for k in range(2, deep - 1):
        total.add(k)
        total.send(k)
        if k < bits:
            doubling(k)
    arrive(core_buf.at[1], c_recv.at[1])
    product(s, keep)
    for k in range(deep - 1, bits):
        doubling(k)
    for r, p in enumerate(peers):
        src, dst = sums_ref.at[bits], sums_ref.at[bits + 1 + s]
        sends.start(None, push(src, dst, s_send.at[bits + r], s_recv.at[bits + r], d, p))
    sums_ref[bits + 1 + s] = sums_ref[bits]
    for copy in loads[4:]:
        copy.wait()
    wide = inner + 2 * N
    heads = inner // P_SIZE
    triple = HEADS // 16
    for b in range(4):
        seat = 2 * (b % 2) + b // 2
        for k in range(4):
            at = (4 * k + b) * STRIPE
            grad_ref[:, at : at + STRIPE] = gate_in[seat, :, k * STRIPE : (k + 1) * STRIPE].astype(F32)
    gout_ref[...] = gout[...].astype(F32)
    gdots_ref[...] = jnp.sum(gout_ref[...] * block_ref[...].astype(F32), axis=1, keepdims=True)
    for r, p in enumerate(peers):
        arrive(sums_ref.at[bits + 1 + p], s_recv.at[bits + r])
    chan = taps_ref.shape[1]
    convs = jnp.zeros((8, chan), F32)
    per_head = jnp.zeros((8, HEADS), F32)
    v = lax.broadcasted_iota(jnp.int32, (wide, chan), 0)
    g = lax.broadcasted_iota(jnp.int32, (wide, chan), 1) + chan * (d * tp + s)
    lane = lax.broadcasted_iota(jnp.int32, (LANES, HEADS), 0)
    head = lax.broadcasted_iota(jnp.int32, (LANES, HEADS), 1)
    place = []
    for p in range(tp):
        b = 2 * (p % 2) + p // 2
        from_v = jnp.where(v < inner, v + 3 * STRIPE * hop(v, STRIPE) + STRIPE * b, v - inner + DI)
        sums = sums_ref[bits + 1 + p]
        convs = convs + dot(sums[:, :wide], jnp.where(from_v == g, 1.0, 0.0), precision=HIGH)
        hit = jnp.logical_and(lane < heads, head == lane + 3 * triple * hop(lane, triple) + triple * b)
        place.append(jnp.where(hit, 1.0, 0.0))
        per_head = per_head + dot(sums[:, wide:], place[p], precision=HIGH)
    taps_ref[...] = convs[:KW]
    bias_ref[...] = convs[KW : KW + 1]
    heads_ref[...] = per_head
    total.add(deep - 1)
    total.finish()
    for p in range(tp):
        handed[p] = final[p * rows : (p + 1) * rows, :]
    for r, p in enumerate(peers):
        sends.start(None, push(handed.at[p], out_ref.at[s], a_send.at[r], a_recv.at[r], d, p))
    out_ref[s] = handed[s]

    arrive(x_buf, x_recv.at[0])

    def last(i):
        m, row = i // (part // 16), (i % (part // 16)) * 16
        lines = pl.ds(pl.multiple_of(row, 16), 16)
        h = tok[m, lines, :].astype(F32)
        r = lax.rsqrt(jnp.mean(h * h, axis=-1, keepdims=True) + EPSILON)
        n = h * r
        grad = (own_ref[m, lines, :] + x_buf[m, lines, :].astype(F32)) * gain_ref[KW + 1 : KW + 2, :]
        grad = grad - n * jnp.mean(grad * n, axis=-1, keepdims=True)
        tokens_ref[m, lines, :] = (cot[m, lines, :].astype(F32) + r * grad).astype(BF16)

    each(micro * (part // 16), last)
    for r, p in enumerate(peers):
        arrive(out_ref.at[p], a_recv.at[r])
    both = [jnp.zeros((rows, N), F32), jnp.zeros((rows, N), F32)]
    steps = jnp.zeros((rows, HEADS), F32)
    for b in range(4):
        seat = 2 * (b % 2) + b // 2
        for k in range(4):
            at = DI + (4 * k + b) * STRIPE
            piece = out_ref[seat, :, k * STRIPE : (k + 1) * STRIPE]
            grad_ref[:, at : at + STRIPE] = piece.astype(F32)
        both[seat % 2] = both[seat % 2] + out_ref[seat, :, inner : inner + N].astype(F32)
        steps = steps + dot(out_ref[seat, :, inner + N :], place[seat].astype(BF16))
    grad_ref[:, 2 * DI : 2 * DI + N] = both[0]
    grad_ref[:, 2 * DI + N : 2 * DI + 2 * N] = both[1]
    grad_ref[:, 2 * DI + 2 * N :] = steps
    dots_ref[...] = jnp.sum(grad_ref[...] * proj_ref[...].astype(F32), axis=1, keepdims=True)
    sends.drain()


def tail(
    normed_t, rows_grad, gates_grad, w_rest, w_gate, tokens, cotangent, gate_in, gout, in_proj, out_proj, gains, wgrad, hgrad, chan, dp
):
    width, count = normed_t.shape
    micro = tokens.shape[0]
    tp = gate_in.shape[0]
    small = (8, wgrad.shape[1] + hgrad.shape[1])
    full = gates_grad.shape[1] + N + LANES
    rows = width // dp // tp
    part = count // micro // tp
    deep = dp // 2
    bits = dp.bit_length() - 1
    block = tp * rows
    dma = pltpu.SemaphoreType.DMA
    vmem = pl.BlockSpec(memory_space=pltpu.VMEM)
    hbm = pl.BlockSpec(memory_space=pl.ANY)
    return pl.pallas_call(
        functools.partial(tail_kernel, dp),
        in_specs=[hbm] * 9 + [vmem] * 5,
        out_specs=[vmem] * 8,
        out_shape=[
            jax.ShapeDtypeStruct(tokens.shape, BF16),
            jax.ShapeDtypeStruct(in_proj.shape, F32),
            jax.ShapeDtypeStruct((rows, 1), F32),
            jax.ShapeDtypeStruct(gout.shape, F32),
            jax.ShapeDtypeStruct((gout.shape[0], 1), F32),
            jax.ShapeDtypeStruct((KW, chan), F32),
            jax.ShapeDtypeStruct((1, chan), F32),
            jax.ShapeDtypeStruct((8, HEADS), F32),
        ],
        scratch_shapes=[
            pltpu.VMEM((tp, rows, full), BF16),
            pltpu.VMEM((micro, part, width), F32),
            pltpu.VMEM((bits + 1 + tp,) + small, F32),
            pltpu.VMEM(tokens.shape, BF16),
            pltpu.VMEM(tokens.shape, BF16),
            pltpu.VMEM(gate_in.shape, BF16),
            pltpu.VMEM(gout.shape, BF16),
            pltpu.VMEM((deep, 2 * block, count), BF16),
            pltpu.VMEM(rows_grad.shape, BF16),
            pltpu.VMEM(gates_grad.shape, BF16),
            pltpu.VMEM(w_rest.shape, BF16),
            pltpu.VMEM(w_gate.shape, BF16),
            pltpu.VMEM((part, min(width, 512)), F32),
            pltpu.VMEM((2 * block, 384), F32),
            pltpu.VMEM((2 * block, 2 * N), F32),
            pltpu.VMEM((2 * block, N), F32),
            pltpu.VMEM((deep, 2 * block, N), BF16),
            pltpu.VMEM((deep, 2 * block, N), BF16),
            pltpu.VMEM((deep, block, full), BF16),
            pltpu.VMEM((deep, block, full), BF16),
            pltpu.VMEM((deep, block, full), BF16),
            pltpu.VMEM((2, deep - 1, block, full), BF16),
            pltpu.VMEM((block, full), BF16),
            pltpu.VMEM((tp, rows, full), BF16),
            pltpu.VMEM((2, micro, part, width), BF16),
            pltpu.VMEM((2, micro, part, width), BF16),
            pltpu.VMEM((micro, part, width), BF16),
            pltpu.VMEM((micro, part, width), BF16),
            pltpu.VMEM((bits,) + small, F32),
            dma((8,)),
            dma((deep,)),
            dma((deep,)),
            dma((deep,)),
            dma((deep,)),
            dma((deep,)),
            dma((2, deep - 1)),
            dma((2, deep - 1)),
            dma((3,)),
            dma((3,)),
            dma((2,)),
            dma((2,)),
            dma((1,)),
            dma((1,)),
            dma((bits + 3,)),
            dma((bits + 3,)),
        ],
        compiler_params=pltpu.CompilerParams(
            collective_id=3, has_side_effects=True, vmem_limit_bytes=62 * 2**20
        ),
        cost_estimate=pl.CostEstimate(flops=6 * 10**10, bytes_accessed=3 * 10**7, transcendentals=0),
        name="gradients_to_owners",
    )(
        normed_t,
        rows_grad,
        gates_grad,
        w_rest,
        w_gate,
        tokens,
        cotangent,
        gate_in,
        gout,
        in_proj,
        out_proj,
        gains,
        wgrad,
        hgrad,
    )


def body(
    tokens,
    in_proj,
    conv_weight,
    conv_bias,
    decay_log,
    step_bias,
    skip_gain,
    norm_gain,
    gated_gain,
    out_proj,
    cotangent,
):
    dp, tp = lax.axis_size("dp"), lax.axis_size("seq")
    s = lax.axis_index("seq")
    micro, part, width = tokens.shape
    heads = HEADS // tp
    inner = heads * P_SIZE
    rows = in_proj.shape[0]
    length = part * tp
    count = micro * length
    wide = inner + 2 * N
    chan = conv_bias.shape[0]

    per_head = jnp.pad(jnp.stack([decay_log, step_bias, skip_gain]), ((0, 5), (0, 0)))
    (
        normed,
        normed_t,
        proj_rest,
        ssd,
        memory,
        gate,
        w_rest,
        w_gate,
        w_out,
        cot,
        taps,
        gains,
        g_gated,
        per_head,
    ) = head(
        in_proj,
        conv_weight,
        conv_bias[None],
        norm_gain[None],
        gated_gain[None],
        per_head,
        tokens,
        cotangent,
        out_proj,
        dp,
        tp,
    )
    proj_rest = proj_rest.reshape(count, wide + LANES)
    w_rest = w_rest.reshape(width, wide + LANES)
    w_gate = w_gate.reshape(width, inner)
    grad_ssd, grad_gate, out_part, grad_out, gate_in = gating(
        ssd, gate, cot, w_out.reshape(inner, width), normed_t, g_gated, dp
    )
    grad_ssd = grad_ssd.reshape(count, inner)
    grad_gate = grad_gate.reshape(count, inner)
    grad_rest, wgrad, hgrad, out_part, grad_out, gate_in = middle(
        proj_rest,
        grad_ssd,
        memory,
        taps,
        per_head,
        out_part.reshape(micro, length, width),
        grad_out.reshape(dp, -1, width),
        gate_in.reshape(dp, tp, rows, inner),
        tokens,
        dp,
        tp,
        heads,
        micro,
    )
    tokens_grad, in_grad, dots, grad_out, gdots, conv_grad, bias_grad, head_grads = tail(
        normed_t,
        grad_rest,
        grad_gate,
        w_rest,
        w_gate,
        tokens,
        cotangent,
        gate_in,
        grad_out,
        in_proj,
        out_proj,
        gains,
        wgrad,
        hgrad,
        chan,
        dp,
    )
    return (
        out_part,
        tokens_grad,
        in_grad,
        conv_grad,
        bias_grad[0],
        head_grads[0],
        head_grads[1],
        head_grads[2],
        dots[:, 0] / norm_gain.astype(F32),
        gdots[:, 0] / gated_gain.astype(F32),
        grad_out,
    )


def solution(mesh):
    both = ("dp", "seq")
    return jax.shard_map(
        body,
        mesh=mesh,
        in_specs=(
            P("dp", "seq", None),
            P(both, None),
            P(None, both),
            P(both),
            P(),
            P(),
            P(),
            P(both),
            P(both),
            P(both, None),
            P("dp", "seq", None),
        ),
        out_specs=(
            P("dp", "seq", None),
            P("dp", "seq", None),
            P(both, None),
            P(None, both),
            P(both),
            P(),
            P(),
            P(),
            P(both),
            P(both),
            P(both, None),
        ),
        check_vma=False,
    )
```

```python
import functools

import jax
import jax.numpy as jnp
from jax import lax
from jax.experimental import pallas as pl
from jax.experimental.pallas import tpu as pltpu
from jax.sharding import PartitionSpec as P

HEADS = 48
P_SIZE = 64
N = 128
KW = 4
DI = 3072
CD = 3328
LANES = 128
FAR = -1e30

EPSILON = 1e-05
F32 = jnp.float32
BF16 = jnp.bfloat16


def dot(a, b, dims=((1,), (0,)), precision=None):
    return lax.dot_general(a, b, (dims, ((), ())), precision=precision, preferred_element_type=F32)


NT = ((1,), (1,))
HIGH = lax.Precision.HIGHEST


def pick(a, p, low):
    return jnp.where(low, a[:, 2 * p : 2 * p + 1], a[:, 2 * p + 1 : 2 * p + 2])


def chunk_parts(heads, rest_ref, xbuf, taps_ref, head_ref):
    size = rest_ref.shape[0]
    wide = taps_ref.shape[1]
    mixed = taps_ref[KW : KW + 1, :] + taps_ref[0:1, :] * xbuf[5 : 5 + size, :]
    for k in range(1, KW):
        mixed = mixed + taps_ref[k : k + 1, :] * xbuf[5 + k : 5 + k + size, :]
    sig = lax.logistic(mixed)
    return (mixed, sig) + step_parts(heads, rest_ref, taps_ref, head_ref)


def step_parts(heads, rest_ref, taps_ref, head_ref):
    size = rest_ref.shape[0]
    wide = taps_ref.shape[1]
    lane = lax.broadcasted_iota(jnp.int32, (1, LANES), 1)
    raw = jnp.where(lane < heads, rest_ref[:, wide:], 0.0) + head_ref[1:2, :]
    step = jnp.maximum(raw, 0.0) + jnp.log1p(jnp.exp(-jnp.abs(raw)))
    decay = -jnp.exp(head_ref[0:1, :]) * step
    i = lax.broadcasted_iota(jnp.int32, (size, size), 0)
    j = lax.broadcasted_iota(jnp.int32, (size, size), 1)
    run = dot(jnp.where(i >= j, 1.0, 0.0), decay, precision=HIGH)
    return raw, step, decay, run


def backward_kernel(
    heads,
    rest_ref,
    prev_ref,
    dy_ref,
    mem_ref,
    taps_ref,
    head_ref,
    out_ref,
    wgrad_ref,
    hgrad_ref,
    xbuf,
    gbuf,
    adj,
    dmix,
    dsum,
    uprod,
    zprod,
    rows_t,
    line,
    acts,
    slopes,
):
    size = rest_ref.shape[0]
    wide = taps_ref.shape[1]
    inner = heads * P_SIZE
    chunks = pl.num_programs(1)
    step_id = pl.program_id(1)
    newest = step_id == 0
    oldest = step_id == chunks - 1
    begin = jnp.logical_and(pl.program_id(0) == 0, newest)
    finish = jnp.logical_and(pl.program_id(0) == pl.num_programs(0) - 1, oldest)

    @pl.when(begin)
    def _():
        wgrad_ref[...] = jnp.zeros_like(wgrad_ref)
        hgrad_ref[...] = jnp.zeros_like(hgrad_ref)
        rows_t[...] = jnp.zeros_like(rows_t)
        line[...] = jnp.zeros_like(line)

    @pl.when(newest)
    def _():
        gbuf[size : size + 8, :] = jnp.zeros((8, wide), F32)
        adj[...] = jnp.zeros_like(adj)

    @pl.when(jnp.logical_not(newest))
    def _():
        gbuf[size : size + 8, :] = gbuf[0:8, :]

    xbuf[0:8, :] = jnp.where(oldest, 0.0, prev_ref[:, :wide])
    xbuf[8 : 8 + size, :] = rest_ref[:, :wide]
    for n in range(wide // LANES):
        at = slice(n * LANES, (n + 1) * LANES)
        mixed = taps_ref[KW : KW + 1, at] + taps_ref[0:1, at] * xbuf[5 : 5 + size, at]
        for k in range(1, KW):
            mixed = mixed + taps_ref[k : k + 1, at] * xbuf[5 + k : 5 + k + size, at]
        sig = lax.logistic(mixed)
        acts[:, at] = mixed * sig
        slopes[:, at] = sig * (1.0 + mixed * (1.0 - sig))
    raw, step, decay, run = step_parts(heads, rest_ref, taps_ref, head_ref)
    run_t = run.T
    closing = run[size - 1 : size, :]
    last = jnp.exp(closing)
    left = jnp.exp(closing - run)
    grown = jnp.exp(run)
    b = acts[:, inner : inner + N].astype(BF16)
    c = acts[:, inner + N :].astype(BF16)
    c_t = acts[:, inner + N :].T.astype(BF16)
    scores_t = dot(b, c, NT)
    low = lax.broadcasted_iota(jnp.int32, (1, LANES), 1) < P_SIZE
    lane = lax.broadcasted_iota(jnp.int32, (1, LANES), 1)
    j = lax.broadcasted_iota(jnp.int32, (size, size), 0)
    i = lax.broadcasted_iota(jnp.int32, (size, size), 1)
    causal = i >= j
    mem_b = mem_ref[0]
    adj_b = adj[...].astype(BF16)
    spread = dot(b, adj_b)
    inherit = dot(c, mem_b)
    scored = jnp.zeros((size, size), F32)
    cols = jnp.zeros((size, LANES), F32)
    for p in range(heads // 2):
        at = slice(p * LANES, (p + 1) * LANES)
        v = acts[:, at]
        size_p = pick(step, p, low)
        xv = size_p * v
        dy = dy_ref[:, at]
        dyb = dy.astype(BF16)
        xvb = xv.astype(BF16)
        dxv = pick(left, p, low) * spread[:, at]
        zprod[:, at] = (dxv * xv).astype(BF16)
        dyg = pick(grown, p, low) * dy
        uprod[:, at] = (dyg * inherit[:, at]).astype(BF16)
        for e in range(2):
            h = 2 * p + e
            keep = low if e == 0 else jnp.logical_not(low)
            mine = jnp.where(keep, dy, 0.0).astype(BF16)
            gap = run_t[h : h + 1, :] - run[:, h : h + 1]
            near = jnp.exp(jnp.where(causal, gap, FAR))
            w_t = scores_t * near
            dw_t = dot(xvb, mine, NT)
            scored = scored + dw_t * near
            g_t = dw_t * w_t
            rows_t[h : h + 1, :] = jnp.sum(g_t, axis=0, keepdims=True)
            cols = jnp.where(lane == h, jnp.sum(g_t, axis=1, keepdims=True), cols)
            dxv = dxv + dot(w_t.astype(BF16), mine)
        dsum[:, at] = (dxv * v).astype(BF16)
        dmix[:, at] = size_p * dxv + pick(head_ref[2:3, :], p, low) * dy
        line[0:1, at] += jnp.sum(dy * v, axis=0, keepdims=True)
        line[1:2, at] = jnp.sum(adj[:, at] * mem_b[:, at].astype(F32), axis=0, keepdims=True) * pick(
            last, p, low
        )
        xc = (pick(left, p, low) * xv).astype(BF16)
        dygb = dyg.astype(BF16)
        db = dot(xc, adj_b[:, at], NT)
        dc = dot(dygb, mem_b[:, at], NT)
        if p == 0:
            dmix[:, inner : inner + N] = db
            dmix[:, inner + N :] = dc
        else:
            dmix[:, inner : inner + N] += db
            dmix[:, inner + N :] += dc
        adj[:, at] = adj[:, at] * pick(last, p, low) + dot(c_t, dygb)
    dmix[:, inner : inner + N] += dot(scored.astype(BF16), c)
    dmix[:, inner + N :] += dot(scored.T.astype(BF16), b)

    group = jnp.where(
        lax.broadcasted_iota(jnp.int32, (inner, LANES), 0) // P_SIZE
        == lax.broadcasted_iota(jnp.int32, (inner, LANES), 1),
        1.0,
        0.0,
    )
    group_b = group.astype(BF16)
    d_step = dot(dsum[...], group_b)
    u = dot(uprod[...], group_b)
    z = dot(zprod[...], group_b)
    sums = dot(line[...], group, precision=HIGH)
    d_run = rows_t[...].T - cols + u - z
    row = lax.broadcasted_iota(jnp.int32, (size, 1), 0)
    ending = sums[1:2, :] + jnp.sum(z, axis=0, keepdims=True)
    d_run = d_run + jnp.where(row == size - 1, ending, 0.0)
    d_decay = dot(jnp.where(causal, 1.0, 0.0), d_run, precision=HIGH)
    d_raw = (d_step - jnp.exp(head_ref[0:1, :]) * d_decay) * lax.logistic(raw)
    d_raw = jnp.where(lane < heads, d_raw, 0.0)
    hgrad_ref[0:1, :] += jnp.sum(d_decay * decay, axis=0, keepdims=True)
    hgrad_ref[1:2, :] += jnp.sum(d_raw, axis=0, keepdims=True)

    @pl.when(finish)
    def _():
        hgrad_ref[2:3, :] = sums[0:1, :]

    for n in range(wide // LANES):
        at = slice(n * LANES, (n + 1) * LANES)
        g = dmix[:, at] * slopes[:, at]
        gbuf[0:size, at] = g
        wgrad_ref[KW : KW + 1, at] += jnp.sum(g, axis=0, keepdims=True)
        for k in range(KW):
            lag = xbuf[5 + k : 5 + k + size, at]
            wgrad_ref[k : k + 1, at] += jnp.sum(g * lag, axis=0, keepdims=True)
        back = taps_ref[KW - 1 : KW, at] * g
        for k in range(KW - 1):
            back = back + taps_ref[k : k + 1, at] * gbuf[3 - k : 3 - k + size, at]
        out_ref[:, at] = back.astype(BF16)
    out_ref[:, wide:] = d_raw.astype(BF16)


MESH = pl.DeviceIdType.MESH


def where_am_i(dp):
    d, s = lax.axis_index("dp"), lax.axis_index("seq")
    z, y = d // 2, d % 2
    x, c = s // 2, s % 2
    peers = [s + 1 - 2 * c, s + 2 - 4 * x, 3 - s]
    return d, s, z, y, x, c, peers, dp // 2


def push(src, dst, send_sem, recv_sem, d, s):
    return pltpu.make_async_remote_copy(
        src_ref=src,
        dst_ref=dst,
        send_sem=send_sem,
        recv_sem=recv_sem,
        device_id={"dp": d, "seq": s},
        device_id_type=MESH,
    )


def greet(partners):
    barrier = pltpu.get_barrier_semaphore()
    for cond, d, s in partners:

        def hello(d=d, s=s):
            pl.semaphore_signal(barrier, inc=1, device_id={"dp": d, "seq": s}, device_id_type=MESH)

        if cond is None:
            hello()
        else:
            pl.when(cond)(hello)
    count = 0
    for cond, _, _ in partners:
        count = count + (1 if cond is None else jnp.where(cond, 1, 0))
    pl.semaphore_wait(barrier, count)


class Sends:
    def __init__(self):
        self.items = []

    def start(self, cond, copy):
        if cond is None:
            copy.start()
        else:
            pl.when(cond)(copy.start)
        self.items.append((cond, copy))

    def drain(self):
        for cond, copy in self.items:
            if cond is None:
                copy.wait_send()
            else:
                pl.when(cond)(copy.wait_send)


STRIPE = DI // 16


def swapped(s):
    return 2 * (s % 2) + s // 2


def stripe_owner(block, dp):
    u = dp // 4
    return block // (4 * u) * u + block % u


def stripe_seat(block, dp):
    return swapped(block // (dp // 4) % 4)


def stripe_block(d, s, dp):
    u = dp // 4
    return (d // u * 4 + swapped(s)) * u + d % u


def forward_chunk(heads, first, rest_ref, taps_ref, head_ref, ssd_ref, mem_ref, xbuf, mem):
    size = rest_ref.shape[0]
    wide = taps_ref.shape[1]
    inner = heads * P_SIZE

    @pl.when(first)
    def _():
        xbuf[0:8, :] = jnp.zeros((8, wide), F32)
        mem[...] = jnp.zeros_like(mem)

    @pl.when(jnp.logical_not(first))
    def _():
        xbuf[0:8, :] = xbuf[size : size + 8, :]

    xbuf[8 : 8 + size, :] = rest_ref[:, :wide]
    mixed, sig, _, step, _, run = chunk_parts(heads, rest_ref, xbuf, taps_ref, head_ref)
    act = mixed * sig
    run_t = run.T
    closing = run[size - 1 : size, :]
    last = jnp.exp(closing)
    left = jnp.exp(closing - run)
    grown = jnp.exp(run)
    b = act[:, inner : inner + N]
    c = act[:, inner + N :].astype(BF16)
    scores = dot(c, b.astype(BF16), NT)
    b_t = b.T.astype(BF16)
    mem_ref[...] = mem[...].astype(BF16)
    inter = dot(c, mem[...].astype(BF16))
    low = lax.broadcasted_iota(jnp.int32, (1, LANES), 1) < P_SIZE
    i = lax.broadcasted_iota(jnp.int32, (size, size), 0)
    j = lax.broadcasted_iota(jnp.int32, (size, size), 1)
    causal = i >= j
    for p in range(heads // 2):
        at = slice(p * LANES, (p + 1) * LANES)
        v = act[:, at]
        xv = pick(step, p, low) * v
        y = pick(head_ref[2:3, :], p, low) * v + pick(grown, p, low) * inter[:, at]
        for e in range(2):
            h = 2 * p + e
            gap = run[:, h : h + 1] - run_t[h : h + 1, :]
            w = (scores * jnp.exp(jnp.where(causal, gap, FAR))).astype(BF16)
            mine = jnp.where(low if e == 0 else jnp.logical_not(low), xv, 0.0).astype(BF16)
            y = y + dot(w, mine)
        ssd_ref[:, at] = y
        xc = (pick(left, p, low) * xv).astype(BF16)
        mem[:, at] = mem[:, at] * pick(last, p, low) + dot(b_t, xc)


def hop(v, size):
    return sum(jnp.where(v >= q * size, 1, 0) for q in range(1, 4))


def head_kernel(
    dp,
    heads,
    proj_ref,
    cw_ref,
    cb_ref,
    ng_ref,
    gg_ref,
    ph_ref,
    tok_ref,
    cot_ref,
    block_ref,
    normed_hbm,
    turned_hbm,
    proj_hbm,
    ssd_hbm,
    mem_hbm,
    gates_hbm,
    rest_hbm,
    gate_hbm,
    out_hbm,
    cot_hbm,
    taps_ref,
    gain_ref,
    gated_ref,
    head_ref,
    line,
    small_stage,
    val_stage,
    half_stage,
    gate_stage,
    small_all,
    val_in,
    half_in,
    gate_in,
    w_val,
    w_half,
    w_other,
    w_tail,
    w_gate,
    out_shard,
    tok,
    flipped,
    proj,
    ssd,
    gates,
    memory,
    xbuf,
    mem,
    l_sem,
    o_sem,
    f_sem,
    p_sem,
    g_sem,
    a_send,
    a_recv,
    z_send,
    z_recv,
    y_send,
    y_recv,
    t_send,
    t_recv,
):
    d, s, z, y, x, c, peers, deep = where_am_i(dp)
    tp, rows = val_stage.shape[:2]
    micro, part, width = tok_ref.shape
    total = dp * tp
    inner = heads * P_SIZE
    wide = inner + 2 * N
    chan, gpiece = cw_ref.shape[1], gg_ref.shape[1]
    up, down, far = d + 2, d - 2, d + 1 - 2 * y
    me = d * tp + s
    to_d, to_s, turned = stripe_owner(me, dp), stripe_seat(me, dp), stripe_block(d, s, dp)
    from_d, from_s = turned // tp, turned % tp
    moves = turned != me

    triple = HEADS // 16
    line[...] = jnp.zeros_like(line)
    line[0:KW, 0:chan] = cw_ref[...].astype(F32)
    line[KW : KW + 1, 0:chan] = cb_ref[...].astype(F32)
    line[KW + 1 : KW + 2, 0:rows] = ng_ref[...].astype(F32)
    line[KW + 2 : KW + 3, 0:gpiece] = gg_ref[...].astype(F32)
    raw = proj_ref[:, 2 * DI + 2 * N :]
    for b in range(4):
        seat = 2 * (b % 2) + b // 2
        for k in range(4):
            to, at = k * STRIPE, (4 * k + b) * STRIPE
            gate_stage[seat, :, to : to + STRIPE] = proj_ref[:, at : at + STRIPE]
            val_stage[seat, :, to : to + STRIPE] = proj_ref[:, DI + at : DI + at + STRIPE]
        at = 2 * DI + N * (seat % 2)
        half_stage[seat] = proj_ref[:, at : at + N]
        v = lax.broadcasted_iota(jnp.int32, (16, HEADS), 0)
        g = lax.broadcasted_iota(jnp.int32, (16, HEADS), 1)
        hit = jnp.logical_and(v < heads, g == v + 3 * triple * hop(v, triple) + triple * b)
        line[16:32, 0:rows] = dot(jnp.where(hit, 1.0, 0.0).astype(BF16), raw, NT)
        small_stage[seat] = line[...].astype(BF16)
    v = lax.broadcasted_iota(jnp.int32, (HEADS, LANES), 1)
    g = lax.broadcasted_iota(jnp.int32, (HEADS, LANES), 0)
    hit = jnp.logical_and(v < heads, g == v + 3 * triple * hop(v, triple) + triple * swapped(s))
    head_ref[...] = dot(ph_ref[...], jnp.where(hit, 1.0, 0.0), precision=HIGH)

    greet(
        [(None, d, p) for p in peers]
        + [(None, far, s), (z < deep - 1, up, s), (z > 0, down, s)]
        + [(moves, to_d, to_s), (moves, from_d, from_s)]
    )
    sends = Sends()

    def arrive(dst, sem):
        push(dst, dst, sem, sem, d, peers[0]).wait_recv()

    def mine(ref, k):
        return ref.at[:, pl.ds(k * part, part), :]

    def exchange(a, stage, target):
        for r, p in enumerate(peers):
            sends.start(
                None, push(stage.at[p], target(s), a_send.at[a, r], a_recv.at[a, r], d, p)
            )

    def exchanged(a, target):
        for r, p in enumerate(peers):
            arrive(target(p), a_recv.at[a, r])

    exchange(0, small_stage, lambda k: small_all.at[d, k])
    exchange(1, half_stage, lambda k: half_in.at[k])
    exchange(2, val_stage, lambda k: val_in.at[k])
    exchange(3, gate_stage, lambda k: gate_in.at[k])
    sends.start(moves, push(block_ref, out_shard, t_send.at[2], t_recv.at[2], to_d, to_s))
    sends.start(None, push(tok_ref, mine(tok, s), t_send.at[0], t_recv.at[0], d, peers[1]))
    sends.start(None, push(tok_ref, mine(tok, s), t_send.at[1], t_recv.at[1], d, peers[0]))
    sends.start(None, push(cot_ref, mine(cot_hbm, s), t_send.at[3], t_recv.at[3], d, peers[1]))
    sends.start(None, push(cot_ref, mine(cot_hbm, s), t_send.at[4], t_recv.at[4], d, peers[0]))
    saves = []

    def save(src, dst):
        copy = pltpu.make_async_copy(src, dst, l_sem.at[len(saves)])
        copy.start()
        saves.append(copy)

    save(cot_ref, mine(cot_hbm, s))
    small_all[d, s] = small_stage[s]
    half_in[s] = half_stage[s]
    val_in[s] = val_stage[s]
    gate_in[s] = gate_stage[s]
    tok[:, pl.ds(pl.multiple_of(s * part, part), part), :] = tok_ref[...]

    @pl.when(jnp.logical_not(moves))
    def _():
        out_shard[...] = block_ref[...]

    def begin(a, shard, dst):
        block = dst.at[d]
        sends.start(z < deep - 1, push(shard, block, z_send.at[a, 0, 0], z_recv.at[a, 0, 0], up, s))
        sends.start(z > 0, push(shard, block, z_send.at[a, 1, 0], z_recv.at[a, 1, 0], down, s))
        sends.start(None, push(shard, block, y_send.at[a, 0, 0], y_recv.at[a, 0, 0], far, s))

    def plan(a, dst, t):
        steps = []
        for way in range(2):
            here = (z >= t) if way == 0 else (z + t <= deep - 1)
            more = jnp.logical_and(here, (z < deep - 1) if way == 0 else (z > 0))
            at = jnp.clip(d - 2 * t if way == 0 else d + 2 * t, 0, dp - 1)
            block = dst.at[at]
            got = z_recv.at[a, way, t - 1]
            on = []
            if t < deep - 1:
                nxt = up if way == 0 else down
                on.append(
                    (more, push(block, block, z_send.at[a, way, t], z_recv.at[a, way, t], nxt, s))
                )
            on.append(
                (here, push(block, block, y_send.at[a, way, t], y_recv.at[a, way, t], far, s))
            )
            steps.append((here, push(block, block, got, got, d, peers[0]), on))
        return steps

    def run(steps):
        for here, wait, on in steps:
            pl.when(here)(wait.wait_recv)
            for cond, copy in on:
                pl.when(cond)(copy.start)

    def remember(steps):
        for _, _, on in steps:
            sends.items.extend(on)

    def relay(a, dst, t):
        steps = plan(a, dst, t)
        run(steps)
        remember(steps)

    def landed(a, dst):
        arrive(dst.at[far], y_recv.at[a, 0, 0])
        for t in range(1, deep):
            for way in range(2):
                here = (z >= t) if way == 0 else (z + t <= deep - 1)
                at = jnp.clip(far - 2 * t if way == 0 else far + 2 * t, 0, dp - 1)
                pl.when(here)(functools.partial(arrive, dst.at[at], y_recv.at[a, way, t]))

    def shard_of(a, pieces, dst):
        exchanged(a, lambda p: pieces.at[p])
        for k in range(tp):
            dst[d, k * rows : (k + 1) * rows, :] = pieces[k]
        begin(a, dst.at[d], dst)

    exchanged(0, lambda p: small_all.at[d, p])
    begin(0, small_all.at[d], small_all)
    shard_of(1, half_in, w_half)
    shard_of(2, val_in, w_val)
    for t in range(1, deep):
        relay(0, small_all, t)
        relay(1, w_half, t)
        relay(2, w_val, t)
    shard_of(3, gate_in, w_gate)
    pl.when(moves)(functools.partial(arrive, out_shard, t_recv.at[2]))
    begin(4, out_shard, out_hbm)
    save(out_shard, out_hbm.at[d])

    landed(0, small_all)

    def one_hot(columns, index, k, length):
        lane = lax.broadcasted_iota(jnp.int32, (LANES, columns), 1)
        at = lax.broadcasted_iota(jnp.int32, (LANES, columns), 0)
        hit = jnp.logical_and(at < length, index(lane) == k * length + at)
        return jnp.where(hit, 1.0, 0.0).astype(BF16)

    taps_ref[...] = jnp.zeros_like(taps_ref)
    gain_ref[...] = jnp.zeros_like(gain_ref)
    gated_ref[...] = jnp.zeros_like(gated_ref)

    def striped(v):
        return v + 3 * STRIPE * hop(v, STRIPE) + STRIPE * swapped(s)

    def lay_out(dd, carry):
        for kk in range(tp):
            k = dd * tp + kk
            values = small_all[dd, kk, 0:16, :]
            chans = one_hot(wide, lambda v: jnp.where(v < inner, striped(v), v - inner + DI), k, chan)
            taps_ref[...] += dot(values, chans)[:8]
            gain_ref[...] += dot(values, one_hot(width, lambda v: v, k, rows))
            gated_ref[...] += dot(values, one_hot(inner, striped, k, gpiece))
            turned = jnp.concatenate(
                [small_all[dd, kk, 16:32, :].astype(F32), jnp.zeros((LANES - 16, LANES), F32)], axis=0
            ).T
            w_tail[dd, kk * rows : (kk + 1) * rows, 2 * N :] = turned[:rows].astype(BF16)
        return carry

    lax.fori_loop(0, dp, lay_out, 0)
    landed(1, w_half)
    sends.start(None, push(w_half, w_other, t_send.at[6], t_recv.at[6], d, peers[0]))
    landed(2, w_val)
    save(w_val, rest_hbm.at[:, :, pl.ds(0, inner)])
    arrive(w_other, t_recv.at[6])

    def both_halves(dd, carry):
        w_tail[dd, :, pl.ds(pl.multiple_of(c * N, N), N)] = w_half[dd]
        w_tail[dd, :, pl.ds(pl.multiple_of((1 - c) * N, N), N)] = w_other[dd]
        return carry

    lax.fori_loop(0, dp, both_halves, 0)
    save(w_tail, rest_hbm.at[:, :, pl.ds(inner, w_tail.shape[2])])
    arrive(mine(tok, peers[1]), t_recv.at[0])
    block = mine(tok, peers[1])
    hand = push(block, block, t_send.at[5], t_recv.at[5], d, peers[0])
    hand.start()
    relay(3, w_gate, 1)
    relay(4, out_hbm, 1)
    arrive(mine(tok, peers[0]), t_recv.at[1])
    arrive(mine(tok, peers[2]), t_recv.at[5])
    hand.wait_send()

    tasks = [(a, ref, t) for t in range(2, deep) for a, ref in ((3, w_gate), (4, out_hbm))]
    chunks = micro * tp
    when = {}
    for n, task in enumerate(tasks):
        when.setdefault(min(n * 4 // len(tasks), chunks - 1), []).append(plan(*task))
    for plans in when.values():
        for steps in plans:
            remember(steps)

    def columns(i):
        return pl.ds(pl.multiple_of(i * part, part), part)

    def chunk(i, carry):
        m, k = i // tp, i % tp
        lines = pl.ds(pl.multiple_of(k * part, part), part)
        h = tok[m, lines, :].astype(F32)
        r = lax.rsqrt(jnp.mean(h * h, axis=-1, keepdims=True) + EPSILON)
        value = h * r * gain_ref[5:6, :]
        tok[m, lines, :] = value.astype(BF16)
        flipped[i] = value.T.astype(BF16)
        proj[i, :, 0:inner] = dot(tok[m, lines, :], w_val[...].reshape(width, inner))
        proj[i, :, inner:] = dot(tok[m, lines, :], w_tail[...].reshape(width, w_tail.shape[2]))
        forward_chunk(
            heads, k == 0, proj.at[i], taps_ref, head_ref, ssd.at[i], memory.at[i], xbuf, mem
        )
        pltpu.make_async_copy(tok.at[m, lines, :], normed_hbm.at[m, lines, :], o_sem.at[i]).start()
        pltpu.make_async_copy(flipped.at[i], turned_hbm.at[:, columns(i)], f_sem.at[i]).start()
        pltpu.make_async_copy(proj.at[i], proj_hbm.at[i], p_sem.at[i]).start()
        for n, plans in when.items():

            @pl.when(i == n)
            def _():
                for steps in plans:
                    run(steps)

        return carry

    lax.fori_loop(0, chunks, chunk, 0)
    save(ssd, ssd_hbm)
    save(memory, mem_hbm)
    arrive(mine(cot_hbm, peers[1]), t_recv.at[3])
    block = mine(cot_hbm, peers[1])
    sends.start(None, push(block, block, t_send.at[7], t_recv.at[7], d, peers[0]))
    landed(3, w_gate)
    save(w_gate, gate_hbm)

    def gating(i, carry):
        m, k = i // tp, i % tp
        lines = pl.ds(pl.multiple_of(k * part, part), part)
        gates[i] = dot(tok[m, lines, :], w_gate[...].reshape(width, inner))
        pltpu.make_async_copy(gates.at[i], gates_hbm.at[i], g_sem.at[i]).start()
        return carry

    lax.fori_loop(0, chunks, gating, 0)
    landed(4, out_hbm)
    arrive(mine(cot_hbm, peers[0]), t_recv.at[4])
    arrive(mine(cot_hbm, peers[2]), t_recv.at[7])

    def saved(i, carry):
        m, k = i // tp, i % tp
        lines = pl.ds(pl.multiple_of(k * part, part), part)
        pltpu.make_async_copy(tok.at[m, lines, :], normed_hbm.at[m, lines, :], o_sem.at[i]).wait()
        pltpu.make_async_copy(flipped.at[i], turned_hbm.at[:, columns(i)], f_sem.at[i]).wait()
        pltpu.make_async_copy(proj.at[i], proj_hbm.at[i], p_sem.at[i]).wait()
        pltpu.make_async_copy(gates.at[i], gates_hbm.at[i], g_sem.at[i]).wait()
        return carry

    lax.fori_loop(0, chunks, saved, 0)
    for copy in saves:
        copy.wait()
    sends.drain()


def head(in_proj, conv_weight, conv_bias, norm_gain, gated_gain, per_head, tokens, cotangent, out_proj, dp, tp):
    rows = in_proj.shape[0]
    heads = HEADS // tp
    inner = heads * P_SIZE
    full = inner + 2 * N + LANES
    micro, part, width = tokens.shape
    deep = dp // 2
    chunks = micro * tp
    block = tp * rows
    dma = pltpu.SemaphoreType.DMA
    vmem = pl.BlockSpec(memory_space=pltpu.VMEM)
    hbm = pl.BlockSpec(memory_space=pl.ANY)
    wide = inner + 2 * N

    def shape(*dims, kind=BF16):
        return jax.ShapeDtypeStruct(dims, kind)

    def room(*dims, kind=BF16):
        return pltpu.VMEM(dims, kind)

    return pl.pallas_call(
        functools.partial(head_kernel, dp, heads),
        in_specs=[vmem] * 9,
        out_specs=[hbm] * 10 + [vmem] * 4,
        out_shape=[
            shape(micro, tp * part, width),
            shape(width, chunks * part),
            shape(chunks, part, full, kind=F32),
            shape(chunks, part, inner, kind=F32),
            shape(chunks, N, inner),
            shape(chunks, part, inner, kind=F32),
            shape(dp, block, full),
            shape(dp, block, inner),
            shape(dp, out_proj.shape[0], width),
            shape(micro, tp * part, width),
            shape(8, wide, kind=F32),
            shape(16, width, kind=F32),
            shape(16, inner, kind=F32),
            shape(8, LANES, kind=F32),
        ],
        scratch_shapes=[
            room(32, LANES, kind=F32),
            room(tp, 32, LANES),
            room(tp, rows, inner),
            room(tp, rows, N),
            room(tp, rows, inner),
            room(dp, tp, 32, LANES),
            room(tp, rows, inner),
            room(tp, rows, N),
            room(tp, rows, inner),
            room(dp, block, inner),
            room(dp, block, N),
            room(dp, block, N),
            room(dp, block, 2 * N + LANES),
            room(dp, block, inner),
            room(*out_proj.shape),
            room(micro, tp * part, width),
            room(chunks, width, part),
            room(chunks, part, full, kind=F32),
            room(chunks, part, inner, kind=F32),
            room(chunks, part, inner, kind=F32),
            room(chunks, N, inner),
            room(part + 8, wide, kind=F32),
            room(N, inner, kind=F32),
            dma((8,)),
            dma((chunks,)),
            dma((chunks,)),
            dma((chunks,)),
            dma((chunks,)),
            dma((4, 3)),
            dma((4, 3)),
            dma((5, 2, deep - 1)),
            dma((5, 2, deep - 1)),
            dma((5, 2, deep)),
            dma((5, 2, deep)),
            dma((8,)),
            dma((8,)),
        ],
        compiler_params=pltpu.CompilerParams(
            collective_id=1, has_side_effects=True, vmem_limit_bytes=62 * 2**20
        ),
        cost_estimate=pl.CostEstimate(flops=10**11, bytes_accessed=5 * 10**7, transcendentals=0),
        name="gather_and_mix",
    )(in_proj, conv_weight, conv_bias, norm_gain, gated_gain, per_head, tokens, cotangent, out_proj)


class OwnerSum:
    def __init__(self, where, sends, source, mine, ybuf, zbuf, final, sems, theirs_ref=None):
        self.where, self.sends = where, sends
        self.mine, self.ybuf, self.zbuf, self.final = mine, ybuf, zbuf, final
        d, s, z, y, _, _, _, deep = where
        self.load_sem, y_send, self.y_recv, z_send, self.z_recv = sems
        lower = z < deep // 2

        def place(j):
            low = jnp.where(j > z, deep - 1 - j, deep - 1 - z + j)
            high = jnp.where(j < z, j, z + deep - 1 - j)
            return jnp.where(j == z, deep - 1, jnp.where(lower, low, high))

        def turn(k):
            low = jnp.where(k < deep - 1 - z, deep - 1 - k, k - (deep - 1 - z))
            high = jnp.where(k < z, k, deep - 1 - (k - z))
            return jnp.where(lower, low, high) if k < deep - 1 else z

        self.order = [turn(k) for k in range(deep)]
        self.y_items, self.loads = [], []
        for k, j in enumerate(self.order):
            theirs = source.at[j * 2 + 1 - y] if theirs_ref is None else theirs_ref.at[k]
            copy = push(theirs, ybuf.at[k], y_send.at[k], self.y_recv.at[k], d + 1 - 2 * y, s)
            self.y_items.append((None, copy))
            if theirs_ref is None:
                own = source.at[j * 2 + y]
                self.loads.append(pltpu.make_async_copy(own, mine.at[k], self.load_sem.at[k]))
        self.z_items = []
        for t in range(deep - 1):
            ways = []
            for way in range(2):
                depth = z if way == 0 else deep - 1 - z
                j = deep - 1 - t + z if way == 0 else t + z - deep + 1
                k = place(jnp.clip(j, 0, deep - 1))
                nxt = d + 2 if way == 0 else d - 2
                dst, ss, rs = zbuf.at[way, t], z_send.at[way, t], self.z_recv.at[way, t]
                first = (depth == 0, push(ybuf.at[k], dst, ss, rs, nxt, s))
                later = None
                if t > 0:
                    cond = jnp.logical_and(depth > 0, depth <= t)
                    later = (cond, push(zbuf.at[way, t - 1], dst, ss, rs, nxt, s))
                ways.append((k, first, later))
            self.z_items.append(ways)
        sends.items.extend(self.y_items)
        for ways in self.z_items:
            for _, first, later in ways:
                sends.items.append(first)
                if later is not None:
                    sends.items.append(later)

    def arrive(self, ref, sem):
        d, s = self.where[:2]
        push(ref, ref, sem, sem, d, self.where[6][0]).wait_recv()

    def begin(self):
        for _, copy in self.y_items:
            copy.start()
        for copy in self.loads:
            copy.start()

    def each(self, work):
        if self.mine.ndim == 4:
            count, cut = self.mine.shape[1], lambda i: i
        else:
            count, cut = self.mine.shape[1] // 16, lambda i: pl.ds(pl.multiple_of(i * 16, 16), 16)
        lax.fori_loop(0, count, lambda i, carry: (work(cut(i)), carry)[1], 0)

    def add(self, k):
        if self.loads:
            self.loads[k].wait()
        self.arrive(self.ybuf.at[k], self.y_recv.at[k])
        ybuf, mine = self.ybuf, self.mine

        def work(i):
            ybuf[k, i] = (ybuf[k, i].astype(F32) + mine[k, i].astype(F32)).astype(BF16)

        self.each(work)

    def send(self, t):
        zbuf, ybuf = self.zbuf, self.ybuf
        for way, (k, first, later) in enumerate(self.z_items[t]):
            pl.when(first[0])(first[1].start)
            if later is None:
                continue

            @pl.when(later[0])
            def _():
                self.arrive(zbuf.at[way, t - 1], self.z_recv.at[way, t - 1])

                def work(i):
                    zbuf[way, t - 1, i] = (
                        zbuf[way, t - 1, i].astype(F32) + ybuf[k, i].astype(F32)
                    ).astype(BF16)

                self.each(work)
                later[1].start()

    def finish(self):
        z, deep = self.where[2], self.where[7]
        zbuf, ybuf, final = self.zbuf, self.ybuf, self.final
        for way in range(2):
            depth = z if way == 0 else deep - 1 - z
            pl.when(depth > 0)(
                functools.partial(self.arrive, zbuf.at[way, deep - 2], self.z_recv.at[way, deep - 2])
            )

        def work(ways, i):
            total = ybuf[deep - 1, i].astype(F32)
            for way in ways:
                total = total + zbuf[way, deep - 2, i].astype(F32)
            final[i] = total.astype(BF16)

        for cond, ways in (
            (z == 0, (1,)),
            (z == deep - 1, (0,)),
            (jnp.logical_and(z > 0, z < deep - 1), (0, 1)),
        ):
            pl.when(cond)(functools.partial(self.each, functools.partial(work, ways)))


def middle_kernel(
    dp,
    heads,
    rest_ref,
    prev_ref,
    dy_ref,
    mem_ref,
    taps_ref,
    head_ref,
    part_hbm,
    gout_hbm,
    ggate_hbm,
    tok_hbm,
    out_ref,
    wgrad_ref,
    hgrad_ref,
    own_hbm,
    gout_out,
    ggate_out,
    xbuf,
    gbuf,
    adj,
    dmix,
    dsum,
    uprod,
    zprod,
    rows_t,
    line,
    acts,
    slopes,
    o_mine,
    o_y,
    o_z,
    o_final,
    g_mine,
    g_y,
    g_z,
    g_final,
    own,
    core_buf,
    x_buf,
    tok,
    result,
    o_load,
    o_ysend,
    o_yrecv,
    o_zsend,
    o_zrecv,
    g_load,
    g_ysend,
    g_yrecv,
    g_zsend,
    g_zrecv,
    b_load,
    c_send,
    c_recv,
    m_send,
    m_recv,
):
    where = where_am_i(dp)
    d, s, z, y, x, c, peers, deep = where
    micro, part, width = result.shape
    step = pl.program_id(0) * pl.num_programs(1) + pl.program_id(1)
    tp = ggate_hbm.shape[1]
    me = d * tp + s
    turned = stripe_block(d, s, dp)
    moves = turned != me
    to_d, to_s = turned // tp, turned % tp
    from_d, from_s = stripe_owner(me, dp), stripe_seat(me, dp)
    sends = Sends()
    gout = OwnerSum(
        where, sends, gout_hbm, o_mine, o_y, o_z, o_final, (o_load, o_ysend, o_yrecv, o_zsend, o_zrecv)
    )
    ggate = OwnerSum(
        where, sends, ggate_hbm, g_mine, g_y, g_z, g_final, (g_load, g_ysend, g_yrecv, g_zsend, g_zrecv)
    )

    def chunk(k):
        return part_hbm.at[:, pl.ds(k * part, part), :]

    cores, loads = [], []
    for q, xx in enumerate((1 - x, x)):
        cores.append(
            push(chunk(xx * 2 + 1 - c), core_buf.at[q], c_send.at[q], c_recv.at[q], d, peers[0])
        )
        loads.append(pltpu.make_async_copy(chunk(xx * 2 + c), own.at[q], b_load.at[q]))
    across = push(core_buf.at[0], x_buf, m_send.at[0], m_recv.at[0], d, peers[1])
    turning = push(o_final, gout_out, m_send.at[1], m_recv.at[1], to_d, to_s)
    staying = pltpu.make_async_copy(o_final, gout_out, b_load.at[2])
    kept = pltpu.make_async_copy(g_final, ggate_out, b_load.at[3])
    saved = pltpu.make_async_copy(result, own_hbm, b_load.at[4])
    loads.append(pltpu.make_async_copy(tok_hbm, tok, b_load.at[5]))
    for copy in cores + [across]:
        sends.items.append((None, copy))
    sends.items.append((moves, turning))
    span = 16

    def by_rows(work):
        def one(i, carry):
            m, row = i // (part // span), (i % (part // span)) * span
            work(m, pl.ds(pl.multiple_of(row, span), span))
            return carry

        lax.fori_loop(0, micro * (part // span), one, 0)

    def start():
        greet(
            [(None, d, p) for p in peers]
            + [(None, d + 1 - 2 * y, s), (z < deep - 1, d + 2, s), (z > 0, d - 2, s)]
            + [(moves, to_d, to_s), (moves, from_d, from_s)]
        )
        for copy in cores + loads:
            copy.start()
        gout.begin()
        ggate.begin()

    def pass_on():
        loads[0].wait()
        cores[0].wait_recv()

        def work(m, rows):
            core_buf[0, m, rows, :] = (
                core_buf[0, m, rows, :].astype(F32) + own[0, m, rows, :].astype(F32)
            ).astype(BF16)

        by_rows(work)
        across.start()

    def collect():
        loads[1].wait()
        loads[2].wait()
        cores[1].wait_recv()
        across.wait_recv()

        def work(m, rows):
            result[m, rows, :] = (
                core_buf[1, m, rows, :].astype(F32)
                + own[1, m, rows, :].astype(F32)
                + x_buf[m, rows, :].astype(F32)
                + tok[m, rows, :].astype(F32)
            ).astype(BF16)

        by_rows(work)
        saved.start()

    def hand_over():
        gout.finish()
        pl.when(moves)(turning.start)
        pl.when(jnp.logical_not(moves))(staying.start)

    def last():
        ggate.add(deep - 1)
        ggate.finish()
        kept.start()
        pl.when(moves)(turning.wait_recv)
        pl.when(jnp.logical_not(moves))(staying.wait)
        kept.wait()
        saved.wait()
        sends.drain()

    stages = {}

    def at(n, task, *args):
        stages.setdefault(n, []).append(functools.partial(task, *args))

    at(0, start)
    at(1, pass_on)
    for k in range(deep - 1):
        n = k * 2 // (deep - 2)
        at(2 + n, gout.add, k)
        at(2 + n, gout.send, k)
    at(4, gout.add, deep - 1)
    at(5, hand_over)
    for k in range(deep - 1):
        n = k * 2 // (deep - 2)
        at(5 + n, ggate.add, k)
        at(5 + n, ggate.send, k)
    at(6, collect)
    for n, tasks in stages.items():

        @pl.when(step == n)
        def _():
            for task in tasks:
                task()

    backward_kernel(
        heads,
        rest_ref,
        prev_ref,
        dy_ref,
        mem_ref,
        taps_ref,
        head_ref,
        out_ref,
        wgrad_ref,
        hgrad_ref,
        xbuf,
        gbuf,
        adj,
        dmix,
        dsum,
        uprod,
        zprod,
        rows_t,
        line,
        acts,
        slopes,
    )
    pl.when(step == pl.num_programs(0) * pl.num_programs(1) - 1)(last)


def middle(rest, dy, memory, taps, head, partial, gout, ggate, tokens, dp, tp, heads, micro):
    count, full = rest.shape
    wide = taps.shape[1]
    inner = heads * P_SIZE
    _, length, width = partial.shape
    part = length // tp
    chunks = length // part
    deep = dp // 2
    dma = pltpu.SemaphoreType.DMA
    hbm = pl.BlockSpec(memory_space=pl.ANY)
    gout = gout.reshape(dp, 2, -1, width)

    def at(m, c):
        return m * chunks + chunks - 1 - c

    def sums(block):
        kinds = [(deep,), (deep,), (2, deep - 1), ()]
        return [pltpu.VMEM(kind + block, BF16) for kind in kinds]

    sems = [dma((deep,))] * 3 + [dma((2, deep - 1))] * 2
    out = pl.pallas_call(
        functools.partial(middle_kernel, dp, heads),
        grid=(micro, chunks),
        in_specs=[
            pl.BlockSpec((part, full), lambda m, c: (at(m, c), 0)),
            pl.BlockSpec((8, full), lambda m, c: (jnp.maximum(at(m, c) * (part // 8) - 1, 0), 0)),
            pl.BlockSpec((part, inner), lambda m, c: (at(m, c), 0)),
            pl.BlockSpec((1, N, inner), lambda m, c: (at(m, c), 0, 0)),
            pl.BlockSpec((8, wide), lambda m, c: (0, 0)),
            pl.BlockSpec((8, LANES), lambda m, c: (0, 0)),
            hbm,
            hbm,
            hbm,
            hbm,
        ],
        out_specs=[
            pl.BlockSpec((part, full), lambda m, c: (at(m, c), 0)),
            pl.BlockSpec((8, wide), lambda m, c: (0, 0)),
            pl.BlockSpec((8, LANES), lambda m, c: (0, 0)),
            hbm,
            hbm,
            hbm,
        ],
        out_shape=[
            jax.ShapeDtypeStruct((count, full), BF16),
            jax.ShapeDtypeStruct((8, wide), F32),
            jax.ShapeDtypeStruct((8, LANES), F32),
            jax.ShapeDtypeStruct((micro, part, width), BF16),
            jax.ShapeDtypeStruct(gout.shape[1:], BF16),
            jax.ShapeDtypeStruct(ggate.shape[1:], BF16),
        ],
        scratch_shapes=[
            pltpu.VMEM((part + 8, wide), F32),
            pltpu.VMEM((part + 8, wide), F32),
            pltpu.VMEM((N, inner), F32),
            pltpu.VMEM((part, wide), F32),
            pltpu.VMEM((part, inner), BF16),
            pltpu.VMEM((part, inner), BF16),
            pltpu.VMEM((part, inner), BF16),
            pltpu.VMEM((LANES, part), F32),
            pltpu.VMEM((8, inner), F32),
            pltpu.VMEM((part, wide), F32),
            pltpu.VMEM((part, wide), F32),
        ]
        + sums(gout.shape[1:])
        + sums(ggate.shape[1:])
        + [
            pltpu.VMEM((2, micro, part, width), BF16),
            pltpu.VMEM((2, micro, part, width), BF16),
            pltpu.VMEM((micro, part, width), BF16),
            pltpu.VMEM((micro, part, width), BF16),
            pltpu.VMEM((micro, part, width), BF16),
        ]
        + sems
        + sems
        + [dma((6,)), dma((2,)), dma((2,)), dma((2,)), dma((2,))],
        compiler_params=pltpu.CompilerParams(
            dimension_semantics=("arbitrary", "arbitrary"),
            collective_id=4,
            has_side_effects=True,
            vmem_limit_bytes=62 * 2**20,
        ),
        cost_estimate=pl.CostEstimate(flops=7 * 10**10, bytes_accessed=4 * 10**7, transcendentals=0),
        name="mixer_backward_and_sums",
    )(rest, rest, dy, memory, taps, head, partial, gout, ggate, tokens)
    rest_grad, wgrad, hgrad, own, gout, ggate = out
    return rest_grad, wgrad, hgrad, own, gout.reshape(-1, width), ggate


def gating_kernel(
    dp,
    ssd_hbm,
    gate_hbm,
    cot_hbm,
    out_hbm,
    turned_hbm,
    gain_ref,
    grad_ssd_hbm,
    grad_gate_hbm,
    part_hbm,
    gout_hbm,
    ggate_hbm,
    ssd,
    gate,
    cot,
    w_out,
    turned,
    weighed,
    shaped_t,
    grad_gate,
    partial,
    gout,
    ggate,
    stats,
    held,
    l_sem,
    c_sem,
    s_sem,
    g_sem,
    p_sem,
    o_sem,
    send,
    recv,
):
    d, s, *_, peers, _ = where_am_i(dp)
    chunks, part, inner = ssd.shape
    width = cot.shape[2]
    count = chunks * part

    def loads(i):
        return [
            pltpu.make_async_copy(cot_hbm.at[i], cot.at[i], c_sem.at[0, i]),
            pltpu.make_async_copy(ssd_hbm.at[i], ssd.at[i], c_sem.at[1, i]),
            pltpu.make_async_copy(gate_hbm.at[i], gate.at[i], c_sem.at[2, i]),
        ]

    first = pltpu.make_async_copy(out_hbm, w_out, l_sem.at[0])
    other = pltpu.make_async_copy(turned_hbm, turned, l_sem.at[1])
    first.start()
    for i in range(chunks):
        for copy in loads(i):
            copy.start()
    other.start()
    greet([(None, d, p) for p in peers])
    first.wait()

    def gated_parts(i):
        g = gate[i]
        sig = lax.logistic(g)
        act = g * sig
        return sig, act, ssd[i] * act

    def measure(i, carry):
        for copy in loads(i):
            copy.wait()
        w = dot(cot[i], w_out[...], NT) * gain_ref[KW + 2 : KW + 3, :]
        weighed[i] = w
        _, _, gated = gated_parts(i)
        lane = lax.broadcasted_iota(jnp.int32, (part, LANES), 1)
        both = jnp.where(lane == 0, jnp.sum(gated * gated, axis=1, keepdims=True), 0.0)
        both = jnp.where(lane == 1, jnp.sum(w * gated, axis=1, keepdims=True), both)
        stats[i] = both.T[:8, :]
        return carry

    lax.fori_loop(0, chunks, measure, 0)
    copies = [push(stats, held.at[r], send.at[r], recv.at[r], d, p) for r, p in enumerate(peers)]
    for copy in copies:
        copy.start()
    for copy in copies:
        copy.wait()

    def out_copies(i):
        return [
            pltpu.make_async_copy(weighed.at[i], grad_ssd_hbm.at[i], s_sem.at[i]),
            pltpu.make_async_copy(grad_gate.at[i], grad_gate_hbm.at[i], g_sem.at[i]),
            pltpu.make_async_copy(partial.at[i], part_hbm.at[i], p_sem.at[i]),
        ]

    def columns(i):
        return pl.ds(pl.multiple_of(i * part, part), part)

    def shape_chunk(i, carry):
        sums = (stats[i] + held[0, i]) + (held[1, i] + held[2, i])
        sums = jnp.concatenate([sums, jnp.zeros((LANES - 8, part), F32)], axis=0).T
        q = lax.rsqrt(sums[:, 0:1] / DI + EPSILON)
        pull = q * q * (sums[:, 1:2] / DI)
        sig, act, gated = gated_parts(i)
        value = gated * q * gain_ref[KW + 2 : KW + 3, :]
        shaped_t[:, columns(i)] = value.T.astype(BF16)
        partial[i] = dot(value.astype(BF16), w_out[...]).astype(BF16)
        grad = q * (weighed[i] - gated * pull)
        grad_gate[i] = (grad * ssd[i] * (sig + act * (1.0 - sig))).astype(BF16)
        weighed[i] = grad * act
        for copy in out_copies(i):
            copy.start()
        return carry

    lax.fori_loop(0, chunks, shape_chunk, 0)
    other.wait()
    high, across = min(384, inner), min(512, width)

    def out_tile(i, carry):
        a = pl.ds(pl.multiple_of(i // (width // across) * high, high), high)
        b = pl.ds(pl.multiple_of(i % (width // across) * across, across), across)
        gout[a, b] = dot(shaped_t[a, :], cot[:, :, b].reshape(count, across)).astype(BF16)
        return carry

    lax.fori_loop(0, (inner // high) * (width // across), out_tile, 0)
    save_out = pltpu.make_async_copy(gout, gout_hbm, o_sem.at[0])
    save_out.start()

    def gate_tile(i, carry):
        a = pl.ds(pl.multiple_of(i // 2 * across, across), across)
        b = pl.ds(pl.multiple_of(i % 2 * (inner // 2), inner // 2), inner // 2)
        ggate[a, b] = dot(turned[a, :], grad_gate[:, :, b].reshape(count, inner // 2)).astype(BF16)
        return carry

    lax.fori_loop(0, (width // across) * 2, gate_tile, 0)
    save_gate = pltpu.make_async_copy(ggate, ggate_hbm, o_sem.at[1])
    save_gate.start()

    def saved(i, carry):
        for copy in out_copies(i):
            copy.wait()
        return carry

    lax.fori_loop(0, chunks, saved, 0)
    save_out.wait()
    save_gate.wait()


def gating(ssd, gate, cot, w_out, normed_t, gains, dp):
    chunks, part, inner = ssd.shape
    width, count = normed_t.shape
    cot = cot.reshape(chunks, part, width)
    dma = pltpu.SemaphoreType.DMA
    vmem = pl.BlockSpec(memory_space=pltpu.VMEM)
    hbm = pl.BlockSpec(memory_space=pl.ANY)

    def shape(*dims, kind=BF16):
        return jax.ShapeDtypeStruct(dims, kind)

    def room(*dims, kind=BF16):
        return pltpu.VMEM(dims, kind)

    return pl.pallas_call(
        functools.partial(gating_kernel, dp),
        in_specs=[hbm] * 5 + [vmem],
        out_specs=[hbm] * 5,
        out_shape=[
            shape(chunks, part, inner, kind=F32),
            shape(chunks, part, inner),
            shape(chunks, part, width),
            shape(inner, width),
            shape(width, inner),
        ],
        scratch_shapes=[
            room(chunks, part, inner, kind=F32),
            room(chunks, part, inner, kind=F32),
            room(chunks, part, width),
            room(inner, width),
            room(width, count),
            room(chunks, part, inner, kind=F32),
            room(inner, count),
            room(chunks, part, inner),
            room(chunks, part, width),
            room(inner, width),
            room(width, inner),
            room(chunks, 8, part, kind=F32),
            room(3, chunks, 8, part, kind=F32),
            dma((2,)),
            dma((3, chunks)),
            dma((chunks,)),
            dma((chunks,)),
            dma((chunks,)),
            dma((2,)),
            dma((3,)),
            dma((3,)),
        ],
        compiler_params=pltpu.CompilerParams(
            collective_id=2, has_side_effects=True, vmem_limit_bytes=63 * 2**20
        ),
        cost_estimate=pl.CostEstimate(flops=3 * 10**10, bytes_accessed=5 * 10**7, transcendentals=0),
        name="gating_and_gradients",
    )(ssd, gate, cot, w_out, normed_t, gains)


def as_row(column):
    size = column.shape[0]
    square = jnp.broadcast_to(column, (size, LANES))
    square = jnp.concatenate([square, jnp.zeros((LANES - size, LANES), F32)], axis=0)
    return square.T[0:1, :size]


def tail_kernel(
    dp,
    normed_hbm,
    rows_hbm,
    gates_hbm,
    w_rest_hbm,
    w_gate_hbm,
    tok_hbm,
    cot_hbm,
    gate_hbm,
    gout_hbm,
    proj_ref,
    block_ref,
    gain_ref,
    wgrad_ref,
    hgrad_ref,
    ng_ref,
    gg_ref,
    tokens_ref,
    grad_ref,
    dots_ref,
    gout_ref,
    gdots_ref,
    taps_ref,
    bias_ref,
    heads_ref,
    out_ref,
    own_ref,
    sums_ref,
    tok,
    cot,
    gate_in,
    gout,
    normed,
    rows_ref,
    gates_ref,
    w_rest,
    w_gate,
    tile,
    wtile,
    btile,
    b_own,
    b_out,
    b_in,
    theirs,
    mine,
    ybuf,
    zbuf,
    final,
    handed,
    core_buf,
    core_out,
    x_buf,
    x_out,
    s_buf,
    l_sem,
    n_sem,
    b_send,
    b_recv,
    g_send,
    g_recv,
    y_send,
    y_recv,
    z_send,
    z_recv,
    a_send,
    a_recv,
    c_send,
    c_recv,
    x_send,
    x_recv,
    s_send,
    s_recv,
):
    where = where_am_i(dp)
    d, s, z, y, x, c, peers, deep = where
    tp, rows = out_ref.shape[:2]
    block = tp * rows
    micro, part, width = own_ref.shape
    inner = gates_ref.shape[1]
    bits = dp.bit_length() - 1
    partners = []
    for k in range(bits):
        step = 2**k
        bit = (d // step) % 2
        partners.append(d + step - 2 * step * bit)
    sends = Sends()
    total = OwnerSum(
        where,
        sends,
        None,
        mine,
        ybuf,
        zbuf,
        final,
        (None, y_send, y_recv, z_send, z_recv),
        theirs,
    )
    loads = [
        pltpu.make_async_copy(src, dst, l_sem.at[k])
        for k, (src, dst) in enumerate(
            (
                (rows_hbm, rows_ref),
                (w_rest_hbm, w_rest),
                (gates_hbm, gates_ref),
                (w_gate_hbm, w_gate),
                (tok_hbm, tok),
                (cot_hbm, cot),
                (gate_hbm.at[s], gate_in.at[s]),
                (gout_hbm, gout),
            )
        )
    ]
    fetches = []
    for k in range(deep):
        lines = pl.ds(pl.multiple_of(total.order[k] * 2 * block, 2 * block), 2 * block)
        fetches.append(pltpu.make_async_copy(normed_hbm.at[lines, :], normed.at[k], n_sem.at[k]))
    for copy in loads + fetches:
        copy.start()
    greet(
        [(None, d, p) for p in peers]
        + [(None, d + 1 - 2 * y, s), (z < deep - 1, d + 2, s), (z > 0, d - 2, s)]
        + [(None, partners[k], s) for k in range(2, bits)]
    )

    def arrive(dst, sem):
        push(dst, dst, sem, sem, d, peers[0]).wait_recv()

    sums_ref[0, :, 0 : wgrad_ref.shape[1]] = wgrad_ref[...]
    sums_ref[0, :, wgrad_ref.shape[1] :] = hgrad_ref[...]

    def each(count, work):
        lax.fori_loop(0, count, lambda i, carry: (work(i), carry)[1], 0)

    across = width // tile.shape[1]
    span = wtile.shape[1]

    def product(owner, use):
        def work(i):
            m, n = i // across, i % across
            row = pl.multiple_of((m * tp + owner) * part, part)
            col = pl.multiple_of(n * tile.shape[1], tile.shape[1])
            lines = pl.ds(col, tile.shape[1])
            tile[...] = dot(rows_ref[pl.ds(row, part), :], w_rest[lines, :], NT) + dot(
                gates_ref[pl.ds(row, part), :], w_gate[lines, :], NT
            )
            use(m, lines)

        each(micro * across, work)

    def weight(k):
        fetches[k].wait()
        far = pl.ds(pl.multiple_of((1 - y) * block, block), block)
        near = pl.ds(pl.multiple_of(y * block, block), block)

        def work(n):
            cols = pl.ds(pl.multiple_of(n * span, span), span)
            wtile[...] = dot(normed[k], rows_ref[:, cols])
            theirs[k, :, cols] = wtile[far, :].astype(BF16)
            mine[k, :, cols] = wtile[near, :].astype(BF16)

        lines = pl.ds(inner, 2 * N)
        btile[...] = dot(normed[k], rows_ref[:, lines])
        ours = pl.ds(pl.multiple_of(c * N, N), N)
        b_out[k] = btile[:, pl.ds(pl.multiple_of((1 - c) * N, N), N)].astype(BF16)
        b_own[...] = btile[:, ours]
        swap = push(b_out.at[k], b_in.at[k], b_send.at[k], b_recv.at[k], d, peers[0])
        sends.start(None, swap)
        each(inner // span, work)
        b_tail = dot(normed[k], rows_ref[:, inner + 2 * N :])
        btile[:, N:] = b_tail
        arrive(b_in.at[k], b_recv.at[k])
        btile[:, 0:N] = b_own[...] + b_in[k].astype(F32)
        theirs[k, :, inner:] = btile[far, :].astype(BF16)
        mine[k, :, inner:] = btile[near, :].astype(BF16)
        total.y_items[k][1].start()

    def doubling(k):
        arrive(s_buf.at[k], s_recv.at[k])
        sums_ref[k + 1] = sums_ref[k] + s_buf[k]
        if k + 1 < bits:
            src = sums_ref.at[k + 1]
            sends.start(
                None, push(src, s_buf.at[k + 1], s_send.at[k + 1], s_recv.at[k + 1], partners[k + 1], s)
            )

    def to_core(q):
        def use(m, lines):
            core_out[q, m, :, lines] = tile[...].astype(BF16)

        return use

    def to_chip(m, lines):
        x_out[m, :, lines] = (tile[...] + core_buf[0, m, :, lines].astype(F32)).astype(BF16)

    def keep(m, lines):
        own_ref[m, :, lines] = tile[...] + core_buf[1, m, :, lines].astype(F32)

    for copy in loads[:4]:
        copy.wait()
    for r, p in enumerate(peers):
        swap = push(gate_hbm.at[p], gate_in.at[s], g_send.at[r], g_recv.at[r], d, p)
        sends.start(None, swap)
    src = sums_ref.at[0]
    sends.start(None, push(src, s_buf.at[0], s_send.at[0], s_recv.at[0], partners[0], s))
    product((1 - x) * 2 + 1 - c, to_core(0))
    sends.start(
        None, push(core_out.at[0], core_buf.at[0], c_send.at[0], c_recv.at[0], d, peers[0])
    )
    weight(0)
    arrive(core_buf.at[0], c_recv.at[0])
    product((1 - x) * 2 + c, to_chip)
    sends.start(None, push(x_out, x_buf, x_send.at[0], x_recv.at[0], d, peers[1]))
    weight(1)
    total.add(0)
    total.send(0)
    doubling(0)
    for k in range(2, deep):
        weight(k)
    total.add(1)
    total.send(1)
    doubling(1)
    product(x * 2 + 1 - c, to_core(1))
    sends.start(
        None, push(core_out.at[1], core_buf.at[1], c_send.at[1], c_recv.at[1], d, peers[0])
    )
    for k in range(2, deep - 1):
        total.add(k)
        total.send(k)
        if k < bits:
            doubling(k)
    arrive(core_buf.at[1], c_recv.at[1])
    product(s, keep)
    for k in range(deep - 1, bits):
        doubling(k)
    for r, p in enumerate(peers):
        src, dst = sums_ref.at[bits], sums_ref.at[bits + 1 + s]
        sends.start(None, push(src, dst, s_send.at[bits + r], s_recv.at[bits + r], d, p))
    sums_ref[bits + 1 + s] = sums_ref[bits]
    for copy in loads[4:]:
        copy.wait()
    for r, p in enumerate(peers):
        arrive(gate_in.at[p], g_recv.at[r])
    wide = inner + 2 * N
    heads = inner // P_SIZE
    triple = HEADS // 16
    for b in range(4):
        seat = 2 * (b % 2) + b // 2
        for k in range(4):
            at = (4 * k + b) * STRIPE
            grad_ref[:, at : at + STRIPE] = gate_in[seat, :, k * STRIPE : (k + 1) * STRIPE].astype(F32)
    gout_ref[...] = gout[...].astype(F32)
    gsum = jnp.sum(gout_ref[...] * block_ref[...].astype(F32), axis=1, keepdims=True)
    gdots_ref[...] = as_row(gsum) / gg_ref[...].astype(F32)
    for r, p in enumerate(peers):
        arrive(sums_ref.at[bits + 1 + p], s_recv.at[bits + r])
    chan = taps_ref.shape[1]
    convs = jnp.zeros((8, chan), F32)
    per_head = jnp.zeros((8, HEADS), F32)
    v = lax.broadcasted_iota(jnp.int32, (wide, chan), 0)
    g = lax.broadcasted_iota(jnp.int32, (wide, chan), 1) + chan * (d * tp + s)
    lane = lax.broadcasted_iota(jnp.int32, (LANES, HEADS), 0)
    head = lax.broadcasted_iota(jnp.int32, (LANES, HEADS), 1)
    place = []
    for p in range(tp):
        b = 2 * (p % 2) + p // 2
        from_v = jnp.where(v < inner, v + 3 * STRIPE * hop(v, STRIPE) + STRIPE * b, v - inner + DI)
        sums = sums_ref[bits + 1 + p]
        convs = convs + dot(sums[:, :wide], jnp.where(from_v == g, 1.0, 0.0), precision=HIGH)
        hit = jnp.logical_and(lane < heads, head == lane + 3 * triple * hop(lane, triple) + triple * b)
        place.append(jnp.where(hit, 1.0, 0.0))
        per_head = per_head + dot(sums[:, wide:], place[p], precision=HIGH)
    taps_ref[...] = convs[:KW]
    bias_ref[...] = convs[KW : KW + 1]
    heads_ref[...] = per_head
    total.add(deep - 1)
    total.finish()
    for p in range(tp):
        handed[p] = final[p * rows : (p + 1) * rows, :]
    for r, p in enumerate(peers):
        sends.start(None, push(handed.at[p], out_ref.at[s], a_send.at[r], a_recv.at[r], d, p))
    out_ref[s] = handed[s]

    arrive(x_buf, x_recv.at[0])

    def last(i):
        m, row = i // (part // 16), (i % (part // 16)) * 16
        lines = pl.ds(pl.multiple_of(row, 16), 16)
        h = tok[m, lines, :].astype(F32)
        r = lax.rsqrt(jnp.mean(h * h, axis=-1, keepdims=True) + EPSILON)
        n = h * r
        grad = (own_ref[m, lines, :] + x_buf[m, lines, :].astype(F32)) * gain_ref[KW + 1 : KW + 2, :]
        grad = grad - n * jnp.mean(grad * n, axis=-1, keepdims=True)
        tokens_ref[m, lines, :] = (cot[m, lines, :].astype(F32) + r * grad).astype(BF16)

    each(micro * (part // 16), last)
    for r, p in enumerate(peers):
        arrive(out_ref.at[p], a_recv.at[r])
    both = [jnp.zeros((rows, N), F32), jnp.zeros((rows, N), F32)]
    steps = jnp.zeros((rows, HEADS), F32)
    for b in range(4):
        seat = 2 * (b % 2) + b // 2
        for k in range(4):
            at = DI + (4 * k + b) * STRIPE
            piece = out_ref[seat, :, k * STRIPE : (k + 1) * STRIPE]
            grad_ref[:, at : at + STRIPE] = piece.astype(F32)
        both[seat % 2] = both[seat % 2] + out_ref[seat, :, inner : inner + N].astype(F32)
        steps = steps + dot(out_ref[seat, :, inner + N :], place[seat].astype(BF16))
    grad_ref[:, 2 * DI : 2 * DI + N] = both[0]
    grad_ref[:, 2 * DI + N : 2 * DI + 2 * N] = both[1]
    grad_ref[:, 2 * DI + 2 * N :] = steps
    nsum = jnp.sum(grad_ref[...] * proj_ref[...].astype(F32), axis=1, keepdims=True)
    dots_ref[...] = as_row(nsum) / ng_ref[...].astype(F32)
    sends.drain()


def tail(
    normed_t, rows_grad, gates_grad, w_rest, w_gate, tokens, cotangent, gate_in, gout, in_proj, out_proj, gains, wgrad, hgrad, norm_gain, gated_gain, chan, dp
):
    width, count = normed_t.shape
    micro = tokens.shape[0]
    tp = gate_in.shape[0]
    small = (8, wgrad.shape[1] + hgrad.shape[1])
    full = gates_grad.shape[1] + N + LANES
    rows = width // dp // tp
    part = count // micro // tp
    deep = dp // 2
    bits = dp.bit_length() - 1
    block = tp * rows
    dma = pltpu.SemaphoreType.DMA
    vmem = pl.BlockSpec(memory_space=pltpu.VMEM)
    hbm = pl.BlockSpec(memory_space=pl.ANY)
    return pl.pallas_call(
        functools.partial(tail_kernel, dp),
        in_specs=[hbm] * 9 + [vmem] * 7,
        out_specs=[vmem] * 8,
        out_shape=[
            jax.ShapeDtypeStruct(tokens.shape, BF16),
            jax.ShapeDtypeStruct(in_proj.shape, F32),
            jax.ShapeDtypeStruct((1, rows), F32),
            jax.ShapeDtypeStruct(gout.shape, F32),
            jax.ShapeDtypeStruct((1, gout.shape[0]), F32),
            jax.ShapeDtypeStruct((KW, chan), F32),
            jax.ShapeDtypeStruct((1, chan), F32),
            jax.ShapeDtypeStruct((8, HEADS), F32),
        ],
        scratch_shapes=[
            pltpu.VMEM((tp, rows, full), BF16),
            pltpu.VMEM((micro, part, width), F32),
            pltpu.VMEM((bits + 1 + tp,) + small, F32),
            pltpu.VMEM(tokens.shape, BF16),
            pltpu.VMEM(tokens.shape, BF16),
            pltpu.VMEM(gate_in.shape, BF16),
            pltpu.VMEM(gout.shape, BF16),
            pltpu.VMEM((deep, 2 * block, count), BF16),
            pltpu.VMEM(rows_grad.shape, BF16),
            pltpu.VMEM(gates_grad.shape, BF16),
            pltpu.VMEM(w_rest.shape, BF16),
            pltpu.VMEM(w_gate.shape, BF16),
            pltpu.VMEM((part, min(width, 512)), F32),
            pltpu.VMEM((2 * block, 384), F32),
            pltpu.VMEM((2 * block, 2 * N), F32),
            pltpu.VMEM((2 * block, N), F32),
            pltpu.VMEM((deep, 2 * block, N), BF16),
            pltpu.VMEM((deep, 2 * block, N), BF16),
            pltpu.VMEM((deep, block, full), BF16),
            pltpu.VMEM((deep, block, full), BF16),
            pltpu.VMEM((deep, block, full), BF16),
            pltpu.VMEM((2, deep - 1, block, full), BF16),
            pltpu.VMEM((block, full), BF16),
            pltpu.VMEM((tp, rows, full), BF16),
            pltpu.VMEM((2, micro, part, width), BF16),
            pltpu.VMEM((2, micro, part, width), BF16),
            pltpu.VMEM((micro, part, width), BF16),
            pltpu.VMEM((micro, part, width), BF16),
            pltpu.VMEM((bits,) + small, F32),
            dma((8,)),
            dma((deep,)),
            dma((deep,)),
            dma((deep,)),
            dma((3,)),
            dma((3,)),
            dma((deep,)),
            dma((deep,)),
            dma((2, deep - 1)),
            dma((2, deep - 1)),
            dma((3,)),
            dma((3,)),
            dma((2,)),
            dma((2,)),
            dma((1,)),
            dma((1,)),
            dma((bits + 3,)),
            dma((bits + 3,)),
        ],
        compiler_params=pltpu.CompilerParams(
            collective_id=3, has_side_effects=True, vmem_limit_bytes=62 * 2**20
        ),
        cost_estimate=pl.CostEstimate(flops=6 * 10**10, bytes_accessed=3 * 10**7, transcendentals=0),
        name="gradients_to_owners",
    )(
        normed_t,
        rows_grad,
        gates_grad,
        w_rest,
        w_gate,
        tokens,
        cotangent,
        gate_in,
        gout,
        in_proj,
        out_proj,
        gains,
        wgrad,
        hgrad,
        norm_gain,
        gated_gain,
    )


def body(
    tokens,
    in_proj,
    conv_weight,
    conv_bias,
    decay_log,
    step_bias,
    skip_gain,
    norm_gain,
    gated_gain,
    out_proj,
    cotangent,
):
    dp, tp = lax.axis_size("dp"), lax.axis_size("seq")
    s = lax.axis_index("seq")
    micro, part, width = tokens.shape
    heads = HEADS // tp
    inner = heads * P_SIZE
    rows = in_proj.shape[0]
    length = part * tp
    count = micro * length
    wide = inner + 2 * N
    chan = conv_bias.shape[0]

    per_head = jnp.pad(jnp.stack([decay_log, step_bias, skip_gain]), ((0, 5), (0, 0)))
    (
        normed,
        normed_t,
        proj_rest,
        ssd,
        memory,
        gate,
        w_rest,
        w_gate,
        w_out,
        cot,
        taps,
        gains,
        g_gated,
        per_head,
    ) = head(
        in_proj,
        conv_weight,
        conv_bias[None],
        norm_gain[None],
        gated_gain[None],
        per_head,
        tokens,
        cotangent,
        out_proj,
        dp,
        tp,
    )
    proj_rest = proj_rest.reshape(count, wide + LANES)
    w_rest = w_rest.reshape(width, wide + LANES)
    w_gate = w_gate.reshape(width, inner)
    grad_ssd, grad_gate, out_part, grad_out, gate_in = gating(
        ssd, gate, cot, w_out.reshape(inner, width), normed_t, g_gated, dp
    )
    grad_ssd = grad_ssd.reshape(count, inner)
    grad_gate = grad_gate.reshape(count, inner)
    grad_rest, wgrad, hgrad, out_part, grad_out, gate_in = middle(
        proj_rest,
        grad_ssd,
        memory,
        taps,
        per_head,
        out_part.reshape(micro, length, width),
        grad_out.reshape(dp, -1, width),
        gate_in.reshape(dp, tp, rows, inner),
        tokens,
        dp,
        tp,
        heads,
        micro,
    )
    tokens_grad, in_grad, dots, grad_out, gdots, conv_grad, bias_grad, head_grads = tail(
        normed_t,
        grad_rest,
        grad_gate,
        w_rest,
        w_gate,
        tokens,
        cotangent,
        gate_in,
        grad_out,
        in_proj,
        out_proj,
        gains,
        wgrad,
        hgrad,
        norm_gain[None],
        gated_gain[None],
        chan,
        dp,
    )
    return (
        out_part,
        tokens_grad,
        in_grad,
        conv_grad,
        bias_grad[0],
        head_grads[0],
        head_grads[1],
        head_grads[2],
        dots[0],
        gdots[0],
        grad_out,
    )


def solution(mesh):
    both = ("dp", "seq")
    return jax.shard_map(
        body,
        mesh=mesh,
        in_specs=(
            P("dp", "seq", None),
            P(both, None),
            P(None, both),
            P(both),
            P(),
            P(),
            P(),
            P(both),
            P(both),
            P(both, None),
            P("dp", "seq", None),
        ),
        out_specs=(
            P("dp", "seq", None),
            P("dp", "seq", None),
            P(both, None),
            P(None, both),
            P(both),
            P(),
            P(),
            P(),
            P(both),
            P(both),
            P(both, None),
        ),
        check_vma=False,
    )
```

```python
import functools

import jax
import jax.numpy as jnp
from jax import lax
from jax.experimental import pallas as pl
from jax.experimental.pallas import tpu as pltpu
from jax.sharding import PartitionSpec as P

HEADS = 48
P_SIZE = 64
N = 128
KW = 4
DI = 3072
CD = 3328
LANES = 128
FAR = -1e30

EPSILON = 1e-05
F32 = jnp.float32
BF16 = jnp.bfloat16


def dot(a, b, dims=((1,), (0,)), precision=None):
    return lax.dot_general(a, b, (dims, ((), ())), precision=precision, preferred_element_type=F32)


NT = ((1,), (1,))
HIGH = lax.Precision.HIGHEST


def pick(a, p, low):
    return jnp.where(low, a[:, 2 * p : 2 * p + 1], a[:, 2 * p + 1 : 2 * p + 2])


def chunk_parts(heads, rest_ref, xbuf, taps_ref, head_ref):
    size = rest_ref.shape[0]
    wide = taps_ref.shape[1]
    mixed = taps_ref[KW : KW + 1, :] + taps_ref[0:1, :] * xbuf[5 : 5 + size, :]
    for k in range(1, KW):
        mixed = mixed + taps_ref[k : k + 1, :] * xbuf[5 + k : 5 + k + size, :]
    sig = lax.logistic(mixed)
    return (mixed, sig) + step_parts(heads, rest_ref, taps_ref, head_ref)


def step_parts(heads, rest_ref, taps_ref, head_ref):
    size = rest_ref.shape[0]
    wide = taps_ref.shape[1]
    lane = lax.broadcasted_iota(jnp.int32, (1, LANES), 1)
    raw = jnp.where(lane < heads, rest_ref[:, wide:], 0.0) + head_ref[1:2, :]
    step = jnp.maximum(raw, 0.0) + jnp.log1p(jnp.exp(-jnp.abs(raw)))
    decay = -jnp.exp(head_ref[0:1, :]) * step
    i = lax.broadcasted_iota(jnp.int32, (size, size), 0)
    j = lax.broadcasted_iota(jnp.int32, (size, size), 1)
    run = dot(jnp.where(i >= j, 1.0, 0.0), decay, precision=HIGH)
    return raw, step, decay, run


def backward_kernel(
    heads,
    rest_ref,
    prev_ref,
    dy_ref,
    mem_ref,
    taps_ref,
    head_ref,
    out_ref,
    wgrad_ref,
    hgrad_ref,
    xbuf,
    gbuf,
    adj,
    dmix,
    dsum,
    uprod,
    zprod,
    rows_t,
    line,
    acts,
    slopes,
):
    size = rest_ref.shape[0]
    wide = taps_ref.shape[1]
    inner = heads * P_SIZE
    chunks = pl.num_programs(1)
    step_id = pl.program_id(1)
    newest = step_id == 0
    oldest = step_id == chunks - 1
    begin = jnp.logical_and(pl.program_id(0) == 0, newest)
    finish = jnp.logical_and(pl.program_id(0) == pl.num_programs(0) - 1, oldest)

    @pl.when(begin)
    def _():
        wgrad_ref[...] = jnp.zeros_like(wgrad_ref)
        hgrad_ref[...] = jnp.zeros_like(hgrad_ref)
        rows_t[...] = jnp.zeros_like(rows_t)
        line[...] = jnp.zeros_like(line)

    @pl.when(newest)
    def _():
        gbuf[size : size + 8, :] = jnp.zeros((8, wide), F32)
        adj[...] = jnp.zeros_like(adj)

    @pl.when(jnp.logical_not(newest))
    def _():
        gbuf[size : size + 8, :] = gbuf[0:8, :]

    xbuf[0:8, :] = jnp.where(oldest, 0.0, prev_ref[:, :wide])
    xbuf[8 : 8 + size, :] = rest_ref[:, :wide]
    for n in range(wide // LANES):
        at = slice(n * LANES, (n + 1) * LANES)
        mixed = taps_ref[KW : KW + 1, at] + taps_ref[0:1, at] * xbuf[5 : 5 + size, at]
        for k in range(1, KW):
            mixed = mixed + taps_ref[k : k + 1, at] * xbuf[5 + k : 5 + k + size, at]
        sig = lax.logistic(mixed)
        acts[:, at] = mixed * sig
        slopes[:, at] = sig * (1.0 + mixed * (1.0 - sig))
    raw, step, decay, run = step_parts(heads, rest_ref, taps_ref, head_ref)
    run_t = run.T
    closing = run[size - 1 : size, :]
    last = jnp.exp(closing)
    left = jnp.exp(closing - run)
    grown = jnp.exp(run)
    b = acts[:, inner : inner + N].astype(BF16)
    c = acts[:, inner + N :].astype(BF16)
    c_t = acts[:, inner + N :].T.astype(BF16)
    scores_t = dot(b, c, NT)
    low = lax.broadcasted_iota(jnp.int32, (1, LANES), 1) < P_SIZE
    lane = lax.broadcasted_iota(jnp.int32, (1, LANES), 1)
    j = lax.broadcasted_iota(jnp.int32, (size, size), 0)
    i = lax.broadcasted_iota(jnp.int32, (size, size), 1)
    causal = i >= j
    mem_b = mem_ref[0]
    adj_b = adj[...].astype(BF16)
    spread = dot(b, adj_b)
    inherit = dot(c, mem_b)
    scored = jnp.zeros((size, size), F32)
    cols = jnp.zeros((size, LANES), F32)
    for p in range(heads // 2):
        at = slice(p * LANES, (p + 1) * LANES)
        v = acts[:, at]
        size_p = pick(step, p, low)
        xv = size_p * v
        dy = dy_ref[:, at]
        dyb = dy.astype(BF16)
        xvb = xv.astype(BF16)
        dxv = pick(left, p, low) * spread[:, at]
        zprod[:, at] = (dxv * xv).astype(BF16)
        dyg = pick(grown, p, low) * dy
        uprod[:, at] = (dyg * inherit[:, at]).astype(BF16)
        for e in range(2):
            h = 2 * p + e
            keep = low if e == 0 else jnp.logical_not(low)
            mine = jnp.where(keep, dy, 0.0).astype(BF16)
            gap = run_t[h : h + 1, :] - run[:, h : h + 1]
            near = jnp.exp(jnp.where(causal, gap, FAR))
            w_t = scores_t * near
            dw_t = dot(xvb, mine, NT)
            scored = scored + dw_t * near
            g_t = dw_t * w_t
            rows_t[h : h + 1, :] = jnp.sum(g_t, axis=0, keepdims=True)
            cols = jnp.where(lane == h, jnp.sum(g_t, axis=1, keepdims=True), cols)
            dxv = dxv + dot(w_t.astype(BF16), mine)
        dsum[:, at] = (dxv * v).astype(BF16)
        dmix[:, at] = size_p * dxv + pick(head_ref[2:3, :], p, low) * dy
        line[0:1, at] += jnp.sum(dy * v, axis=0, keepdims=True)
        line[1:2, at] = jnp.sum(adj[:, at] * mem_b[:, at].astype(F32), axis=0, keepdims=True) * pick(
            last, p, low
        )
        xc = (pick(left, p, low) * xv).astype(BF16)
        dygb = dyg.astype(BF16)
        db = dot(xc, adj_b[:, at], NT)
        dc = dot(dygb, mem_b[:, at], NT)
        if p == 0:
            dmix[:, inner : inner + N] = db
            dmix[:, inner + N :] = dc
        else:
            dmix[:, inner : inner + N] += db
            dmix[:, inner + N :] += dc
        adj[:, at] = adj[:, at] * pick(last, p, low) + dot(c_t, dygb)
    dmix[:, inner : inner + N] += dot(scored.astype(BF16), c)
    dmix[:, inner + N :] += dot(scored.T.astype(BF16), b)

    group = jnp.where(
        lax.broadcasted_iota(jnp.int32, (inner, LANES), 0) // P_SIZE
        == lax.broadcasted_iota(jnp.int32, (inner, LANES), 1),
        1.0,
        0.0,
    )
    group_b = group.astype(BF16)
    d_step = dot(dsum[...], group_b)
    u = dot(uprod[...], group_b)
    z = dot(zprod[...], group_b)
    sums = dot(line[...], group, precision=HIGH)
    d_run = rows_t[...].T - cols + u - z
    row = lax.broadcasted_iota(jnp.int32, (size, 1), 0)
    ending = sums[1:2, :] + jnp.sum(z, axis=0, keepdims=True)
    d_run = d_run + jnp.where(row == size - 1, ending, 0.0)
    d_decay = dot(jnp.where(causal, 1.0, 0.0), d_run, precision=HIGH)
    d_raw = (d_step - jnp.exp(head_ref[0:1, :]) * d_decay) * lax.logistic(raw)
    d_raw = jnp.where(lane < heads, d_raw, 0.0)
    hgrad_ref[0:1, :] += jnp.sum(d_decay * decay, axis=0, keepdims=True)
    hgrad_ref[1:2, :] += jnp.sum(d_raw, axis=0, keepdims=True)

    @pl.when(finish)
    def _():
        hgrad_ref[2:3, :] = sums[0:1, :]

    for n in range(wide // LANES):
        at = slice(n * LANES, (n + 1) * LANES)
        g = dmix[:, at] * slopes[:, at]
        gbuf[0:size, at] = g
        wgrad_ref[KW : KW + 1, at] += jnp.sum(g, axis=0, keepdims=True)
        for k in range(KW):
            lag = xbuf[5 + k : 5 + k + size, at]
            wgrad_ref[k : k + 1, at] += jnp.sum(g * lag, axis=0, keepdims=True)
        back = taps_ref[KW - 1 : KW, at] * g
        for k in range(KW - 1):
            back = back + taps_ref[k : k + 1, at] * gbuf[3 - k : 3 - k + size, at]
        out_ref[:, at] = back.astype(BF16)
    out_ref[:, wide:] = d_raw.astype(BF16)


MESH = pl.DeviceIdType.MESH


def where_am_i(dp):
    d, s = lax.axis_index("dp"), lax.axis_index("seq")
    z, y = d // 2, d % 2
    x, c = s // 2, s % 2
    peers = [s + 1 - 2 * c, s + 2 - 4 * x, 3 - s]
    return d, s, z, y, x, c, peers, dp // 2


def push(src, dst, send_sem, recv_sem, d, s):
    return pltpu.make_async_remote_copy(
        src_ref=src,
        dst_ref=dst,
        send_sem=send_sem,
        recv_sem=recv_sem,
        device_id={"dp": d, "seq": s},
        device_id_type=MESH,
    )


def greet(partners):
    barrier = pltpu.get_barrier_semaphore()
    for cond, d, s in partners:

        def hello(d=d, s=s):
            pl.semaphore_signal(barrier, inc=1, device_id={"dp": d, "seq": s}, device_id_type=MESH)

        if cond is None:
            hello()
        else:
            pl.when(cond)(hello)
    count = 0
    for cond, _, _ in partners:
        count = count + (1 if cond is None else jnp.where(cond, 1, 0))
    pl.semaphore_wait(barrier, count)


class Sends:
    def __init__(self):
        self.items = []

    def start(self, cond, copy):
        if cond is None:
            copy.start()
        else:
            pl.when(cond)(copy.start)
        self.items.append((cond, copy))

    def drain(self):
        for cond, copy in self.items:
            if cond is None:
                copy.wait_send()
            else:
                pl.when(cond)(copy.wait_send)


STRIPE = DI // 16


def swapped(s):
    return 2 * (s % 2) + s // 2


def stripe_owner(block, dp):
    u = dp // 4
    return block // (4 * u) * u + block % u


def stripe_seat(block, dp):
    return swapped(block // (dp // 4) % 4)


def stripe_block(d, s, dp):
    u = dp // 4
    return (d // u * 4 + swapped(s)) * u + d % u


def forward_chunk(heads, first, rest_ref, taps_ref, head_ref, ssd_ref, mem_ref, xbuf, mem):
    size = rest_ref.shape[0]
    wide = taps_ref.shape[1]
    inner = heads * P_SIZE

    @pl.when(first)
    def _():
        xbuf[0:8, :] = jnp.zeros((8, wide), F32)
        mem[...] = jnp.zeros_like(mem)

    @pl.when(jnp.logical_not(first))
    def _():
        xbuf[0:8, :] = xbuf[size : size + 8, :]

    xbuf[8 : 8 + size, :] = rest_ref[:, :wide]
    mixed, sig, _, step, _, run = chunk_parts(heads, rest_ref, xbuf, taps_ref, head_ref)
    act = mixed * sig
    run_t = run.T
    closing = run[size - 1 : size, :]
    last = jnp.exp(closing)
    left = jnp.exp(closing - run)
    grown = jnp.exp(run)
    b = act[:, inner : inner + N]
    c = act[:, inner + N :].astype(BF16)
    scores = dot(c, b.astype(BF16), NT)
    b_t = b.T.astype(BF16)
    mem_ref[...] = mem[...].astype(BF16)
    inter = dot(c, mem[...].astype(BF16))
    low = lax.broadcasted_iota(jnp.int32, (1, LANES), 1) < P_SIZE
    i = lax.broadcasted_iota(jnp.int32, (size, size), 0)
    j = lax.broadcasted_iota(jnp.int32, (size, size), 1)
    causal = i >= j
    for p in range(heads // 2):
        at = slice(p * LANES, (p + 1) * LANES)
        v = act[:, at]
        xv = pick(step, p, low) * v
        y = pick(head_ref[2:3, :], p, low) * v + pick(grown, p, low) * inter[:, at]
        for e in range(2):
            h = 2 * p + e
            gap = run[:, h : h + 1] - run_t[h : h + 1, :]
            w = (scores * jnp.exp(jnp.where(causal, gap, FAR))).astype(BF16)
            mine = jnp.where(low if e == 0 else jnp.logical_not(low), xv, 0.0).astype(BF16)
            y = y + dot(w, mine)
        ssd_ref[:, at] = y
        xc = (pick(left, p, low) * xv).astype(BF16)
        mem[:, at] = mem[:, at] * pick(last, p, low) + dot(b_t, xc)


def hop(v, size):
    return sum(jnp.where(v >= q * size, 1, 0) for q in range(1, 4))


def head_kernel(
    dp,
    heads,
    proj_ref,
    cw_ref,
    cb_ref,
    ng_ref,
    gg_ref,
    dl_ref,
    sb_ref,
    sg_ref,
    tok_ref,
    cot_ref,
    block_ref,
    normed_hbm,
    turned_hbm,
    proj_hbm,
    ssd_hbm,
    mem_hbm,
    gates_hbm,
    rest_hbm,
    gate_hbm,
    out_hbm,
    cot_hbm,
    taps_ref,
    gain_ref,
    gated_ref,
    head_ref,
    line,
    small_stage,
    val_stage,
    half_stage,
    gate_stage,
    small_all,
    val_in,
    half_in,
    gate_in,
    w_val,
    w_half,
    w_other,
    w_tail,
    w_gate,
    out_shard,
    tok,
    flipped,
    proj,
    ssd,
    gates,
    memory,
    xbuf,
    mem,
    l_sem,
    o_sem,
    f_sem,
    p_sem,
    g_sem,
    a_send,
    a_recv,
    z_send,
    z_recv,
    y_send,
    y_recv,
    t_send,
    t_recv,
):
    d, s, z, y, x, c, peers, deep = where_am_i(dp)
    tp, rows = val_stage.shape[:2]
    micro, part, width = tok_ref.shape
    total = dp * tp
    inner = heads * P_SIZE
    wide = inner + 2 * N
    chan, gpiece = cw_ref.shape[1], gg_ref.shape[1]
    up, down, far = d + 2, d - 2, d + 1 - 2 * y
    me = d * tp + s
    to_d, to_s, turned = stripe_owner(me, dp), stripe_seat(me, dp), stripe_block(d, s, dp)
    from_d, from_s = turned // tp, turned % tp
    moves = turned != me

    triple = HEADS // 16
    line[...] = jnp.zeros_like(line)
    line[0:KW, 0:chan] = cw_ref[...].astype(F32)
    line[KW : KW + 1, 0:chan] = cb_ref[...].astype(F32)
    line[KW + 1 : KW + 2, 0:rows] = ng_ref[...].astype(F32)
    line[KW + 2 : KW + 3, 0:gpiece] = gg_ref[...].astype(F32)
    raw = proj_ref[:, 2 * DI + 2 * N :]
    for b in range(4):
        seat = 2 * (b % 2) + b // 2
        for k in range(4):
            to, at = k * STRIPE, (4 * k + b) * STRIPE
            gate_stage[seat, :, to : to + STRIPE] = proj_ref[:, at : at + STRIPE]
            val_stage[seat, :, to : to + STRIPE] = proj_ref[:, DI + at : DI + at + STRIPE]
        at = 2 * DI + N * (seat % 2)
        half_stage[seat] = proj_ref[:, at : at + N]
        v = lax.broadcasted_iota(jnp.int32, (16, HEADS), 0)
        g = lax.broadcasted_iota(jnp.int32, (16, HEADS), 1)
        hit = jnp.logical_and(v < heads, g == v + 3 * triple * hop(v, triple) + triple * b)
        line[16:32, 0:rows] = dot(jnp.where(hit, 1.0, 0.0).astype(BF16), raw, NT)
        small_stage[seat] = line[...].astype(BF16)
    v = lax.broadcasted_iota(jnp.int32, (HEADS, LANES), 1)
    g = lax.broadcasted_iota(jnp.int32, (HEADS, LANES), 0)
    hit = jnp.logical_and(v < heads, g == v + 3 * triple * hop(v, triple) + triple * swapped(s))
    line[...] = jnp.zeros_like(line)
    for k, row in enumerate((dl_ref, sb_ref, sg_ref)):
        line[k : k + 1, 0:HEADS] = row[...]
    head_ref[...] = dot(line[0:8, 0:HEADS], jnp.where(hit, 1.0, 0.0), precision=HIGH)

    greet(
        [(None, d, p) for p in peers]
        + [(None, far, s), (z < deep - 1, up, s), (z > 0, down, s)]
        + [(moves, to_d, to_s), (moves, from_d, from_s)]
    )
    sends = Sends()

    def arrive(dst, sem):
        push(dst, dst, sem, sem, d, peers[0]).wait_recv()

    def mine(ref, k):
        return ref.at[:, pl.ds(k * part, part), :]

    def exchange(a, stage, target):
        for r, p in enumerate(peers):
            sends.start(
                None, push(stage.at[p], target(s), a_send.at[a, r], a_recv.at[a, r], d, p)
            )

    def exchanged(a, target):
        for r, p in enumerate(peers):
            arrive(target(p), a_recv.at[a, r])

    exchange(0, small_stage, lambda k: small_all.at[d, k])
    exchange(1, half_stage, lambda k: half_in.at[k])
    exchange(2, val_stage, lambda k: val_in.at[k])
    exchange(3, gate_stage, lambda k: gate_in.at[k])
    sends.start(moves, push(block_ref, out_shard, t_send.at[2], t_recv.at[2], to_d, to_s))
    sends.start(None, push(tok_ref, mine(tok, s), t_send.at[0], t_recv.at[0], d, peers[1]))
    sends.start(None, push(tok_ref, mine(tok, s), t_send.at[1], t_recv.at[1], d, peers[0]))
    sends.start(None, push(cot_ref, mine(cot_hbm, s), t_send.at[3], t_recv.at[3], d, peers[1]))
    sends.start(None, push(cot_ref, mine(cot_hbm, s), t_send.at[4], t_recv.at[4], d, peers[0]))
    saves = []

    def save(src, dst):
        copy = pltpu.make_async_copy(src, dst, l_sem.at[len(saves)])
        copy.start()
        saves.append(copy)

    save(cot_ref, mine(cot_hbm, s))
    small_all[d, s] = small_stage[s]
    half_in[s] = half_stage[s]
    val_in[s] = val_stage[s]
    gate_in[s] = gate_stage[s]
    tok[:, pl.ds(pl.multiple_of(s * part, part), part), :] = tok_ref[...]

    @pl.when(jnp.logical_not(moves))
    def _():
        out_shard[...] = block_ref[...]

    def begin(a, shard, dst):
        block = dst.at[d]
        sends.start(z < deep - 1, push(shard, block, z_send.at[a, 0, 0], z_recv.at[a, 0, 0], up, s))
        sends.start(z > 0, push(shard, block, z_send.at[a, 1, 0], z_recv.at[a, 1, 0], down, s))
        sends.start(None, push(shard, block, y_send.at[a, 0, 0], y_recv.at[a, 0, 0], far, s))

    def plan(a, dst, t):
        steps = []
        for way in range(2):
            here = (z >= t) if way == 0 else (z + t <= deep - 1)
            more = jnp.logical_and(here, (z < deep - 1) if way == 0 else (z > 0))
            at = jnp.clip(d - 2 * t if way == 0 else d + 2 * t, 0, dp - 1)
            block = dst.at[at]
            got = z_recv.at[a, way, t - 1]
            on = []
            if t < deep - 1:
                nxt = up if way == 0 else down
                on.append(
                    (more, push(block, block, z_send.at[a, way, t], z_recv.at[a, way, t], nxt, s))
                )
            on.append(
                (here, push(block, block, y_send.at[a, way, t], y_recv.at[a, way, t], far, s))
            )
            steps.append((here, push(block, block, got, got, d, peers[0]), on))
        return steps

    def run(steps):
        for here, wait, on in steps:
            pl.when(here)(wait.wait_recv)
            for cond, copy in on:
                pl.when(cond)(copy.start)

    def remember(steps):
        for _, _, on in steps:
            sends.items.extend(on)

    def relay(a, dst, t):
        steps = plan(a, dst, t)
        run(steps)
        remember(steps)

    def landed(a, dst):
        arrive(dst.at[far], y_recv.at[a, 0, 0])
        for t in range(1, deep):
            for way in range(2):
                here = (z >= t) if way == 0 else (z + t <= deep - 1)
                at = jnp.clip(far - 2 * t if way == 0 else far + 2 * t, 0, dp - 1)
                pl.when(here)(functools.partial(arrive, dst.at[at], y_recv.at[a, way, t]))

    def shard_of(a, pieces, dst):
        exchanged(a, lambda p: pieces.at[p])
        for k in range(tp):
            dst[d, k * rows : (k + 1) * rows, :] = pieces[k]
        begin(a, dst.at[d], dst)

    exchanged(0, lambda p: small_all.at[d, p])
    begin(0, small_all.at[d], small_all)
    shard_of(1, half_in, w_half)
    shard_of(2, val_in, w_val)
    for t in range(1, deep):
        relay(0, small_all, t)
        relay(1, w_half, t)
        relay(2, w_val, t)
    shard_of(3, gate_in, w_gate)
    pl.when(moves)(functools.partial(arrive, out_shard, t_recv.at[2]))
    begin(4, out_shard, out_hbm)
    save(out_shard, out_hbm.at[d])

    landed(0, small_all)

    def one_hot(columns, index, k, length):
        lane = lax.broadcasted_iota(jnp.int32, (LANES, columns), 1)
        at = lax.broadcasted_iota(jnp.int32, (LANES, columns), 0)
        hit = jnp.logical_and(at < length, index(lane) == k * length + at)
        return jnp.where(hit, 1.0, 0.0).astype(BF16)

    taps_ref[...] = jnp.zeros_like(taps_ref)
    gain_ref[...] = jnp.zeros_like(gain_ref)
    gated_ref[...] = jnp.zeros_like(gated_ref)

    def striped(v):
        return v + 3 * STRIPE * hop(v, STRIPE) + STRIPE * swapped(s)

    def lay_out(dd, carry):
        for kk in range(tp):
            k = dd * tp + kk
            values = small_all[dd, kk, 0:16, :]
            chans = one_hot(wide, lambda v: jnp.where(v < inner, striped(v), v - inner + DI), k, chan)
            taps_ref[...] += dot(values, chans)[:8]
            gain_ref[...] += dot(values, one_hot(width, lambda v: v, k, rows))
            gated_ref[...] += dot(values, one_hot(inner, striped, k, gpiece))
            turned = jnp.concatenate(
                [small_all[dd, kk, 16:32, :].astype(F32), jnp.zeros((LANES - 16, LANES), F32)], axis=0
            ).T
            w_tail[dd, kk * rows : (kk + 1) * rows, 2 * N :] = turned[:rows].astype(BF16)
        return carry

    lax.fori_loop(0, dp, lay_out, 0)
    landed(1, w_half)
    sends.start(None, push(w_half, w_other, t_send.at[6], t_recv.at[6], d, peers[0]))
    landed(2, w_val)
    save(w_val, rest_hbm.at[:, :, pl.ds(0, inner)])
    arrive(w_other, t_recv.at[6])

    def both_halves(dd, carry):
        w_tail[dd, :, pl.ds(pl.multiple_of(c * N, N), N)] = w_half[dd]
        w_tail[dd, :, pl.ds(pl.multiple_of((1 - c) * N, N), N)] = w_other[dd]
        return carry

    lax.fori_loop(0, dp, both_halves, 0)
    save(w_tail, rest_hbm.at[:, :, pl.ds(inner, w_tail.shape[2])])
    arrive(mine(tok, peers[1]), t_recv.at[0])
    block = mine(tok, peers[1])
    hand = push(block, block, t_send.at[5], t_recv.at[5], d, peers[0])
    hand.start()
    relay(3, w_gate, 1)
    relay(4, out_hbm, 1)
    arrive(mine(tok, peers[0]), t_recv.at[1])
    arrive(mine(tok, peers[2]), t_recv.at[5])
    hand.wait_send()

    tasks = [(a, ref, t) for t in range(2, deep) for a, ref in ((3, w_gate), (4, out_hbm))]
    chunks = micro * tp
    when = {}
    for n, task in enumerate(tasks):
        when.setdefault(min(1 + n * 4 // len(tasks), chunks - 1), []).append(plan(*task))
    for plans in when.values():
        for steps in plans:
            remember(steps)

    def columns(i):
        return pl.ds(pl.multiple_of(i * part, part), part)

    def chunk(i, carry):
        m, k = i // tp, i % tp
        lines = pl.ds(pl.multiple_of(k * part, part), part)
        h = tok[m, lines, :].astype(F32)
        r = lax.rsqrt(jnp.mean(h * h, axis=-1, keepdims=True) + EPSILON)
        value = h * r * gain_ref[5:6, :]
        tok[m, lines, :] = value.astype(BF16)
        flipped[i] = value.T.astype(BF16)
        proj[i, :, 0:inner] = dot(tok[m, lines, :], w_val[...].reshape(width, inner))
        proj[i, :, inner:] = dot(tok[m, lines, :], w_tail[...].reshape(width, w_tail.shape[2]))
        forward_chunk(
            heads, k == 0, proj.at[i], taps_ref, head_ref, ssd.at[i], memory.at[i], xbuf, mem
        )
        pltpu.make_async_copy(tok.at[m, lines, :], normed_hbm.at[m, lines, :], o_sem.at[i]).start()
        pltpu.make_async_copy(flipped.at[i], turned_hbm.at[:, columns(i)], f_sem.at[i]).start()
        pltpu.make_async_copy(proj.at[i], proj_hbm.at[i], p_sem.at[i]).start()
        for n, plans in when.items():

            @pl.when(i == n)
            def _():
                for steps in plans:
                    run(steps)

        return carry

    lax.fori_loop(0, chunks, chunk, 0)
    save(ssd, ssd_hbm)
    save(memory, mem_hbm)
    arrive(mine(cot_hbm, peers[1]), t_recv.at[3])
    block = mine(cot_hbm, peers[1])
    sends.start(None, push(block, block, t_send.at[7], t_recv.at[7], d, peers[0]))
    landed(3, w_gate)
    save(w_gate, gate_hbm)

    def gating(i, carry):
        m, k = i // tp, i % tp
        lines = pl.ds(pl.multiple_of(k * part, part), part)
        gates[i] = dot(tok[m, lines, :], w_gate[...].reshape(width, inner))
        pltpu.make_async_copy(gates.at[i], gates_hbm.at[i], g_sem.at[i]).start()
        return carry

    lax.fori_loop(0, chunks, gating, 0)
    landed(4, out_hbm)
    arrive(mine(cot_hbm, peers[0]), t_recv.at[4])
    arrive(mine(cot_hbm, peers[2]), t_recv.at[7])

    def saved(i, carry):
        m, k = i // tp, i % tp
        lines = pl.ds(pl.multiple_of(k * part, part), part)
        pltpu.make_async_copy(tok.at[m, lines, :], normed_hbm.at[m, lines, :], o_sem.at[i]).wait()
        pltpu.make_async_copy(flipped.at[i], turned_hbm.at[:, columns(i)], f_sem.at[i]).wait()
        pltpu.make_async_copy(proj.at[i], proj_hbm.at[i], p_sem.at[i]).wait()
        pltpu.make_async_copy(gates.at[i], gates_hbm.at[i], g_sem.at[i]).wait()
        return carry

    lax.fori_loop(0, chunks, saved, 0)
    for copy in saves:
        copy.wait()
    sends.drain()


def head(in_proj, conv_weight, conv_bias, norm_gain, gated_gain, d_log, s_bias, s_gain, tokens, cotangent, out_proj, dp, tp):
    rows = in_proj.shape[0]
    heads = HEADS // tp
    inner = heads * P_SIZE
    full = inner + 2 * N + LANES
    micro, part, width = tokens.shape
    deep = dp // 2
    chunks = micro * tp
    block = tp * rows
    dma = pltpu.SemaphoreType.DMA
    vmem = pl.BlockSpec(memory_space=pltpu.VMEM)
    hbm = pl.BlockSpec(memory_space=pl.ANY)
    wide = inner + 2 * N

    def shape(*dims, kind=BF16):
        return jax.ShapeDtypeStruct(dims, kind)

    def room(*dims, kind=BF16):
        return pltpu.VMEM(dims, kind)

    return pl.pallas_call(
        functools.partial(head_kernel, dp, heads),
        in_specs=[vmem] * 11,
        out_specs=[hbm] * 10 + [vmem] * 4,
        out_shape=[
            shape(micro, tp * part, width),
            shape(width, chunks * part),
            shape(chunks, part, full, kind=F32),
            shape(chunks, part, inner, kind=F32),
            shape(chunks, N, inner),
            shape(chunks, part, inner, kind=F32),
            shape(dp, block, full),
            shape(dp, block, inner),
            shape(dp, out_proj.shape[0], width),
            shape(micro, tp * part, width),
            shape(8, wide, kind=F32),
            shape(16, width, kind=F32),
            shape(16, inner, kind=F32),
            shape(8, LANES, kind=F32),
        ],
        scratch_shapes=[
            room(32, LANES, kind=F32),
            room(tp, 32, LANES),
            room(tp, rows, inner),
            room(tp, rows, N),
            room(tp, rows, inner),
            room(dp, tp, 32, LANES),
            room(tp, rows, inner),
            room(tp, rows, N),
            room(tp, rows, inner),
            room(dp, block, inner),
            room(dp, block, N),
            room(dp, block, N),
            room(dp, block, 2 * N + LANES),
            room(dp, block, inner),
            room(*out_proj.shape),
            room(micro, tp * part, width),
            room(chunks, width, part),
            room(chunks, part, full, kind=F32),
            room(chunks, part, inner, kind=F32),
            room(chunks, part, inner, kind=F32),
            room(chunks, N, inner),
            room(part + 8, wide, kind=F32),
            room(N, inner, kind=F32),
            dma((8,)),
            dma((chunks,)),
            dma((chunks,)),
            dma((chunks,)),
            dma((chunks,)),
            dma((4, 3)),
            dma((4, 3)),
            dma((5, 2, deep - 1)),
            dma((5, 2, deep - 1)),
            dma((5, 2, deep)),
            dma((5, 2, deep)),
            dma((8,)),
            dma((8,)),
        ],
        compiler_params=pltpu.CompilerParams(
            collective_id=1, has_side_effects=True, vmem_limit_bytes=62 * 2**20
        ),
        cost_estimate=pl.CostEstimate(flops=10**11, bytes_accessed=5 * 10**7, transcendentals=0),
        name="gather_and_mix",
    )(
        in_proj,
        conv_weight,
        conv_bias,
        norm_gain,
        gated_gain,
        d_log,
        s_bias,
        s_gain,
        tokens,
        cotangent,
        out_proj,
    )


class OwnerSum:
    def __init__(self, where, sends, source, mine, ybuf, zbuf, final, sems, theirs_ref=None):
        self.where, self.sends = where, sends
        self.mine, self.ybuf, self.zbuf, self.final = mine, ybuf, zbuf, final
        d, s, z, y, _, _, _, deep = where
        self.load_sem, y_send, self.y_recv, z_send, self.z_recv = sems
        lower = z < deep // 2

        def place(j):
            low = jnp.where(j > z, deep - 1 - j, deep - 1 - z + j)
            high = jnp.where(j < z, j, z + deep - 1 - j)
            return jnp.where(j == z, deep - 1, jnp.where(lower, low, high))

        def turn(k):
            low = jnp.where(k < deep - 1 - z, deep - 1 - k, k - (deep - 1 - z))
            high = jnp.where(k < z, k, deep - 1 - (k - z))
            return jnp.where(lower, low, high) if k < deep - 1 else z

        self.order = [turn(k) for k in range(deep)]
        self.y_items, self.loads = [], []
        for k, j in enumerate(self.order):
            theirs = source.at[j * 2 + 1 - y] if theirs_ref is None else theirs_ref.at[k]
            copy = push(theirs, ybuf.at[k], y_send.at[k], self.y_recv.at[k], d + 1 - 2 * y, s)
            self.y_items.append((None, copy))
            if theirs_ref is None:
                own = source.at[j * 2 + y]
                self.loads.append(pltpu.make_async_copy(own, mine.at[k], self.load_sem.at[k]))
        self.z_items = []
        for t in range(deep - 1):
            ways = []
            for way in range(2):
                depth = z if way == 0 else deep - 1 - z
                j = deep - 1 - t + z if way == 0 else t + z - deep + 1
                k = place(jnp.clip(j, 0, deep - 1))
                nxt = d + 2 if way == 0 else d - 2
                dst, ss, rs = zbuf.at[way, t], z_send.at[way, t], self.z_recv.at[way, t]
                first = (depth == 0, push(ybuf.at[k], dst, ss, rs, nxt, s))
                later = None
                if t > 0:
                    cond = jnp.logical_and(depth > 0, depth <= t)
                    later = (cond, push(zbuf.at[way, t - 1], dst, ss, rs, nxt, s))
                ways.append((k, first, later))
            self.z_items.append(ways)
        sends.items.extend(self.y_items)
        for ways in self.z_items:
            for _, first, later in ways:
                sends.items.append(first)
                if later is not None:
                    sends.items.append(later)

    def arrive(self, ref, sem):
        d, s = self.where[:2]
        push(ref, ref, sem, sem, d, self.where[6][0]).wait_recv()

    def begin(self):
        for _, copy in self.y_items:
            copy.start()
        for copy in self.loads:
            copy.start()

    def each(self, work):
        if self.mine.ndim == 4:
            count, cut = self.mine.shape[1], lambda i: i
        else:
            count, cut = self.mine.shape[1] // 16, lambda i: pl.ds(pl.multiple_of(i * 16, 16), 16)
        lax.fori_loop(0, count, lambda i, carry: (work(cut(i)), carry)[1], 0)

    def add(self, k):
        if self.loads:
            self.loads[k].wait()
        self.arrive(self.ybuf.at[k], self.y_recv.at[k])
        ybuf, mine = self.ybuf, self.mine

        def work(i):
            ybuf[k, i] = (ybuf[k, i].astype(F32) + mine[k, i].astype(F32)).astype(BF16)

        self.each(work)

    def send(self, t):
        zbuf, ybuf = self.zbuf, self.ybuf
        for way, (k, first, later) in enumerate(self.z_items[t]):
            pl.when(first[0])(first[1].start)
            if later is None:
                continue

            @pl.when(later[0])
            def _():
                self.arrive(zbuf.at[way, t - 1], self.z_recv.at[way, t - 1])

                def work(i):
                    zbuf[way, t - 1, i] = (
                        zbuf[way, t - 1, i].astype(F32) + ybuf[k, i].astype(F32)
                    ).astype(BF16)

                self.each(work)
                later[1].start()

    def finish(self):
        z, deep = self.where[2], self.where[7]
        zbuf, ybuf, final = self.zbuf, self.ybuf, self.final
        for way in range(2):
            depth = z if way == 0 else deep - 1 - z
            pl.when(depth > 0)(
                functools.partial(self.arrive, zbuf.at[way, deep - 2], self.z_recv.at[way, deep - 2])
            )

        def work(ways, i):
            total = ybuf[deep - 1, i].astype(F32)
            for way in ways:
                total = total + zbuf[way, deep - 2, i].astype(F32)
            final[i] = total.astype(BF16)

        for cond, ways in (
            (z == 0, (1,)),
            (z == deep - 1, (0,)),
            (jnp.logical_and(z > 0, z < deep - 1), (0, 1)),
        ):
            pl.when(cond)(functools.partial(self.each, functools.partial(work, ways)))


def middle_kernel(
    dp,
    heads,
    rest_ref,
    prev_ref,
    dy_ref,
    mem_ref,
    taps_ref,
    head_ref,
    part_hbm,
    gout_hbm,
    ggate_hbm,
    tok_hbm,
    out_ref,
    wgrad_ref,
    hgrad_ref,
    own_hbm,
    gout_out,
    ggate_out,
    xbuf,
    gbuf,
    adj,
    dmix,
    dsum,
    uprod,
    zprod,
    rows_t,
    line,
    acts,
    slopes,
    o_mine,
    o_y,
    o_z,
    o_final,
    g_mine,
    g_y,
    g_z,
    g_final,
    own,
    core_buf,
    x_buf,
    tok,
    result,
    o_load,
    o_ysend,
    o_yrecv,
    o_zsend,
    o_zrecv,
    g_load,
    g_ysend,
    g_yrecv,
    g_zsend,
    g_zrecv,
    b_load,
    c_send,
    c_recv,
    m_send,
    m_recv,
):
    where = where_am_i(dp)
    d, s, z, y, x, c, peers, deep = where
    micro, part, width = result.shape
    step = pl.program_id(0) * pl.num_programs(1) + pl.program_id(1)
    tp = ggate_hbm.shape[1]
    me = d * tp + s
    turned = stripe_block(d, s, dp)
    moves = turned != me
    to_d, to_s = turned // tp, turned % tp
    from_d, from_s = stripe_owner(me, dp), stripe_seat(me, dp)
    sends = Sends()
    gout = OwnerSum(
        where, sends, gout_hbm, o_mine, o_y, o_z, o_final, (o_load, o_ysend, o_yrecv, o_zsend, o_zrecv)
    )
    ggate = OwnerSum(
        where, sends, ggate_hbm, g_mine, g_y, g_z, g_final, (g_load, g_ysend, g_yrecv, g_zsend, g_zrecv)
    )

    def chunk(k):
        return part_hbm.at[:, pl.ds(k * part, part), :]

    cores, loads = [], []
    for q, xx in enumerate((1 - x, x)):
        cores.append(
            push(chunk(xx * 2 + 1 - c), core_buf.at[q], c_send.at[q], c_recv.at[q], d, peers[0])
        )
        loads.append(pltpu.make_async_copy(chunk(xx * 2 + c), own.at[q], b_load.at[q]))
    across = push(core_buf.at[0], x_buf, m_send.at[0], m_recv.at[0], d, peers[1])
    turning = push(o_final, gout_out, m_send.at[1], m_recv.at[1], to_d, to_s)
    staying = pltpu.make_async_copy(o_final, gout_out, b_load.at[2])
    kept = pltpu.make_async_copy(g_final, ggate_out, b_load.at[3])
    saved = pltpu.make_async_copy(result, own_hbm, b_load.at[4])
    loads.append(pltpu.make_async_copy(tok_hbm, tok, b_load.at[5]))
    for copy in cores + [across]:
        sends.items.append((None, copy))
    sends.items.append((moves, turning))
    span = 16

    def by_rows(work):
        def one(i, carry):
            m, row = i // (part // span), (i % (part // span)) * span
            work(m, pl.ds(pl.multiple_of(row, span), span))
            return carry

        lax.fori_loop(0, micro * (part // span), one, 0)

    def start():
        greet(
            [(None, d, p) for p in peers]
            + [(None, d + 1 - 2 * y, s), (z < deep - 1, d + 2, s), (z > 0, d - 2, s)]
            + [(moves, to_d, to_s), (moves, from_d, from_s)]
        )
        for copy in cores + loads:
            copy.start()
        gout.begin()
        ggate.begin()

    def pass_on():
        loads[0].wait()
        cores[0].wait_recv()

        def work(m, rows):
            core_buf[0, m, rows, :] = (
                core_buf[0, m, rows, :].astype(F32) + own[0, m, rows, :].astype(F32)
            ).astype(BF16)

        by_rows(work)
        across.start()

    def collect():
        loads[1].wait()
        loads[2].wait()
        cores[1].wait_recv()
        across.wait_recv()

        def work(m, rows):
            result[m, rows, :] = (
                core_buf[1, m, rows, :].astype(F32)
                + own[1, m, rows, :].astype(F32)
                + x_buf[m, rows, :].astype(F32)
                + tok[m, rows, :].astype(F32)
            ).astype(BF16)

        by_rows(work)
        saved.start()

    def hand_over():
        gout.finish()
        pl.when(moves)(turning.start)
        pl.when(jnp.logical_not(moves))(staying.start)

    def last():
        ggate.add(deep - 1)
        ggate.finish()
        kept.start()
        pl.when(moves)(turning.wait_recv)
        pl.when(jnp.logical_not(moves))(staying.wait)
        kept.wait()
        saved.wait()
        sends.drain()

    stages = {}

    def at(n, task, *args):
        stages.setdefault(n, []).append(functools.partial(task, *args))

    at(0, start)
    at(1, pass_on)
    for k in range(deep - 1):
        n = k * 2 // (deep - 2)
        at(2 + n, gout.add, k)
        at(2 + n, gout.send, k)
    at(4, gout.add, deep - 1)
    at(5, hand_over)
    for k in range(deep - 1):
        n = k * 2 // (deep - 2)
        at(5 + n, ggate.add, k)
        at(5 + n, ggate.send, k)
    at(6, collect)
    for n, tasks in stages.items():

        @pl.when(step == n)
        def _():
            for task in tasks:
                task()

    backward_kernel(
        heads,
        rest_ref,
        prev_ref,
        dy_ref,
        mem_ref,
        taps_ref,
        head_ref,
        out_ref,
        wgrad_ref,
        hgrad_ref,
        xbuf,
        gbuf,
        adj,
        dmix,
        dsum,
        uprod,
        zprod,
        rows_t,
        line,
        acts,
        slopes,
    )
    pl.when(step == pl.num_programs(0) * pl.num_programs(1) - 1)(last)


def middle(rest, dy, memory, taps, head, partial, gout, ggate, tokens, dp, tp, heads, micro):
    count, full = rest.shape
    wide = taps.shape[1]
    inner = heads * P_SIZE
    _, length, width = partial.shape
    part = length // tp
    chunks = length // part
    deep = dp // 2
    dma = pltpu.SemaphoreType.DMA
    hbm = pl.BlockSpec(memory_space=pl.ANY)
    gout = gout.reshape(dp, 2, -1, width)

    def at(m, c):
        return m * chunks + chunks - 1 - c

    def sums(block):
        kinds = [(deep,), (deep,), (2, deep - 1), ()]
        return [pltpu.VMEM(kind + block, BF16) for kind in kinds]

    sems = [dma((deep,))] * 3 + [dma((2, deep - 1))] * 2
    out = pl.pallas_call(
        functools.partial(middle_kernel, dp, heads),
        grid=(micro, chunks),
        in_specs=[
            pl.BlockSpec((part, full), lambda m, c: (at(m, c), 0)),
            pl.BlockSpec((8, full), lambda m, c: (jnp.maximum(at(m, c) * (part // 8) - 1, 0), 0)),
            pl.BlockSpec((part, inner), lambda m, c: (at(m, c), 0)),
            pl.BlockSpec((1, N, inner), lambda m, c: (at(m, c), 0, 0)),
            pl.BlockSpec((8, wide), lambda m, c: (0, 0)),
            pl.BlockSpec((8, LANES), lambda m, c: (0, 0)),
            hbm,
            hbm,
            hbm,
            hbm,
        ],
        out_specs=[
            pl.BlockSpec((part, full), lambda m, c: (at(m, c), 0)),
            pl.BlockSpec((8, wide), lambda m, c: (0, 0)),
            pl.BlockSpec((8, LANES), lambda m, c: (0, 0)),
            hbm,
            hbm,
            hbm,
        ],
        out_shape=[
            jax.ShapeDtypeStruct((count, full), BF16),
            jax.ShapeDtypeStruct((8, wide), F32),
            jax.ShapeDtypeStruct((8, LANES), F32),
            jax.ShapeDtypeStruct((micro, part, width), BF16),
            jax.ShapeDtypeStruct(gout.shape[1:], BF16),
            jax.ShapeDtypeStruct(ggate.shape[1:], BF16),
        ],
        scratch_shapes=[
            pltpu.VMEM((part + 8, wide), F32),
            pltpu.VMEM((part + 8, wide), F32),
            pltpu.VMEM((N, inner), F32),
            pltpu.VMEM((part, wide), F32),
            pltpu.VMEM((part, inner), BF16),
            pltpu.VMEM((part, inner), BF16),
            pltpu.VMEM((part, inner), BF16),
            pltpu.VMEM((LANES, part), F32),
            pltpu.VMEM((8, inner), F32),
            pltpu.VMEM((part, wide), F32),
            pltpu.VMEM((part, wide), F32),
        ]
        + sums(gout.shape[1:])
        + sums(ggate.shape[1:])
        + [
            pltpu.VMEM((2, micro, part, width), BF16),
            pltpu.VMEM((2, micro, part, width), BF16),
            pltpu.VMEM((micro, part, width), BF16),
            pltpu.VMEM((micro, part, width), BF16),
            pltpu.VMEM((micro, part, width), BF16),
        ]
        + sems
        + sems
        + [dma((6,)), dma((2,)), dma((2,)), dma((2,)), dma((2,))],
        compiler_params=pltpu.CompilerParams(
            dimension_semantics=("arbitrary", "arbitrary"),
            collective_id=4,
            has_side_effects=True,
            vmem_limit_bytes=62 * 2**20,
        ),
        cost_estimate=pl.CostEstimate(flops=7 * 10**10, bytes_accessed=4 * 10**7, transcendentals=0),
        name="mixer_backward_and_sums",
    )(rest, rest, dy, memory, taps, head, partial, gout, ggate, tokens)
    rest_grad, wgrad, hgrad, own, gout, ggate = out
    return rest_grad, wgrad, hgrad, own, gout.reshape(-1, width), ggate


def gating_kernel(
    dp,
    ssd_hbm,
    gate_hbm,
    cot_hbm,
    out_hbm,
    turned_hbm,
    gain_ref,
    grad_ssd_hbm,
    grad_gate_hbm,
    part_hbm,
    gout_hbm,
    ggate_hbm,
    ssd,
    gate,
    cot,
    w_out,
    turned,
    weighed,
    shaped_t,
    grad_gate,
    partial,
    gout,
    ggate,
    stats,
    held,
    l_sem,
    c_sem,
    s_sem,
    g_sem,
    p_sem,
    o_sem,
    send,
    recv,
):
    d, s, *_, peers, _ = where_am_i(dp)
    chunks, part, inner = ssd.shape
    width = cot.shape[2]
    count = chunks * part

    def loads(i):
        return [
            pltpu.make_async_copy(cot_hbm.at[i], cot.at[i], c_sem.at[0, i]),
            pltpu.make_async_copy(ssd_hbm.at[i], ssd.at[i], c_sem.at[1, i]),
            pltpu.make_async_copy(gate_hbm.at[i], gate.at[i], c_sem.at[2, i]),
        ]

    first = pltpu.make_async_copy(out_hbm, w_out, l_sem.at[0])
    other = pltpu.make_async_copy(turned_hbm, turned, l_sem.at[1])
    first.start()
    for i in range(chunks):
        for copy in loads(i):
            copy.start()
    other.start()
    greet([(None, d, p) for p in peers])
    first.wait()

    def gated_parts(i):
        g = gate[i]
        sig = lax.logistic(g)
        act = g * sig
        return sig, act, ssd[i] * act

    def measure(i, carry):
        for copy in loads(i):
            copy.wait()
        w = dot(cot[i], w_out[...], NT) * gain_ref[KW + 2 : KW + 3, :]
        weighed[i] = w
        _, _, gated = gated_parts(i)
        lane = lax.broadcasted_iota(jnp.int32, (part, LANES), 1)
        both = jnp.where(lane == 0, jnp.sum(gated * gated, axis=1, keepdims=True), 0.0)
        both = jnp.where(lane == 1, jnp.sum(w * gated, axis=1, keepdims=True), both)
        stats[i] = both.T[:8, :]
        return carry

    lax.fori_loop(0, chunks, measure, 0)
    copies = [push(stats, held.at[r], send.at[r], recv.at[r], d, p) for r, p in enumerate(peers)]
    for copy in copies:
        copy.start()
    for copy in copies:
        copy.wait()

    def out_copies(i):
        return [
            pltpu.make_async_copy(weighed.at[i], grad_ssd_hbm.at[i], s_sem.at[i]),
            pltpu.make_async_copy(grad_gate.at[i], grad_gate_hbm.at[i], g_sem.at[i]),
            pltpu.make_async_copy(partial.at[i], part_hbm.at[i], p_sem.at[i]),
        ]

    def columns(i):
        return pl.ds(pl.multiple_of(i * part, part), part)

    def shape_chunk(i, carry):
        sums = (stats[i] + held[0, i]) + (held[1, i] + held[2, i])
        sums = jnp.concatenate([sums, jnp.zeros((LANES - 8, part), F32)], axis=0).T
        q = lax.rsqrt(sums[:, 0:1] / DI + EPSILON)
        pull = q * q * (sums[:, 1:2] / DI)
        sig, act, gated = gated_parts(i)
        value = gated * q * gain_ref[KW + 2 : KW + 3, :]
        shaped_t[:, columns(i)] = value.T.astype(BF16)
        partial[i] = dot(value.astype(BF16), w_out[...]).astype(BF16)
        grad = q * (weighed[i] - gated * pull)
        grad_gate[i] = (grad * ssd[i] * (sig + act * (1.0 - sig))).astype(BF16)
        weighed[i] = grad * act
        for copy in out_copies(i):
            copy.start()
        return carry

    lax.fori_loop(0, chunks, shape_chunk, 0)
    other.wait()
    high, across = min(384, inner), min(512, width)

    def out_tile(i, carry):
        a = pl.ds(pl.multiple_of(i // (width // across) * high, high), high)
        b = pl.ds(pl.multiple_of(i % (width // across) * across, across), across)
        gout[a, b] = dot(shaped_t[a, :], cot[:, :, b].reshape(count, across)).astype(BF16)
        return carry

    lax.fori_loop(0, (inner // high) * (width // across), out_tile, 0)
    save_out = pltpu.make_async_copy(gout, gout_hbm, o_sem.at[0])
    save_out.start()

    def gate_tile(i, carry):
        a = pl.ds(pl.multiple_of(i // 2 * across, across), across)
        b = pl.ds(pl.multiple_of(i % 2 * (inner // 2), inner // 2), inner // 2)
        ggate[a, b] = dot(turned[a, :], grad_gate[:, :, b].reshape(count, inner // 2)).astype(BF16)
        return carry

    lax.fori_loop(0, (width // across) * 2, gate_tile, 0)
    save_gate = pltpu.make_async_copy(ggate, ggate_hbm, o_sem.at[1])
    save_gate.start()

    def saved(i, carry):
        for copy in out_copies(i):
            copy.wait()
        return carry

    lax.fori_loop(0, chunks, saved, 0)
    save_out.wait()
    save_gate.wait()


def gating(ssd, gate, cot, w_out, normed_t, gains, dp):
    chunks, part, inner = ssd.shape
    width, count = normed_t.shape
    cot = cot.reshape(chunks, part, width)
    dma = pltpu.SemaphoreType.DMA
    vmem = pl.BlockSpec(memory_space=pltpu.VMEM)
    hbm = pl.BlockSpec(memory_space=pl.ANY)

    def shape(*dims, kind=BF16):
        return jax.ShapeDtypeStruct(dims, kind)

    def room(*dims, kind=BF16):
        return pltpu.VMEM(dims, kind)

    return pl.pallas_call(
        functools.partial(gating_kernel, dp),
        in_specs=[hbm] * 5 + [vmem],
        out_specs=[hbm] * 5,
        out_shape=[
            shape(chunks, part, inner, kind=F32),
            shape(chunks, part, inner),
            shape(chunks, part, width),
            shape(inner, width),
            shape(width, inner),
        ],
        scratch_shapes=[
            room(chunks, part, inner, kind=F32),
            room(chunks, part, inner, kind=F32),
            room(chunks, part, width),
            room(inner, width),
            room(width, count),
            room(chunks, part, inner, kind=F32),
            room(inner, count),
            room(chunks, part, inner),
            room(chunks, part, width),
            room(inner, width),
            room(width, inner),
            room(chunks, 8, part, kind=F32),
            room(3, chunks, 8, part, kind=F32),
            dma((2,)),
            dma((3, chunks)),
            dma((chunks,)),
            dma((chunks,)),
            dma((chunks,)),
            dma((2,)),
            dma((3,)),
            dma((3,)),
        ],
        compiler_params=pltpu.CompilerParams(
            collective_id=2, has_side_effects=True, vmem_limit_bytes=63 * 2**20
        ),
        cost_estimate=pl.CostEstimate(flops=3 * 10**10, bytes_accessed=5 * 10**7, transcendentals=0),
        name="gating_and_gradients",
    )(ssd, gate, cot, w_out, normed_t, gains)


def as_row(column):
    size = column.shape[0]
    square = jnp.broadcast_to(column, (size, LANES))
    square = jnp.concatenate([square, jnp.zeros((LANES - size, LANES), F32)], axis=0)
    return square.T[0:1, :size]


def tail_kernel(
    dp,
    normed_hbm,
    rows_hbm,
    gates_hbm,
    w_rest_hbm,
    w_gate_hbm,
    tok_hbm,
    cot_hbm,
    gate_hbm,
    gout_hbm,
    proj_ref,
    block_ref,
    gain_ref,
    wgrad_ref,
    hgrad_ref,
    ng_ref,
    gg_ref,
    tokens_ref,
    grad_ref,
    dots_ref,
    gout_ref,
    gdots_ref,
    taps_ref,
    bias_ref,
    heads_ref,
    out_ref,
    own_ref,
    sums_ref,
    tok,
    cot,
    gate_in,
    gout,
    normed,
    rows_ref,
    gates_ref,
    w_rest,
    w_gate,
    tile,
    wtile,
    btile,
    b_own,
    b_out,
    b_in,
    theirs,
    mine,
    ybuf,
    zbuf,
    final,
    handed,
    core_buf,
    core_out,
    x_buf,
    x_out,
    s_buf,
    l_sem,
    n_sem,
    b_send,
    b_recv,
    g_send,
    g_recv,
    y_send,
    y_recv,
    z_send,
    z_recv,
    a_send,
    a_recv,
    c_send,
    c_recv,
    x_send,
    x_recv,
    s_send,
    s_recv,
):
    where = where_am_i(dp)
    d, s, z, y, x, c, peers, deep = where
    tp, rows = out_ref.shape[:2]
    block = tp * rows
    micro, part, width = own_ref.shape
    inner = gates_ref.shape[1]
    bits = dp.bit_length() - 1
    partners = []
    for k in range(bits):
        step = 2**k
        bit = (d // step) % 2
        partners.append(d + step - 2 * step * bit)
    sends = Sends()
    total = OwnerSum(
        where,
        sends,
        None,
        mine,
        ybuf,
        zbuf,
        final,
        (None, y_send, y_recv, z_send, z_recv),
        theirs,
    )
    loads = [
        pltpu.make_async_copy(src, dst, l_sem.at[k])
        for k, (src, dst) in enumerate(
            (
                (rows_hbm, rows_ref),
                (w_rest_hbm, w_rest),
                (gates_hbm, gates_ref),
                (w_gate_hbm, w_gate),
                (tok_hbm, tok),
                (cot_hbm, cot),
                (gate_hbm.at[s], gate_in.at[s]),
                (gout_hbm, gout),
            )
        )
    ]
    fetches = []
    for k in range(deep):
        lines = pl.ds(pl.multiple_of(total.order[k] * 2 * block, 2 * block), 2 * block)
        fetches.append(pltpu.make_async_copy(normed_hbm.at[lines, :], normed.at[k], n_sem.at[k]))
    for copy in loads + fetches:
        copy.start()
    greet(
        [(None, d, p) for p in peers]
        + [(None, d + 1 - 2 * y, s), (z < deep - 1, d + 2, s), (z > 0, d - 2, s)]
        + [(None, partners[k], s) for k in range(2, bits)]
    )

    def arrive(dst, sem):
        push(dst, dst, sem, sem, d, peers[0]).wait_recv()

    sums_ref[0, :, 0 : wgrad_ref.shape[1]] = wgrad_ref[...]
    sums_ref[0, :, wgrad_ref.shape[1] :] = hgrad_ref[...]

    def each(count, work):
        lax.fori_loop(0, count, lambda i, carry: (work(i), carry)[1], 0)

    across = width // tile.shape[1]
    span = wtile.shape[1]

    def product(owner, use):
        def work(i):
            m, n = i // across, i % across
            row = pl.multiple_of((m * tp + owner) * part, part)
            col = pl.multiple_of(n * tile.shape[1], tile.shape[1])
            lines = pl.ds(col, tile.shape[1])
            tile[...] = dot(rows_ref[pl.ds(row, part), :], w_rest[lines, :], NT) + dot(
                gates_ref[pl.ds(row, part), :], w_gate[lines, :], NT
            )
            use(m, lines)

        each(micro * across, work)

    def weight(k):
        fetches[k].wait()
        far = pl.ds(pl.multiple_of((1 - y) * block, block), block)
        near = pl.ds(pl.multiple_of(y * block, block), block)

        def work(n):
            cols = pl.ds(pl.multiple_of(n * span, span), span)
            wtile[...] = dot(normed[k], rows_ref[:, cols])
            theirs[k, :, cols] = wtile[far, :].astype(BF16)
            mine[k, :, cols] = wtile[near, :].astype(BF16)

        lines = pl.ds(inner, 2 * N)
        btile[...] = dot(normed[k], rows_ref[:, lines])
        ours = pl.ds(pl.multiple_of(c * N, N), N)
        b_out[k] = btile[:, pl.ds(pl.multiple_of((1 - c) * N, N), N)].astype(BF16)
        b_own[...] = btile[:, ours]
        swap = push(b_out.at[k], b_in.at[k], b_send.at[k], b_recv.at[k], d, peers[0])
        sends.start(None, swap)
        each(inner // span, work)
        b_tail = dot(normed[k], rows_ref[:, inner + 2 * N :])
        btile[:, N:] = b_tail
        arrive(b_in.at[k], b_recv.at[k])
        btile[:, 0:N] = b_own[...] + b_in[k].astype(F32)
        theirs[k, :, inner:] = btile[far, :].astype(BF16)
        mine[k, :, inner:] = btile[near, :].astype(BF16)
        total.y_items[k][1].start()

    def doubling(k):
        arrive(s_buf.at[k], s_recv.at[k])
        sums_ref[k + 1] = sums_ref[k] + s_buf[k]
        if k + 1 < bits:
            src = sums_ref.at[k + 1]
            sends.start(
                None, push(src, s_buf.at[k + 1], s_send.at[k + 1], s_recv.at[k + 1], partners[k + 1], s)
            )

    def to_core(q):
        def use(m, lines):
            core_out[q, m, :, lines] = tile[...].astype(BF16)

        return use

    def to_chip(m, lines):
        x_out[m, :, lines] = (tile[...] + core_buf[0, m, :, lines].astype(F32)).astype(BF16)

    def keep(m, lines):
        own_ref[m, :, lines] = tile[...] + core_buf[1, m, :, lines].astype(F32)

    for copy in loads[:4]:
        copy.wait()
    for r, p in enumerate(peers):
        swap = push(gate_hbm.at[p], gate_in.at[s], g_send.at[r], g_recv.at[r], d, p)
        sends.start(None, swap)
    src = sums_ref.at[0]
    sends.start(None, push(src, s_buf.at[0], s_send.at[0], s_recv.at[0], partners[0], s))
    product((1 - x) * 2 + 1 - c, to_core(0))
    sends.start(
        None, push(core_out.at[0], core_buf.at[0], c_send.at[0], c_recv.at[0], d, peers[0])
    )
    weight(0)
    arrive(core_buf.at[0], c_recv.at[0])
    product((1 - x) * 2 + c, to_chip)
    sends.start(None, push(x_out, x_buf, x_send.at[0], x_recv.at[0], d, peers[1]))
    weight(1)
    total.add(0)
    total.send(0)
    doubling(0)
    for k in range(2, deep):
        weight(k)
    total.add(1)
    total.send(1)
    doubling(1)
    product(x * 2 + 1 - c, to_core(1))
    sends.start(
        None, push(core_out.at[1], core_buf.at[1], c_send.at[1], c_recv.at[1], d, peers[0])
    )
    for k in range(2, deep - 1):
        total.add(k)
        total.send(k)
        if k < bits:
            doubling(k)
    arrive(core_buf.at[1], c_recv.at[1])
    product(s, keep)
    for k in range(deep - 1, bits):
        doubling(k)
    for r, p in enumerate(peers):
        src, dst = sums_ref.at[bits], sums_ref.at[bits + 1 + s]
        sends.start(None, push(src, dst, s_send.at[bits + r], s_recv.at[bits + r], d, p))
    sums_ref[bits + 1 + s] = sums_ref[bits]
    for copy in loads[4:]:
        copy.wait()
    for r, p in enumerate(peers):
        arrive(gate_in.at[p], g_recv.at[r])
    wide = inner + 2 * N
    heads = inner // P_SIZE
    triple = HEADS // 16
    for b in range(4):
        seat = 2 * (b % 2) + b // 2
        for k in range(4):
            at = (4 * k + b) * STRIPE
            grad_ref[:, at : at + STRIPE] = gate_in[seat, :, k * STRIPE : (k + 1) * STRIPE].astype(F32)
    gout_ref[...] = gout[...].astype(F32)
    gsum = jnp.sum(gout_ref[...] * block_ref[...].astype(F32), axis=1, keepdims=True)
    gdots_ref[...] = as_row(gsum) / gg_ref[...].astype(F32)
    for r, p in enumerate(peers):
        arrive(sums_ref.at[bits + 1 + p], s_recv.at[bits + r])
    chan = taps_ref.shape[1]
    convs = jnp.zeros((8, chan), F32)
    per_head = jnp.zeros((8, HEADS), F32)
    v = lax.broadcasted_iota(jnp.int32, (wide, chan), 0)
    g = lax.broadcasted_iota(jnp.int32, (wide, chan), 1) + chan * (d * tp + s)
    lane = lax.broadcasted_iota(jnp.int32, (LANES, HEADS), 0)
    head = lax.broadcasted_iota(jnp.int32, (LANES, HEADS), 1)
    place = []
    for p in range(tp):
        b = 2 * (p % 2) + p // 2
        from_v = jnp.where(v < inner, v + 3 * STRIPE * hop(v, STRIPE) + STRIPE * b, v - inner + DI)
        sums = sums_ref[bits + 1 + p]
        convs = convs + dot(sums[:, :wide], jnp.where(from_v == g, 1.0, 0.0), precision=HIGH)
        hit = jnp.logical_and(lane < heads, head == lane + 3 * triple * hop(lane, triple) + triple * b)
        place.append(jnp.where(hit, 1.0, 0.0))
        per_head = per_head + dot(sums[:, wide:], place[p], precision=HIGH)
    taps_ref[...] = convs[:KW]
    bias_ref[...] = convs[KW : KW + 1]
    heads_ref[...] = per_head
    total.add(deep - 1)
    total.finish()
    for p in range(tp):
        handed[p] = final[p * rows : (p + 1) * rows, :]
    for r, p in enumerate(peers):
        sends.start(None, push(handed.at[p], out_ref.at[s], a_send.at[r], a_recv.at[r], d, p))
    out_ref[s] = handed[s]

    arrive(x_buf, x_recv.at[0])

    def last(i):
        m, row = i // (part // 16), (i % (part // 16)) * 16
        lines = pl.ds(pl.multiple_of(row, 16), 16)
        h = tok[m, lines, :].astype(F32)
        r = lax.rsqrt(jnp.mean(h * h, axis=-1, keepdims=True) + EPSILON)
        n = h * r
        grad = (own_ref[m, lines, :] + x_buf[m, lines, :].astype(F32)) * gain_ref[KW + 1 : KW + 2, :]
        grad = grad - n * jnp.mean(grad * n, axis=-1, keepdims=True)
        tokens_ref[m, lines, :] = (cot[m, lines, :].astype(F32) + r * grad).astype(BF16)

    each(micro * (part // 16), last)
    for r, p in enumerate(peers):
        arrive(out_ref.at[p], a_recv.at[r])
    both = [jnp.zeros((rows, N), F32), jnp.zeros((rows, N), F32)]
    steps = jnp.zeros((rows, HEADS), F32)
    for b in range(4):
        seat = 2 * (b % 2) + b // 2
        for k in range(4):
            at = DI + (4 * k + b) * STRIPE
            piece = out_ref[seat, :, k * STRIPE : (k + 1) * STRIPE]
            grad_ref[:, at : at + STRIPE] = piece.astype(F32)
        both[seat % 2] = both[seat % 2] + out_ref[seat, :, inner : inner + N].astype(F32)
        steps = steps + dot(out_ref[seat, :, inner + N :], place[seat].astype(BF16))
    grad_ref[:, 2 * DI : 2 * DI + N] = both[0]
    grad_ref[:, 2 * DI + N : 2 * DI + 2 * N] = both[1]
    grad_ref[:, 2 * DI + 2 * N :] = steps
    nsum = jnp.sum(grad_ref[...] * proj_ref[...].astype(F32), axis=1, keepdims=True)
    dots_ref[...] = as_row(nsum) / ng_ref[...].astype(F32)
    sends.drain()


def tail(
    normed_t, rows_grad, gates_grad, w_rest, w_gate, tokens, cotangent, gate_in, gout, in_proj, out_proj, gains, wgrad, hgrad, norm_gain, gated_gain, chan, dp
):
    width, count = normed_t.shape
    micro = tokens.shape[0]
    tp = gate_in.shape[0]
    small = (8, wgrad.shape[1] + hgrad.shape[1])
    full = gates_grad.shape[1] + N + LANES
    rows = width // dp // tp
    part = count // micro // tp
    deep = dp // 2
    bits = dp.bit_length() - 1
    block = tp * rows
    dma = pltpu.SemaphoreType.DMA
    vmem = pl.BlockSpec(memory_space=pltpu.VMEM)
    hbm = pl.BlockSpec(memory_space=pl.ANY)
    return pl.pallas_call(
        functools.partial(tail_kernel, dp),
        in_specs=[hbm] * 9 + [vmem] * 7,
        out_specs=[vmem] * 8,
        out_shape=[
            jax.ShapeDtypeStruct(tokens.shape, BF16),
            jax.ShapeDtypeStruct(in_proj.shape, F32),
            jax.ShapeDtypeStruct((1, rows), F32),
            jax.ShapeDtypeStruct(gout.shape, F32),
            jax.ShapeDtypeStruct((1, gout.shape[0]), F32),
            jax.ShapeDtypeStruct((KW, chan), F32),
            jax.ShapeDtypeStruct((1, chan), F32),
            jax.ShapeDtypeStruct((8, HEADS), F32),
        ],
        scratch_shapes=[
            pltpu.VMEM((tp, rows, full), BF16),
            pltpu.VMEM((micro, part, width), F32),
            pltpu.VMEM((bits + 1 + tp,) + small, F32),
            pltpu.VMEM(tokens.shape, BF16),
            pltpu.VMEM(tokens.shape, BF16),
            pltpu.VMEM(gate_in.shape, BF16),
            pltpu.VMEM(gout.shape, BF16),
            pltpu.VMEM((deep, 2 * block, count), BF16),
            pltpu.VMEM(rows_grad.shape, BF16),
            pltpu.VMEM(gates_grad.shape, BF16),
            pltpu.VMEM(w_rest.shape, BF16),
            pltpu.VMEM(w_gate.shape, BF16),
            pltpu.VMEM((part, min(width, 512)), F32),
            pltpu.VMEM((2 * block, 384), F32),
            pltpu.VMEM((2 * block, 2 * N), F32),
            pltpu.VMEM((2 * block, N), F32),
            pltpu.VMEM((deep, 2 * block, N), BF16),
            pltpu.VMEM((deep, 2 * block, N), BF16),
            pltpu.VMEM((deep, block, full), BF16),
            pltpu.VMEM((deep, block, full), BF16),
            pltpu.VMEM((deep, block, full), BF16),
            pltpu.VMEM((2, deep - 1, block, full), BF16),
            pltpu.VMEM((block, full), BF16),
            pltpu.VMEM((tp, rows, full), BF16),
            pltpu.VMEM((2, micro, part, width), BF16),
            pltpu.VMEM((2, micro, part, width), BF16),
            pltpu.VMEM((micro, part, width), BF16),
            pltpu.VMEM((micro, part, width), BF16),
            pltpu.VMEM((bits,) + small, F32),
            dma((8,)),
            dma((deep,)),
            dma((deep,)),
            dma((deep,)),
            dma((3,)),
            dma((3,)),
            dma((deep,)),
            dma((deep,)),
            dma((2, deep - 1)),
            dma((2, deep - 1)),
            dma((3,)),
            dma((3,)),
            dma((2,)),
            dma((2,)),
            dma((1,)),
            dma((1,)),
            dma((bits + 3,)),
            dma((bits + 3,)),
        ],
        compiler_params=pltpu.CompilerParams(
            collective_id=3, has_side_effects=True, vmem_limit_bytes=62 * 2**20
        ),
        cost_estimate=pl.CostEstimate(flops=6 * 10**10, bytes_accessed=3 * 10**7, transcendentals=0),
        name="gradients_to_owners",
    )(
        normed_t,
        rows_grad,
        gates_grad,
        w_rest,
        w_gate,
        tokens,
        cotangent,
        gate_in,
        gout,
        in_proj,
        out_proj,
        gains,
        wgrad,
        hgrad,
        norm_gain,
        gated_gain,
    )


def body(
    tokens,
    in_proj,
    conv_weight,
    conv_bias,
    decay_log,
    step_bias,
    skip_gain,
    norm_gain,
    gated_gain,
    out_proj,
    cotangent,
):
    dp, tp = lax.axis_size("dp"), lax.axis_size("seq")
    s = lax.axis_index("seq")
    micro, part, width = tokens.shape
    heads = HEADS // tp
    inner = heads * P_SIZE
    rows = in_proj.shape[0]
    length = part * tp
    count = micro * length
    wide = inner + 2 * N
    chan = conv_bias.shape[0]

    (
        normed,
        normed_t,
        proj_rest,
        ssd,
        memory,
        gate,
        w_rest,
        w_gate,
        w_out,
        cot,
        taps,
        gains,
        g_gated,
        per_head,
    ) = head(
        in_proj,
        conv_weight,
        conv_bias[None],
        norm_gain[None],
        gated_gain[None],
        decay_log[None],
        step_bias[None],
        skip_gain[None],
        tokens,
        cotangent,
        out_proj,
        dp,
        tp,
    )
    proj_rest = proj_rest.reshape(count, wide + LANES)
    w_rest = w_rest.reshape(width, wide + LANES)
    w_gate = w_gate.reshape(width, inner)
    grad_ssd, grad_gate, out_part, grad_out, gate_in = gating(
        ssd, gate, cot, w_out.reshape(inner, width), normed_t, g_gated, dp
    )
    grad_ssd = grad_ssd.reshape(count, inner)
    grad_gate = grad_gate.reshape(count, inner)
    grad_rest, wgrad, hgrad, out_part, grad_out, gate_in = middle(
        proj_rest,
        grad_ssd,
        memory,
        taps,
        per_head,
        out_part.reshape(micro, length, width),
        grad_out.reshape(dp, -1, width),
        gate_in.reshape(dp, tp, rows, inner),
        tokens,
        dp,
        tp,
        heads,
        micro,
    )
    tokens_grad, in_grad, dots, grad_out, gdots, conv_grad, bias_grad, head_grads = tail(
        normed_t,
        grad_rest,
        grad_gate,
        w_rest,
        w_gate,
        tokens,
        cotangent,
        gate_in,
        grad_out,
        in_proj,
        out_proj,
        gains,
        wgrad,
        hgrad,
        norm_gain[None],
        gated_gain[None],
        chan,
        dp,
    )
    return (
        out_part,
        tokens_grad,
        in_grad,
        conv_grad,
        bias_grad[0],
        head_grads[0],
        head_grads[1],
        head_grads[2],
        dots[0],
        gdots[0],
        grad_out,
    )


def solution(mesh):
    both = ("dp", "seq")
    return jax.shard_map(
        body,
        mesh=mesh,
        in_specs=(
            P("dp", "seq", None),
            P(both, None),
            P(None, both),
            P(both),
            P(),
            P(),
            P(),
            P(both),
            P(both),
            P(both, None),
            P("dp", "seq", None),
        ),
        out_specs=(
            P("dp", "seq", None),
            P("dp", "seq", None),
            P(both, None),
            P(None, both),
            P(both),
            P(),
            P(),
            P(),
            P(both),
            P(both),
            P(both, None),
        ),
        check_vma=False,
    )
```

```python
import functools

import jax
import jax.numpy as jnp
from jax import lax
from jax.experimental import pallas as pl
from jax.experimental.pallas import tpu as pltpu
from jax.sharding import PartitionSpec as P

HEADS = 48
P_SIZE = 64
N = 128
KW = 4
DI = 3072
CD = 3328
LANES = 128
FAR = -1e30

EPSILON = 1e-05
F32 = jnp.float32
BF16 = jnp.bfloat16


def dot(a, b, dims=((1,), (0,)), precision=None):
    return lax.dot_general(a, b, (dims, ((), ())), precision=precision, preferred_element_type=F32)


NT = ((1,), (1,))
HIGH = lax.Precision.HIGHEST


def pick(a, p, low):
    return jnp.where(low, a[:, 2 * p : 2 * p + 1], a[:, 2 * p + 1 : 2 * p + 2])


def chunk_parts(heads, rest_ref, xbuf, taps_ref, head_ref):
    size = rest_ref.shape[0]
    wide = taps_ref.shape[1]
    mixed = taps_ref[KW : KW + 1, :] + taps_ref[0:1, :] * xbuf[5 : 5 + size, :]
    for k in range(1, KW):
        mixed = mixed + taps_ref[k : k + 1, :] * xbuf[5 + k : 5 + k + size, :]
    sig = lax.logistic(mixed)
    return (mixed, sig) + step_parts(heads, rest_ref, taps_ref, head_ref)


def step_parts(heads, rest_ref, taps_ref, head_ref):
    size = rest_ref.shape[0]
    wide = taps_ref.shape[1]
    lane = lax.broadcasted_iota(jnp.int32, (1, LANES), 1)
    raw = jnp.where(lane < heads, rest_ref[:, wide:], 0.0) + head_ref[1:2, :]
    step = jnp.maximum(raw, 0.0) + jnp.log1p(jnp.exp(-jnp.abs(raw)))
    decay = -jnp.exp(head_ref[0:1, :]) * step
    i = lax.broadcasted_iota(jnp.int32, (size, size), 0)
    j = lax.broadcasted_iota(jnp.int32, (size, size), 1)
    run = dot(jnp.where(i >= j, 1.0, 0.0), decay, precision=HIGH)
    return raw, step, decay, run


def backward_kernel(
    heads,
    rest_ref,
    prev_ref,
    dy_ref,
    mem_ref,
    taps_ref,
    head_ref,
    out_ref,
    wgrad_ref,
    hgrad_ref,
    xbuf,
    gbuf,
    adj,
    dmix,
    dsum,
    uprod,
    zprod,
    rows_t,
    line,
    acts,
    slopes,
):
    size = rest_ref.shape[0]
    wide = taps_ref.shape[1]
    inner = heads * P_SIZE
    chunks = pl.num_programs(1)
    step_id = pl.program_id(1)
    newest = step_id == 0
    oldest = step_id == chunks - 1
    begin = jnp.logical_and(pl.program_id(0) == 0, newest)
    finish = jnp.logical_and(pl.program_id(0) == pl.num_programs(0) - 1, oldest)

    @pl.when(begin)
    def _():
        wgrad_ref[...] = jnp.zeros_like(wgrad_ref)
        hgrad_ref[...] = jnp.zeros_like(hgrad_ref)
        rows_t[...] = jnp.zeros_like(rows_t)
        line[...] = jnp.zeros_like(line)

    @pl.when(newest)
    def _():
        gbuf[size : size + 8, :] = jnp.zeros((8, wide), F32)
        adj[...] = jnp.zeros_like(adj)

    @pl.when(jnp.logical_not(newest))
    def _():
        gbuf[size : size + 8, :] = gbuf[0:8, :]

    xbuf[0:8, :] = jnp.where(oldest, 0.0, prev_ref[:, :wide])
    xbuf[8 : 8 + size, :] = rest_ref[:, :wide]
    for n in range(wide // LANES):
        at = slice(n * LANES, (n + 1) * LANES)
        mixed = taps_ref[KW : KW + 1, at] + taps_ref[0:1, at] * xbuf[5 : 5 + size, at]
        for k in range(1, KW):
            mixed = mixed + taps_ref[k : k + 1, at] * xbuf[5 + k : 5 + k + size, at]
        sig = lax.logistic(mixed)
        acts[:, at] = mixed * sig
        slopes[:, at] = sig * (1.0 + mixed * (1.0 - sig))
    raw, step, decay, run = step_parts(heads, rest_ref, taps_ref, head_ref)
    run_t = run.T
    closing = run[size - 1 : size, :]
    last = jnp.exp(closing)
    left = jnp.exp(closing - run)
    grown = jnp.exp(run)
    b = acts[:, inner : inner + N].astype(BF16)
    c = acts[:, inner + N :].astype(BF16)
    c_t = acts[:, inner + N :].T.astype(BF16)
    scores_t = dot(b, c, NT)
    low = lax.broadcasted_iota(jnp.int32, (1, LANES), 1) < P_SIZE
    lane = lax.broadcasted_iota(jnp.int32, (1, LANES), 1)
    j = lax.broadcasted_iota(jnp.int32, (size, size), 0)
    i = lax.broadcasted_iota(jnp.int32, (size, size), 1)
    causal = i >= j
    mem_b = mem_ref[0]
    adj_b = adj[...].astype(BF16)
    spread = dot(b, adj_b)
    inherit = dot(c, mem_b)
    scored = jnp.zeros((size, size), F32)
    cols = jnp.zeros((size, LANES), F32)
    for p in range(heads // 2):
        at = slice(p * LANES, (p + 1) * LANES)
        v = acts[:, at]
        size_p = pick(step, p, low)
        xv = size_p * v
        dy = dy_ref[:, at]
        dyb = dy.astype(BF16)
        xvb = xv.astype(BF16)
        dxv = pick(left, p, low) * spread[:, at]
        zprod[:, at] = (dxv * xv).astype(BF16)
        dyg = pick(grown, p, low) * dy
        uprod[:, at] = (dyg * inherit[:, at]).astype(BF16)
        for e in range(2):
            h = 2 * p + e
            keep = low if e == 0 else jnp.logical_not(low)
            mine = jnp.where(keep, dy, 0.0).astype(BF16)
            gap = run_t[h : h + 1, :] - run[:, h : h + 1]
            near = jnp.exp(jnp.where(causal, gap, FAR))
            w_t = scores_t * near
            dw_t = dot(xvb, mine, NT)
            scored = scored + dw_t * near
            g_t = dw_t * w_t
            rows_t[h : h + 1, :] = jnp.sum(g_t, axis=0, keepdims=True)
            cols = jnp.where(lane == h, jnp.sum(g_t, axis=1, keepdims=True), cols)
            dxv = dxv + dot(w_t.astype(BF16), mine)
        dsum[:, at] = (dxv * v).astype(BF16)
        dmix[:, at] = size_p * dxv + pick(head_ref[2:3, :], p, low) * dy
        line[0:1, at] += jnp.sum(dy * v, axis=0, keepdims=True)
        line[1:2, at] = jnp.sum(adj[:, at] * mem_b[:, at].astype(F32), axis=0, keepdims=True) * pick(
            last, p, low
        )
        xc = (pick(left, p, low) * xv).astype(BF16)
        dygb = dyg.astype(BF16)
        db = dot(xc, adj_b[:, at], NT)
        dc = dot(dygb, mem_b[:, at], NT)
        if p == 0:
            dmix[:, inner : inner + N] = db
            dmix[:, inner + N :] = dc
        else:
            dmix[:, inner : inner + N] += db
            dmix[:, inner + N :] += dc
        adj[:, at] = adj[:, at] * pick(last, p, low) + dot(c_t, dygb)
    dmix[:, inner : inner + N] += dot(scored.astype(BF16), c)
    dmix[:, inner + N :] += dot(scored.T.astype(BF16), b)

    group = jnp.where(
        lax.broadcasted_iota(jnp.int32, (inner, LANES), 0) // P_SIZE
        == lax.broadcasted_iota(jnp.int32, (inner, LANES), 1),
        1.0,
        0.0,
    )
    group_b = group.astype(BF16)
    d_step = dot(dsum[...], group_b)
    u = dot(uprod[...], group_b)
    z = dot(zprod[...], group_b)
    sums = dot(line[...], group, precision=HIGH)
    d_run = rows_t[...].T - cols + u - z
    row = lax.broadcasted_iota(jnp.int32, (size, 1), 0)
    ending = sums[1:2, :] + jnp.sum(z, axis=0, keepdims=True)
    d_run = d_run + jnp.where(row == size - 1, ending, 0.0)
    d_decay = dot(jnp.where(causal, 1.0, 0.0), d_run, precision=HIGH)
    d_raw = (d_step - jnp.exp(head_ref[0:1, :]) * d_decay) * lax.logistic(raw)
    d_raw = jnp.where(lane < heads, d_raw, 0.0)
    hgrad_ref[0:1, :] += jnp.sum(d_decay * decay, axis=0, keepdims=True)
    hgrad_ref[1:2, :] += jnp.sum(d_raw, axis=0, keepdims=True)

    @pl.when(finish)
    def _():
        hgrad_ref[2:3, :] = sums[0:1, :]

    for n in range(wide // LANES):
        at = slice(n * LANES, (n + 1) * LANES)
        g = dmix[:, at] * slopes[:, at]
        gbuf[0:size, at] = g
        wgrad_ref[KW : KW + 1, at] += jnp.sum(g, axis=0, keepdims=True)
        for k in range(KW):
            lag = xbuf[5 + k : 5 + k + size, at]
            wgrad_ref[k : k + 1, at] += jnp.sum(g * lag, axis=0, keepdims=True)
        back = taps_ref[KW - 1 : KW, at] * g
        for k in range(KW - 1):
            back = back + taps_ref[k : k + 1, at] * gbuf[3 - k : 3 - k + size, at]
        out_ref[:, at] = back.astype(BF16)
    out_ref[:, wide:] = d_raw.astype(BF16)


MESH = pl.DeviceIdType.MESH


def where_am_i(dp):
    d, s = lax.axis_index("dp"), lax.axis_index("seq")
    z, y = d // 2, d % 2
    x, c = s // 2, s % 2
    peers = [s + 1 - 2 * c, s + 2 - 4 * x, 3 - s]
    return d, s, z, y, x, c, peers, dp // 2


def push(src, dst, send_sem, recv_sem, d, s):
    return pltpu.make_async_remote_copy(
        src_ref=src,
        dst_ref=dst,
        send_sem=send_sem,
        recv_sem=recv_sem,
        device_id={"dp": d, "seq": s},
        device_id_type=MESH,
    )


def greet(partners):
    barrier = pltpu.get_barrier_semaphore()
    for cond, d, s in partners:

        def hello(d=d, s=s):
            pl.semaphore_signal(barrier, inc=1, device_id={"dp": d, "seq": s}, device_id_type=MESH)

        if cond is None:
            hello()
        else:
            pl.when(cond)(hello)
    count = 0
    for cond, _, _ in partners:
        count = count + (1 if cond is None else jnp.where(cond, 1, 0))
    pl.semaphore_wait(barrier, count)


class Sends:
    def __init__(self):
        self.items = []

    def start(self, cond, copy):
        if cond is None:
            copy.start()
        else:
            pl.when(cond)(copy.start)
        self.items.append((cond, copy))

    def drain(self):
        for cond, copy in self.items:
            if cond is None:
                copy.wait_send()
            else:
                pl.when(cond)(copy.wait_send)


STRIPE = DI // 16


def swapped(s):
    return 2 * (s % 2) + s // 2


def stripe_owner(block, dp):
    u = dp // 4
    return block // (4 * u) * u + block % u


def stripe_seat(block, dp):
    return swapped(block // (dp // 4) % 4)


def stripe_block(d, s, dp):
    u = dp // 4
    return (d // u * 4 + swapped(s)) * u + d % u


def forward_chunk(heads, first, rest_ref, taps_ref, head_ref, ssd_ref, mem_ref, xbuf, mem):
    size = rest_ref.shape[0]
    wide = taps_ref.shape[1]
    inner = heads * P_SIZE

    @pl.when(first)
    def _():
        xbuf[0:8, :] = jnp.zeros((8, wide), F32)
        mem[...] = jnp.zeros_like(mem)

    @pl.when(jnp.logical_not(first))
    def _():
        xbuf[0:8, :] = xbuf[size : size + 8, :]

    xbuf[8 : 8 + size, :] = rest_ref[:, :wide]
    mixed, sig, _, step, _, run = chunk_parts(heads, rest_ref, xbuf, taps_ref, head_ref)
    act = mixed * sig
    run_t = run.T
    closing = run[size - 1 : size, :]
    last = jnp.exp(closing)
    left = jnp.exp(closing - run)
    grown = jnp.exp(run)
    b = act[:, inner : inner + N]
    c = act[:, inner + N :].astype(BF16)
    scores = dot(c, b.astype(BF16), NT)
    b_t = b.T.astype(BF16)
    mem_ref[...] = mem[...].astype(BF16)
    inter = dot(c, mem[...].astype(BF16))
    low = lax.broadcasted_iota(jnp.int32, (1, LANES), 1) < P_SIZE
    i = lax.broadcasted_iota(jnp.int32, (size, size), 0)
    j = lax.broadcasted_iota(jnp.int32, (size, size), 1)
    causal = i >= j
    for p in range(heads // 2):
        at = slice(p * LANES, (p + 1) * LANES)
        v = act[:, at]
        xv = pick(step, p, low) * v
        y = pick(head_ref[2:3, :], p, low) * v + pick(grown, p, low) * inter[:, at]
        for e in range(2):
            h = 2 * p + e
            gap = run[:, h : h + 1] - run_t[h : h + 1, :]
            w = (scores * jnp.exp(jnp.where(causal, gap, FAR))).astype(BF16)
            mine = jnp.where(low if e == 0 else jnp.logical_not(low), xv, 0.0).astype(BF16)
            y = y + dot(w, mine)
        ssd_ref[:, at] = y
        xc = (pick(left, p, low) * xv).astype(BF16)
        mem[:, at] = mem[:, at] * pick(last, p, low) + dot(b_t, xc)


def hop(v, size):
    return sum(jnp.where(v >= q * size, 1, 0) for q in range(1, 4))


def head_kernel(
    dp,
    heads,
    proj_ref,
    cw_ref,
    cb_ref,
    ng_ref,
    gg_ref,
    dl_ref,
    sb_ref,
    sg_ref,
    tok_ref,
    cot_ref,
    block_ref,
    normed_hbm,
    turned_hbm,
    proj_hbm,
    ssd_hbm,
    mem_hbm,
    gates_hbm,
    rest_hbm,
    gate_hbm,
    out_hbm,
    cot_hbm,
    taps_ref,
    gain_ref,
    gated_ref,
    head_ref,
    line,
    small_stage,
    val_stage,
    half_stage,
    gate_stage,
    small_all,
    val_in,
    half_in,
    gate_in,
    w_val,
    w_half,
    w_other,
    w_tail,
    w_gate,
    out_shard,
    tok,
    flipped,
    proj,
    ssd,
    gates,
    memory,
    xbuf,
    mem,
    l_sem,
    o_sem,
    f_sem,
    p_sem,
    g_sem,
    a_send,
    a_recv,
    z_send,
    z_recv,
    y_send,
    y_recv,
    t_send,
    t_recv,
):
    d, s, z, y, x, c, peers, deep = where_am_i(dp)
    tp, rows = val_stage.shape[:2]
    micro, part, width = tok_ref.shape
    total = dp * tp
    inner = heads * P_SIZE
    wide = inner + 2 * N
    chan, gpiece = cw_ref.shape[1], gg_ref.shape[1]
    up, down, far = d + 2, d - 2, d + 1 - 2 * y
    me = d * tp + s
    to_d, to_s, turned = stripe_owner(me, dp), stripe_seat(me, dp), stripe_block(d, s, dp)
    from_d, from_s = turned // tp, turned % tp
    moves = turned != me

    triple = HEADS // 16
    line[...] = jnp.zeros_like(line)
    line[0:KW, 0:chan] = cw_ref[...].astype(F32)
    line[KW : KW + 1, 0:chan] = cb_ref[...].astype(F32)
    line[KW + 1 : KW + 2, 0:rows] = ng_ref[...].astype(F32)
    line[KW + 2 : KW + 3, 0:gpiece] = gg_ref[...].astype(F32)
    raw = proj_ref[:, 2 * DI + 2 * N :]
    for b in range(4):
        seat = 2 * (b % 2) + b // 2
        for k in range(4):
            to, at = k * STRIPE, (4 * k + b) * STRIPE
            gate_stage[seat, :, to : to + STRIPE] = proj_ref[:, at : at + STRIPE]
            val_stage[seat, :, to : to + STRIPE] = proj_ref[:, DI + at : DI + at + STRIPE]
        at = 2 * DI + N * (seat % 2)
        half_stage[seat] = proj_ref[:, at : at + N]
        v = lax.broadcasted_iota(jnp.int32, (16, HEADS), 0)
        g = lax.broadcasted_iota(jnp.int32, (16, HEADS), 1)
        hit = jnp.logical_and(v < heads, g == v + 3 * triple * hop(v, triple) + triple * b)
        line[16:32, 0:rows] = dot(jnp.where(hit, 1.0, 0.0).astype(BF16), raw, NT)
        small_stage[seat] = line[...].astype(BF16)
    v = lax.broadcasted_iota(jnp.int32, (HEADS, LANES), 1)
    g = lax.broadcasted_iota(jnp.int32, (HEADS, LANES), 0)
    hit = jnp.logical_and(v < heads, g == v + 3 * triple * hop(v, triple) + triple * swapped(s))
    line[...] = jnp.zeros_like(line)
    for k, row in enumerate((dl_ref, sb_ref, sg_ref)):
        line[k : k + 1, 0:HEADS] = row[...]
    head_ref[...] = dot(line[0:8, 0:HEADS], jnp.where(hit, 1.0, 0.0), precision=HIGH)

    greet(
        [(None, d, p) for p in peers]
        + [(None, far, s), (z < deep - 1, up, s), (z > 0, down, s)]
        + [(moves, to_d, to_s), (moves, from_d, from_s)]
    )
    sends = Sends()

    def arrive(dst, sem):
        push(dst, dst, sem, sem, d, peers[0]).wait_recv()

    def mine(ref, k):
        return ref.at[:, pl.ds(k * part, part), :]

    def exchange(a, stage, target):
        for r, p in enumerate(peers):
            sends.start(
                None, push(stage.at[p], target(s), a_send.at[a, r], a_recv.at[a, r], d, p)
            )

    def exchanged(a, target):
        for r, p in enumerate(peers):
            arrive(target(p), a_recv.at[a, r])

    exchange(0, small_stage, lambda k: small_all.at[d, k])
    exchange(1, half_stage, lambda k: half_in.at[k])
    exchange(2, val_stage, lambda k: val_in.at[k])
    exchange(3, gate_stage, lambda k: gate_in.at[k])
    sends.start(moves, push(block_ref, out_shard, t_send.at[2], t_recv.at[2], to_d, to_s))
    sends.start(None, push(tok_ref, mine(tok, s), t_send.at[0], t_recv.at[0], d, peers[1]))
    sends.start(None, push(tok_ref, mine(tok, s), t_send.at[1], t_recv.at[1], d, peers[0]))
    sends.start(None, push(cot_ref, mine(cot_hbm, s), t_send.at[3], t_recv.at[3], d, peers[1]))
    sends.start(None, push(cot_ref, mine(cot_hbm, s), t_send.at[4], t_recv.at[4], d, peers[0]))
    saves = []

    def save(src, dst):
        copy = pltpu.make_async_copy(src, dst, l_sem.at[len(saves)])
        copy.start()
        saves.append(copy)

    save(cot_ref, mine(cot_hbm, s))
    small_all[d, s] = small_stage[s]
    half_in[s] = half_stage[s]
    val_in[s] = val_stage[s]
    gate_in[s] = gate_stage[s]
    tok[:, pl.ds(pl.multiple_of(s * part, part), part), :] = tok_ref[...]

    @pl.when(jnp.logical_not(moves))
    def _():
        out_shard[...] = block_ref[...]

    def begin(a, shard, dst):
        block = dst.at[d]
        sends.start(z < deep - 1, push(shard, block, z_send.at[a, 0, 0], z_recv.at[a, 0, 0], up, s))
        sends.start(z > 0, push(shard, block, z_send.at[a, 1, 0], z_recv.at[a, 1, 0], down, s))
        sends.start(None, push(shard, block, y_send.at[a, 0, 0], y_recv.at[a, 0, 0], far, s))

    def plan(a, dst, t):
        steps = []
        for way in range(2):
            here = (z >= t) if way == 0 else (z + t <= deep - 1)
            more = jnp.logical_and(here, (z < deep - 1) if way == 0 else (z > 0))
            at = jnp.clip(d - 2 * t if way == 0 else d + 2 * t, 0, dp - 1)
            block = dst.at[at]
            got = z_recv.at[a, way, t - 1]
            on = []
            if t < deep - 1:
                nxt = up if way == 0 else down
                on.append(
                    (more, push(block, block, z_send.at[a, way, t], z_recv.at[a, way, t], nxt, s))
                )
            on.append(
                (here, push(block, block, y_send.at[a, way, t], y_recv.at[a, way, t], far, s))
            )
            steps.append((here, push(block, block, got, got, d, peers[0]), on))
        return steps

    def run(steps):
        for here, wait, on in steps:
            pl.when(here)(wait.wait_recv)
            for cond, copy in on:
                pl.when(cond)(copy.start)

    def remember(steps):
        for _, _, on in steps:
            sends.items.extend(on)

    def relay(a, dst, t):
        steps = plan(a, dst, t)
        run(steps)
        remember(steps)

    def landed(a, dst):
        arrive(dst.at[far], y_recv.at[a, 0, 0])
        for t in range(1, deep):
            for way in range(2):
                here = (z >= t) if way == 0 else (z + t <= deep - 1)
                at = jnp.clip(far - 2 * t if way == 0 else far + 2 * t, 0, dp - 1)
                pl.when(here)(functools.partial(arrive, dst.at[at], y_recv.at[a, way, t]))

    def shard_of(a, pieces, dst):
        exchanged(a, lambda p: pieces.at[p])
        for k in range(tp):
            dst[d, k * rows : (k + 1) * rows, :] = pieces[k]
        begin(a, dst.at[d], dst)

    exchanged(0, lambda p: small_all.at[d, p])
    begin(0, small_all.at[d], small_all)
    shard_of(1, half_in, w_half)
    shard_of(2, val_in, w_val)
    for t in range(1, deep):
        relay(0, small_all, t)
        relay(1, w_half, t)
        relay(2, w_val, t)
    shard_of(3, gate_in, w_gate)
    pl.when(moves)(functools.partial(arrive, out_shard, t_recv.at[2]))
    begin(4, out_shard, out_hbm)
    save(out_shard, out_hbm.at[d])

    landed(0, small_all)

    def one_hot(columns, index, k, length):
        lane = lax.broadcasted_iota(jnp.int32, (LANES, columns), 1)
        at = lax.broadcasted_iota(jnp.int32, (LANES, columns), 0)
        hit = jnp.logical_and(at < length, index(lane) == k * length + at)
        return jnp.where(hit, 1.0, 0.0).astype(BF16)

    taps_ref[...] = jnp.zeros_like(taps_ref)
    gain_ref[...] = jnp.zeros_like(gain_ref)
    gated_ref[...] = jnp.zeros_like(gated_ref)

    def striped(v):
        return v + 3 * STRIPE * hop(v, STRIPE) + STRIPE * swapped(s)

    def lay_out(dd, carry):
        for kk in range(tp):
            k = dd * tp + kk
            values = small_all[dd, kk, 0:16, :]
            chans = one_hot(wide, lambda v: jnp.where(v < inner, striped(v), v - inner + DI), k, chan)
            taps_ref[...] += dot(values, chans)[:8]
            gain_ref[...] += dot(values, one_hot(width, lambda v: v, k, rows))
            gated_ref[...] += dot(values, one_hot(inner, striped, k, gpiece))
            turned = jnp.concatenate(
                [small_all[dd, kk, 16:32, :].astype(F32), jnp.zeros((LANES - 16, LANES), F32)], axis=0
            ).T
            w_tail[dd, kk * rows : (kk + 1) * rows, 2 * N :] = turned[:rows].astype(BF16)
        return carry

    lax.fori_loop(0, dp, lay_out, 0)
    landed(1, w_half)
    sends.start(None, push(w_half, w_other, t_send.at[6], t_recv.at[6], d, peers[0]))
    landed(2, w_val)
    save(w_val, rest_hbm.at[:, :, pl.ds(0, inner)])
    arrive(w_other, t_recv.at[6])

    def both_halves(dd, carry):
        w_tail[dd, :, pl.ds(pl.multiple_of(c * N, N), N)] = w_half[dd]
        w_tail[dd, :, pl.ds(pl.multiple_of((1 - c) * N, N), N)] = w_other[dd]
        return carry

    lax.fori_loop(0, dp, both_halves, 0)
    save(w_tail, rest_hbm.at[:, :, pl.ds(inner, w_tail.shape[2])])
    arrive(mine(tok, peers[1]), t_recv.at[0])
    block = mine(tok, peers[1])
    hand = push(block, block, t_send.at[5], t_recv.at[5], d, peers[0])
    hand.start()
    relay(3, w_gate, 1)
    relay(4, out_hbm, 1)
    arrive(mine(tok, peers[0]), t_recv.at[1])
    arrive(mine(tok, peers[2]), t_recv.at[5])
    hand.wait_send()

    tasks = [(a, ref, t) for t in range(2, deep) for a, ref in ((3, w_gate), (4, out_hbm))]
    chunks = micro * tp
    when = {}
    for n, task in enumerate(tasks):
        when.setdefault(min(2 + n * 4 // len(tasks), chunks - 1), []).append(plan(*task))
    for plans in when.values():
        for steps in plans:
            remember(steps)

    def columns(i):
        return pl.ds(pl.multiple_of(i * part, part), part)

    def chunk(i, carry):
        m, k = i // tp, i % tp
        lines = pl.ds(pl.multiple_of(k * part, part), part)
        h = tok[m, lines, :].astype(F32)
        r = lax.rsqrt(jnp.mean(h * h, axis=-1, keepdims=True) + EPSILON)
        value = h * r * gain_ref[5:6, :]
        tok[m, lines, :] = value.astype(BF16)
        flipped[i] = value.T.astype(BF16)
        proj[i, :, 0:inner] = dot(tok[m, lines, :], w_val[...].reshape(width, inner))
        proj[i, :, inner:] = dot(tok[m, lines, :], w_tail[...].reshape(width, w_tail.shape[2]))
        forward_chunk(
            heads, k == 0, proj.at[i], taps_ref, head_ref, ssd.at[i], memory.at[i], xbuf, mem
        )
        pltpu.make_async_copy(tok.at[m, lines, :], normed_hbm.at[m, lines, :], o_sem.at[i]).start()
        pltpu.make_async_copy(flipped.at[i], turned_hbm.at[:, columns(i)], f_sem.at[i]).start()
        pltpu.make_async_copy(proj.at[i], proj_hbm.at[i], p_sem.at[i]).start()
        for n, plans in when.items():

            @pl.when(i == n)
            def _():
                for steps in plans:
                    run(steps)

        return carry

    lax.fori_loop(0, chunks, chunk, 0)
    save(ssd, ssd_hbm)
    save(memory, mem_hbm)
    arrive(mine(cot_hbm, peers[1]), t_recv.at[3])
    block = mine(cot_hbm, peers[1])
    sends.start(None, push(block, block, t_send.at[7], t_recv.at[7], d, peers[0]))
    landed(3, w_gate)
    save(w_gate, gate_hbm)

    def gating(i, carry):
        m, k = i // tp, i % tp
        lines = pl.ds(pl.multiple_of(k * part, part), part)
        gates[i] = dot(tok[m, lines, :], w_gate[...].reshape(width, inner))
        pltpu.make_async_copy(gates.at[i], gates_hbm.at[i], g_sem.at[i]).start()
        return carry

    lax.fori_loop(0, chunks, gating, 0)
    landed(4, out_hbm)
    arrive(mine(cot_hbm, peers[0]), t_recv.at[4])
    arrive(mine(cot_hbm, peers[2]), t_recv.at[7])

    def saved(i, carry):
        m, k = i // tp, i % tp
        lines = pl.ds(pl.multiple_of(k * part, part), part)
        pltpu.make_async_copy(tok.at[m, lines, :], normed_hbm.at[m, lines, :], o_sem.at[i]).wait()
        pltpu.make_async_copy(flipped.at[i], turned_hbm.at[:, columns(i)], f_sem.at[i]).wait()
        pltpu.make_async_copy(proj.at[i], proj_hbm.at[i], p_sem.at[i]).wait()
        pltpu.make_async_copy(gates.at[i], gates_hbm.at[i], g_sem.at[i]).wait()
        return carry

    lax.fori_loop(0, chunks, saved, 0)
    for copy in saves:
        copy.wait()
    sends.drain()


def head(in_proj, conv_weight, conv_bias, norm_gain, gated_gain, d_log, s_bias, s_gain, tokens, cotangent, out_proj, dp, tp):
    rows = in_proj.shape[0]
    heads = HEADS // tp
    inner = heads * P_SIZE
    full = inner + 2 * N + LANES
    micro, part, width = tokens.shape
    deep = dp // 2
    chunks = micro * tp
    block = tp * rows
    dma = pltpu.SemaphoreType.DMA
    vmem = pl.BlockSpec(memory_space=pltpu.VMEM)
    hbm = pl.BlockSpec(memory_space=pl.ANY)
    wide = inner + 2 * N

    def shape(*dims, kind=BF16):
        return jax.ShapeDtypeStruct(dims, kind)

    def room(*dims, kind=BF16):
        return pltpu.VMEM(dims, kind)

    return pl.pallas_call(
        functools.partial(head_kernel, dp, heads),
        in_specs=[vmem] * 11,
        out_specs=[hbm] * 10 + [vmem] * 4,
        out_shape=[
            shape(micro, tp * part, width),
            shape(width, chunks * part),
            shape(chunks, part, full, kind=F32),
            shape(chunks, part, inner, kind=F32),
            shape(chunks, N, inner),
            shape(chunks, part, inner, kind=F32),
            shape(dp, block, full),
            shape(dp, block, inner),
            shape(dp, out_proj.shape[0], width),
            shape(micro, tp * part, width),
            shape(8, wide, kind=F32),
            shape(16, width, kind=F32),
            shape(16, inner, kind=F32),
            shape(8, LANES, kind=F32),
        ],
        scratch_shapes=[
            room(32, LANES, kind=F32),
            room(tp, 32, LANES),
            room(tp, rows, inner),
            room(tp, rows, N),
            room(tp, rows, inner),
            room(dp, tp, 32, LANES),
            room(tp, rows, inner),
            room(tp, rows, N),
            room(tp, rows, inner),
            room(dp, block, inner),
            room(dp, block, N),
            room(dp, block, N),
            room(dp, block, 2 * N + LANES),
            room(dp, block, inner),
            room(*out_proj.shape),
            room(micro, tp * part, width),
            room(chunks, width, part),
            room(chunks, part, full, kind=F32),
            room(chunks, part, inner, kind=F32),
            room(chunks, part, inner, kind=F32),
            room(chunks, N, inner),
            room(part + 8, wide, kind=F32),
            room(N, inner, kind=F32),
            dma((8,)),
            dma((chunks,)),
            dma((chunks,)),
            dma((chunks,)),
            dma((chunks,)),
            dma((4, 3)),
            dma((4, 3)),
            dma((5, 2, deep - 1)),
            dma((5, 2, deep - 1)),
            dma((5, 2, deep)),
            dma((5, 2, deep)),
            dma((8,)),
            dma((8,)),
        ],
        compiler_params=pltpu.CompilerParams(
            collective_id=1, has_side_effects=True, vmem_limit_bytes=62 * 2**20
        ),
        cost_estimate=pl.CostEstimate(flops=10**11, bytes_accessed=5 * 10**7, transcendentals=0),
        name="gather_and_mix",
    )(
        in_proj,
        conv_weight,
        conv_bias,
        norm_gain,
        gated_gain,
        d_log,
        s_bias,
        s_gain,
        tokens,
        cotangent,
        out_proj,
    )


class OwnerSum:
    def __init__(self, where, sends, source, mine, ybuf, zbuf, final, sems, theirs_ref=None):
        self.where, self.sends = where, sends
        self.mine, self.ybuf, self.zbuf, self.final = mine, ybuf, zbuf, final
        d, s, z, y, _, _, _, deep = where
        self.load_sem, y_send, self.y_recv, z_send, self.z_recv = sems
        lower = z < deep // 2

        def place(j):
            low = jnp.where(j > z, deep - 1 - j, deep - 1 - z + j)
            high = jnp.where(j < z, j, z + deep - 1 - j)
            return jnp.where(j == z, deep - 1, jnp.where(lower, low, high))

        def turn(k):
            low = jnp.where(k < deep - 1 - z, deep - 1 - k, k - (deep - 1 - z))
            high = jnp.where(k < z, k, deep - 1 - (k - z))
            return jnp.where(lower, low, high) if k < deep - 1 else z

        self.order = [turn(k) for k in range(deep)]
        self.y_items, self.loads = [], []
        for k, j in enumerate(self.order):
            theirs = source.at[j * 2 + 1 - y] if theirs_ref is None else theirs_ref.at[k]
            copy = push(theirs, ybuf.at[k], y_send.at[k], self.y_recv.at[k], d + 1 - 2 * y, s)
            self.y_items.append((None, copy))
            if theirs_ref is None:
                own = source.at[j * 2 + y]
                self.loads.append(pltpu.make_async_copy(own, mine.at[k], self.load_sem.at[k]))
        self.z_items = []
        for t in range(deep - 1):
            ways = []
            for way in range(2):
                depth = z if way == 0 else deep - 1 - z
                j = deep - 1 - t + z if way == 0 else t + z - deep + 1
                k = place(jnp.clip(j, 0, deep - 1))
                nxt = d + 2 if way == 0 else d - 2
                dst, ss, rs = zbuf.at[way, t], z_send.at[way, t], self.z_recv.at[way, t]
                first = (depth == 0, push(ybuf.at[k], dst, ss, rs, nxt, s))
                later = None
                if t > 0:
                    cond = jnp.logical_and(depth > 0, depth <= t)
                    later = (cond, push(zbuf.at[way, t - 1], dst, ss, rs, nxt, s))
                ways.append((k, first, later))
            self.z_items.append(ways)
        sends.items.extend(self.y_items)
        for ways in self.z_items:
            for _, first, later in ways:
                sends.items.append(first)
                if later is not None:
                    sends.items.append(later)

    def arrive(self, ref, sem):
        d, s = self.where[:2]
        push(ref, ref, sem, sem, d, self.where[6][0]).wait_recv()

    def begin(self):
        for _, copy in self.y_items:
            copy.start()
        for copy in self.loads:
            copy.start()

    def each(self, work):
        if self.mine.ndim == 4:
            count, cut = self.mine.shape[1], lambda i: i
        else:
            count, cut = self.mine.shape[1] // 16, lambda i: pl.ds(pl.multiple_of(i * 16, 16), 16)
        lax.fori_loop(0, count, lambda i, carry: (work(cut(i)), carry)[1], 0)

    def add(self, k):
        if self.loads:
            self.loads[k].wait()
        self.arrive(self.ybuf.at[k], self.y_recv.at[k])
        ybuf, mine = self.ybuf, self.mine

        def work(i):
            ybuf[k, i] = (ybuf[k, i].astype(F32) + mine[k, i].astype(F32)).astype(BF16)

        self.each(work)

    def send(self, t):
        zbuf, ybuf = self.zbuf, self.ybuf
        for way, (k, first, later) in enumerate(self.z_items[t]):
            pl.when(first[0])(first[1].start)
            if later is None:
                continue

            @pl.when(later[0])
            def _():
                self.arrive(zbuf.at[way, t - 1], self.z_recv.at[way, t - 1])

                def work(i):
                    zbuf[way, t - 1, i] = (
                        zbuf[way, t - 1, i].astype(F32) + ybuf[k, i].astype(F32)
                    ).astype(BF16)

                self.each(work)
                later[1].start()

    def finish(self):
        z, deep = self.where[2], self.where[7]
        zbuf, ybuf, final = self.zbuf, self.ybuf, self.final
        for way in range(2):
            depth = z if way == 0 else deep - 1 - z
            pl.when(depth > 0)(
                functools.partial(self.arrive, zbuf.at[way, deep - 2], self.z_recv.at[way, deep - 2])
            )

        def work(ways, i):
            total = ybuf[deep - 1, i].astype(F32)
            for way in ways:
                total = total + zbuf[way, deep - 2, i].astype(F32)
            final[i] = total.astype(BF16)

        for cond, ways in (
            (z == 0, (1,)),
            (z == deep - 1, (0,)),
            (jnp.logical_and(z > 0, z < deep - 1), (0, 1)),
        ):
            pl.when(cond)(functools.partial(self.each, functools.partial(work, ways)))


def middle_kernel(
    dp,
    heads,
    rest_ref,
    prev_ref,
    dy_ref,
    mem_ref,
    taps_ref,
    head_ref,
    part_hbm,
    gout_hbm,
    ggate_hbm,
    tok_hbm,
    out_ref,
    wgrad_ref,
    hgrad_ref,
    own_hbm,
    gout_out,
    ggate_out,
    xbuf,
    gbuf,
    adj,
    dmix,
    dsum,
    uprod,
    zprod,
    rows_t,
    line,
    acts,
    slopes,
    o_mine,
    o_y,
    o_z,
    o_final,
    g_mine,
    g_y,
    g_z,
    g_final,
    own,
    core_buf,
    x_buf,
    tok,
    result,
    o_load,
    o_ysend,
    o_yrecv,
    o_zsend,
    o_zrecv,
    g_load,
    g_ysend,
    g_yrecv,
    g_zsend,
    g_zrecv,
    b_load,
    c_send,
    c_recv,
    m_send,
    m_recv,
):
    where = where_am_i(dp)
    d, s, z, y, x, c, peers, deep = where
    micro, part, width = result.shape
    step = pl.program_id(0) * pl.num_programs(1) + pl.program_id(1)
    tp = ggate_hbm.shape[1]
    me = d * tp + s
    turned = stripe_block(d, s, dp)
    moves = turned != me
    to_d, to_s = turned // tp, turned % tp
    from_d, from_s = stripe_owner(me, dp), stripe_seat(me, dp)
    sends = Sends()
    gout = OwnerSum(
        where, sends, gout_hbm, o_mine, o_y, o_z, o_final, (o_load, o_ysend, o_yrecv, o_zsend, o_zrecv)
    )
    ggate = OwnerSum(
        where, sends, ggate_hbm, g_mine, g_y, g_z, g_final, (g_load, g_ysend, g_yrecv, g_zsend, g_zrecv)
    )

    def chunk(k):
        return part_hbm.at[:, pl.ds(k * part, part), :]

    cores, loads = [], []
    for q, xx in enumerate((1 - x, x)):
        cores.append(
            push(chunk(xx * 2 + 1 - c), core_buf.at[q], c_send.at[q], c_recv.at[q], d, peers[0])
        )
        loads.append(pltpu.make_async_copy(chunk(xx * 2 + c), own.at[q], b_load.at[q]))
    across = push(core_buf.at[0], x_buf, m_send.at[0], m_recv.at[0], d, peers[1])
    turning = push(o_final, gout_out, m_send.at[1], m_recv.at[1], to_d, to_s)
    staying = pltpu.make_async_copy(o_final, gout_out, b_load.at[2])
    kept = pltpu.make_async_copy(g_final, ggate_out, b_load.at[3])
    saved = pltpu.make_async_copy(result, own_hbm, b_load.at[4])
    loads.append(pltpu.make_async_copy(tok_hbm, tok, b_load.at[5]))
    for copy in cores + [across]:
        sends.items.append((None, copy))
    sends.items.append((moves, turning))
    span = 16

    def by_rows(work):
        def one(i, carry):
            m, row = i // (part // span), (i % (part // span)) * span
            work(m, pl.ds(pl.multiple_of(row, span), span))
            return carry

        lax.fori_loop(0, micro * (part // span), one, 0)

    def start():
        greet(
            [(None, d, p) for p in peers]
            + [(None, d + 1 - 2 * y, s), (z < deep - 1, d + 2, s), (z > 0, d - 2, s)]
            + [(moves, to_d, to_s), (moves, from_d, from_s)]
        )
        for copy in cores + loads:
            copy.start()
        gout.begin()
        ggate.begin()

    def pass_on():
        loads[0].wait()
        cores[0].wait_recv()

        def work(m, rows):
            core_buf[0, m, rows, :] = (
                core_buf[0, m, rows, :].astype(F32) + own[0, m, rows, :].astype(F32)
            ).astype(BF16)

        by_rows(work)
        across.start()

    def collect():
        loads[1].wait()
        loads[2].wait()
        cores[1].wait_recv()
        across.wait_recv()

        def work(m, rows):
            result[m, rows, :] = (
                core_buf[1, m, rows, :].astype(F32)
                + own[1, m, rows, :].astype(F32)
                + x_buf[m, rows, :].astype(F32)
                + tok[m, rows, :].astype(F32)
            ).astype(BF16)

        by_rows(work)
        saved.start()

    def hand_over():
        gout.finish()
        pl.when(moves)(turning.start)
        pl.when(jnp.logical_not(moves))(staying.start)

    def last():
        ggate.add(deep - 1)
        ggate.finish()
        kept.start()
        pl.when(moves)(turning.wait_recv)
        pl.when(jnp.logical_not(moves))(staying.wait)
        kept.wait()
        saved.wait()
        sends.drain()

    stages = {}

    def at(n, task, *args):
        stages.setdefault(n, []).append(functools.partial(task, *args))

    at(0, start)
    at(1, pass_on)
    for k in range(deep - 1):
        n = k * 2 // (deep - 2)
        at(2 + n, gout.add, k)
        at(2 + n, gout.send, k)
    at(4, gout.add, deep - 1)
    at(5, hand_over)
    for k in range(deep - 1):
        n = k * 2 // (deep - 2)
        at(5 + n, ggate.add, k)
        at(5 + n, ggate.send, k)
    at(6, collect)
    for n, tasks in stages.items():

        @pl.when(step == n)
        def _():
            for task in tasks:
                task()

    backward_kernel(
        heads,
        rest_ref,
        prev_ref,
        dy_ref,
        mem_ref,
        taps_ref,
        head_ref,
        out_ref,
        wgrad_ref,
        hgrad_ref,
        xbuf,
        gbuf,
        adj,
        dmix,
        dsum,
        uprod,
        zprod,
        rows_t,
        line,
        acts,
        slopes,
    )
    pl.when(step == pl.num_programs(0) * pl.num_programs(1) - 1)(last)


def middle(rest, dy, memory, taps, head, partial, gout, ggate, tokens, dp, tp, heads, micro):
    count, full = rest.shape
    wide = taps.shape[1]
    inner = heads * P_SIZE
    _, length, width = partial.shape
    part = length // tp
    chunks = length // part
    deep = dp // 2
    dma = pltpu.SemaphoreType.DMA
    hbm = pl.BlockSpec(memory_space=pl.ANY)
    gout = gout.reshape(dp, 2, -1, width)

    def at(m, c):
        return m * chunks + chunks - 1 - c

    def sums(block):
        kinds = [(deep,), (deep,), (2, deep - 1), ()]
        return [pltpu.VMEM(kind + block, BF16) for kind in kinds]

    sems = [dma((deep,))] * 3 + [dma((2, deep - 1))] * 2
    out = pl.pallas_call(
        functools.partial(middle_kernel, dp, heads),
        grid=(micro, chunks),
        in_specs=[
            pl.BlockSpec((part, full), lambda m, c: (at(m, c), 0)),
            pl.BlockSpec((8, full), lambda m, c: (jnp.maximum(at(m, c) * (part // 8) - 1, 0), 0)),
            pl.BlockSpec((part, inner), lambda m, c: (at(m, c), 0)),
            pl.BlockSpec((1, N, inner), lambda m, c: (at(m, c), 0, 0)),
            pl.BlockSpec((8, wide), lambda m, c: (0, 0)),
            pl.BlockSpec((8, LANES), lambda m, c: (0, 0)),
            hbm,
            hbm,
            hbm,
            hbm,
        ],
        out_specs=[
            pl.BlockSpec((part, full), lambda m, c: (at(m, c), 0)),
            pl.BlockSpec((8, wide), lambda m, c: (0, 0)),
            pl.BlockSpec((8, LANES), lambda m, c: (0, 0)),
            hbm,
            hbm,
            hbm,
        ],
        out_shape=[
            jax.ShapeDtypeStruct((count, full), BF16),
            jax.ShapeDtypeStruct((8, wide), F32),
            jax.ShapeDtypeStruct((8, LANES), F32),
            jax.ShapeDtypeStruct((micro, part, width), BF16),
            jax.ShapeDtypeStruct(gout.shape[1:], BF16),
            jax.ShapeDtypeStruct(ggate.shape[1:], BF16),
        ],
        scratch_shapes=[
            pltpu.VMEM((part + 8, wide), F32),
            pltpu.VMEM((part + 8, wide), F32),
            pltpu.VMEM((N, inner), F32),
            pltpu.VMEM((part, wide), F32),
            pltpu.VMEM((part, inner), BF16),
            pltpu.VMEM((part, inner), BF16),
            pltpu.VMEM((part, inner), BF16),
            pltpu.VMEM((LANES, part), F32),
            pltpu.VMEM((8, inner), F32),
            pltpu.VMEM((part, wide), F32),
            pltpu.VMEM((part, wide), F32),
        ]
        + sums(gout.shape[1:])
        + sums(ggate.shape[1:])
        + [
            pltpu.VMEM((2, micro, part, width), BF16),
            pltpu.VMEM((2, micro, part, width), BF16),
            pltpu.VMEM((micro, part, width), BF16),
            pltpu.VMEM((micro, part, width), BF16),
            pltpu.VMEM((micro, part, width), BF16),
        ]
        + sems
        + sems
        + [dma((6,)), dma((2,)), dma((2,)), dma((2,)), dma((2,))],
        compiler_params=pltpu.CompilerParams(
            dimension_semantics=("arbitrary", "arbitrary"),
            collective_id=4,
            has_side_effects=True,
            vmem_limit_bytes=62 * 2**20,
        ),
        cost_estimate=pl.CostEstimate(flops=7 * 10**10, bytes_accessed=4 * 10**7, transcendentals=0),
        name="mixer_backward_and_sums",
    )(rest, rest, dy, memory, taps, head, partial, gout, ggate, tokens)
    rest_grad, wgrad, hgrad, own, gout, ggate = out
    return rest_grad, wgrad, hgrad, own, gout.reshape(-1, width), ggate


def gating_kernel(
    dp,
    ssd_hbm,
    gate_hbm,
    cot_hbm,
    out_hbm,
    turned_hbm,
    gain_ref,
    grad_ssd_hbm,
    grad_gate_hbm,
    part_hbm,
    gout_hbm,
    ggate_hbm,
    ssd,
    gate,
    cot,
    w_out,
    turned,
    weighed,
    shaped_t,
    grad_gate,
    partial,
    gout,
    ggate,
    stats,
    held,
    l_sem,
    c_sem,
    s_sem,
    g_sem,
    p_sem,
    o_sem,
    send,
    recv,
):
    d, s, *_, peers, _ = where_am_i(dp)
    chunks, part, inner = ssd.shape
    width = cot.shape[2]
    count = chunks * part

    def loads(i):
        return [
            pltpu.make_async_copy(cot_hbm.at[i], cot.at[i], c_sem.at[0, i]),
            pltpu.make_async_copy(ssd_hbm.at[i], ssd.at[i], c_sem.at[1, i]),
            pltpu.make_async_copy(gate_hbm.at[i], gate.at[i], c_sem.at[2, i]),
        ]

    first = pltpu.make_async_copy(out_hbm, w_out, l_sem.at[0])
    other = pltpu.make_async_copy(turned_hbm, turned, l_sem.at[1])
    first.start()
    for i in range(chunks):
        for copy in loads(i):
            copy.start()
    other.start()
    greet([(None, d, p) for p in peers])
    first.wait()

    def gated_parts(i):
        g = gate[i]
        sig = lax.logistic(g)
        act = g * sig
        return sig, act, ssd[i] * act

    def measure(i, carry):
        for copy in loads(i):
            copy.wait()
        w = dot(cot[i], w_out[...], NT) * gain_ref[KW + 2 : KW + 3, :]
        weighed[i] = w
        _, _, gated = gated_parts(i)
        lane = lax.broadcasted_iota(jnp.int32, (part, LANES), 1)
        both = jnp.where(lane == 0, jnp.sum(gated * gated, axis=1, keepdims=True), 0.0)
        both = jnp.where(lane == 1, jnp.sum(w * gated, axis=1, keepdims=True), both)
        stats[i] = both.T[:8, :]
        return carry

    lax.fori_loop(0, chunks, measure, 0)
    copies = [push(stats, held.at[r], send.at[r], recv.at[r], d, p) for r, p in enumerate(peers)]
    for copy in copies:
        copy.start()
    for copy in copies:
        copy.wait()

    def out_copies(i):
        return [
            pltpu.make_async_copy(weighed.at[i], grad_ssd_hbm.at[i], s_sem.at[i]),
            pltpu.make_async_copy(grad_gate.at[i], grad_gate_hbm.at[i], g_sem.at[i]),
            pltpu.make_async_copy(partial.at[i], part_hbm.at[i], p_sem.at[i]),
        ]

    def columns(i):
        return pl.ds(pl.multiple_of(i * part, part), part)

    def shape_chunk(i, carry):
        sums = (stats[i] + held[0, i]) + (held[1, i] + held[2, i])
        sums = jnp.concatenate([sums, jnp.zeros((LANES - 8, part), F32)], axis=0).T
        q = lax.rsqrt(sums[:, 0:1] / DI + EPSILON)
        pull = q * q * (sums[:, 1:2] / DI)
        sig, act, gated = gated_parts(i)
        value = gated * q * gain_ref[KW + 2 : KW + 3, :]
        shaped_t[:, columns(i)] = value.T.astype(BF16)
        partial[i] = dot(value.astype(BF16), w_out[...]).astype(BF16)
        grad = q * (weighed[i] - gated * pull)
        grad_gate[i] = (grad * ssd[i] * (sig + act * (1.0 - sig))).astype(BF16)
        weighed[i] = grad * act
        for copy in out_copies(i):
            copy.start()
        return carry

    lax.fori_loop(0, chunks, shape_chunk, 0)
    other.wait()
    high, across = min(384, inner), min(512, width)

    def out_tile(i, carry):
        a = pl.ds(pl.multiple_of(i // (width // across) * high, high), high)
        b = pl.ds(pl.multiple_of(i % (width // across) * across, across), across)
        gout[a, b] = dot(shaped_t[a, :], cot[:, :, b].reshape(count, across)).astype(BF16)
        return carry

    lax.fori_loop(0, (inner // high) * (width // across), out_tile, 0)
    save_out = pltpu.make_async_copy(gout, gout_hbm, o_sem.at[0])
    save_out.start()

    def gate_tile(i, carry):
        a = pl.ds(pl.multiple_of(i // 2 * across, across), across)
        b = pl.ds(pl.multiple_of(i % 2 * (inner // 2), inner // 2), inner // 2)
        ggate[a, b] = dot(turned[a, :], grad_gate[:, :, b].reshape(count, inner // 2)).astype(BF16)
        return carry

    lax.fori_loop(0, (width // across) * 2, gate_tile, 0)
    save_gate = pltpu.make_async_copy(ggate, ggate_hbm, o_sem.at[1])
    save_gate.start()

    def saved(i, carry):
        for copy in out_copies(i):
            copy.wait()
        return carry

    lax.fori_loop(0, chunks, saved, 0)
    save_out.wait()
    save_gate.wait()


def gating(ssd, gate, cot, w_out, normed_t, gains, dp):
    chunks, part, inner = ssd.shape
    width, count = normed_t.shape
    cot = cot.reshape(chunks, part, width)
    dma = pltpu.SemaphoreType.DMA
    vmem = pl.BlockSpec(memory_space=pltpu.VMEM)
    hbm = pl.BlockSpec(memory_space=pl.ANY)

    def shape(*dims, kind=BF16):
        return jax.ShapeDtypeStruct(dims, kind)

    def room(*dims, kind=BF16):
        return pltpu.VMEM(dims, kind)

    return pl.pallas_call(
        functools.partial(gating_kernel, dp),
        in_specs=[hbm] * 5 + [vmem],
        out_specs=[hbm] * 5,
        out_shape=[
            shape(chunks, part, inner, kind=F32),
            shape(chunks, part, inner),
            shape(chunks, part, width),
            shape(inner, width),
            shape(width, inner),
        ],
        scratch_shapes=[
            room(chunks, part, inner, kind=F32),
            room(chunks, part, inner, kind=F32),
            room(chunks, part, width),
            room(inner, width),
            room(width, count),
            room(chunks, part, inner, kind=F32),
            room(inner, count),
            room(chunks, part, inner),
            room(chunks, part, width),
            room(inner, width),
            room(width, inner),
            room(chunks, 8, part, kind=F32),
            room(3, chunks, 8, part, kind=F32),
            dma((2,)),
            dma((3, chunks)),
            dma((chunks,)),
            dma((chunks,)),
            dma((chunks,)),
            dma((2,)),
            dma((3,)),
            dma((3,)),
        ],
        compiler_params=pltpu.CompilerParams(
            collective_id=2, has_side_effects=True, vmem_limit_bytes=63 * 2**20
        ),
        cost_estimate=pl.CostEstimate(flops=3 * 10**10, bytes_accessed=5 * 10**7, transcendentals=0),
        name="gating_and_gradients",
    )(ssd, gate, cot, w_out, normed_t, gains)


def as_row(column):
    size = column.shape[0]
    square = jnp.broadcast_to(column, (size, LANES))
    square = jnp.concatenate([square, jnp.zeros((LANES - size, LANES), F32)], axis=0)
    return square.T[0:1, :size]


def tail_kernel(
    dp,
    normed_hbm,
    rows_hbm,
    gates_hbm,
    w_rest_hbm,
    w_gate_hbm,
    tok_hbm,
    cot_hbm,
    gate_hbm,
    gout_hbm,
    proj_ref,
    block_ref,
    gain_ref,
    wgrad_ref,
    hgrad_ref,
    ng_ref,
    gg_ref,
    tokens_ref,
    grad_ref,
    dots_ref,
    gout_ref,
    gdots_ref,
    taps_ref,
    bias_ref,
    heads_ref,
    out_ref,
    own_ref,
    sums_ref,
    tok,
    cot,
    gate_in,
    gout,
    normed,
    rows_ref,
    gates_ref,
    w_rest,
    w_gate,
    tile,
    wtile,
    btile,
    b_own,
    b_out,
    b_in,
    theirs,
    mine,
    ybuf,
    zbuf,
    final,
    handed,
    core_buf,
    core_out,
    x_buf,
    x_out,
    s_buf,
    l_sem,
    n_sem,
    b_send,
    b_recv,
    g_send,
    g_recv,
    y_send,
    y_recv,
    z_send,
    z_recv,
    a_send,
    a_recv,
    c_send,
    c_recv,
    x_send,
    x_recv,
    s_send,
    s_recv,
):
    where = where_am_i(dp)
    d, s, z, y, x, c, peers, deep = where
    tp, rows = out_ref.shape[:2]
    block = tp * rows
    micro, part, width = own_ref.shape
    inner = gates_ref.shape[1]
    bits = dp.bit_length() - 1
    partners = []
    for k in range(bits):
        step = 2**k
        bit = (d // step) % 2
        partners.append(d + step - 2 * step * bit)
    sends = Sends()
    total = OwnerSum(
        where,
        sends,
        None,
        mine,
        ybuf,
        zbuf,
        final,
        (None, y_send, y_recv, z_send, z_recv),
        theirs,
    )
    loads = [
        pltpu.make_async_copy(src, dst, l_sem.at[k])
        for k, (src, dst) in enumerate(
            (
                (rows_hbm, rows_ref),
                (w_rest_hbm, w_rest),
                (gates_hbm, gates_ref),
                (w_gate_hbm, w_gate),
                (tok_hbm, tok),
                (cot_hbm, cot),
                (gate_hbm.at[s], gate_in.at[s]),
                (gout_hbm, gout),
            )
        )
    ]
    fetches = []
    for k in range(deep):
        lines = pl.ds(pl.multiple_of(total.order[k] * 2 * block, 2 * block), 2 * block)
        fetches.append(pltpu.make_async_copy(normed_hbm.at[lines, :], normed.at[k], n_sem.at[k]))
    for copy in loads + fetches:
        copy.start()
    greet(
        [(None, d, p) for p in peers]
        + [(None, d + 1 - 2 * y, s), (z < deep - 1, d + 2, s), (z > 0, d - 2, s)]
        + [(None, partners[k], s) for k in range(2, bits)]
    )

    def arrive(dst, sem):
        push(dst, dst, sem, sem, d, peers[0]).wait_recv()

    sums_ref[0, :, 0 : wgrad_ref.shape[1]] = wgrad_ref[...]
    sums_ref[0, :, wgrad_ref.shape[1] :] = hgrad_ref[...]

    def each(count, work):
        lax.fori_loop(0, count, lambda i, carry: (work(i), carry)[1], 0)

    across = width // tile.shape[1]
    span = wtile.shape[1]

    def product(owner, use):
        def work(i):
            m, n = i // across, i % across
            row = pl.multiple_of((m * tp + owner) * part, part)
            col = pl.multiple_of(n * tile.shape[1], tile.shape[1])
            lines = pl.ds(col, tile.shape[1])
            tile[...] = dot(rows_ref[pl.ds(row, part), :], w_rest[lines, :], NT) + dot(
                gates_ref[pl.ds(row, part), :], w_gate[lines, :], NT
            )
            use(m, lines)

        each(micro * across, work)

    def weight(k):
        fetches[k].wait()
        far = pl.ds(pl.multiple_of((1 - y) * block, block), block)
        near = pl.ds(pl.multiple_of(y * block, block), block)

        def work(n):
            cols = pl.ds(pl.multiple_of(n * span, span), span)
            wtile[...] = dot(normed[k], rows_ref[:, cols])
            theirs[k, :, cols] = wtile[far, :].astype(BF16)
            mine[k, :, cols] = wtile[near, :].astype(BF16)

        lines = pl.ds(inner, 2 * N)
        btile[...] = dot(normed[k], rows_ref[:, lines])
        ours = pl.ds(pl.multiple_of(c * N, N), N)
        b_out[k] = btile[:, pl.ds(pl.multiple_of((1 - c) * N, N), N)].astype(BF16)
        b_own[...] = btile[:, ours]
        swap = push(b_out.at[k], b_in.at[k], b_send.at[k], b_recv.at[k], d, peers[0])
        sends.start(None, swap)
        each(inner // span, work)
        b_tail = dot(normed[k], rows_ref[:, inner + 2 * N :])
        btile[:, N:] = b_tail
        arrive(b_in.at[k], b_recv.at[k])
        btile[:, 0:N] = b_own[...] + b_in[k].astype(F32)
        theirs[k, :, inner:] = btile[far, :].astype(BF16)
        mine[k, :, inner:] = btile[near, :].astype(BF16)
        total.y_items[k][1].start()

    def doubling(k):
        arrive(s_buf.at[k], s_recv.at[k])
        sums_ref[k + 1] = sums_ref[k] + s_buf[k]
        if k + 1 < bits:
            src = sums_ref.at[k + 1]
            sends.start(
                None, push(src, s_buf.at[k + 1], s_send.at[k + 1], s_recv.at[k + 1], partners[k + 1], s)
            )

    def to_core(q):
        def use(m, lines):
            core_out[q, m, :, lines] = tile[...].astype(BF16)

        return use

    def to_chip(m, lines):
        x_out[m, :, lines] = (tile[...] + core_buf[0, m, :, lines].astype(F32)).astype(BF16)

    def keep(m, lines):
        own_ref[m, :, lines] = tile[...] + core_buf[1, m, :, lines].astype(F32)

    for copy in loads[:4]:
        copy.wait()
    for r, p in enumerate(peers):
        swap = push(gate_hbm.at[p], gate_in.at[s], g_send.at[r], g_recv.at[r], d, p)
        sends.start(None, swap)
    src = sums_ref.at[0]
    sends.start(None, push(src, s_buf.at[0], s_send.at[0], s_recv.at[0], partners[0], s))
    product((1 - x) * 2 + 1 - c, to_core(0))
    sends.start(
        None, push(core_out.at[0], core_buf.at[0], c_send.at[0], c_recv.at[0], d, peers[0])
    )
    weight(0)
    arrive(core_buf.at[0], c_recv.at[0])
    product((1 - x) * 2 + c, to_chip)
    sends.start(None, push(x_out, x_buf, x_send.at[0], x_recv.at[0], d, peers[1]))
    weight(1)
    total.add(0)
    total.send(0)
    doubling(0)
    for k in range(2, deep):
        weight(k)
    total.add(1)
    total.send(1)
    doubling(1)
    product(x * 2 + 1 - c, to_core(1))
    sends.start(
        None, push(core_out.at[1], core_buf.at[1], c_send.at[1], c_recv.at[1], d, peers[0])
    )
    for k in range(2, deep - 1):
        total.add(k)
        total.send(k)
        if k < bits:
            doubling(k)
    arrive(core_buf.at[1], c_recv.at[1])
    product(s, keep)
    for k in range(deep - 1, bits):
        doubling(k)
    for r, p in enumerate(peers):
        src, dst = sums_ref.at[bits], sums_ref.at[bits + 1 + s]
        sends.start(None, push(src, dst, s_send.at[bits + r], s_recv.at[bits + r], d, p))
    sums_ref[bits + 1 + s] = sums_ref[bits]
    for copy in loads[4:]:
        copy.wait()
    for r, p in enumerate(peers):
        arrive(gate_in.at[p], g_recv.at[r])
    wide = inner + 2 * N
    heads = inner // P_SIZE
    triple = HEADS // 16
    for b in range(4):
        seat = 2 * (b % 2) + b // 2
        for k in range(4):
            at = (4 * k + b) * STRIPE
            grad_ref[:, at : at + STRIPE] = gate_in[seat, :, k * STRIPE : (k + 1) * STRIPE].astype(F32)
    gout_ref[...] = gout[...].astype(F32)
    gsum = jnp.sum(gout_ref[...] * block_ref[...].astype(F32), axis=1, keepdims=True)
    gdots_ref[...] = as_row(gsum) / gg_ref[...].astype(F32)
    for r, p in enumerate(peers):
        arrive(sums_ref.at[bits + 1 + p], s_recv.at[bits + r])
    chan = taps_ref.shape[1]
    convs = jnp.zeros((8, chan), F32)
    per_head = jnp.zeros((8, HEADS), F32)
    v = lax.broadcasted_iota(jnp.int32, (wide, chan), 0)
    g = lax.broadcasted_iota(jnp.int32, (wide, chan), 1) + chan * (d * tp + s)
    lane = lax.broadcasted_iota(jnp.int32, (LANES, HEADS), 0)
    head = lax.broadcasted_iota(jnp.int32, (LANES, HEADS), 1)
    place = []
    for p in range(tp):
        b = 2 * (p % 2) + p // 2
        from_v = jnp.where(v < inner, v + 3 * STRIPE * hop(v, STRIPE) + STRIPE * b, v - inner + DI)
        sums = sums_ref[bits + 1 + p]
        convs = convs + dot(sums[:, :wide], jnp.where(from_v == g, 1.0, 0.0), precision=HIGH)
        hit = jnp.logical_and(lane < heads, head == lane + 3 * triple * hop(lane, triple) + triple * b)
        place.append(jnp.where(hit, 1.0, 0.0))
        per_head = per_head + dot(sums[:, wide:], place[p], precision=HIGH)
    taps_ref[...] = convs[:KW]
    bias_ref[...] = convs[KW : KW + 1]
    heads_ref[...] = per_head
    total.add(deep - 1)
    total.finish()
    for p in range(tp):
        handed[p] = final[p * rows : (p + 1) * rows, :]
    for r, p in enumerate(peers):
        sends.start(None, push(handed.at[p], out_ref.at[s], a_send.at[r], a_recv.at[r], d, p))
    out_ref[s] = handed[s]

    arrive(x_buf, x_recv.at[0])

    def last(i):
        m, row = i // (part // 16), (i % (part // 16)) * 16
        lines = pl.ds(pl.multiple_of(row, 16), 16)
        h = tok[m, lines, :].astype(F32)
        r = lax.rsqrt(jnp.mean(h * h, axis=-1, keepdims=True) + EPSILON)
        n = h * r
        grad = (own_ref[m, lines, :] + x_buf[m, lines, :].astype(F32)) * gain_ref[KW + 1 : KW + 2, :]
        grad = grad - n * jnp.mean(grad * n, axis=-1, keepdims=True)
        tokens_ref[m, lines, :] = (cot[m, lines, :].astype(F32) + r * grad).astype(BF16)

    each(micro * (part // 16), last)
    for r, p in enumerate(peers):
        arrive(out_ref.at[p], a_recv.at[r])
    both = [jnp.zeros((rows, N), F32), jnp.zeros((rows, N), F32)]
    steps = jnp.zeros((rows, HEADS), F32)
    for b in range(4):
        seat = 2 * (b % 2) + b // 2
        for k in range(4):
            at = DI + (4 * k + b) * STRIPE
            piece = out_ref[seat, :, k * STRIPE : (k + 1) * STRIPE]
            grad_ref[:, at : at + STRIPE] = piece.astype(F32)
        both[seat % 2] = both[seat % 2] + out_ref[seat, :, inner : inner + N].astype(F32)
        steps = steps + dot(out_ref[seat, :, inner + N :], place[seat].astype(BF16))
    grad_ref[:, 2 * DI : 2 * DI + N] = both[0]
    grad_ref[:, 2 * DI + N : 2 * DI + 2 * N] = both[1]
    grad_ref[:, 2 * DI + 2 * N :] = steps
    nsum = jnp.sum(grad_ref[...] * proj_ref[...].astype(F32), axis=1, keepdims=True)
    dots_ref[...] = as_row(nsum) / ng_ref[...].astype(F32)
    sends.drain()


def tail(
    normed_t, rows_grad, gates_grad, w_rest, w_gate, tokens, cotangent, gate_in, gout, in_proj, out_proj, gains, wgrad, hgrad, norm_gain, gated_gain, chan, dp
):
    width, count = normed_t.shape
    micro = tokens.shape[0]
    tp = gate_in.shape[0]
    small = (8, wgrad.shape[1] + hgrad.shape[1])
    full = gates_grad.shape[1] + N + LANES
    rows = width // dp // tp
    part = count // micro // tp
    deep = dp // 2
    bits = dp.bit_length() - 1
    block = tp * rows
    dma = pltpu.SemaphoreType.DMA
    vmem = pl.BlockSpec(memory_space=pltpu.VMEM)
    hbm = pl.BlockSpec(memory_space=pl.ANY)
    return pl.pallas_call(
        functools.partial(tail_kernel, dp),
        in_specs=[hbm] * 9 + [vmem] * 7,
        out_specs=[vmem] * 8,
        out_shape=[
            jax.ShapeDtypeStruct(tokens.shape, BF16),
            jax.ShapeDtypeStruct(in_proj.shape, F32),
            jax.ShapeDtypeStruct((1, rows), F32),
            jax.ShapeDtypeStruct(gout.shape, F32),
            jax.ShapeDtypeStruct((1, gout.shape[0]), F32),
            jax.ShapeDtypeStruct((KW, chan), F32),
            jax.ShapeDtypeStruct((1, chan), F32),
            jax.ShapeDtypeStruct((8, HEADS), F32),
        ],
        scratch_shapes=[
            pltpu.VMEM((tp, rows, full), BF16),
            pltpu.VMEM((micro, part, width), F32),
            pltpu.VMEM((bits + 1 + tp,) + small, F32),
            pltpu.VMEM(tokens.shape, BF16),
            pltpu.VMEM(tokens.shape, BF16),
            pltpu.VMEM(gate_in.shape, BF16),
            pltpu.VMEM(gout.shape, BF16),
            pltpu.VMEM((deep, 2 * block, count), BF16),
            pltpu.VMEM(rows_grad.shape, BF16),
            pltpu.VMEM(gates_grad.shape, BF16),
            pltpu.VMEM(w_rest.shape, BF16),
            pltpu.VMEM(w_gate.shape, BF16),
            pltpu.VMEM((part, min(width, 512)), F32),
            pltpu.VMEM((2 * block, 384), F32),
            pltpu.VMEM((2 * block, 2 * N), F32),
            pltpu.VMEM((2 * block, N), F32),
            pltpu.VMEM((deep, 2 * block, N), BF16),
            pltpu.VMEM((deep, 2 * block, N), BF16),
            pltpu.VMEM((deep, block, full), BF16),
            pltpu.VMEM((deep, block, full), BF16),
            pltpu.VMEM((deep, block, full), BF16),
            pltpu.VMEM((2, deep - 1, block, full), BF16),
            pltpu.VMEM((block, full), BF16),
            pltpu.VMEM((tp, rows, full), BF16),
            pltpu.VMEM((2, micro, part, width), BF16),
            pltpu.VMEM((2, micro, part, width), BF16),
            pltpu.VMEM((micro, part, width), BF16),
            pltpu.VMEM((micro, part, width), BF16),
            pltpu.VMEM((bits,) + small, F32),
            dma((8,)),
            dma((deep,)),
            dma((deep,)),
            dma((deep,)),
            dma((3,)),
            dma((3,)),
            dma((deep,)),
            dma((deep,)),
            dma((2, deep - 1)),
            dma((2, deep - 1)),
            dma((3,)),
            dma((3,)),
            dma((2,)),
            dma((2,)),
            dma((1,)),
            dma((1,)),
            dma((bits + 3,)),
            dma((bits + 3,)),
        ],
        compiler_params=pltpu.CompilerParams(
            collective_id=3, has_side_effects=True, vmem_limit_bytes=62 * 2**20
        ),
        cost_estimate=pl.CostEstimate(flops=6 * 10**10, bytes_accessed=3 * 10**7, transcendentals=0),
        name="gradients_to_owners",
    )(
        normed_t,
        rows_grad,
        gates_grad,
        w_rest,
        w_gate,
        tokens,
        cotangent,
        gate_in,
        gout,
        in_proj,
        out_proj,
        gains,
        wgrad,
        hgrad,
        norm_gain,
        gated_gain,
    )


def body(
    tokens,
    in_proj,
    conv_weight,
    conv_bias,
    decay_log,
    step_bias,
    skip_gain,
    norm_gain,
    gated_gain,
    out_proj,
    cotangent,
):
    dp, tp = lax.axis_size("dp"), lax.axis_size("seq")
    s = lax.axis_index("seq")
    micro, part, width = tokens.shape
    heads = HEADS // tp
    inner = heads * P_SIZE
    rows = in_proj.shape[0]
    length = part * tp
    count = micro * length
    wide = inner + 2 * N
    chan = conv_bias.shape[0]

    (
        normed,
        normed_t,
        proj_rest,
        ssd,
        memory,
        gate,
        w_rest,
        w_gate,
        w_out,
        cot,
        taps,
        gains,
        g_gated,
        per_head,
    ) = head(
        in_proj,
        conv_weight,
        conv_bias[None],
        norm_gain[None],
        gated_gain[None],
        decay_log[None],
        step_bias[None],
        skip_gain[None],
        tokens,
        cotangent,
        out_proj,
        dp,
        tp,
    )
    proj_rest = proj_rest.reshape(count, wide + LANES)
    w_rest = w_rest.reshape(width, wide + LANES)
    w_gate = w_gate.reshape(width, inner)
    grad_ssd, grad_gate, out_part, grad_out, gate_in = gating(
        ssd, gate, cot, w_out.reshape(inner, width), normed_t, g_gated, dp
    )
    grad_ssd = grad_ssd.reshape(count, inner)
    grad_gate = grad_gate.reshape(count, inner)
    grad_rest, wgrad, hgrad, out_part, grad_out, gate_in = middle(
        proj_rest,
        grad_ssd,
        memory,
        taps,
        per_head,
        out_part.reshape(micro, length, width),
        grad_out.reshape(dp, -1, width),
        gate_in.reshape(dp, tp, rows, inner),
        tokens,
        dp,
        tp,
        heads,
        micro,
    )
    tokens_grad, in_grad, dots, grad_out, gdots, conv_grad, bias_grad, head_grads = tail(
        normed_t,
        grad_rest,
        grad_gate,
        w_rest,
        w_gate,
        tokens,
        cotangent,
        gate_in,
        grad_out,
        in_proj,
        out_proj,
        gains,
        wgrad,
        hgrad,
        norm_gain[None],
        gated_gain[None],
        chan,
        dp,
    )
    return (
        out_part,
        tokens_grad,
        in_grad,
        conv_grad,
        bias_grad[0],
        head_grads[0],
        head_grads[1],
        head_grads[2],
        dots[0],
        gdots[0],
        grad_out,
    )


def solution(mesh):
    both = ("dp", "seq")
    return jax.shard_map(
        body,
        mesh=mesh,
        in_specs=(
            P("dp", "seq", None),
            P(both, None),
            P(None, both),
            P(both),
            P(),
            P(),
            P(),
            P(both),
            P(both),
            P(both, None),
            P("dp", "seq", None),
        ),
        out_specs=(
            P("dp", "seq", None),
            P("dp", "seq", None),
            P(both, None),
            P(None, both),
            P(both),
            P(),
            P(),
            P(),
            P(both),
            P(both),
            P(both, None),
        ),
        check_vma=False,
    )
```
